32 devices in a mesh: dp: 4 (over y, x), ctx: 4 (over z), tensor: 2 (over core).
Axes of the slice: x: 2, y: 2, z: 4, core: 2. Of those that a mesh axis runs over, the one named last changes fastest.
Arguments:
- layer_input: bfloat16 [8192, 1536], P(('dp', 'ctx', 'tensor')), may hold values from -6 to 6
- teacher: bfloat16 [8192, 1536], P(('dp', 'ctx', 'tensor')), may hold values from -6 to 6
- cotangent: bfloat16 [8192, 1536], P(('dp', 'ctx', 'tensor')), may hold values from -6 to 6
- segment_ids: int32 [8192], P('dp'), may hold values from 0 to 8191, as said below
- positions: int32 [8192], P('dp'), may hold values from 0 to 2047, as said below
- valid_mask: int32 [8192], P('dp'), may hold values from 0 to 1
- gain_attn: bfloat16 [1536], replicated, may hold values from 0.5 to 1.5
- query_weight: bfloat16 [1536, 1536], P(('dp', 'ctx'), 'tensor'), may hold values from -0.15625 to 0.15625
- query_bias: bfloat16 [1536], replicated, may hold values from -3 to 3
- key_weight: bfloat16 [1536, 256], P(('dp', 'ctx'), 'tensor'), may hold values from -0.15625 to 0.15625
- key_bias: bfloat16 [256], replicated, may hold values from -3 to 3
- value_weight: bfloat16 [1536, 256], P(('dp', 'ctx'), 'tensor'), may hold values from -0.15625 to 0.15625
- value_bias: bfloat16 [256], replicated, may hold values from -3 to 3
- out_weight: bfloat16 [1536, 1536], P('tensor', ('dp', 'ctx')), may hold values from -1.25 to 1.25
- gain_mlp: bfloat16 [1536], replicated, may hold values from 0.5 to 1.5
- gate_weight: bfloat16 [1536, 8960], P(('dp', 'ctx'), 'tensor'), may hold values from -0.15625 to 0.15625
- up_weight: bfloat16 [1536, 8960], P(('dp', 'ctx'), 'tensor'), may hold values from -0.15625 to 0.15625
- down_weight: bfloat16 [8960, 1536], P('tensor', ('dp', 'ctx')), may hold values from -0.0625 to 0.0625
Outputs:
- layer_out: bfloat16 [8192, 1536], P(('dp', 'ctx', 'tensor'))
- loss: float32 [], replicated
- grad_input: float32 [8192, 1536], P(('dp', 'ctx', 'tensor'))
- grad_gain_attn: float32 [1536], replicated
- grad_query: float32 [1536, 1536], P(('dp', 'ctx'), 'tensor')
- grad_query_bias: float32 [1536], replicated
- grad_key: float32 [1536, 256], P(('dp', 'ctx'), 'tensor')
- grad_key_bias: float32 [256], replicated
- grad_value: float32 [1536, 256], P(('dp', 'ctx'), 'tensor')
- grad_value_bias: float32 [256], replicated
- grad_out: float32 [1536, 1536], P('tensor', ('dp', 'ctx'))
- grad_gain_mlp: float32 [1536], replicated
- grad_gate: float32 [1536, 8960], P(('dp', 'ctx'), 'tensor')
- grad_up: float32 [1536, 8960], P(('dp', 'ctx'), 'tensor')
- grad_down: float32 [8960, 1536], P('tensor', ('dp', 'ctx'))
The draws below stay inside these ranges and needn't reach their ends.
Inputs may be any that keep to these rules, and one draw needn't show every extreme that they name: `segment_ids`: the index of the first token of the token's document; never falls along the tokens, every sequence of 2048 tokens begins a new document, and the last token alone forms a document. `positions`: 0 at a document's first token, rising by one token by token within the document; the first sequence is one document.
All inputs are finite; a program needn't handle non-finite values.
Results may differ from the reference program's by a relative error of at most 0.024.
Values may be sent and summed in bfloat16 or wider, within the bound.
A program may use at most 192 MiB of HBM per device.

```python
import math
import jax
import jax.numpy as jnp
from jax import lax

D = 1536
FF = 8960
HEADS = 12
KV_HEADS = 2
HEAD = 128
SEQ_LEN = 2048
SEQS = 4
TOKENS = 8192


def document_starts(key):
    base_key = jax.random.fold_in(key, 11)
    token_index = jnp.arange(TOKENS, dtype=jnp.int32)
    levels = jax.random.randint(jax.random.fold_in(base_key, 1), (TOKENS // 512 + 1,), 0, 4)
    token_level = levels[token_index // 512]
    period = jnp.left_shift(jnp.ones_like(token_level), 3 + 2 * token_level)
    draws = jax.random.randint(jax.random.fold_in(base_key, 2), (TOKENS,), 0, 1 << 30)
    inner = (draws % period == 0) & (token_index >= SEQ_LEN)
    starting = inner | (token_index % SEQ_LEN == 0) | (token_index == TOKENS - 1)
    last_start = lax.cummax(jnp.where(starting, token_index, 0), axis=0)
    return (last_start.astype(jnp.int32), token_index)


def draw_segment_ids(key, part):
    last_start, token_index = document_starts(key)
    return last_start


def draw_positions(key, part):
    last_start, token_index = document_starts(key)
    return (token_index - last_start).astype(jnp.int32)


def draw_valid_mask(key, part):
    token_index = jnp.arange(TOKENS, dtype=jnp.int32)
    draws = jax.random.randint(jax.random.fold_in(key, 29), (TOKENS,), 0, 4 * TOKENS)
    return (draws < TOKENS + 3 * token_index).astype(jnp.int32)


def spiked(values, key, source, target, parts, factor):
    def block_of(position):
        return (jnp.arange(values.shape[position]) // (values.shape[position] // parts)).reshape((-1,) + (1,) * (values.ndim - 1 - position))

    first = jax.random.permutation(key, parts)[block_of(target)]
    second = (block_of(target) + parts // 2) % parts
    return jnp.where((block_of(source) == first) | (block_of(source) == second), factor * values, values)


def level_of(own_key, shape, shards, low, high):
    factor_of, own = 1.0, jax.random.fold_in(own_key, 6)
    for dim, blocks in shards:
        steps = jnp.exp(jax.random.uniform(jax.random.fold_in(own, dim), (blocks,), jnp.float32, low / len(shards), high / len(shards)))
        factor_of = factor_of * jnp.repeat(steps, shape[dim] // blocks).reshape([-1 if axis == dim else 1 for axis in range(len(shape))])
    return factor_of


def gaussian(stream_key, dims, spread, bound, split=(), kind=jnp.bfloat16):
    array = spread * jax.random.normal(stream_key, dims, jnp.float32)
    if split:
        array = array * level_of(stream_key, dims, split, -0.22, 0.18)
    return jnp.clip(array, -bound, bound).astype(kind)


def heavy_noise(own_key, shape, deviation, most, cuts, heavy, held_as=jnp.bfloat16):
    entries = deviation * jax.random.normal(own_key, shape, jnp.float32)
    if cuts:
        entries = entries * level_of(own_key, shape, cuts, -0.22, 0.18)
    return jnp.clip(spiked(entries, jax.random.fold_in(own_key, 3), *heavy), -most, most).astype(held_as)


def setup_inputs(seed: int = 0) -> dict:
    streams_of = jax.random.split(jax.random.key(seed), 19)
    layer_input = heavy_noise(streams_of[0], (TOKENS, D), 1.0, 6.0, ((0, 32),), (0, 1, 32, 2.75))
    teacher = gaussian(streams_of[1], (TOKENS, D), 1.0, 6.0, ((0, 32),))
    cotangent = heavy_noise(streams_of[2], (TOKENS, D), 1.0, 6.0, ((0, 32),), (0, 1, 32, 2.75))
    segment_ids = draw_segment_ids(jax.random.fold_in(streams_of[18], 71), 0)
    positions = draw_positions(jax.random.fold_in(streams_of[18], 71), 0)
    valid_mask = draw_valid_mask(jax.random.fold_in(streams_of[18], 71), 0)
    gain_attn = jnp.clip(1.0 + 0.1 * jax.random.normal(streams_of[6], (D,), jnp.float32), 0.5, 1.5).astype(jnp.bfloat16)
    query_weight = gaussian(streams_of[7], (D, HEADS * HEAD), D ** -0.5, 0.15625, ((0, 16), (1, 2)))
    query_bias = gaussian(streams_of[8], (HEADS * HEAD,), 0.5, 3.0)
    key_weight = gaussian(streams_of[9], (D, KV_HEADS * HEAD), D ** -0.5, 0.15625, ((0, 16), (1, 2)))
    key_bias = gaussian(streams_of[10], (KV_HEADS * HEAD,), 0.5, 3.0)
    value_weight = gaussian(streams_of[11], (D, KV_HEADS * HEAD), D ** -0.5, 0.15625, ((0, 16), (1, 2)))
    value_bias = gaussian(streams_of[12], (KV_HEADS * HEAD,), 0.5, 3.0)
    out_weight = gaussian(streams_of[13], (HEADS * HEAD, D), (HEADS * HEAD // 64) ** -0.5, 1.25, ((0, 2), (1, 16)))
    gain_mlp = jnp.clip(1.0 + 0.1 * jax.random.normal(streams_of[14], (D,), jnp.float32), 0.5, 1.5).astype(jnp.bfloat16)
    gate_weight = gaussian(streams_of[15], (D, FF), D ** -0.5, 0.15625, ((0, 16), (1, 2)))
    up_weight = gaussian(streams_of[16], (D, FF), D ** -0.5, 0.15625, ((0, 16), (1, 2)))
    down_weight = gaussian(streams_of[17], (FF, D), FF ** -0.5, 0.0625, ((0, 2), (1, 16)))
    return dict(layer_input=layer_input, teacher=teacher, cotangent=cotangent, segment_ids=segment_ids, positions=positions, valid_mask=valid_mask, gain_attn=gain_attn, query_weight=query_weight, query_bias=query_bias, key_weight=key_weight, key_bias=key_bias, value_weight=value_weight, value_bias=value_bias, out_weight=out_weight, gain_mlp=gain_mlp, gate_weight=gate_weight, up_weight=up_weight, down_weight=down_weight)


EPS = 1e-06
THETA = 10000.0
HIGH = lax.Precision.HIGHEST

@jax.custom_vjp
def low(v):
    return lax.optimization_barrier(v.astype(jnp.bfloat16)).astype(jnp.float32)

@jax.custom_vjp
def low_back(v):
    return v

def low_keep(v):
    return (low(v), None)

def low_pass(kept, grad):
    return (grad,)

def back_keep(v):
    return (v, None)

def back_low(kept, grad):
    return (low(grad),)
low.defvjp(low_keep, low_pass)
low_back.defvjp(back_keep, back_low)

def rope_tables(places):
    half_dim = HEAD // 2
    frequency = THETA ** (-(jnp.arange(half_dim, dtype=jnp.float32) * 2.0 / HEAD))
    angles = places.astype(jnp.float32)[:, None] * frequency[None, :]
    return (jnp.cos(angles), jnp.sin(angles))

def rotate(stacked, cosine, sine_table):
    half_dim = HEAD // 2
    first_half = stacked[..., :half_dim]
    second_half = stacked[..., half_dim:]
    cosine = cosine[:, None, :]
    sine_table = sine_table[:, None, :]
    return jnp.concatenate([first_half * cosine - second_half * sine_table, second_half * cosine + first_half * sine_table], axis=-1)

def matmul(first_op, second_op):
    return jnp.dot(first_op, second_op, precision=HIGH, preferred_element_type=jnp.float32)

def rms_norm(stacked, gain):
    inverse = lax.rsqrt(lax.optimization_barrier(jnp.mean(stacked * stacked, axis=-1, keepdims=True)) + EPS)
    return stacked * inverse * gain

def sequence(params, tokens, targets, segments, places, valid_tokens):
    gain_attn, query_weight, query_bias, key_weight, key_bias, value_weight, value_bias, out_weight, gain_mlp, gate_weight, up_weight, down_weight = params
    length = tokens.shape[0]
    group_size = HEADS // KV_HEADS
    score_scale = 1.0 / math.sqrt(HEAD)
    normed_rows = low(rms_norm(tokens, gain_attn))
    query_pre = low_back(matmul(normed_rows, query_weight) + query_bias)
    key_pre = low_back(matmul(normed_rows, key_weight) + key_bias)
    value_rows = low(low_back(matmul(normed_rows, value_weight) + value_bias)).reshape(length, KV_HEADS, HEAD)
    cosine, sine_table = rope_tables(places)
    queries = low(rotate(query_pre.reshape(length, HEADS, HEAD), cosine, sine_table)).reshape(length, KV_HEADS, group_size, HEAD)
    key_rows = low(rotate(key_pre.reshape(length, KV_HEADS, HEAD), cosine, sine_table))
    block_rows = math.gcd(512, length)
    key_index = jnp.arange(length, dtype=jnp.int32)
    key_valid = valid_tokens > 0

    def rows_block(offset):
        query_block = lax.dynamic_slice_in_dim(queries, offset, block_rows, 0)
        raw_scores = jnp.einsum('icgd,jcd->cgij', query_block, key_rows, precision=HIGH) * score_scale
        scores = low_back(raw_scores)
        query_index = offset + jnp.arange(block_rows, dtype=jnp.int32)
        query_seg = lax.dynamic_slice_in_dim(segments, offset, block_rows, 0)
        same_doc = query_seg[:, None] == segments[None, :]
        earlier = key_index[None, :] <= query_index[:, None]
        itself = key_index[None, :] == query_index[:, None]
        allowed = same_doc & earlier & (key_valid[None, :] | itself)
        scores = jnp.where(allowed, scores, -jnp.inf)
        attn_probs = jax.nn.softmax(scores, axis=3)
        mixture = jnp.einsum('cgij,jcd->icgd', low(attn_probs), value_rows, precision=HIGH)
        return mixture.reshape(block_rows, HEADS * HEAD)
    starts = jnp.arange(0, length, block_rows, dtype=jnp.int32)
    heads_out = lax.map(jax.checkpoint(rows_block), starts).reshape(length, HEADS * HEAD)
    heads_out = low(low_back(heads_out))
    attention = low_back(matmul(heads_out, out_weight))
    residual_mid = tokens + attention
    mlp_rows = low(rms_norm(residual_mid, gain_mlp))
    gate_act = low_back(matmul(mlp_rows, gate_weight))
    up_act = low_back(matmul(mlp_rows, up_weight))
    hidden = low(jax.nn.silu(gate_act) * up_act)
    branch = low_back(matmul(hidden, down_weight))
    layer_result = residual_mid + branch
    squared_err = jnp.sum(valid_tokens.astype(layer_result.dtype)[:, None] * (layer_result - targets) ** 2)
    return (layer_result, squared_err)

def reference(layer_input, teacher, cotangent, segment_ids, positions, valid_mask, gain_attn, query_weight, query_bias, key_weight, key_bias, value_weight, value_bias, out_weight, gain_mlp, gate_weight, up_weight, down_weight):
    params = tuple((weight.astype(jnp.float32) for weight in (gain_attn, query_weight, query_bias, key_weight, key_bias, value_weight, value_bias, out_weight, gain_mlp, gate_weight, up_weight, down_weight)))
    tokens = layer_input.astype(jnp.float32).reshape(SEQS, SEQ_LEN, D)
    targets = teacher.astype(jnp.float32).reshape(SEQS, SEQ_LEN, D)
    segments = segment_ids.reshape(SEQS, SEQ_LEN)
    places = positions.reshape(SEQS, SEQ_LEN)
    valid_tokens = valid_mask.reshape(SEQS, SEQ_LEN)
    valid_count = jnp.sum(valid_mask).astype(jnp.float32)

    def forward(params, tokens):

        def per_sequence(seq_item):
            return jax.checkpoint(sequence)(params, seq_item[0], seq_item[1], seq_item[2], seq_item[3], seq_item[4])
        results, errors = lax.map(per_sequence, (tokens, targets, segments, places, valid_tokens))
        return (results, jnp.sum(errors) / (valid_count * D))
    (results, loss_value), pullback = jax.vjp(forward, params, tokens)
    seed_grad = cotangent.astype(jnp.float32).reshape(SEQS, SEQ_LEN, D)
    param_grads, grad_tokens = pullback((seed_grad, jnp.ones((), loss_value.dtype)))
    return (results.reshape(TOKENS, D).astype(jnp.bfloat16), loss_value, grad_tokens.reshape(TOKENS, D), param_grads[0], param_grads[1], param_grads[2], param_grads[3], param_grads[4], param_grads[5], param_grads[6], param_grads[7], param_grads[8], param_grads[9], param_grads[10], param_grads[11])
```

```python
import functools
import math

import jax
import jax.numpy as jnp
from jax import lax
from jax.experimental import pallas as pl
from jax.experimental.pallas import tpu as pltpu
from jax.sharding import PartitionSpec as P

D = 1536
HEAD = 128


EPS = 1e-06
THETA = 10000.0
VERY_LOW = -1e30


def rope_tables(places):
    half_dim = HEAD // 2
    frequency = THETA ** (-(jnp.arange(half_dim, dtype=jnp.float32) * 2.0 / HEAD))
    angles = places.astype(jnp.float32)[:, None] * frequency[None, :]
    return (jnp.cos(angles), jnp.sin(angles))


def rotate(stacked, cosine, sine_table):
    half_dim = HEAD // 2
    first_half = stacked[..., :half_dim]
    second_half = stacked[..., half_dim:]
    cosine = cosine[:, None, :]
    sine_table = sine_table[:, None, :]
    return jnp.concatenate(
        [
            first_half * cosine - second_half * sine_table,
            second_half * cosine + first_half * sine_table,
        ],
        axis=-1,
    )


def matmul(first_op, second_op):
    return jnp.dot(first_op, second_op, preferred_element_type=jnp.float32)


def matmul_tn(first_op, second_op):
    return lax.dot_general(
        first_op, second_op, (((0,), (0,)), ((), ())), preferred_element_type=jnp.float32
    )


def matmul_nt(first_op, second_op):
    return lax.dot_general(
        first_op, second_op, (((1,), (1,)), ((), ())), preferred_element_type=jnp.float32
    )


def norm_back(grad_normed, normed, inverse, gain):
    scaled = grad_normed * gain
    return inverse * (scaled - normed * jnp.mean(scaled * normed, axis=1, keepdims=True))


def exchange(blocks, axis):
    size = lax.axis_size(axis)
    rank = lax.axis_index(axis)
    received = [(rank, lax.dynamic_index_in_dim(blocks, rank, 0, keepdims=False))]
    for step in range(1, size):
        going = lax.dynamic_index_in_dim(blocks, (rank + step) % size, 0, keepdims=False)
        came = lax.ppermute(going, axis, [(i, (i + step) % size) for i in range(size)])
        received.append(((rank - step + size) % size, came))
    return received


def to_columns(shard, width):
    size = lax.axis_size("ctx")
    rows, columns = shard.shape
    padded = jnp.pad(shard, ((0, 0), (0, size * width - columns)))
    blocks = jnp.stack([padded[:, j * width : (j + 1) * width] for j in range(size)])
    gathered = jnp.zeros((size, rows, width), shard.dtype)
    for rank, block in exchange(blocks, "ctx"):
        gathered = lax.dynamic_update_index_in_dim(gathered, block, rank, 0)
    return lax.all_gather(gathered.reshape(size * rows, width), "dp", axis=0, tiled=True)


def to_rows(grad, columns):
    size = lax.axis_size("ctx")
    summed = lax.psum_scatter(grad, "dp", scatter_dimension=0, tiled=True)
    rows, width = summed.shape[0] // size, summed.shape[1]
    shard = jnp.zeros((rows, size * width), jnp.bfloat16)
    for rank, block in exchange(summed.reshape(size, rows, width), "ctx"):
        shard = lax.dynamic_update_slice_in_dim(shard, block, rank * width, 1)
    return shard[:, :columns].astype(jnp.float32)


def sum_everywhere(value):
    for axis in ("tensor", "ctx", "dp"):
        size = lax.axis_size(axis)
        if size & (size - 1):
            value = lax.psum(value, axis)
            continue
        step = 1
        while step < size:
            value = value + lax.ppermute(value, axis, [(i, i ^ step) for i in range(size)])
            step *= 2
    return value


def mask_into(bias_ref, first, seg_ref, place_ref):
    keys, rows = bias_ref.shape
    key_index = lax.broadcasted_iota(jnp.int32, (keys, rows), 0)
    row_index = lax.broadcasted_iota(jnp.int32, (keys, rows), 1) + first
    place = jnp.broadcast_to(place_ref[...], (keys, rows))
    start = jnp.broadcast_to(seg_ref[...], (keys, rows))
    allowed = ((place >= start) & (place <= row_index)) | (key_index == row_index)
    bias_ref[...] = jnp.where(allowed, 0.0, VERY_LOW)


def nn(first_op, second_op):
    return jnp.dot(first_op, second_op, preferred_element_type=jnp.float32)


def attend_kernel(scale, first_ref, seg_ref, place_ref, q_ref, k_ref, vt_ref, o_ref, lse_ref, bias_ref):
    @pl.when(pl.program_id(1) == 0)
    def _():
        mask_into(bias_ref, first_ref[0] + pl.program_id(0) * q_ref.shape[0], seg_ref, place_ref)

    scores = matmul_nt(k_ref[...], q_ref[...]) * scale + bias_ref[...]
    top = jnp.max(scores, axis=0, keepdims=True)
    powers = jnp.exp(scores - top)
    total = jnp.sum(powers, axis=0, keepdims=True)
    mixture = nn(vt_ref[...], powers.astype(jnp.bfloat16)) / total
    o_ref[...] = mixture.T.astype(jnp.bfloat16)
    lse_ref[0] = top + jnp.log(total)


def attend_back_kernel(
    scale, first_ref, seg_ref, place_ref, q_ref, do_ref, lse_ref, k_ref, v_ref, kt_ref,
    dq_ref, dkv_ref, bias_ref, dk_ref, dv_ref,
):
    block, head = pl.program_id(0), pl.program_id(1)

    @pl.when(head == 0)
    def _():
        mask_into(bias_ref, first_ref[0] + block * q_ref.shape[0], seg_ref, place_ref)

    @pl.when((head == 0) & (block == 0))
    def _():
        dk_ref[...] = jnp.zeros_like(dk_ref)
        dv_ref[...] = jnp.zeros_like(dv_ref)

    query, grad = q_ref[...], do_ref[...]
    scores = matmul_nt(k_ref[...], query) * scale + bias_ref[...]
    probs = jnp.exp(scores - lse_ref[0])
    grad_probs = matmul_nt(v_ref[...], grad)
    delta = jnp.sum(probs * grad_probs, axis=0, keepdims=True)
    grad_scores = (probs * (grad_probs - delta)).astype(jnp.bfloat16)
    dv_ref[...] += nn(probs.astype(jnp.bfloat16), grad)
    dk_ref[...] += nn(grad_scores, query)
    dq_ref[...] = (nn(kt_ref[...], grad_scores) * scale).T

    @pl.when((head == pl.num_programs(1) - 1) & (block == pl.num_programs(0) - 1))
    def _():
        dkv_ref[:, :HEAD] = (dk_ref[...] * scale).astype(jnp.bfloat16)
        dkv_ref[:, HEAD:] = dv_ref[...].astype(jnp.bfloat16)


def attention_calls(rows, keys, heads):
    block = math.gcd(256, rows)
    scale = 1.0 / math.sqrt(HEAD)
    smem = pl.BlockSpec(memory_space=pltpu.SMEM)
    seg = pl.BlockSpec((1, block), lambda i, h: (0, i))
    place = pl.BlockSpec((keys, 1), lambda i, h: (0, 0))
    head = pl.BlockSpec((block, HEAD), lambda i, h: (i, h))
    lse = pl.BlockSpec((1, 1, block), lambda i, h: (h, 0, i))
    tall = pl.BlockSpec((keys, HEAD), lambda i, h: (0, 0))
    wide = pl.BlockSpec((HEAD, keys), lambda i, h: (0, 0))
    params = pltpu.CompilerParams(vmem_limit_bytes=60000000)
    grid = (rows // block, heads)
    size = heads * rows * keys
    forward = pl.pallas_call(
        functools.partial(attend_kernel, scale),
        grid=grid,
        in_specs=[smem, seg, place, head, tall, wide],
        out_specs=[head, lse],
        out_shape=[
            jax.ShapeDtypeStruct((rows, heads * HEAD), jnp.bfloat16),
            jax.ShapeDtypeStruct((heads, 1, rows), jnp.float32),
        ],
        scratch_shapes=[pltpu.VMEM((keys, block), jnp.float32)],
        compiler_params=params,
        cost_estimate=pl.CostEstimate(flops=4 * size * HEAD, bytes_accessed=4 * rows * heads * HEAD, transcendentals=size),
        name="attend",
    )
    backward = pl.pallas_call(
        functools.partial(attend_back_kernel, scale),
        grid=grid,
        in_specs=[smem, seg, place, head, head, lse, tall, tall, wide],
        out_specs=[head, pl.BlockSpec((keys, 2 * HEAD), lambda i, h: (0, 0))],
        out_shape=[
            jax.ShapeDtypeStruct((rows, heads * HEAD), jnp.float32),
            jax.ShapeDtypeStruct((keys, 2 * HEAD), jnp.bfloat16),
        ],
        scratch_shapes=[
            pltpu.VMEM((keys, block), jnp.float32),
            pltpu.VMEM((keys, HEAD), jnp.float32),
            pltpu.VMEM((keys, HEAD), jnp.float32),
        ],
        compiler_params=params,
        cost_estimate=pl.CostEstimate(flops=10 * size * HEAD, bytes_accessed=8 * rows * heads * HEAD, transcendentals=size),
        name="attend_back",
    )
    return forward, backward


def per_device(
    layer_input,
    teacher,
    cotangent,
    segment_ids,
    positions,
    valid_mask,
    gain_attn,
    query_weight,
    query_bias,
    key_weight,
    key_bias,
    value_weight,
    value_bias,
    out_weight,
    gain_mlp,
    gate_weight,
    up_weight,
    down_weight,
):
    tensor_rank = lax.axis_index("tensor")
    ctx_rank = lax.axis_index("ctx")
    tensor_size, ctx_size = lax.axis_size("tensor"), lax.axis_size("ctx")
    own_rows = layer_input.shape[0]
    shard_rows = own_rows * tensor_size
    seq_len = segment_ids.shape[0]
    q_width = query_weight.shape[1]
    kv_width = key_weight.shape[1]
    kv_local = kv_width // HEAD
    group = q_width // kv_width
    hidden_width = gate_weight.shape[1]
    slice_width = -(-hidden_width // (128 * ctx_size)) * 128
    first_row = ctx_rank * shard_rows
    own_first = first_row + tensor_rank * own_rows

    inputs = layer_input.astype(jnp.float32)
    gain_one = gain_attn.astype(jnp.float32)
    gain_two = gain_mlp.astype(jnp.float32)
    scale_attn = lax.rsqrt(jnp.mean(inputs * inputs, axis=1, keepdims=True) + EPS)
    normed_attn = inputs * scale_attn
    normed_rows = lax.all_gather(
        (normed_attn * gain_one).astype(jnp.bfloat16), "tensor", axis=0, tiled=True
    )
    full_qkv = lax.all_gather(
        jnp.concatenate([query_weight, key_weight, value_weight], axis=1),
        ("dp", "ctx"),
        axis=0,
        tiled=True,
    )
    full_out = lax.all_gather(out_weight.T, ("dp", "ctx"), axis=0, tiled=True)
    full_gate = to_columns(gate_weight, slice_width)
    full_up = to_columns(up_weight, slice_width)
    full_down = to_columns(down_weight.T, slice_width)
    valid_count = jnp.sum(valid_mask.astype(jnp.float32))
    counts = [valid_count]
    dp_size = lax.axis_size("dp")
    for step in range(1, dp_size):
        counts.append(
            lax.ppermute(
                jnp.full((8, 128), valid_count), "dp", [(i, (i + step) % dp_size) for i in range(dp_size)]
            )[0, 0]
        )
    valid_count = sum(counts)

    bias = jnp.concatenate(
        [
            lax.dynamic_slice_in_dim(query_bias, tensor_rank * q_width, q_width),
            lax.dynamic_slice_in_dim(key_bias, tensor_rank * kv_width, kv_width),
            lax.dynamic_slice_in_dim(value_bias, tensor_rank * kv_width, kv_width),
        ]
    ).astype(jnp.float32)
    places = lax.dynamic_slice_in_dim(positions, first_row, shard_rows)
    cosine, sine_table = rope_tables(places)
    qkv_pre = matmul(normed_rows, full_qkv) + bias
    turned = q_width + kv_width
    rotated = (
        rotate(qkv_pre[:, :turned].reshape(shard_rows, turned // HEAD, HEAD), cosine, sine_table)
        .astype(jnp.bfloat16)
        .reshape(shard_rows, turned)
    )
    queries = rotated[:, :q_width]
    own_kv = jnp.concatenate([rotated[:, q_width:], qkv_pre[:, turned:].astype(jnp.bfloat16)], axis=1)
    all_kv = lax.all_gather(own_kv, "ctx", axis=0, tiled=True)

    key_index = jnp.arange(seq_len, dtype=jnp.int32)
    key_place = jnp.where(valid_mask > 0, key_index, -1)[:, None]
    seq_first = lax.axis_index("dp") * seq_len
    doc_start = (lax.dynamic_slice_in_dim(segment_ids, first_row, shard_rows) - seq_first)[None, :]
    first = jnp.reshape(first_row, (1,)).astype(jnp.int32)
    forward, backward = attention_calls(shard_rows, seq_len, group)
    kept = []
    for c in range(kv_local):
        key = all_kv[:, c * HEAD : (c + 1) * HEAD]
        value = all_kv[:, kv_width + c * HEAD : kv_width + (c + 1) * HEAD]
        query = queries[:, c * group * HEAD : (c + 1) * group * HEAD]
        kept.append((query, key, value) + tuple(forward(first, doc_start, key_place, query, key, value.T)))
    heads_out = jnp.concatenate([k[3] for k in kept], axis=1)
    attention = lax.psum_scatter(
        matmul_nt(heads_out, full_out), "tensor", scatter_dimension=0, tiled=True
    )
    residual_mid = inputs + attention
    scale_mlp = lax.rsqrt(jnp.mean(residual_mid * residual_mid, axis=1, keepdims=True) + EPS)
    normed_mlp = residual_mid * scale_mlp
    mlp_rows = lax.all_gather(
        (normed_mlp * gain_two).astype(jnp.bfloat16), ("ctx", "tensor"), axis=0, tiled=True
    )
    gate_act = matmul(mlp_rows, full_gate)
    up_act = matmul(mlp_rows, full_up)
    sigmoid = jax.nn.sigmoid(gate_act)
    silu_gate = gate_act * sigmoid
    hidden = (silu_gate * up_act).astype(jnp.bfloat16)
    branch = lax.psum_scatter(
        matmul_nt(hidden, full_down).astype(jnp.bfloat16), ("ctx", "tensor"), scatter_dimension=0, tiled=True
    ).astype(jnp.float32)
    layer_result = residual_mid + branch
    valid_own = lax.dynamic_slice_in_dim(valid_mask, own_first, own_rows).astype(jnp.float32)
    difference = layer_result - teacher.astype(jnp.float32)
    squared_sum = jnp.sum(valid_own[:, None] * difference * difference)
    grad_result = cotangent.astype(jnp.float32) + 2.0 * valid_own[:, None] * difference / (
        valid_count * D
    )
    grad_branch = lax.all_gather(grad_result.astype(jnp.bfloat16), ("ctx", "tensor"), axis=0, tiled=True)
    grad_hidden = matmul(grad_branch, full_down)
    grad_gate_act = (grad_hidden * up_act * sigmoid * (1.0 + gate_act * (1.0 - sigmoid))).astype(
        jnp.bfloat16
    )
    grad_up_act = (grad_hidden * silu_gate).astype(jnp.bfloat16)
    grad_mlp_rows = lax.psum_scatter(
        (matmul_nt(grad_gate_act, full_gate) + matmul_nt(grad_up_act, full_up)).astype(
            jnp.bfloat16
        ),
        ("ctx", "tensor"),
        scatter_dimension=0,
        tiled=True,
    ).astype(jnp.float32)
    shard_down = to_rows(matmul_tn(grad_branch, hidden).astype(jnp.bfloat16), hidden_width).T
    shard_gate = to_rows(matmul_tn(mlp_rows, grad_gate_act).astype(jnp.bfloat16), hidden_width)
    shard_up = to_rows(matmul_tn(mlp_rows, grad_up_act).astype(jnp.bfloat16), hidden_width)
    grad_gain_mlp = jnp.sum(grad_mlp_rows * normed_mlp, axis=0)
    grad_mid = grad_result + norm_back(grad_mlp_rows, normed_mlp, scale_mlp, gain_two)
    grad_attn_rows = lax.all_gather(grad_mid.astype(jnp.bfloat16), "tensor", axis=0, tiled=True)
    grad_heads = matmul(grad_attn_rows, full_out).astype(jnp.bfloat16)
    grad_out = matmul_tn(grad_attn_rows, heads_out).astype(jnp.bfloat16)

    def scatter(grad):
        grad = lax.psum_scatter(grad, "dp", scatter_dimension=0, tiled=True)
        return lax.psum_scatter(grad, "ctx", scatter_dimension=0, tiled=True).astype(jnp.float32)

    shard_out = scatter(grad_out).T
    query_grads, key_grads, value_grads = [], [], []
    for c in range(kv_local):
        query, key, value, _, log_total = kept[c]
        span = slice(c * group * HEAD, (c + 1) * group * HEAD)
        grad_query, grad_kv = backward(
            first, doc_start, key_place, query, grad_heads[:, span], log_total, key, value, key.T
        )
        query_grads.append(grad_query)
        key_grads.append(grad_kv[:, :HEAD])
        value_grads.append(grad_kv[:, HEAD:])
    grad_kv = grad_kv if kv_local == 1 else jnp.concatenate(key_grads + value_grads, axis=1)
    grad_kv = lax.psum_scatter(grad_kv, "ctx", scatter_dimension=0, tiled=True)
    back = jnp.concatenate(query_grads + [grad_kv[:, :kv_width].astype(jnp.float32)], axis=1)
    grad_pre = jnp.concatenate(
        [
            rotate(back.reshape(shard_rows, turned // HEAD, HEAD), cosine, -sine_table)
            .reshape(shard_rows, turned)
            .astype(jnp.bfloat16),
            grad_kv[:, kv_width:],
        ],
        axis=1,
    )
    shard_qkv = scatter(matmul_tn(normed_rows, grad_pre).astype(jnp.bfloat16))
    grad_normed = lax.psum_scatter(
        matmul_nt(grad_pre, full_qkv).astype(jnp.bfloat16), "tensor", scatter_dimension=0, tiled=True
    ).astype(jnp.float32)
    grad_gain_attn = jnp.sum(grad_normed * normed_attn, axis=0)
    grad_input = grad_mid + norm_back(grad_normed, normed_attn, scale_attn, gain_one)
    bias_sum = jnp.sum(grad_pre.astype(jnp.float32), axis=0)

    def spread(part, size):
        return lax.dynamic_update_slice_in_dim(
            jnp.zeros((size,), jnp.float32), part, tensor_rank * part.shape[0], 0
        )

    loss_part = jnp.zeros((128,), jnp.float32).at[0].set(squared_sum)
    parts = [
        grad_gain_attn,
        grad_gain_mlp,
        spread(bias_sum[:q_width], query_bias.shape[0]),
        spread(bias_sum[q_width:turned], key_bias.shape[0]),
        spread(bias_sum[turned:], value_bias.shape[0]),
        loss_part,
    ]
    sums = sum_everywhere(jnp.concatenate(parts).reshape(-1, 128)).reshape(-1)
    pieces, offset = [], 0
    for part in parts:
        pieces.append(sums[offset : offset + part.shape[0]])
        offset += part.shape[0]
    return (
        layer_result.astype(jnp.bfloat16),
        pieces[5][0] / (valid_count * D),
        grad_input,
        pieces[0],
        shard_qkv[:, :q_width],
        pieces[2],
        shard_qkv[:, q_width:turned],
        pieces[3],
        shard_qkv[:, turned:],
        pieces[4],
        shard_out,
        pieces[1],
        shard_gate,
        shard_up,
        shard_down,
    )


def solution(mesh):
    in_specs = (
        P(("dp", "ctx", "tensor"), None),
        P(("dp", "ctx", "tensor"), None),
        P(("dp", "ctx", "tensor"), None),
        P("dp"),
        P("dp"),
        P("dp"),
        P(),
        P(("dp", "ctx"), "tensor"),
        P(),
        P(("dp", "ctx"), "tensor"),
        P(),
        P(("dp", "ctx"), "tensor"),
        P(),
        P("tensor", ("dp", "ctx")),
        P(),
        P(("dp", "ctx"), "tensor"),
        P(("dp", "ctx"), "tensor"),
        P("tensor", ("dp", "ctx")),
    )
    out_specs = (
        P(("dp", "ctx", "tensor"), None),
        P(),
        P(("dp", "ctx", "tensor"), None),
        P(),
        P(("dp", "ctx"), "tensor"),
        P(),
        P(("dp", "ctx"), "tensor"),
        P(),
        P(("dp", "ctx"), "tensor"),
        P(),
        P("tensor", ("dp", "ctx")),
        P(),
        P(("dp", "ctx"), "tensor"),
        P(("dp", "ctx"), "tensor"),
        P("tensor", ("dp", "ctx")),
    )
    return jax.shard_map(
        per_device, mesh=mesh, in_specs=in_specs, out_specs=out_specs, check_vma=False
    )
```

```python
import functools
import math

import jax
import jax.numpy as jnp
from jax import lax
from jax.experimental import pallas as pl
from jax.experimental.pallas import tpu as pltpu
from jax.sharding import PartitionSpec as P

D = 1536
HEAD = 128


EPS = 1e-06
THETA = 10000.0
VERY_LOW = -1e30


def rope_tables(places):
    half_dim = HEAD // 2
    frequency = THETA ** (-(jnp.arange(half_dim, dtype=jnp.float32) * 2.0 / HEAD))
    angles = places.astype(jnp.float32)[:, None] * frequency[None, :]
    return (jnp.cos(angles), jnp.sin(angles))


def rotate(stacked, cosine, sine_table):
    half_dim = HEAD // 2
    first_half = stacked[..., :half_dim]
    second_half = stacked[..., half_dim:]
    cosine = cosine[:, None, :]
    sine_table = sine_table[:, None, :]
    return jnp.concatenate(
        [
            first_half * cosine - second_half * sine_table,
            second_half * cosine + first_half * sine_table,
        ],
        axis=-1,
    )


def matmul(first_op, second_op):
    return jnp.dot(first_op, second_op, preferred_element_type=jnp.float32)


def matmul_tn(first_op, second_op):
    return lax.dot_general(
        first_op, second_op, (((0,), (0,)), ((), ())), preferred_element_type=jnp.float32
    )


def matmul_nt(first_op, second_op):
    return lax.dot_general(
        first_op, second_op, (((1,), (1,)), ((), ())), preferred_element_type=jnp.float32
    )


def norm_back(grad_normed, normed, inverse, gain):
    scaled = grad_normed * gain
    return inverse * (scaled - normed * jnp.mean(scaled * normed, axis=1, keepdims=True))


def exchange(blocks, axis):
    size = lax.axis_size(axis)
    rank = lax.axis_index(axis)
    received = [(rank, lax.dynamic_index_in_dim(blocks, rank, 0, keepdims=False))]
    for step in range(1, size):
        going = lax.dynamic_index_in_dim(blocks, (rank + step) % size, 0, keepdims=False)
        came = lax.ppermute(going, axis, [(i, (i + step) % size) for i in range(size)])
        received.append(((rank - step + size) % size, came))
    return received


def to_rows(grad, columns):
    size = lax.axis_size("ctx")
    summed = lax.psum_scatter(grad, "dp", scatter_dimension=0, tiled=True)
    rows, width = summed.shape[0] // size, summed.shape[1]
    shard = jnp.zeros((rows, size * width), jnp.bfloat16)
    for rank, block in exchange(summed.reshape(size, rows, width), "ctx"):
        shard = lax.dynamic_update_slice_in_dim(shard, block, rank * width, 1)
    return shard[:, :columns].astype(jnp.float32)


def sum_everywhere(value):
    for axis in ("tensor", "ctx", "dp"):
        size = lax.axis_size(axis)
        if size & (size - 1):
            value = lax.psum(value, axis)
            continue
        step = 1
        while step < size:
            value = value + lax.ppermute(value, axis, [(i, i ^ step) for i in range(size)])
            step *= 2
    return value


MESH = pl.DeviceIdType.MESH
ANY = pl.BlockSpec(memory_space=pl.ANY)
IN_VMEM = pl.BlockSpec(memory_space=pltpu.VMEM)


def remote(source, target, send_sem, recv_sem, device):
    return pltpu.make_async_remote_copy(
        src_ref=source,
        dst_ref=target,
        send_sem=send_sem,
        recv_sem=recv_sem,
        device_id=device,
        device_id_type=MESH,
    )


def greet(barrier, device):
    pl.semaphore_signal(barrier, inc=1, device_id=device, device_id_type=MESH)


def greet_chain(size, paired):
    place = lax.axis_index("ctx")
    barrier = pltpu.get_barrier_semaphore()
    if size > 1:
        pl.when(place < size - 1)(lambda: greet(barrier, {"ctx": place + 1}))
        pl.when(place > 0)(lambda: greet(barrier, {"ctx": place - 1}))
    if paired:
        greet(barrier, {"tensor": 1 - lax.axis_index("tensor")})
    if size == 1:
        pl.semaphore_wait(barrier, 1)
        return
    ends = (place == 0) | (place == size - 1)
    pl.when(ends)(lambda: pl.semaphore_wait(barrier, 1 + paired))
    pl.when(jnp.logical_not(ends))(lambda: pl.semaphore_wait(barrier, 2 + paired))


def gather_kernel(size, paired, pieces, x_ref, o_ref, local_sem, up_send, up_recv, down_send, down_recv, mate_send, mate_recv):
    place = lax.axis_index("ctx") if size > 1 else 0
    core = lax.axis_index("tensor")
    rows = x_ref.shape[0]
    part = rows // pieces
    greet_chain(size, paired)

    def block(rank, which, p):
        index = rank * 2 + which if paired else rank
        return o_ref.at[pl.ds(pl.multiple_of(index * rows + p * part, part), part)]

    def source(rank, k, p):
        return x_ref.at[pl.ds(p * part, part)] if k == 0 else block(rank, core, p)

    def going_up(k, p):
        return remote(
            source(place - k, k, p), block(place - k, core, p), up_send.at[k, p], up_recv.at[k, p], {"ctx": place + 1}
        )

    def going_down(k, p):
        return remote(
            source(place + k, k, p), block(place + k, core, p), down_send.at[k, p], down_recv.at[k, p], {"ctx": place - 1}
        )

    def to_mate(rank, k, p):
        return remote(
            source(rank, k, p), block(rank, core, p), mate_send.at[k, p], mate_recv.at[rank, p], {"tensor": 1 - core}
        )

    def from_mate(rank, p):
        there = block(rank, 1 - core, p)
        return remote(there, there, mate_send.at[0, p], mate_recv.at[rank, p], {"tensor": 1 - core})

    own = pltpu.make_async_copy(x_ref, o_ref.at[pl.ds(pl.multiple_of((place * 2 + core if paired else place) * rows, rows), rows)], local_sem)
    for p in range(pieces):
        if size > 1:
            pl.when(place < size - 1)(lambda p=p: going_up(0, p).start())
            pl.when(place > 0)(lambda p=p: going_down(0, p).start())
    for p in range(pieces):
        if paired:
            to_mate(place, 0, p).start()
    own.start()
    for k in range(size - 1):
        for p in range(pieces):

            @pl.when(place - 1 - k >= 0)
            def _(k=k, p=p):
                there = block(place - 1 - k, core, p)
                remote(there, there, up_send.at[k, p], up_recv.at[k, p], {"ctx": place - 1}).wait_recv()
                if k + 1 < size - 1:
                    pl.when(place < size - 1)(lambda: going_up(k + 1, p).start())
                if paired:
                    to_mate(place - 1 - k, 1 + k, p).start()

            @pl.when(place + 1 + k <= size - 1)
            def _(k=k, p=p):
                there = block(place + 1 + k, core, p)
                remote(there, there, down_send.at[k, p], down_recv.at[k, p], {"ctx": place + 1}).wait_recv()
                if k + 1 < size - 1:
                    pl.when(place > 0)(lambda: going_down(k + 1, p).start())
                if paired:
                    to_mate(place + 1 + k, size + k, p).start()

    own.wait()
    for p in range(pieces):
        if paired:
            for rank in range(size):
                from_mate(rank, p).wait_recv()
            to_mate(place, 0, p).wait_send()
        for k in range(size - 1):
            pl.when((place < size - 1) & (place - k >= 0))(lambda k=k, p=p: going_up(k, p).wait_send())
            pl.when((place > 0) & (place + k <= size - 1))(lambda k=k, p=p: going_down(k, p).wait_send())
            if paired:
                pl.when(place - 1 - k >= 0)(lambda k=k, p=p: to_mate(place - 1 - k, 1 + k, p).wait_send())
                pl.when(place + 1 + k <= size - 1)(lambda k=k, p=p: to_mate(place + 1 + k, size + k, p).wait_send())


def pieces_of(rows, columns):
    return math.gcd(4, rows // 64) if rows * columns >= 1 << 18 else 1


def gather(x, size, paired, ident):
    copies = size * 2 if paired else size
    wide = max(size, 2)
    pieces = pieces_of(*x.shape)
    dma = pltpu.SemaphoreType.DMA
    return pl.pallas_call(
        functools.partial(gather_kernel, size, paired, pieces),
        in_specs=[IN_VMEM],
        out_specs=ANY,
        out_shape=jax.ShapeDtypeStruct((copies * x.shape[0], x.shape[1]), x.dtype),
        scratch_shapes=[dma] + [dma((wide, pieces))] * 4 + [dma((2 * wide, pieces)), dma((wide, pieces))],
        compiler_params=pltpu.CompilerParams(collective_id=ident, has_side_effects=True),
        cost_estimate=pl.CostEstimate(flops=0, bytes_accessed=30 * copies * x.size, transcendentals=0),
        name="gather",
    )(x)


def add_blocks(target, parts):
    rows = target.shape[0]
    step = math.gcd(rows, 32)

    def some(i, carry):
        span = pl.ds(pl.multiple_of(i * step, step), step)
        total = parts[0][span].astype(jnp.float32)
        for part in parts[1:]:
            total += part[span].astype(jnp.float32)
        target[span] = total.astype(target.dtype)
        return carry

    lax.fori_loop(0, rows // step, some, 0)


def scatter_kernel(
    size, paired, pieces, x_ref, o_ref, mine, mate, above, below, own_sem, mate_send, mate_recv, up_send, up_recv, down_send, down_recv
):
    place = lax.axis_index("ctx") if size > 1 else 0
    core = lax.axis_index("tensor")
    rows = o_ref.shape[0]
    part = rows // pieces
    order = sorted(range(size), key=lambda d: min(d, size - 1 - d))
    every = [(d, p) for d in order for p in range(pieces)]

    def block(rank, which, p):
        index = rank * 2 + which if paired else rank
        return x_ref.at[pl.ds(pl.multiple_of(index * rows + p * part, part), part)]

    def at(ref, d, p):
        return ref.at[d, pl.ds(p * part, part)]

    def load(d, p):
        return pltpu.make_async_copy(block(d, core, p), at(mine, d, p), own_sem.at[d, p])

    def to_mate(d, p):
        return remote(
            block(d, 1 - core, p), at(mate, d, p), mate_send.at[d, p], mate_recv.at[d, p], {"tensor": 1 - core}
        )

    def going_up(d, p):
        return remote(at(mine, d, p), at(below, d, p), up_send.at[d, p], up_recv.at[d, p], {"ctx": place + 1})

    def going_down(d, p):
        return remote(at(mine, d, p), at(above, d, p), down_send.at[d, p], down_recv.at[d, p], {"ctx": place - 1})

    for d, p in every:
        load(d, p).start()
    greet_chain(size, paired)
    if paired:
        for d, p in every:
            to_mate(d, p).start()

    def here(d, p):
        load(d, p).wait()
        if paired:
            to_mate(d, p).wait_recv()
            return [at(mine, d, p), at(mate, d, p)]
        return [at(mine, d, p)]

    for k in range(size - 1):
        for p in range(pieces):

            @pl.when(place < size - 1 - k)
            def _(d=size - 1 - k, p=p):
                parts = here(d, p)

                @pl.when(place > 0)
                def _():
                    going_up(d, p).wait_recv()
                    add_blocks(at(mine, d, p), parts + [at(below, d, p)])

                if paired:
                    pl.when(place == 0)(lambda: add_blocks(at(mine, d, p), parts))
                going_up(d, p).start()

            @pl.when(place > k)
            def _(d=k, p=p):
                parts = here(d, p)

                @pl.when(place < size - 1)
                def _():
                    going_down(d, p).wait_recv()
                    add_blocks(at(mine, d, p), parts + [at(above, d, p)])

                if paired:
                    pl.when(place == size - 1)(lambda: add_blocks(at(mine, d, p), parts))
                going_down(d, p).start()

    for d in range(size):

        @pl.when(place == d)
        def _(d=d):
            for p in range(pieces):
                parts = here(d, p)
                if d > 0:
                    going_up(d, p).wait_recv()
                    parts = parts + [at(below, d, p)]
                if d < size - 1:
                    going_down(d, p).wait_recv()
                    parts = parts + [at(above, d, p)]
                add_blocks(o_ref.at[pl.ds(p * part, part)], parts)

    for d, p in every:
        if d > 0:
            pl.when(place < d)(lambda d=d, p=p: going_up(d, p).wait_send())
        if d < size - 1:
            pl.when(place > d)(lambda d=d, p=p: going_down(d, p).wait_send())
        if paired:
            to_mate(d, p).wait_send()


def scatter(x, size, paired, ident):
    copies = size * 2 if paired else size
    rows = x.shape[0] // copies
    pieces = pieces_of(rows, x.shape[1])
    dma = pltpu.SemaphoreType.DMA
    slots = pltpu.VMEM((size, rows, x.shape[1]), x.dtype)
    one = pltpu.VMEM((1, 32, 128), x.dtype)
    chain = slots if size > 1 else one
    return pl.pallas_call(
        functools.partial(scatter_kernel, size, paired, pieces),
        in_specs=[ANY],
        out_specs=IN_VMEM,
        out_shape=jax.ShapeDtypeStruct((rows, x.shape[1]), jnp.float32),
        scratch_shapes=[slots, slots if paired else one, chain, chain] + [dma((size, pieces))] * 7,
        compiler_params=pltpu.CompilerParams(collective_id=ident, has_side_effects=True, vmem_limit_bytes=60000000),
        cost_estimate=pl.CostEstimate(flops=0, bytes_accessed=30 * x.size, transcendentals=0),
        name="scatter",
    )(x)


def front_kernel(
    size, groups, a_ref, b_ref, g_ref, u_ref, d_ref, fa_ref, fb_ref, og_ref, ou_ref, od_ref,
    local_sem, up_send, up_recv, down_send, down_recv, far_send, far_recv, swap_send, swap_recv,
):
    place, group = lax.axis_index("ctx"), lax.axis_index("dp")
    rows, width = a_ref.shape[0], og_ref.shape[1]
    wholes, owns = (fa_ref, fb_ref), (a_ref, b_ref)
    parts, slices = (g_ref, u_ref, d_ref), (og_ref, ou_ref, od_ref)
    barrier = pltpu.get_barrier_semaphore()
    for step in range(1, size):
        greet(barrier, {"ctx": lax.rem(place + step, size)})
    for step in range(1, groups):
        greet(barrier, {"dp": lax.rem(group + step, groups)})
    pl.semaphore_wait(barrier, size + groups - 2)

    def chunk(which, in_group, rank):
        return wholes[which].at[pl.ds(pl.multiple_of((in_group * size + rank) * rows, rows), rows)]

    def source(which, rank, k):
        return owns[which] if k == 0 else chunk(which, group, rank)

    def going_up(which, k):
        return remote(
            source(which, place - k, k), chunk(which, group, place - k),
            up_send.at[which, k], up_recv.at[which, k], {"ctx": place + 1},
        )

    def going_down(which, k):
        return remote(
            source(which, place + k, k), chunk(which, group, place + k),
            down_send.at[which, k], down_recv.at[which, k], {"ctx": place - 1},
        )

    def across(which, rank, step, k):
        return remote(
            source(which, rank, k), chunk(which, group, rank),
            far_send.at[which, rank, step], far_recv.at[which, rank, step], {"dp": lax.rem(group + step, groups)},
        )

    def from_across(which, rank, step):
        there = chunk(which, lax.rem(group - step + groups, groups), rank)
        return remote(there, there, far_send.at[which, rank, step], far_recv.at[which, rank, step], {"dp": lax.rem(group + step, groups)})

    def columns(which, rank):
        return parts[which].at[:, pl.ds(pl.multiple_of(rank * width, 128), width)]

    def swap(which, step):
        return remote(
            columns(which, lax.rem(place + step, size)),
            slices[which].at[pl.ds(pl.multiple_of(place * rows, rows), rows)],
            swap_send.at[which, step], swap_recv.at[which, step], {"ctx": lax.rem(place + step, size)},
        )

    def swapped(which, step):
        there = slices[which].at[pl.ds(pl.multiple_of(lax.rem(place - step + size, size) * rows, rows), rows)]
        return remote(there, there, swap_send.at[which, step], swap_recv.at[which, step], {"ctx": lax.rem(place + step, size)})

    locals_ = [pltpu.make_async_copy(owns[w], chunk(w, group, place), local_sem.at[w]) for w in range(2)]
    locals_ += [
        pltpu.make_async_copy(
            columns(w, place), slices[w].at[pl.ds(pl.multiple_of(place * rows, rows), rows)], local_sem.at[2 + w]
        )
        for w in range(3)
    ]
    for w in range(2):
        pl.when(place < size - 1)(lambda w=w: going_up(w, 0).start())
        pl.when(place > 0)(lambda w=w: going_down(w, 0).start())
        for step in range(1, groups):
            across(w, place, step, 0).start()
    for copy in locals_:
        copy.start()
    for k in range(size - 1):
        for w in range(2):

            @pl.when(place - 1 - k >= 0)
            def _(k=k, w=w):
                there = chunk(w, group, place - 1 - k)
                remote(there, there, up_send.at[w, k], up_recv.at[w, k], {"ctx": place - 1}).wait_recv()
                if k + 1 < size - 1:
                    pl.when(place < size - 1)(lambda: going_up(w, k + 1).start())
                for step in range(1, groups):
                    across(w, place - 1 - k, step, 1).start()

            @pl.when(place + 1 + k <= size - 1)
            def _(k=k, w=w):
                there = chunk(w, group, place + 1 + k)
                remote(there, there, down_send.at[w, k], down_recv.at[w, k], {"ctx": place + 1}).wait_recv()
                if k + 1 < size - 1:
                    pl.when(place > 0)(lambda: going_down(w, k + 1).start())
                for step in range(1, groups):
                    across(w, place + 1 + k, step, 1).start()

    for w in range(3):
        for step in range(1, size):
            swap(w, step).start()
    for rank in range(size):
        for w in range(2):
            for step in range(1, groups):
                from_across(w, rank, step).wait_recv()
    for w in range(3):
        for step in range(1, size):
            swapped(w, step).wait_recv()
    for copy in locals_:
        copy.wait()
    for w in range(2):
        for k in range(size - 1):
            pl.when((place < size - 1) & (place - k >= 0))(lambda k=k, w=w: going_up(w, k).wait_send())
            pl.when((place > 0) & (place + k <= size - 1))(lambda k=k, w=w: going_down(w, k).wait_send())
        for rank in range(size):
            for step in range(1, groups):
                across(w, rank, step, 1).wait_send()
    for w in range(3):
        for step in range(1, size):
            swap(w, step).wait_send()


def front(a, b, parts, width, ident):
    size, groups = lax.axis_size("ctx"), lax.axis_size("dp")
    rows = a.shape[0]
    dma = pltpu.SemaphoreType.DMA
    slices = jax.ShapeDtypeStruct((size * rows, width), a.dtype)
    return pl.pallas_call(
        functools.partial(front_kernel, size, groups),
        in_specs=[IN_VMEM] * 5,
        out_specs=[ANY] * 5,
        out_shape=[jax.ShapeDtypeStruct((groups * size * rows, x.shape[1]), x.dtype) for x in (a, b)] + [slices] * 3,
        scratch_shapes=[dma((5,))] + [dma((2, size))] * 4 + [dma((2, size, groups))] * 2 + [dma((3, size))] * 2,
        compiler_params=pltpu.CompilerParams(collective_id=ident, has_side_effects=True),
        cost_estimate=pl.CostEstimate(flops=0, bytes_accessed=200000000, transcendentals=0),
        name="front",
    )(a, b, *parts)


def mask_into(bias_ref, first, seg_ref, place_ref):
    keys, rows = bias_ref.shape
    key_index = lax.broadcasted_iota(jnp.int32, (keys, rows), 0)
    row_index = lax.broadcasted_iota(jnp.int32, (keys, rows), 1) + first
    place = jnp.broadcast_to(place_ref[...], (keys, rows))
    start = jnp.broadcast_to(seg_ref[...], (keys, rows))
    allowed = ((place >= start) & (place <= row_index)) | (key_index == row_index)
    bias_ref[...] = jnp.where(allowed, 0.0, VERY_LOW)


def nn(first_op, second_op):
    return jnp.dot(first_op, second_op, preferred_element_type=jnp.float32)


def attend_kernel(scale, first_ref, seg_ref, place_ref, q_ref, k_ref, vt_ref, o_ref, lse_ref, bias_ref):
    @pl.when(pl.program_id(1) == 0)
    def _():
        mask_into(bias_ref, first_ref[0] + pl.program_id(0) * q_ref.shape[0], seg_ref, place_ref)

    scores = matmul_nt(k_ref[...], q_ref[...]) * scale + bias_ref[...]
    top = jnp.max(scores, axis=0, keepdims=True)
    powers = jnp.exp(scores - top)
    total = jnp.sum(powers, axis=0, keepdims=True)
    mixture = nn(vt_ref[...], powers.astype(jnp.bfloat16)) / total
    o_ref[...] = mixture.T.astype(jnp.bfloat16)
    lse_ref[0] = top + jnp.log(total)


def attend_back_kernel(
    scale, first_ref, seg_ref, place_ref, q_ref, do_ref, lse_ref, k_ref, v_ref, kt_ref,
    dq_ref, dkv_ref, bias_ref, dk_ref, dv_ref,
):
    block, head = pl.program_id(0), pl.program_id(1)

    @pl.when(head == 0)
    def _():
        mask_into(bias_ref, first_ref[0] + block * q_ref.shape[0], seg_ref, place_ref)

    @pl.when((head == 0) & (block == 0))
    def _():
        dk_ref[...] = jnp.zeros_like(dk_ref)
        dv_ref[...] = jnp.zeros_like(dv_ref)

    query, grad = q_ref[...], do_ref[...]
    scores = matmul_nt(k_ref[...], query) * scale + bias_ref[...]
    probs = jnp.exp(scores - lse_ref[0])
    grad_probs = matmul_nt(v_ref[...], grad)
    delta = jnp.sum(probs * grad_probs, axis=0, keepdims=True)
    grad_scores = (probs * (grad_probs - delta)).astype(jnp.bfloat16)
    dv_ref[...] += nn(probs.astype(jnp.bfloat16), grad)
    dk_ref[...] += nn(grad_scores, query)
    dq_ref[...] = (nn(kt_ref[...], grad_scores) * scale).T

    @pl.when((head == pl.num_programs(1) - 1) & (block == pl.num_programs(0) - 1))
    def _():
        dkv_ref[:, :HEAD] = (dk_ref[...] * scale).astype(jnp.bfloat16)
        dkv_ref[:, HEAD:] = dv_ref[...].astype(jnp.bfloat16)


def attention_calls(rows, keys, heads):
    block = math.gcd(256, rows)
    scale = 1.0 / math.sqrt(HEAD)
    smem = pl.BlockSpec(memory_space=pltpu.SMEM)
    seg = pl.BlockSpec((1, block), lambda i, h: (0, i))
    place = pl.BlockSpec((keys, 1), lambda i, h: (0, 0))
    head = pl.BlockSpec((block, HEAD), lambda i, h: (i, h))
    lse = pl.BlockSpec((1, 1, block), lambda i, h: (h, 0, i))
    tall = pl.BlockSpec((keys, HEAD), lambda i, h: (0, 0))
    wide = pl.BlockSpec((HEAD, keys), lambda i, h: (0, 0))
    params = pltpu.CompilerParams(vmem_limit_bytes=60000000)
    grid = (rows // block, heads)
    size = heads * rows * keys
    forward = pl.pallas_call(
        functools.partial(attend_kernel, scale),
        grid=grid,
        in_specs=[smem, seg, place, head, tall, wide],
        out_specs=[head, lse],
        out_shape=[
            jax.ShapeDtypeStruct((rows, heads * HEAD), jnp.bfloat16),
            jax.ShapeDtypeStruct((heads, 1, rows), jnp.float32),
        ],
        scratch_shapes=[pltpu.VMEM((keys, block), jnp.float32)],
        compiler_params=params,
        cost_estimate=pl.CostEstimate(flops=4 * size * HEAD, bytes_accessed=4 * rows * heads * HEAD, transcendentals=size),
        name="attend",
    )
    backward = pl.pallas_call(
        functools.partial(attend_back_kernel, scale),
        grid=grid,
        in_specs=[smem, seg, place, head, head, lse, tall, tall, wide],
        out_specs=[head, pl.BlockSpec((keys, 2 * HEAD), lambda i, h: (0, 0))],
        out_shape=[
            jax.ShapeDtypeStruct((rows, heads * HEAD), jnp.float32),
            jax.ShapeDtypeStruct((keys, 2 * HEAD), jnp.bfloat16),
        ],
        scratch_shapes=[
            pltpu.VMEM((keys, block), jnp.float32),
            pltpu.VMEM((keys, HEAD), jnp.float32),
            pltpu.VMEM((keys, HEAD), jnp.float32),
        ],
        compiler_params=params,
        cost_estimate=pl.CostEstimate(flops=10 * size * HEAD, bytes_accessed=8 * rows * heads * HEAD, transcendentals=size),
        name="attend_back",
    )
    return forward, backward


def per_device(
    layer_input,
    teacher,
    cotangent,
    segment_ids,
    positions,
    valid_mask,
    gain_attn,
    query_weight,
    query_bias,
    key_weight,
    key_bias,
    value_weight,
    value_bias,
    out_weight,
    gain_mlp,
    gate_weight,
    up_weight,
    down_weight,
):
    tensor_rank = lax.axis_index("tensor")
    ctx_rank = lax.axis_index("ctx")
    tensor_size, ctx_size = lax.axis_size("tensor"), lax.axis_size("ctx")
    own_rows = layer_input.shape[0]
    shard_rows = own_rows * tensor_size
    seq_len = segment_ids.shape[0]
    q_width = query_weight.shape[1]
    kv_width = key_weight.shape[1]
    kv_local = kv_width // HEAD
    group = q_width // kv_width
    hidden_width = gate_weight.shape[1]
    slice_width = -(-hidden_width // (128 * ctx_size)) * 128
    first_row = ctx_rank * shard_rows
    own_first = first_row + tensor_rank * own_rows

    inputs = layer_input.astype(jnp.float32)
    gain_one = gain_attn.astype(jnp.float32)
    gain_two = gain_mlp.astype(jnp.float32)
    scale_attn = lax.rsqrt(jnp.mean(inputs * inputs, axis=1, keepdims=True) + EPS)
    normed_attn = inputs * scale_attn
    extra = ((0, 0), (0, ctx_size * slice_width - hidden_width))
    full_qkv, full_out, *slices = front(
        jnp.concatenate([query_weight, key_weight, value_weight], axis=1),
        out_weight.T,
        [jnp.pad(w, extra) for w in (gate_weight, up_weight, down_weight.T)],
        slice_width,
        1,
    )
    full_gate, full_up, full_down = [lax.all_gather(w, "dp", axis=0, tiled=True) for w in slices]
    normed_rows = gather((normed_attn * gain_one).astype(jnp.bfloat16), 1, True, 2)
    valid_count = jnp.sum(valid_mask.astype(jnp.float32))
    counts = [valid_count]
    dp_size = lax.axis_size("dp")
    for step in range(1, dp_size):
        counts.append(
            lax.ppermute(
                jnp.full((8, 128), valid_count), "dp", [(i, (i + step) % dp_size) for i in range(dp_size)]
            )[0, 0]
        )
    valid_count = sum(counts)

    bias = jnp.concatenate(
        [
            lax.dynamic_slice_in_dim(query_bias, tensor_rank * q_width, q_width),
            lax.dynamic_slice_in_dim(key_bias, tensor_rank * kv_width, kv_width),
            lax.dynamic_slice_in_dim(value_bias, tensor_rank * kv_width, kv_width),
        ]
    ).astype(jnp.float32)
    places = lax.dynamic_slice_in_dim(positions, first_row, shard_rows)
    cosine, sine_table = rope_tables(places)
    qkv_pre = matmul(normed_rows, full_qkv) + bias
    turned = q_width + kv_width
    rotated = (
        rotate(qkv_pre[:, :turned].reshape(shard_rows, turned // HEAD, HEAD), cosine, sine_table)
        .astype(jnp.bfloat16)
        .reshape(shard_rows, turned)
    )
    queries = rotated[:, :q_width]
    own_kv = jnp.concatenate([rotated[:, q_width:], qkv_pre[:, turned:].astype(jnp.bfloat16)], axis=1)
    all_kv = gather(own_kv, ctx_size, False, 3)

    key_index = jnp.arange(seq_len, dtype=jnp.int32)
    key_place = jnp.where(valid_mask > 0, key_index, -1)[:, None]
    seq_first = lax.axis_index("dp") * seq_len
    doc_start = (lax.dynamic_slice_in_dim(segment_ids, first_row, shard_rows) - seq_first)[None, :]
    first = jnp.reshape(first_row, (1,)).astype(jnp.int32)
    forward, backward = attention_calls(shard_rows, seq_len, group)
    kept = []
    for c in range(kv_local):
        key = all_kv[:, c * HEAD : (c + 1) * HEAD]
        value = all_kv[:, kv_width + c * HEAD : kv_width + (c + 1) * HEAD]
        query = queries[:, c * group * HEAD : (c + 1) * group * HEAD]
        kept.append((query, key, value) + tuple(forward(first, doc_start, key_place, query, key, value.T)))
    heads_out = jnp.concatenate([k[3] for k in kept], axis=1)
    attention = scatter(matmul_nt(heads_out, full_out), 1, True, 4)
    residual_mid = inputs + attention
    scale_mlp = lax.rsqrt(jnp.mean(residual_mid * residual_mid, axis=1, keepdims=True) + EPS)
    normed_mlp = residual_mid * scale_mlp
    mlp_rows = gather((normed_mlp * gain_two).astype(jnp.bfloat16), ctx_size, True, 5)
    gate_act = matmul(mlp_rows, full_gate)
    up_act = matmul(mlp_rows, full_up)
    sigmoid = jax.nn.sigmoid(gate_act)
    silu_gate = gate_act * sigmoid
    hidden = (silu_gate * up_act).astype(jnp.bfloat16)
    branch = scatter(matmul_nt(hidden, full_down).astype(jnp.bfloat16), ctx_size, True, 6)
    layer_result = residual_mid + branch
    valid_own = lax.dynamic_slice_in_dim(valid_mask, own_first, own_rows).astype(jnp.float32)
    difference = layer_result - teacher.astype(jnp.float32)
    squared_sum = jnp.sum(valid_own[:, None] * difference * difference)
    grad_result = cotangent.astype(jnp.float32) + 2.0 * valid_own[:, None] * difference / (
        valid_count * D
    )
    grad_branch = gather(grad_result.astype(jnp.bfloat16), ctx_size, True, 5)
    grad_hidden = matmul(grad_branch, full_down)
    grad_gate_act = (grad_hidden * up_act * sigmoid * (1.0 + gate_act * (1.0 - sigmoid))).astype(
        jnp.bfloat16
    )
    grad_up_act = (grad_hidden * silu_gate).astype(jnp.bfloat16)
    grad_mlp_rows = lax.psum_scatter(
        (matmul_nt(grad_gate_act, full_gate) + matmul_nt(grad_up_act, full_up)).astype(
            jnp.bfloat16
        ),
        ("ctx", "tensor"),
        scatter_dimension=0,
        tiled=True,
    ).astype(jnp.float32)
    shard_down = to_rows(matmul_tn(grad_branch, hidden).astype(jnp.bfloat16), hidden_width).T
    shard_gate = to_rows(matmul_tn(mlp_rows, grad_gate_act).astype(jnp.bfloat16), hidden_width)
    shard_up = to_rows(matmul_tn(mlp_rows, grad_up_act).astype(jnp.bfloat16), hidden_width)
    grad_gain_mlp = jnp.sum(grad_mlp_rows * normed_mlp, axis=0)
    grad_mid = grad_result + norm_back(grad_mlp_rows, normed_mlp, scale_mlp, gain_two)
    grad_attn_rows = gather(grad_mid.astype(jnp.bfloat16), 1, True, 2)
    grad_heads = matmul(grad_attn_rows, full_out).astype(jnp.bfloat16)
    grad_out = matmul_tn(grad_attn_rows, heads_out).astype(jnp.bfloat16)

    def to_owner(grad):
        grad = lax.psum_scatter(grad, "dp", scatter_dimension=0, tiled=True)
        return lax.psum_scatter(grad, "ctx", scatter_dimension=0, tiled=True).astype(jnp.float32)

    shard_out = to_owner(grad_out).T
    query_grads, key_grads, value_grads = [], [], []
    for c in range(kv_local):
        query, key, value, _, log_total = kept[c]
        span = slice(c * group * HEAD, (c + 1) * group * HEAD)
        grad_query, grad_kv = backward(
            first, doc_start, key_place, query, grad_heads[:, span], log_total, key, value, key.T
        )
        query_grads.append(grad_query)
        key_grads.append(grad_kv[:, :HEAD])
        value_grads.append(grad_kv[:, HEAD:])
    grad_kv = grad_kv if kv_local == 1 else jnp.concatenate(key_grads + value_grads, axis=1)
    grad_kv = scatter(grad_kv, ctx_size, False, 7)
    back = jnp.concatenate(query_grads + [grad_kv[:, :kv_width]], axis=1)
    grad_pre = jnp.concatenate(
        [
            rotate(back.reshape(shard_rows, turned // HEAD, HEAD), cosine, -sine_table)
            .reshape(shard_rows, turned)
            .astype(jnp.bfloat16),
            grad_kv[:, kv_width:].astype(jnp.bfloat16),
        ],
        axis=1,
    )
    shard_qkv = to_owner(matmul_tn(normed_rows, grad_pre).astype(jnp.bfloat16))
    grad_normed = scatter(matmul_nt(grad_pre, full_qkv), 1, True, 4)
    grad_gain_attn = jnp.sum(grad_normed * normed_attn, axis=0)
    grad_input = grad_mid + norm_back(grad_normed, normed_attn, scale_attn, gain_one)
    bias_sum = jnp.sum(grad_pre.astype(jnp.float32), axis=0)

    def spread(part, size):
        return lax.dynamic_update_slice_in_dim(
            jnp.zeros((size,), jnp.float32), part, tensor_rank * part.shape[0], 0
        )

    loss_part = jnp.zeros((128,), jnp.float32).at[0].set(squared_sum)
    parts = [
        grad_gain_attn,
        grad_gain_mlp,
        spread(bias_sum[:q_width], query_bias.shape[0]),
        spread(bias_sum[q_width:turned], key_bias.shape[0]),
        spread(bias_sum[turned:], value_bias.shape[0]),
        loss_part,
    ]
    sums = sum_everywhere(jnp.concatenate(parts).reshape(-1, 128)).reshape(-1)
    pieces, offset = [], 0
    for part in parts:
        pieces.append(sums[offset : offset + part.shape[0]])
        offset += part.shape[0]
    return (
        layer_result.astype(jnp.bfloat16),
        pieces[5][0] / (valid_count * D),
        grad_input,
        pieces[0],
        shard_qkv[:, :q_width],
        pieces[2],
        shard_qkv[:, q_width:turned],
        pieces[3],
        shard_qkv[:, turned:],
        pieces[4],
        shard_out,
        pieces[1],
        shard_gate,
        shard_up,
        shard_down,
    )


def solution(mesh):
    in_specs = (
        P(("dp", "ctx", "tensor"), None),
        P(("dp", "ctx", "tensor"), None),
        P(("dp", "ctx", "tensor"), None),
        P("dp"),
        P("dp"),
        P("dp"),
        P(),
        P(("dp", "ctx"), "tensor"),
        P(),
        P(("dp", "ctx"), "tensor"),
        P(),
        P(("dp", "ctx"), "tensor"),
        P(),
        P("tensor", ("dp", "ctx")),
        P(),
        P(("dp", "ctx"), "tensor"),
        P(("dp", "ctx"), "tensor"),
        P("tensor", ("dp", "ctx")),
    )
    out_specs = (
        P(("dp", "ctx", "tensor"), None),
        P(),
        P(("dp", "ctx", "tensor"), None),
        P(),
        P(("dp", "ctx"), "tensor"),
        P(),
        P(("dp", "ctx"), "tensor"),
        P(),
        P(("dp", "ctx"), "tensor"),
        P(),
        P("tensor", ("dp", "ctx")),
        P(),
        P(("dp", "ctx"), "tensor"),
        P(("dp", "ctx"), "tensor"),
        P("tensor", ("dp", "ctx")),
    )
    return jax.shard_map(
        per_device, mesh=mesh, in_specs=in_specs, out_specs=out_specs, check_vma=False
    )
```

```python
import functools
import math

import jax
import jax.numpy as jnp
from jax import lax
from jax.experimental import pallas as pl
from jax.experimental.pallas import tpu as pltpu
from jax.sharding import PartitionSpec as P


D = 1536
HEAD = 128


EPS = 1e-06
THETA = 10000.0
VERY_LOW = -1e30


def rope_tables(places):
    half_dim = HEAD // 2
    frequency = THETA ** (-(jnp.arange(half_dim, dtype=jnp.float32) * 2.0 / HEAD))
    angles = places.astype(jnp.float32)[:, None] * frequency[None, :]
    return (jnp.cos(angles), jnp.sin(angles))


def rotate(stacked, cosine, sine_table):
    half_dim = HEAD // 2
    first_half = stacked[..., :half_dim]
    second_half = stacked[..., half_dim:]
    cosine = cosine[:, None, :]
    sine_table = sine_table[:, None, :]
    return jnp.concatenate(
        [
            first_half * cosine - second_half * sine_table,
            second_half * cosine + first_half * sine_table,
        ],
        axis=-1,
    )


def matmul(first_op, second_op):
    return jnp.dot(first_op, second_op, preferred_element_type=jnp.float32)


def matmul_tn(first_op, second_op):
    return lax.dot_general(
        first_op, second_op, (((0,), (0,)), ((), ())), preferred_element_type=jnp.float32
    )


def matmul_nt(first_op, second_op):
    return lax.dot_general(
        first_op, second_op, (((1,), (1,)), ((), ())), preferred_element_type=jnp.float32
    )


def norm_back(grad_normed, normed, inverse, gain):
    scaled = grad_normed * gain
    return inverse * (scaled - normed * jnp.mean(scaled * normed, axis=1, keepdims=True))


def exchange(blocks, axis):
    size = lax.axis_size(axis)
    rank = lax.axis_index(axis)
    received = [(rank, lax.dynamic_index_in_dim(blocks, rank, 0, keepdims=False))]
    for step in range(1, size):
        going = lax.dynamic_index_in_dim(blocks, (rank + step) % size, 0, keepdims=False)
        came = lax.ppermute(going, axis, [(i, (i + step) % size) for i in range(size)])
        received.append(((rank - step + size) % size, came))
    return received


def to_rows(summed, columns):
    size = lax.axis_size("ctx")
    rows, width = summed[0].shape[0] // size, summed[0].shape[1]
    blocks = jnp.stack([s.reshape(size, rows, width) for s in summed], axis=1)
    shards = jnp.zeros((len(summed), rows, size * width), jnp.bfloat16)
    for rank, block in exchange(blocks, "ctx"):
        shards = lax.dynamic_update_slice_in_dim(shards, block, rank * width, 2)
    return [s[:, :columns].astype(jnp.float32) for s in shards]


def sum_everywhere(value):
    for axis in ("tensor", "ctx", "dp"):
        size = lax.axis_size(axis)
        if size & (size - 1):
            value = lax.psum(value, axis)
            continue
        step = 1
        while step < size:
            value = value + lax.ppermute(value, axis, [(i, i ^ step) for i in range(size)])
            step *= 2
    return value


MESH = pl.DeviceIdType.MESH
ANY = pl.BlockSpec(memory_space=pl.ANY)
IN_VMEM = pl.BlockSpec(memory_space=pltpu.VMEM)


def remote(source, target, send_sem, recv_sem, device):
    return pltpu.make_async_remote_copy(
        src_ref=source,
        dst_ref=target,
        send_sem=send_sem,
        recv_sem=recv_sem,
        device_id=device,
        device_id_type=MESH,
    )


def greet(barrier, device):
    pl.semaphore_signal(barrier, inc=1, device_id=device, device_id_type=MESH)


def greet_chain(size, paired):
    place = lax.axis_index("ctx")
    barrier = pltpu.get_barrier_semaphore()
    if size > 1:
        pl.when(place < size - 1)(lambda: greet(barrier, {"ctx": place + 1}))
        pl.when(place > 0)(lambda: greet(barrier, {"ctx": place - 1}))
    if paired:
        greet(barrier, {"tensor": 1 - lax.axis_index("tensor")})
    if size == 1:
        pl.semaphore_wait(barrier, 1)
        return
    ends = (place == 0) | (place == size - 1)
    pl.when(ends)(lambda: pl.semaphore_wait(barrier, 1 + paired))
    pl.when(jnp.logical_not(ends))(lambda: pl.semaphore_wait(barrier, 2 + paired))


def gather_kernel(size, paired, pieces, x_ref, o_ref, local_sem, up_send, up_recv, down_send, down_recv, mate_send, mate_recv):
    place = lax.axis_index("ctx") if size > 1 else 0
    core = lax.axis_index("tensor")
    rows = x_ref.shape[0]
    part = rows // pieces
    greet_chain(size, paired)

    def block(rank, which, p):
        index = rank * 2 + which if paired else rank
        return o_ref.at[pl.ds(pl.multiple_of(index * rows + p * part, part), part)]

    def source(rank, k, p):
        return x_ref.at[pl.ds(p * part, part)] if k == 0 else block(rank, core, p)

    def going_up(k, p):
        return remote(
            source(place - k, k, p), block(place - k, core, p), up_send.at[k, p], up_recv.at[k, p], {"ctx": place + 1}
        )

    def going_down(k, p):
        return remote(
            source(place + k, k, p), block(place + k, core, p), down_send.at[k, p], down_recv.at[k, p], {"ctx": place - 1}
        )

    def to_mate(rank, k, p):
        return remote(
            source(rank, k, p), block(rank, core, p), mate_send.at[k, p], mate_recv.at[rank, p], {"tensor": 1 - core}
        )

    def from_mate(rank, p):
        there = block(rank, 1 - core, p)
        return remote(there, there, mate_send.at[0, p], mate_recv.at[rank, p], {"tensor": 1 - core})

    own = pltpu.make_async_copy(x_ref, o_ref.at[pl.ds(pl.multiple_of((place * 2 + core if paired else place) * rows, rows), rows)], local_sem)
    for p in range(pieces):
        if size > 1:
            pl.when(place < size - 1)(lambda p=p: going_up(0, p).start())
            pl.when(place > 0)(lambda p=p: going_down(0, p).start())
    for p in range(pieces):
        if paired:
            to_mate(place, 0, p).start()
    own.start()
    for k in range(size - 1):
        for p in range(pieces):

            @pl.when(place - 1 - k >= 0)
            def _(k=k, p=p):
                there = block(place - 1 - k, core, p)
                remote(there, there, up_send.at[k, p], up_recv.at[k, p], {"ctx": place - 1}).wait_recv()
                if k + 1 < size - 1:
                    pl.when(place < size - 1)(lambda: going_up(k + 1, p).start())
                if paired:
                    to_mate(place - 1 - k, 1 + k, p).start()

            @pl.when(place + 1 + k <= size - 1)
            def _(k=k, p=p):
                there = block(place + 1 + k, core, p)
                remote(there, there, down_send.at[k, p], down_recv.at[k, p], {"ctx": place + 1}).wait_recv()
                if k + 1 < size - 1:
                    pl.when(place > 0)(lambda: going_down(k + 1, p).start())
                if paired:
                    to_mate(place + 1 + k, size + k, p).start()

    own.wait()
    for p in range(pieces):
        if paired:
            for rank in range(size):
                from_mate(rank, p).wait_recv()
            to_mate(place, 0, p).wait_send()
        for k in range(size - 1):
            pl.when((place < size - 1) & (place - k >= 0))(lambda k=k, p=p: going_up(k, p).wait_send())
            pl.when((place > 0) & (place + k <= size - 1))(lambda k=k, p=p: going_down(k, p).wait_send())
            if paired:
                pl.when(place - 1 - k >= 0)(lambda k=k, p=p: to_mate(place - 1 - k, 1 + k, p).wait_send())
                pl.when(place + 1 + k <= size - 1)(lambda k=k, p=p: to_mate(place + 1 + k, size + k, p).wait_send())


def pieces_of(rows, columns):
    return math.gcd(4, rows // 64) if rows * columns >= 1 << 18 else 1


def gather(x, size, paired, ident):
    copies = size * 2 if paired else size
    wide = max(size, 2)
    pieces = pieces_of(*x.shape)
    dma = pltpu.SemaphoreType.DMA
    return pl.pallas_call(
        functools.partial(gather_kernel, size, paired, pieces),
        in_specs=[IN_VMEM],
        out_specs=ANY,
        out_shape=jax.ShapeDtypeStruct((copies * x.shape[0], x.shape[1]), x.dtype),
        scratch_shapes=[dma] + [dma((wide, pieces))] * 4 + [dma((2 * wide, pieces)), dma((wide, pieces))],
        compiler_params=pltpu.CompilerParams(collective_id=ident, has_side_effects=True),
        cost_estimate=pl.CostEstimate(flops=0, bytes_accessed=30 * copies * x.size, transcendentals=0),
        name="gather",
    )(x)


def add_blocks(target, parts):
    rows = target.shape[0]
    step = math.gcd(rows, 32)

    def some(i, carry):
        span = pl.ds(pl.multiple_of(i * step, step), step)
        total = parts[0][span].astype(jnp.float32)
        for part in parts[1:]:
            total += part[span].astype(jnp.float32)
        target[span] = total.astype(target.dtype)
        return carry

    lax.fori_loop(0, rows // step, some, 0)


def scatter_kernel(
    size, paired, pieces, x_ref, o_ref, mine, mate, above, below, own_sem, mate_send, mate_recv, up_send, up_recv, down_send, down_recv
):
    place = lax.axis_index("ctx") if size > 1 else 0
    core = lax.axis_index("tensor")
    rows = o_ref.shape[0]
    part = rows // pieces
    order = sorted(range(size), key=lambda d: min(d, size - 1 - d))
    every = [(d, p) for d in order for p in range(pieces)]

    def block(rank, which, p):
        index = rank * 2 + which if paired else rank
        return x_ref.at[pl.ds(pl.multiple_of(index * rows + p * part, part), part)]

    def at(ref, d, p):
        return ref.at[d, pl.ds(p * part, part)]

    def load(d, p):
        return pltpu.make_async_copy(block(d, core, p), at(mine, d, p), own_sem.at[d, p])

    def to_mate(d, p):
        return remote(
            block(d, 1 - core, p), at(mate, d, p), mate_send.at[d, p], mate_recv.at[d, p], {"tensor": 1 - core}
        )

    def going_up(d, p):
        return remote(at(mine, d, p), at(below, d, p), up_send.at[d, p], up_recv.at[d, p], {"ctx": place + 1})

    def going_down(d, p):
        return remote(at(mine, d, p), at(above, d, p), down_send.at[d, p], down_recv.at[d, p], {"ctx": place - 1})

    for d, p in every:
        load(d, p).start()
    greet_chain(size, paired)
    if paired:
        for d, p in every:
            to_mate(d, p).start()

    def here(d, p):
        load(d, p).wait()
        if paired:
            to_mate(d, p).wait_recv()
            return [at(mine, d, p), at(mate, d, p)]
        return [at(mine, d, p)]

    for k in range(size - 1):
        for p in range(pieces):

            @pl.when(place < size - 1 - k)
            def _(d=size - 1 - k, p=p):
                parts = here(d, p)

                @pl.when(place > 0)
                def _():
                    going_up(d, p).wait_recv()
                    add_blocks(at(mine, d, p), parts + [at(below, d, p)])

                if paired:
                    pl.when(place == 0)(lambda: add_blocks(at(mine, d, p), parts))
                going_up(d, p).start()

            @pl.when(place > k)
            def _(d=k, p=p):
                parts = here(d, p)

                @pl.when(place < size - 1)
                def _():
                    going_down(d, p).wait_recv()
                    add_blocks(at(mine, d, p), parts + [at(above, d, p)])

                if paired:
                    pl.when(place == size - 1)(lambda: add_blocks(at(mine, d, p), parts))
                going_down(d, p).start()

    for d in range(size):

        @pl.when(place == d)
        def _(d=d):
            for p in range(pieces):
                parts = here(d, p)
                if d > 0:
                    going_up(d, p).wait_recv()
                    parts = parts + [at(below, d, p)]
                if d < size - 1:
                    going_down(d, p).wait_recv()
                    parts = parts + [at(above, d, p)]
                add_blocks(o_ref.at[pl.ds(p * part, part)], parts)

    for d, p in every:
        if d > 0:
            pl.when(place < d)(lambda d=d, p=p: going_up(d, p).wait_send())
        if d < size - 1:
            pl.when(place > d)(lambda d=d, p=p: going_down(d, p).wait_send())
        if paired:
            to_mate(d, p).wait_send()


def scatter(x, size, paired, ident):
    copies = size * 2 if paired else size
    rows = x.shape[0] // copies
    pieces = pieces_of(rows, x.shape[1])
    dma = pltpu.SemaphoreType.DMA
    slots = pltpu.VMEM((size, rows, x.shape[1]), x.dtype)
    one = pltpu.VMEM((1, 32, 128), x.dtype)
    chain = slots if size > 1 else one
    return pl.pallas_call(
        functools.partial(scatter_kernel, size, paired, pieces),
        in_specs=[ANY],
        out_specs=IN_VMEM,
        out_shape=jax.ShapeDtypeStruct((rows, x.shape[1]), jnp.float32),
        scratch_shapes=[slots, slots if paired else one, chain, chain] + [dma((size, pieces))] * 7,
        compiler_params=pltpu.CompilerParams(collective_id=ident, has_side_effects=True, vmem_limit_bytes=60000000),
        cost_estimate=pl.CostEstimate(flops=0, bytes_accessed=30 * x.size, transcendentals=0),
        name="scatter",
    )(x)


def front_kernel(
    size, groups, a_ref, b_ref, g_ref, u_ref, d_ref, fa_ref, fb_ref, og_ref, ou_ref, od_ref,
    local_sem, up_send, up_recv, down_send, down_recv, far_send, far_recv, swap_send, swap_recv,
):
    place, group = lax.axis_index("ctx"), lax.axis_index("dp")
    rows, width = a_ref.shape[0], og_ref.shape[1]
    wholes, owns = (fa_ref, fb_ref), (a_ref, b_ref)
    parts, slices = (g_ref, u_ref, d_ref), (og_ref, ou_ref, od_ref)
    barrier = pltpu.get_barrier_semaphore()
    for step in range(1, size):
        greet(barrier, {"ctx": lax.rem(place + step, size)})
    for step in range(1, groups):
        greet(barrier, {"dp": lax.rem(group + step, groups)})
    pl.semaphore_wait(barrier, size + groups - 2)

    def chunk(which, in_group, rank):
        return wholes[which].at[pl.ds(pl.multiple_of((in_group * size + rank) * rows, rows), rows)]

    def source(which, rank, k):
        return owns[which] if k == 0 else chunk(which, group, rank)

    def going_up(which, k):
        return remote(
            source(which, place - k, k), chunk(which, group, place - k),
            up_send.at[which, k], up_recv.at[which, k], {"ctx": place + 1},
        )

    def going_down(which, k):
        return remote(
            source(which, place + k, k), chunk(which, group, place + k),
            down_send.at[which, k], down_recv.at[which, k], {"ctx": place - 1},
        )

    def across(which, rank, step, k):
        return remote(
            source(which, rank, k), chunk(which, group, rank),
            far_send.at[which, rank, step], far_recv.at[which, rank, step], {"dp": lax.rem(group + step, groups)},
        )

    def from_across(which, rank, step):
        there = chunk(which, lax.rem(group - step + groups, groups), rank)
        return remote(there, there, far_send.at[which, rank, step], far_recv.at[which, rank, step], {"dp": lax.rem(group + step, groups)})

    def columns(which, rank):
        return parts[which].at[:, pl.ds(pl.multiple_of(rank * width, 128), width)]

    def swap(which, step):
        return remote(
            columns(which, lax.rem(place + step, size)),
            slices[which].at[pl.ds(pl.multiple_of(place * rows, rows), rows)],
            swap_send.at[which, step], swap_recv.at[which, step], {"ctx": lax.rem(place + step, size)},
        )

    def swapped(which, step):
        there = slices[which].at[pl.ds(pl.multiple_of(lax.rem(place - step + size, size) * rows, rows), rows)]
        return remote(there, there, swap_send.at[which, step], swap_recv.at[which, step], {"ctx": lax.rem(place + step, size)})

    locals_ = [pltpu.make_async_copy(owns[w], chunk(w, group, place), local_sem.at[w]) for w in range(2)]
    locals_ += [
        pltpu.make_async_copy(
            columns(w, place), slices[w].at[pl.ds(pl.multiple_of(place * rows, rows), rows)], local_sem.at[2 + w]
        )
        for w in range(3)
    ]
    for w in range(2):
        pl.when(place < size - 1)(lambda w=w: going_up(w, 0).start())
        pl.when(place > 0)(lambda w=w: going_down(w, 0).start())
        for step in range(1, groups):
            across(w, place, step, 0).start()
    for copy in locals_:
        copy.start()
    for k in range(size - 1):
        for w in range(2):

            @pl.when(place - 1 - k >= 0)
            def _(k=k, w=w):
                there = chunk(w, group, place - 1 - k)
                remote(there, there, up_send.at[w, k], up_recv.at[w, k], {"ctx": place - 1}).wait_recv()
                if k + 1 < size - 1:
                    pl.when(place < size - 1)(lambda: going_up(w, k + 1).start())
                for step in range(1, groups):
                    across(w, place - 1 - k, step, 1).start()

            @pl.when(place + 1 + k <= size - 1)
            def _(k=k, w=w):
                there = chunk(w, group, place + 1 + k)
                remote(there, there, down_send.at[w, k], down_recv.at[w, k], {"ctx": place + 1}).wait_recv()
                if k + 1 < size - 1:
                    pl.when(place > 0)(lambda: going_down(w, k + 1).start())
                for step in range(1, groups):
                    across(w, place + 1 + k, step, 1).start()

    for w in range(3):
        for step in range(1, size):
            swap(w, step).start()
    for rank in range(size):
        for w in range(2):
            for step in range(1, groups):
                from_across(w, rank, step).wait_recv()
    for w in range(3):
        for step in range(1, size):
            swapped(w, step).wait_recv()
    for copy in locals_:
        copy.wait()
    for w in range(2):
        for k in range(size - 1):
            pl.when((place < size - 1) & (place - k >= 0))(lambda k=k, w=w: going_up(w, k).wait_send())
            pl.when((place > 0) & (place + k <= size - 1))(lambda k=k, w=w: going_down(w, k).wait_send())
        for rank in range(size):
            for step in range(1, groups):
                across(w, rank, step, 1).wait_send()
    for w in range(3):
        for step in range(1, size):
            swap(w, step).wait_send()


def front(a, b, parts, width, ident):
    size, groups = lax.axis_size("ctx"), lax.axis_size("dp")
    rows = a.shape[0]
    dma = pltpu.SemaphoreType.DMA
    slices = jax.ShapeDtypeStruct((size * rows, width), a.dtype)
    return pl.pallas_call(
        functools.partial(front_kernel, size, groups),
        in_specs=[IN_VMEM] * 5,
        out_specs=[ANY] * 5,
        out_shape=[jax.ShapeDtypeStruct((groups * size * rows, x.shape[1]), x.dtype) for x in (a, b)] + [slices] * 3,
        scratch_shapes=[dma((5,))] + [dma((2, size))] * 4 + [dma((2, size, groups))] * 2 + [dma((3, size))] * 2,
        compiler_params=pltpu.CompilerParams(collective_id=ident, has_side_effects=True),
        cost_estimate=pl.CostEstimate(flops=0, bytes_accessed=200000000, transcendentals=0),
        name="front",
    )(a, b, *parts)


def back_kernel(size, groups, x_ref, o_ref, mine, far, near, own_sem, far_send, far_recv, near_send, near_recv):
    place, group = lax.axis_index("ctx"), lax.axis_index("dp")
    rows = o_ref.shape[0]
    barrier = pltpu.get_barrier_semaphore()

    def rank_at(k):
        return lax.rem(place + 1 + k, size)

    def block(in_group, rank):
        return x_ref.at[pl.ds(pl.multiple_of((in_group * size + rank) * rows, rows), rows)]

    def load(k):
        return pltpu.make_async_copy(block(group, rank_at(k)), mine.at[k], own_sem.at[k])

    def across(k, step):
        to = lax.rem(group + step, groups)
        return remote(block(to, rank_at(k)), far.at[k, step], far_send.at[k, step], far_recv.at[k, step], {"dp": to})

    def along(k):
        return remote(mine.at[k], near.at[k], near_send.at[k], near_recv.at[k], {"ctx": rank_at(k)})

    for k in range(size):
        load(k).start()
    for step in range(1, size):
        greet(barrier, {"ctx": lax.rem(place + step, size)})
    for step in range(1, groups):
        greet(barrier, {"dp": lax.rem(group + step, groups)})
    pl.semaphore_wait(barrier, size + groups - 2)
    for k in range(size):
        for step in range(1, groups):
            across(k, step).start()
    for k in range(size):
        load(k).wait()
        for step in range(1, groups):
            across(k, step).wait_recv()
        parts = [mine.at[k]] + [far.at[k, step] for step in range(1, groups)]
        if k < size - 1:
            add_blocks(mine.at[k], parts)
            along(k).start()
    for k in range(size - 1):
        along(k).wait_recv()
        parts.append(near.at[k])
    add_blocks(o_ref, parts)
    for k in range(size):
        for step in range(1, groups):
            across(k, step).wait_send()
        if k < size - 1:
            along(k).wait_send()


def back(x, ident):
    size, groups = lax.axis_size("ctx"), lax.axis_size("dp")
    rows, columns = x.shape[0] // (size * groups), x.shape[1]
    dma = pltpu.SemaphoreType.DMA
    return pl.pallas_call(
        functools.partial(back_kernel, size, groups),
        in_specs=[ANY],
        out_specs=IN_VMEM,
        out_shape=jax.ShapeDtypeStruct((rows, columns), jnp.float32),
        scratch_shapes=[
            pltpu.VMEM((size, rows, columns), x.dtype),
            pltpu.VMEM((size, groups, rows, columns), x.dtype),
            pltpu.VMEM((size, rows, columns), x.dtype),
            dma((size,)),
            dma((size, groups)),
            dma((size, groups)),
            dma((size,)),
            dma((size,)),
        ],
        compiler_params=pltpu.CompilerParams(collective_id=ident, has_side_effects=True, vmem_limit_bytes=60000000),
        cost_estimate=pl.CostEstimate(flops=0, bytes_accessed=100 * x.size, transcendentals=0),
        name="back",
    )(x)


def mask_into(bias_ref, first, seg_ref, place_ref):
    keys, rows = bias_ref.shape
    key_index = lax.broadcasted_iota(jnp.int32, (keys, rows), 0)
    row_index = lax.broadcasted_iota(jnp.int32, (keys, rows), 1) + first
    place = jnp.broadcast_to(place_ref[...], (keys, rows))
    start = jnp.broadcast_to(seg_ref[...], (keys, rows))
    allowed = ((place >= start) & (place <= row_index)) | (key_index == row_index)
    bias_ref[...] = jnp.where(allowed, 0.0, VERY_LOW)


def nn(first_op, second_op):
    return jnp.dot(first_op, second_op, preferred_element_type=jnp.float32)


def attend_kernel(scale, first_ref, seg_ref, place_ref, q_ref, k_ref, vt_ref, o_ref, lse_ref, bias_ref):
    @pl.when(pl.program_id(1) == 0)
    def _():
        mask_into(bias_ref, first_ref[0] + pl.program_id(0) * q_ref.shape[0], seg_ref, place_ref)

    scores = matmul_nt(k_ref[...], q_ref[...]) * scale + bias_ref[...]
    top = jnp.max(scores, axis=0, keepdims=True)
    powers = jnp.exp(scores - top)
    total = jnp.sum(powers, axis=0, keepdims=True)
    mixture = nn(vt_ref[...], powers.astype(jnp.bfloat16)) / total
    o_ref[...] = mixture.T.astype(jnp.bfloat16)
    lse_ref[0] = top + jnp.log(total)


def attend_back_kernel(
    scale, first_ref, seg_ref, place_ref, q_ref, do_ref, lse_ref, k_ref, v_ref, kt_ref,
    dq_ref, dkv_ref, bias_ref, dk_ref, dv_ref,
):
    block, head = pl.program_id(0), pl.program_id(1)

    @pl.when(head == 0)
    def _():
        mask_into(bias_ref, first_ref[0] + block * q_ref.shape[0], seg_ref, place_ref)

    @pl.when((head == 0) & (block == 0))
    def _():
        dk_ref[...] = jnp.zeros_like(dk_ref)
        dv_ref[...] = jnp.zeros_like(dv_ref)

    query, grad = q_ref[...], do_ref[...]
    scores = matmul_nt(k_ref[...], query) * scale + bias_ref[...]
    probs = jnp.exp(scores - lse_ref[0])
    grad_probs = matmul_nt(v_ref[...], grad)
    delta = jnp.sum(probs * grad_probs, axis=0, keepdims=True)
    grad_scores = (probs * (grad_probs - delta)).astype(jnp.bfloat16)
    dv_ref[...] += nn(probs.astype(jnp.bfloat16), grad)
    dk_ref[...] += nn(grad_scores, query)
    dq_ref[...] = (nn(kt_ref[...], grad_scores) * scale).T

    @pl.when((head == pl.num_programs(1) - 1) & (block == pl.num_programs(0) - 1))
    def _():
        dkv_ref[:, :HEAD] = (dk_ref[...] * scale).astype(jnp.bfloat16)
        dkv_ref[:, HEAD:] = dv_ref[...].astype(jnp.bfloat16)


def attention_calls(rows, keys, heads):
    block = math.gcd(256, rows)
    scale = 1.0 / math.sqrt(HEAD)
    smem = pl.BlockSpec(memory_space=pltpu.SMEM)
    seg = pl.BlockSpec((1, block), lambda i, h: (0, i))
    place = pl.BlockSpec((keys, 1), lambda i, h: (0, 0))
    head = pl.BlockSpec((block, HEAD), lambda i, h: (i, h))
    lse = pl.BlockSpec((1, 1, block), lambda i, h: (h, 0, i))
    tall = pl.BlockSpec((keys, HEAD), lambda i, h: (0, 0))
    wide = pl.BlockSpec((HEAD, keys), lambda i, h: (0, 0))
    params = pltpu.CompilerParams(vmem_limit_bytes=60000000)
    grid = (rows // block, heads)
    size = heads * rows * keys
    forward = pl.pallas_call(
        functools.partial(attend_kernel, scale),
        grid=grid,
        in_specs=[smem, seg, place, head, tall, wide],
        out_specs=[head, lse],
        out_shape=[
            jax.ShapeDtypeStruct((rows, heads * HEAD), jnp.bfloat16),
            jax.ShapeDtypeStruct((heads, 1, rows), jnp.float32),
        ],
        scratch_shapes=[pltpu.VMEM((keys, block), jnp.float32)],
        compiler_params=params,
        cost_estimate=pl.CostEstimate(flops=4 * size * HEAD, bytes_accessed=4 * rows * heads * HEAD, transcendentals=size),
        name="attend",
    )
    backward = pl.pallas_call(
        functools.partial(attend_back_kernel, scale),
        grid=grid,
        in_specs=[smem, seg, place, head, head, lse, tall, tall, wide],
        out_specs=[head, pl.BlockSpec((keys, 2 * HEAD), lambda i, h: (0, 0))],
        out_shape=[
            jax.ShapeDtypeStruct((rows, heads * HEAD), jnp.float32),
            jax.ShapeDtypeStruct((keys, 2 * HEAD), jnp.bfloat16),
        ],
        scratch_shapes=[
            pltpu.VMEM((keys, block), jnp.float32),
            pltpu.VMEM((keys, HEAD), jnp.float32),
            pltpu.VMEM((keys, HEAD), jnp.float32),
        ],
        compiler_params=params,
        cost_estimate=pl.CostEstimate(flops=10 * size * HEAD, bytes_accessed=8 * rows * heads * HEAD, transcendentals=size),
        name="attend_back",
    )
    return forward, backward


def per_device(
    layer_input,
    teacher,
    cotangent,
    segment_ids,
    positions,
    valid_mask,
    gain_attn,
    query_weight,
    query_bias,
    key_weight,
    key_bias,
    value_weight,
    value_bias,
    out_weight,
    gain_mlp,
    gate_weight,
    up_weight,
    down_weight,
):
    tensor_rank = lax.axis_index("tensor")
    ctx_rank = lax.axis_index("ctx")
    tensor_size, ctx_size = lax.axis_size("tensor"), lax.axis_size("ctx")
    own_rows = layer_input.shape[0]
    shard_rows = own_rows * tensor_size
    seq_len = segment_ids.shape[0]
    q_width = query_weight.shape[1]
    kv_width = key_weight.shape[1]
    kv_local = kv_width // HEAD
    group = q_width // kv_width
    hidden_width = gate_weight.shape[1]
    slice_width = -(-hidden_width // (128 * ctx_size)) * 128
    first_row = ctx_rank * shard_rows
    own_first = first_row + tensor_rank * own_rows

    inputs = layer_input.astype(jnp.float32)
    gain_one = gain_attn.astype(jnp.float32)
    gain_two = gain_mlp.astype(jnp.float32)
    scale_attn = lax.rsqrt(jnp.mean(inputs * inputs, axis=1, keepdims=True) + EPS)
    normed_attn = inputs * scale_attn
    extra = ((0, 0), (0, ctx_size * slice_width - hidden_width))
    full_qkv, full_out, *slices = front(
        jnp.concatenate([query_weight, key_weight, value_weight], axis=1),
        out_weight.T,
        [jnp.pad(w, extra) for w in (gate_weight, up_weight, down_weight.T)],
        slice_width,
        1,
    )
    full_gate, full_up, full_down = [lax.all_gather(w, "dp", axis=0, tiled=True) for w in slices]
    normed_rows = gather((normed_attn * gain_one).astype(jnp.bfloat16), 1, True, 2)
    valid_count = jnp.sum(valid_mask.astype(jnp.float32))
    counts = [valid_count]
    dp_size = lax.axis_size("dp")
    for step in range(1, dp_size):
        counts.append(
            lax.ppermute(
                jnp.full((8, 128), valid_count), "dp", [(i, (i + step) % dp_size) for i in range(dp_size)]
            )[0, 0]
        )
    valid_count = sum(counts)

    bias = jnp.concatenate(
        [
            lax.dynamic_slice_in_dim(query_bias, tensor_rank * q_width, q_width),
            lax.dynamic_slice_in_dim(key_bias, tensor_rank * kv_width, kv_width),
            lax.dynamic_slice_in_dim(value_bias, tensor_rank * kv_width, kv_width),
        ]
    ).astype(jnp.float32)
    places = lax.dynamic_slice_in_dim(positions, first_row, shard_rows)
    cosine, sine_table = rope_tables(places)
    qkv_pre = matmul(normed_rows, full_qkv) + bias
    turned = q_width + kv_width
    rotated = (
        rotate(qkv_pre[:, :turned].reshape(shard_rows, turned // HEAD, HEAD), cosine, sine_table)
        .astype(jnp.bfloat16)
        .reshape(shard_rows, turned)
    )
    queries = rotated[:, :q_width]
    own_kv = jnp.concatenate([rotated[:, q_width:], qkv_pre[:, turned:].astype(jnp.bfloat16)], axis=1)
    all_kv = gather(own_kv, ctx_size, False, 3)

    key_index = jnp.arange(seq_len, dtype=jnp.int32)
    key_place = jnp.where(valid_mask > 0, key_index, -1)[:, None]
    seq_first = lax.axis_index("dp") * seq_len
    doc_start = (lax.dynamic_slice_in_dim(segment_ids, first_row, shard_rows) - seq_first)[None, :]
    first = jnp.reshape(first_row, (1,)).astype(jnp.int32)
    forward, backward = attention_calls(shard_rows, seq_len, group)
    kept = []
    for c in range(kv_local):
        key = all_kv[:, c * HEAD : (c + 1) * HEAD]
        value = all_kv[:, kv_width + c * HEAD : kv_width + (c + 1) * HEAD]
        query = queries[:, c * group * HEAD : (c + 1) * group * HEAD]
        kept.append((query, key, value) + tuple(forward(first, doc_start, key_place, query, key, value.T)))
    heads_out = jnp.concatenate([k[3] for k in kept], axis=1)
    attention = scatter(matmul_nt(heads_out, full_out), 1, True, 4)
    residual_mid = inputs + attention
    scale_mlp = lax.rsqrt(jnp.mean(residual_mid * residual_mid, axis=1, keepdims=True) + EPS)
    normed_mlp = residual_mid * scale_mlp
    mlp_rows = gather((normed_mlp * gain_two).astype(jnp.bfloat16), ctx_size, True, 5)
    gate_act = matmul(mlp_rows, full_gate)
    up_act = matmul(mlp_rows, full_up)
    sigmoid = jax.nn.sigmoid(gate_act)
    silu_gate = gate_act * sigmoid
    hidden = (silu_gate * up_act).astype(jnp.bfloat16)
    branch = scatter(matmul_nt(hidden, full_down).astype(jnp.bfloat16), ctx_size, True, 6)
    layer_result = residual_mid + branch
    valid_own = lax.dynamic_slice_in_dim(valid_mask, own_first, own_rows).astype(jnp.float32)
    difference = layer_result - teacher.astype(jnp.float32)
    squared_sum = jnp.sum(valid_own[:, None] * difference * difference)
    grad_result = cotangent.astype(jnp.float32) + 2.0 * valid_own[:, None] * difference / (
        valid_count * D
    )
    grad_branch = gather(grad_result.astype(jnp.bfloat16), ctx_size, True, 5)
    grad_hidden = matmul(grad_branch, full_down)
    grad_gate_act = (grad_hidden * up_act * sigmoid * (1.0 + gate_act * (1.0 - sigmoid))).astype(
        jnp.bfloat16
    )
    grad_up_act = (grad_hidden * silu_gate).astype(jnp.bfloat16)
    summed = []
    for left, right in ((grad_branch, hidden), (mlp_rows, grad_gate_act), (mlp_rows, grad_up_act)):
        grad = matmul_tn(left, right).astype(jnp.bfloat16)
        grad_gate_act, grad_up_act, grad = lax.optimization_barrier((grad_gate_act, grad_up_act, grad))
        summed.append(lax.psum_scatter(grad, "dp", scatter_dimension=0, tiled=True))
    grad_mlp_rows = (matmul_nt(grad_gate_act, full_gate) + matmul_nt(grad_up_act, full_up)).astype(jnp.bfloat16)
    grad_mlp_rows = scatter(grad_mlp_rows, ctx_size, True, 6)
    grad_gain_mlp = jnp.sum(grad_mlp_rows * normed_mlp, axis=0)
    grad_mid = grad_result + norm_back(grad_mlp_rows, normed_mlp, scale_mlp, gain_two)
    grad_attn_rows = gather(grad_mid.astype(jnp.bfloat16), 1, True, 2)
    grad_heads = matmul(grad_attn_rows, full_out).astype(jnp.bfloat16)
    grad_out = matmul_tn(grad_attn_rows, heads_out).astype(jnp.bfloat16)

    grad_out = lax.psum_scatter(grad_out, "dp", scatter_dimension=0, tiled=True)
    query_grads, key_grads, value_grads = [], [], []
    for c in range(kv_local):
        query, key, value, _, log_total = kept[c]
        span = slice(c * group * HEAD, (c + 1) * group * HEAD)
        grad_query, grad_kv = backward(
            first, doc_start, key_place, query, grad_heads[:, span], log_total, key, value, key.T
        )
        query_grads.append(grad_query)
        key_grads.append(grad_kv[:, :HEAD])
        value_grads.append(grad_kv[:, HEAD:])
    grad_kv = grad_kv if kv_local == 1 else jnp.concatenate(key_grads + value_grads, axis=1)
    grad_kv, *summed = lax.optimization_barrier((grad_kv, *summed))
    shard_down, shard_gate, shard_up = to_rows(summed, hidden_width)
    shard_down = shard_down.T
    grad_kv = scatter(grad_kv, ctx_size, False, 7)
    grad_turned = jnp.concatenate(query_grads + [grad_kv[:, :kv_width]], axis=1)
    grad_pre = jnp.concatenate(
        [
            rotate(grad_turned.reshape(shard_rows, turned // HEAD, HEAD), cosine, -sine_table)
            .reshape(shard_rows, turned)
            .astype(jnp.bfloat16),
            grad_kv[:, kv_width:].astype(jnp.bfloat16),
        ],
        axis=1,
    )
    grad_pre, grad_out = lax.optimization_barrier((grad_pre, grad_out))
    shard_out = lax.psum_scatter(grad_out, "ctx", scatter_dimension=0, tiled=True).astype(jnp.float32).T
    shard_qkv = back(matmul_tn(normed_rows, grad_pre).astype(jnp.bfloat16), 8)
    grad_normed = scatter(matmul_nt(grad_pre, full_qkv), 1, True, 4)
    grad_gain_attn = jnp.sum(grad_normed * normed_attn, axis=0)
    grad_input = grad_mid + norm_back(grad_normed, normed_attn, scale_attn, gain_one)
    bias_sum = jnp.sum(grad_pre.astype(jnp.float32), axis=0)

    def spread(part, size):
        return lax.dynamic_update_slice_in_dim(
            jnp.zeros((size,), jnp.float32), part, tensor_rank * part.shape[0], 0
        )

    loss_part = jnp.zeros((128,), jnp.float32).at[0].set(squared_sum)
    parts = [
        grad_gain_attn,
        grad_gain_mlp,
        spread(bias_sum[:q_width], query_bias.shape[0]),
        spread(bias_sum[q_width:turned], key_bias.shape[0]),
        spread(bias_sum[turned:], value_bias.shape[0]),
        loss_part,
    ]
    sums = sum_everywhere(jnp.concatenate(parts).reshape(-1, 128)).reshape(-1)
    pieces, offset = [], 0
    for part in parts:
        pieces.append(sums[offset : offset + part.shape[0]])
        offset += part.shape[0]
    return (
        layer_result.astype(jnp.bfloat16),
        pieces[5][0] / (valid_count * D),
        grad_input,
        pieces[0],
        shard_qkv[:, :q_width],
        pieces[2],
        shard_qkv[:, q_width:turned],
        pieces[3],
        shard_qkv[:, turned:],
        pieces[4],
        shard_out,
        pieces[1],
        shard_gate,
        shard_up,
        shard_down,
    )


def solution(mesh):
    in_specs = (
        P(("dp", "ctx", "tensor"), None),
        P(("dp", "ctx", "tensor"), None),
        P(("dp", "ctx", "tensor"), None),
        P("dp"),
        P("dp"),
        P("dp"),
        P(),
        P(("dp", "ctx"), "tensor"),
        P(),
        P(("dp", "ctx"), "tensor"),
        P(),
        P(("dp", "ctx"), "tensor"),
        P(),
        P("tensor", ("dp", "ctx")),
        P(),
        P(("dp", "ctx"), "tensor"),
        P(("dp", "ctx"), "tensor"),
        P("tensor", ("dp", "ctx")),
    )
    out_specs = (
        P(("dp", "ctx", "tensor"), None),
        P(),
        P(("dp", "ctx", "tensor"), None),
        P(),
        P(("dp", "ctx"), "tensor"),
        P(),
        P(("dp", "ctx"), "tensor"),
        P(),
        P(("dp", "ctx"), "tensor"),
        P(),
        P("tensor", ("dp", "ctx")),
        P(),
        P(("dp", "ctx"), "tensor"),
        P(("dp", "ctx"), "tensor"),
        P("tensor", ("dp", "ctx")),
    )

    return jax.shard_map(per_device, mesh=mesh, in_specs=in_specs, out_specs=out_specs, check_vma=False)
```

```python
import functools
import math

import jax
import jax.numpy as jnp
from jax import lax
from jax.experimental import pallas as pl
from jax.experimental.pallas import tpu as pltpu
from jax.sharding import PartitionSpec as P


D = 1536
HEAD = 128


EPS = 1e-06
THETA = 10000.0
VERY_LOW = -1e30


def rope_tables(places):
    half_dim = HEAD // 2
    frequency = THETA ** (-(jnp.arange(half_dim, dtype=jnp.float32) * 2.0 / HEAD))
    angles = places.astype(jnp.float32)[:, None] * frequency[None, :]
    return (jnp.cos(angles), jnp.sin(angles))


def rotate(stacked, cosine, sine_table):
    half_dim = HEAD // 2
    first_half = stacked[..., :half_dim]
    second_half = stacked[..., half_dim:]
    cosine = cosine[:, None, :]
    sine_table = sine_table[:, None, :]
    return jnp.concatenate(
        [
            first_half * cosine - second_half * sine_table,
            second_half * cosine + first_half * sine_table,
        ],
        axis=-1,
    )


def matmul(first_op, second_op):
    return jnp.dot(first_op, second_op, preferred_element_type=jnp.float32)


def matmul_tn(first_op, second_op):
    return lax.dot_general(
        first_op, second_op, (((0,), (0,)), ((), ())), preferred_element_type=jnp.float32
    )


def matmul_nt(first_op, second_op):
    return lax.dot_general(
        first_op, second_op, (((1,), (1,)), ((), ())), preferred_element_type=jnp.float32
    )


def norm_back(grad_normed, normed, inverse, gain):
    scaled = grad_normed * gain
    return inverse * (scaled - normed * jnp.mean(scaled * normed, axis=1, keepdims=True))


def exchange(blocks, axis):
    size = lax.axis_size(axis)
    rank = lax.axis_index(axis)
    received = [(rank, lax.dynamic_index_in_dim(blocks, rank, 0, keepdims=False))]
    for step in range(1, size):
        going = lax.dynamic_index_in_dim(blocks, (rank + step) % size, 0, keepdims=False)
        came = lax.ppermute(going, axis, [(i, (i + step) % size) for i in range(size)])
        received.append(((rank - step + size) % size, came))
    return received


def to_rows(summed, columns):
    size = lax.axis_size("ctx")
    rows, width = summed[0].shape[0] // size, summed[0].shape[1]
    blocks = jnp.stack([s.reshape(size, rows, width) for s in summed], axis=1)
    shards = jnp.zeros((len(summed), rows, size * width), jnp.bfloat16)
    for rank, block in exchange(blocks, "ctx"):
        shards = lax.dynamic_update_slice_in_dim(shards, block, rank * width, 2)
    return [s[:, :columns].astype(jnp.float32) for s in shards]


def nn(first_op, second_op):
    return jnp.dot(first_op, second_op, preferred_element_type=jnp.float32)


MESH = pl.DeviceIdType.MESH
ANY = pl.BlockSpec(memory_space=pl.ANY)
IN_VMEM = pl.BlockSpec(memory_space=pltpu.VMEM)


def remote(source, target, send_sem, recv_sem, device):
    return pltpu.make_async_remote_copy(
        src_ref=source,
        dst_ref=target,
        send_sem=send_sem,
        recv_sem=recv_sem,
        device_id=device,
        device_id_type=MESH,
    )


def greet(barrier, device):
    pl.semaphore_signal(barrier, inc=1, device_id=device, device_id_type=MESH)


def greet_chain(size, paired):
    place = lax.axis_index("ctx")
    barrier = pltpu.get_barrier_semaphore()
    if size > 1:
        pl.when(place < size - 1)(lambda: greet(barrier, {"ctx": place + 1}))
        pl.when(place > 0)(lambda: greet(barrier, {"ctx": place - 1}))
    if paired:
        greet(barrier, {"tensor": 1 - lax.axis_index("tensor")})
    if size == 1:
        pl.semaphore_wait(barrier, 1)
        return
    ends = (place == 0) | (place == size - 1)
    pl.when(ends)(lambda: pl.semaphore_wait(barrier, 1 + paired))
    pl.when(jnp.logical_not(ends))(lambda: pl.semaphore_wait(barrier, 2 + paired))


def gather_kernel(size, paired, pieces, x_ref, o_ref, local_sem, up_send, up_recv, down_send, down_recv, mate_send, mate_recv):
    place = lax.axis_index("ctx") if size > 1 else 0
    core = lax.axis_index("tensor")
    rows = x_ref.shape[0]
    part = rows // pieces
    greet_chain(size, paired)

    def block(rank, which, p):
        index = rank * 2 + which if paired else rank
        return o_ref.at[pl.ds(pl.multiple_of(index * rows + p * part, part), part)]

    def source(rank, k, p):
        return x_ref.at[pl.ds(p * part, part)] if k == 0 else block(rank, core, p)

    def going_up(k, p):
        return remote(
            source(place - k, k, p), block(place - k, core, p), up_send.at[k, p], up_recv.at[k, p], {"ctx": place + 1}
        )

    def going_down(k, p):
        return remote(
            source(place + k, k, p), block(place + k, core, p), down_send.at[k, p], down_recv.at[k, p], {"ctx": place - 1}
        )

    def to_mate(rank, k, p):
        return remote(
            source(rank, k, p), block(rank, core, p), mate_send.at[k, p], mate_recv.at[rank, p], {"tensor": 1 - core}
        )

    def from_mate(rank, p):
        there = block(rank, 1 - core, p)
        return remote(there, there, mate_send.at[0, p], mate_recv.at[rank, p], {"tensor": 1 - core})

    own = pltpu.make_async_copy(x_ref, o_ref.at[pl.ds(pl.multiple_of((place * 2 + core if paired else place) * rows, rows), rows)], local_sem)
    for p in range(pieces):
        if size > 1:
            pl.when(place < size - 1)(lambda p=p: going_up(0, p).start())
            pl.when(place > 0)(lambda p=p: going_down(0, p).start())
    for p in range(pieces):
        if paired:
            to_mate(place, 0, p).start()
    own.start()
    for k in range(size - 1):
        for p in range(pieces):

            @pl.when(place - 1 - k >= 0)
            def _(k=k, p=p):
                there = block(place - 1 - k, core, p)
                remote(there, there, up_send.at[k, p], up_recv.at[k, p], {"ctx": place - 1}).wait_recv()
                if k + 1 < size - 1:
                    pl.when(place < size - 1)(lambda: going_up(k + 1, p).start())
                if paired:
                    to_mate(place - 1 - k, 1 + k, p).start()

            @pl.when(place + 1 + k <= size - 1)
            def _(k=k, p=p):
                there = block(place + 1 + k, core, p)
                remote(there, there, down_send.at[k, p], down_recv.at[k, p], {"ctx": place + 1}).wait_recv()
                if k + 1 < size - 1:
                    pl.when(place > 0)(lambda: going_down(k + 1, p).start())
                if paired:
                    to_mate(place + 1 + k, size + k, p).start()

    own.wait()
    for p in range(pieces):
        if paired:
            for rank in range(size):
                from_mate(rank, p).wait_recv()
            to_mate(place, 0, p).wait_send()
        for k in range(size - 1):
            pl.when((place < size - 1) & (place - k >= 0))(lambda k=k, p=p: going_up(k, p).wait_send())
            pl.when((place > 0) & (place + k <= size - 1))(lambda k=k, p=p: going_down(k, p).wait_send())
            if paired:
                pl.when(place - 1 - k >= 0)(lambda k=k, p=p: to_mate(place - 1 - k, 1 + k, p).wait_send())
                pl.when(place + 1 + k <= size - 1)(lambda k=k, p=p: to_mate(place + 1 + k, size + k, p).wait_send())


def pieces_of(rows, columns):
    return math.gcd(4, rows // 64) if rows * columns >= 1 << 18 else 1


def gather(x, size, paired, ident):
    copies = size * 2 if paired else size
    wide = max(size, 2)
    pieces = pieces_of(*x.shape)
    dma = pltpu.SemaphoreType.DMA
    return pl.pallas_call(
        functools.partial(gather_kernel, size, paired, pieces),
        in_specs=[IN_VMEM],
        out_specs=ANY,
        out_shape=jax.ShapeDtypeStruct((copies * x.shape[0], x.shape[1]), x.dtype),
        scratch_shapes=[dma] + [dma((wide, pieces))] * 4 + [dma((2 * wide, pieces)), dma((wide, pieces))],
        compiler_params=pltpu.CompilerParams(collective_id=ident, has_side_effects=True),
        cost_estimate=pl.CostEstimate(flops=0, bytes_accessed=30 * copies * x.size, transcendentals=0),
        name="gather",
    )(x)


def add_blocks(target, parts):
    rows = target.shape[0]
    step = math.gcd(rows, 32)

    def some(i, carry):
        span = pl.ds(pl.multiple_of(i * step, step), step)
        total = parts[0][span].astype(jnp.float32)
        for part in parts[1:]:
            total += part[span].astype(jnp.float32)
        target[span] = total.astype(target.dtype)
        return carry

    lax.fori_loop(0, rows // step, some, 0)


def scatter_kernel(
    size, paired, pieces, x_ref, o_ref, mine, mate, above, below, own_sem, mate_send, mate_recv, up_send, up_recv, down_send, down_recv
):
    place = lax.axis_index("ctx") if size > 1 else 0
    core = lax.axis_index("tensor")
    rows = o_ref.shape[0]
    part = rows // pieces
    order = sorted(range(size), key=lambda d: min(d, size - 1 - d))
    every = [(d, p) for d in order for p in range(pieces)]

    def block(rank, which, p):
        index = rank * 2 + which if paired else rank
        return x_ref.at[pl.ds(pl.multiple_of(index * rows + p * part, part), part)]

    def at(ref, d, p):
        return ref.at[d, pl.ds(p * part, part)]

    def load(d, p):
        return pltpu.make_async_copy(block(d, core, p), at(mine, d, p), own_sem.at[d, p])

    def to_mate(d, p):
        return remote(
            block(d, 1 - core, p), at(mate, d, p), mate_send.at[d, p], mate_recv.at[d, p], {"tensor": 1 - core}
        )

    def going_up(d, p):
        return remote(at(mine, d, p), at(below, d, p), up_send.at[d, p], up_recv.at[d, p], {"ctx": place + 1})

    def going_down(d, p):
        return remote(at(mine, d, p), at(above, d, p), down_send.at[d, p], down_recv.at[d, p], {"ctx": place - 1})

    for d, p in every:
        load(d, p).start()
    greet_chain(size, paired)
    if paired:
        for d, p in every:
            to_mate(d, p).start()

    def here(d, p):
        load(d, p).wait()
        if paired:
            to_mate(d, p).wait_recv()
            return [at(mine, d, p), at(mate, d, p)]
        return [at(mine, d, p)]

    for k in range(size - 1):
        for p in range(pieces):

            @pl.when(place < size - 1 - k)
            def _(d=size - 1 - k, p=p):
                parts = here(d, p)

                @pl.when(place > 0)
                def _():
                    going_up(d, p).wait_recv()
                    add_blocks(at(mine, d, p), parts + [at(below, d, p)])

                if paired:
                    pl.when(place == 0)(lambda: add_blocks(at(mine, d, p), parts))
                going_up(d, p).start()

            @pl.when(place > k)
            def _(d=k, p=p):
                parts = here(d, p)

                @pl.when(place < size - 1)
                def _():
                    going_down(d, p).wait_recv()
                    add_blocks(at(mine, d, p), parts + [at(above, d, p)])

                if paired:
                    pl.when(place == size - 1)(lambda: add_blocks(at(mine, d, p), parts))
                going_down(d, p).start()

    for d in range(size):

        @pl.when(place == d)
        def _(d=d):
            for p in range(pieces):
                parts = here(d, p)
                if d > 0:
                    going_up(d, p).wait_recv()
                    parts = parts + [at(below, d, p)]
                if d < size - 1:
                    going_down(d, p).wait_recv()
                    parts = parts + [at(above, d, p)]
                add_blocks(o_ref.at[pl.ds(p * part, part)], parts)

    for d, p in every:
        if d > 0:
            pl.when(place < d)(lambda d=d, p=p: going_up(d, p).wait_send())
        if d < size - 1:
            pl.when(place > d)(lambda d=d, p=p: going_down(d, p).wait_send())
        if paired:
            to_mate(d, p).wait_send()


def scatter(x, size, paired, ident):
    copies = size * 2 if paired else size
    rows = x.shape[0] // copies
    pieces = pieces_of(rows, x.shape[1])
    dma = pltpu.SemaphoreType.DMA
    slots = pltpu.VMEM((size, rows, x.shape[1]), x.dtype)
    one = pltpu.VMEM((1, 32, 128), x.dtype)
    chain = slots if size > 1 else one
    return pl.pallas_call(
        functools.partial(scatter_kernel, size, paired, pieces),
        in_specs=[ANY],
        out_specs=IN_VMEM,
        out_shape=jax.ShapeDtypeStruct((rows, x.shape[1]), jnp.float32),
        scratch_shapes=[slots, slots if paired else one, chain, chain] + [dma((size, pieces))] * 7,
        compiler_params=pltpu.CompilerParams(collective_id=ident, has_side_effects=True, vmem_limit_bytes=60000000),
        cost_estimate=pl.CostEstimate(flops=0, bytes_accessed=30 * x.size, transcendentals=0),
        name="scatter",
    )(x)


def front_kernel(
    size, groups, a_ref, b_ref, g_ref, u_ref, d_ref, fa_ref, fb_ref, og_ref, ou_ref, od_ref,
    local_sem, up_send, up_recv, down_send, down_recv, far_send, far_recv, swap_send, swap_recv,
):
    place, group = lax.axis_index("ctx"), lax.axis_index("dp")
    rows, width = a_ref.shape[0], og_ref.shape[1]
    wholes, owns = (fa_ref, fb_ref), (a_ref, b_ref)
    parts, slices = (g_ref, u_ref, d_ref), (og_ref, ou_ref, od_ref)
    barrier = pltpu.get_barrier_semaphore()
    for step in range(1, size):
        greet(barrier, {"ctx": lax.rem(place + step, size)})
    for step in range(1, groups):
        greet(barrier, {"dp": lax.rem(group + step, groups)})
    pl.semaphore_wait(barrier, size + groups - 2)

    def chunk(which, in_group, rank):
        return wholes[which].at[pl.ds(pl.multiple_of((in_group * size + rank) * rows, rows), rows)]

    def source(which, rank, k):
        return owns[which] if k == 0 else chunk(which, group, rank)

    def going_up(which, k):
        return remote(
            source(which, place - k, k), chunk(which, group, place - k),
            up_send.at[which, k], up_recv.at[which, k], {"ctx": place + 1},
        )

    def going_down(which, k):
        return remote(
            source(which, place + k, k), chunk(which, group, place + k),
            down_send.at[which, k], down_recv.at[which, k], {"ctx": place - 1},
        )

    def across(which, rank, step, k):
        return remote(
            source(which, rank, k), chunk(which, group, rank),
            far_send.at[which, rank, step], far_recv.at[which, rank, step], {"dp": lax.rem(group + step, groups)},
        )

    def from_across(which, rank, step):
        there = chunk(which, lax.rem(group - step + groups, groups), rank)
        return remote(there, there, far_send.at[which, rank, step], far_recv.at[which, rank, step], {"dp": lax.rem(group + step, groups)})

    def columns(which, rank):
        return parts[which].at[:, pl.ds(pl.multiple_of(rank * width, 128), width)]

    def swap(which, step):
        return remote(
            columns(which, lax.rem(place + step, size)),
            slices[which].at[pl.ds(pl.multiple_of(place * rows, rows), rows)],
            swap_send.at[which, step], swap_recv.at[which, step], {"ctx": lax.rem(place + step, size)},
        )

    def swapped(which, step):
        there = slices[which].at[pl.ds(pl.multiple_of(lax.rem(place - step + size, size) * rows, rows), rows)]
        return remote(there, there, swap_send.at[which, step], swap_recv.at[which, step], {"ctx": lax.rem(place + step, size)})

    locals_ = [pltpu.make_async_copy(owns[w], chunk(w, group, place), local_sem.at[w]) for w in range(2)]
    locals_ += [
        pltpu.make_async_copy(
            columns(w, place), slices[w].at[pl.ds(pl.multiple_of(place * rows, rows), rows)], local_sem.at[2 + w]
        )
        for w in range(3)
    ]
    for w in range(2):
        pl.when(place < size - 1)(lambda w=w: going_up(w, 0).start())
        pl.when(place > 0)(lambda w=w: going_down(w, 0).start())
        for step in range(1, groups):
            across(w, place, step, 0).start()
    for copy in locals_:
        copy.start()
    for k in range(size - 1):
        for w in range(2):

            @pl.when(place - 1 - k >= 0)
            def _(k=k, w=w):
                there = chunk(w, group, place - 1 - k)
                remote(there, there, up_send.at[w, k], up_recv.at[w, k], {"ctx": place - 1}).wait_recv()
                if k + 1 < size - 1:
                    pl.when(place < size - 1)(lambda: going_up(w, k + 1).start())
                for step in range(1, groups):
                    across(w, place - 1 - k, step, 1).start()

            @pl.when(place + 1 + k <= size - 1)
            def _(k=k, w=w):
                there = chunk(w, group, place + 1 + k)
                remote(there, there, down_send.at[w, k], down_recv.at[w, k], {"ctx": place + 1}).wait_recv()
                if k + 1 < size - 1:
                    pl.when(place > 0)(lambda: going_down(w, k + 1).start())
                for step in range(1, groups):
                    across(w, place + 1 + k, step, 1).start()

    for w in range(3):
        for step in range(1, size):
            swap(w, step).start()
    for rank in range(size):
        for w in range(2):
            for step in range(1, groups):
                from_across(w, rank, step).wait_recv()
    for w in range(3):
        for step in range(1, size):
            swapped(w, step).wait_recv()
    for copy in locals_:
        copy.wait()
    for w in range(2):
        for k in range(size - 1):
            pl.when((place < size - 1) & (place - k >= 0))(lambda k=k, w=w: going_up(w, k).wait_send())
            pl.when((place > 0) & (place + k <= size - 1))(lambda k=k, w=w: going_down(w, k).wait_send())
        for rank in range(size):
            for step in range(1, groups):
                across(w, rank, step, 1).wait_send()
    for w in range(3):
        for step in range(1, size):
            swap(w, step).wait_send()


def front(a, b, parts, width, ident):
    size, groups = lax.axis_size("ctx"), lax.axis_size("dp")
    rows = a.shape[0]
    dma = pltpu.SemaphoreType.DMA
    slices = jax.ShapeDtypeStruct((size * rows, width), a.dtype)
    return pl.pallas_call(
        functools.partial(front_kernel, size, groups),
        in_specs=[IN_VMEM] * 5,
        out_specs=[ANY] * 5,
        out_shape=[jax.ShapeDtypeStruct((groups * size * rows, x.shape[1]), x.dtype) for x in (a, b)] + [slices] * 3,
        scratch_shapes=[dma((5,))] + [dma((2, size))] * 4 + [dma((2, size, groups))] * 2 + [dma((3, size))] * 2,
        compiler_params=pltpu.CompilerParams(collective_id=ident, has_side_effects=True),
        cost_estimate=pl.CostEstimate(flops=0, bytes_accessed=200000000, transcendentals=0),
        name="front",
    )(a, b, *parts)


def back_kernel(
    size, groups, x_ref, s_ref, o_ref, t_ref, mine, far, near, pair, crowd, row,
    own_sem, far_send, far_recv, near_send, near_recv, pair_sems, crowd_send, crowd_recv, row_send, row_recv,
):
    place, group = lax.axis_index("ctx"), lax.axis_index("dp")
    core = lax.axis_index("tensor")
    rows = o_ref.shape[0]
    barrier = pltpu.get_barrier_semaphore()

    def rank_at(k):
        return lax.rem(place + 1 + k, size)

    def block(in_group, rank):
        return x_ref.at[pl.ds(pl.multiple_of((in_group * size + rank) * rows, rows), rows)]

    def load(k):
        return pltpu.make_async_copy(block(group, rank_at(k)), mine.at[k], own_sem.at[k])

    def across(k, step):
        to = lax.rem(group + step, groups)
        return remote(block(to, rank_at(k)), far.at[k, step], far_send.at[k, step], far_recv.at[k, step], {"dp": to})

    def along(k):
        return remote(mine.at[k], near.at[k], near_send.at[k], near_recv.at[k], {"ctx": rank_at(k)})

    to_mate = remote(s_ref, pair, pair_sems.at[0], pair_sems.at[1], {"tensor": 1 - core})

    def to_crowd(step):
        return remote(
            crowd.at[group], crowd.at[group], crowd_send.at[step], crowd_recv.at[step],
            {"dp": lax.rem(group + step, groups)},
        )

    def to_row(step):
        return remote(
            row.at[place], row.at[place], row_send.at[step], row_recv.at[step], {"ctx": lax.rem(place + step, size)}
        )

    for k in range(size):
        load(k).start()
    for step in range(1, size):
        greet(barrier, {"ctx": lax.rem(place + step, size)})
    for step in range(1, groups):
        greet(barrier, {"dp": lax.rem(group + step, groups)})
    greet(barrier, {"tensor": 1 - core})
    pl.semaphore_wait(barrier, size + groups - 1)
    to_mate.start()
    to_mate.wait_recv()
    crowd[group] = s_ref[...] + pair[...]
    for step in range(1, groups):
        to_crowd(step).start()
    for k in range(size):
        for step in range(1, groups):
            across(k, step).start()
    for step in range(1, groups):
        to_crowd(step).wait_recv()
    total = crowd[0]
    for g in range(1, groups):
        total += crowd[g]
    row[place] = total
    for step in range(1, size):
        to_row(step).start()
    for k in range(size):
        load(k).wait()
        for step in range(1, groups):
            across(k, step).wait_recv()
        parts = [mine.at[k]] + [far.at[k, step] for step in range(1, groups)]
        if k < size - 1:
            add_blocks(mine.at[k], parts)
            along(k).start()
    for k in range(size - 1):
        along(k).wait_recv()
        parts.append(near.at[k])
    add_blocks(o_ref, parts)
    for step in range(1, size):
        to_row(step).wait_recv()
    total = row[0]
    for c in range(1, size):
        total += row[c]
    t_ref[...] = total
    to_mate.wait_send()
    for step in range(1, groups):
        to_crowd(step).wait_send()
    for step in range(1, size):
        to_row(step).wait_send()
    for k in range(size):
        for step in range(1, groups):
            across(k, step).wait_send()
        if k < size - 1:
            along(k).wait_send()


def back(x, small, ident):
    size, groups = lax.axis_size("ctx"), lax.axis_size("dp")
    rows, columns = x.shape[0] // (size * groups), x.shape[1]
    dma = pltpu.SemaphoreType.DMA
    return pl.pallas_call(
        functools.partial(back_kernel, size, groups),
        in_specs=[ANY, IN_VMEM],
        out_specs=[IN_VMEM, IN_VMEM],
        out_shape=[
            jax.ShapeDtypeStruct((rows, columns), jnp.float32),
            jax.ShapeDtypeStruct(small.shape, jnp.float32),
        ],
        scratch_shapes=[
            pltpu.VMEM((size, rows, columns), x.dtype),
            pltpu.VMEM((size, groups, rows, columns), x.dtype),
            pltpu.VMEM((size, rows, columns), x.dtype),
            pltpu.VMEM(small.shape, jnp.float32),
            pltpu.VMEM((groups,) + small.shape, jnp.float32),
            pltpu.VMEM((size,) + small.shape, jnp.float32),
            dma((size,)),
            dma((size, groups)),
            dma((size, groups)),
            dma((size,)),
            dma((size,)),
            dma((2,)),
            dma((groups,)),
            dma((groups,)),
            dma((size,)),
            dma((size,)),
        ],
        compiler_params=pltpu.CompilerParams(collective_id=ident, has_side_effects=True, vmem_limit_bytes=60000000),
        cost_estimate=pl.CostEstimate(flops=0, bytes_accessed=100 * x.size, transcendentals=0),
        name="back",
    )(x, small)


def column_step(width):
    return max(t for t in (384, 256, 128) if width % t == 0)


def expand_block(x_ref, weights, extra, stage):
    step = column_step(weights[0].shape[1])

    def some(j, carry):
        span = pl.ds(pl.multiple_of(j * step, step), step)
        gate = nn(x_ref[...], weights[0][:, span])
        up = nn(x_ref[...], weights[1][:, span])
        stage[0, :, span] = gate.astype(jnp.bfloat16)
        stage[1, :, span] = up.astype(jnp.bfloat16)
        stage[2, :, span] = (gate * jax.nn.sigmoid(gate) * up).astype(jnp.bfloat16)
        return carry

    lax.fori_loop(0, weights[0].shape[1] // step, some, 0)


def shrink_block(x_ref, weights, extra, stage):
    step = column_step(weights[0].shape[1])

    def some(j, carry):
        span = pl.ds(pl.multiple_of(j * step, step), step)
        grad = nn(x_ref[...], weights[0][:, span])
        gate = extra[0, :, span].astype(jnp.float32)
        up = extra[1, :, span].astype(jnp.float32)
        sigmoid = jax.nn.sigmoid(gate)
        stage[0, :, span] = (grad * up * sigmoid * (1.0 + gate * (1.0 - sigmoid))).astype(jnp.bfloat16)
        stage[1, :, span] = (grad * gate * sigmoid).astype(jnp.bfloat16)
        return carry

    lax.fori_loop(0, weights[0].shape[1] // step, some, 0)


def gather_apply_kernel(size, pieces, work, n_weights, n_extra, n_made, *refs):
    x_ref, refs = refs[0], refs[1:]
    weights_from, refs = refs[:n_weights], refs[n_weights:]
    extra_from, refs = refs[:n_extra], refs[n_extra:]
    o_ref, refs = refs[0], refs[1:]
    made_to, refs = refs[:n_made], refs[n_made:]
    weights, refs = refs[:n_weights], refs[n_weights:]
    extra, stage, refs = refs[0], refs[1], refs[2:]
    local_sem, weight_sem, extra_sem, stage_sem = refs[:4]
    up_send, up_recv, down_send, down_recv, mate_send, mate_recv = refs[4:]
    place = lax.axis_index("ctx")
    core = lax.axis_index("tensor")
    rows = x_ref.shape[0]
    part = rows // pieces
    last = size - 1

    loads = [pltpu.make_async_copy(weights_from[w], weights[w], weight_sem.at[w]) for w in range(n_weights)]
    for load in loads:
        load.start()

    def first_of(rank, which):
        return pl.multiple_of((rank * 2 + which) * rows, rows)

    def block(rank, which, p):
        return o_ref.at[pl.ds(pl.multiple_of((rank * 2 + which) * rows + p * part, part), part)]

    def going_up(k, p):
        there = block(place - k, core, p)
        return remote(there, there, up_send.at[k, p], up_recv.at[k, p], {"ctx": place + 1})

    def going_down(k, p):
        there = block(place + k, core, p)
        return remote(there, there, down_send.at[k, p], down_recv.at[k, p], {"ctx": place - 1})

    def coming_up(k, p):
        there = block(place - 1 - k, core, p)
        return remote(there, there, up_send.at[k, p], up_recv.at[k, p], {"ctx": place - 1})

    def coming_down(k, p):
        there = block(place + 1 + k, core, p)
        return remote(there, there, down_send.at[k, p], down_recv.at[k, p], {"ctx": place + 1})

    def to_mate(rank, p):
        there = block(rank, core, p)
        return remote(there, there, mate_send.at[rank, p], mate_recv.at[rank, p], {"tensor": 1 - core})

    def from_mate(rank, p):
        there = block(rank, 1 - core, p)
        return remote(there, there, mate_send.at[rank, p], mate_recv.at[rank, p], {"tensor": 1 - core})

    own = pltpu.make_async_copy(x_ref, o_ref.at[pl.ds(first_of(place, core), rows)], local_sem)
    own.start()
    greet_chain(size, True)
    own.wait()
    for p in range(pieces):
        pl.when(place < last)(lambda p=p: going_up(0, p).start())
        pl.when(place > 0)(lambda p=p: going_down(0, p).start())
    for p in range(pieces):
        to_mate(place, p).start()

    def forward(d):
        for p in range(pieces):

            @pl.when(place - d >= 0)
            def _(p=p):
                coming_up(d - 1, p).wait_recv()
                pl.when(place < last)(lambda: going_up(d, p).start())
                to_mate(place - d, p).start()

            @pl.when(place + d <= last)
            def _(p=p):
                coming_down(d - 1, p).wait_recv()
                pl.when(place > 0)(lambda: going_down(d, p).start())
                to_mate(place + d, p).start()

    for load in loads:
        load.wait()
    short = jnp.minimum(place, last - place)

    def distance(s):
        return jnp.where(s <= 2 * short, (s + 1) // 2, s - short)

    def extra_load(rank, which, slot, e):
        return pltpu.make_async_copy(
            extra_from[e].at[pl.ds(first_of(rank, which), rows)], extra.at[slot, e], extra_sem.at[slot, e]
        )

    def store(rank, which, slot, m):
        return pltpu.make_async_copy(
            stage.at[slot, m], made_to[m].at[pl.ds(first_of(rank, which), rows)], stage_sem.at[slot, m]
        )

    def visit(s, carry):
        d = distance(s)
        below = jnp.where(s <= 2 * short, s % 2 == 1, place > last - place)
        rank = jnp.where(below, place - d, place + d)
        for slot, which in enumerate((core, 1 - core)):
            for e in range(n_extra):
                extra_load(rank, which, slot, e).start()
        pl.when((s > 0) & (d != distance(s - 1)))(lambda: forward(d))
        for slot, which in enumerate((core, 1 - core)):
            if slot == 1:
                for p in range(pieces):
                    from_mate(rank, p).wait_recv()
            for e in range(n_extra):
                extra_load(rank, which, slot, e).wait()

            @pl.when(s > 0)
            def _():
                for m in range(n_made):
                    store(rank, which, slot, m).wait()

            work(o_ref.at[pl.ds(first_of(rank, which), rows)], weights, extra.at[slot], stage.at[slot])
            for m in range(n_made):
                store(rank, which, slot, m).start()
        return carry

    lax.fori_loop(0, size, visit, 0)
    for slot, which in enumerate((core, 1 - core)):
        for m in range(n_made):
            store(place, which, slot, m).wait()
    for p in range(pieces):
        for k in range(last):
            pl.when((place < last) & (place - k >= 0))(lambda k=k, p=p: going_up(k, p).wait_send())
            pl.when((place > 0) & (place + k <= last))(lambda k=k, p=p: going_down(k, p).wait_send())
        for rank in range(size):
            to_mate(rank, p).wait_send()


def gather_apply(x, weights, extra, work, n_made, ident):
    size = lax.axis_size("ctx")
    rows, width = x.shape[0], weights[0].shape[1]
    total = 2 * size * rows
    pieces = pieces_of(*x.shape)
    dma = pltpu.SemaphoreType.DMA
    made = jax.ShapeDtypeStruct((total, width), jnp.bfloat16)
    slots = max(1, len(extra))
    return pl.pallas_call(
        functools.partial(gather_apply_kernel, size, pieces, work, len(weights), len(extra), n_made),
        in_specs=[IN_VMEM] + [ANY] * (len(weights) + len(extra)),
        out_specs=[IN_VMEM] + [ANY] * n_made,
        out_shape=[jax.ShapeDtypeStruct((total, x.shape[1]), x.dtype)] + [made] * n_made,
        scratch_shapes=[pltpu.VMEM(w.shape, w.dtype) for w in weights]
        + [
            pltpu.VMEM((2, slots, rows, width) if extra else (2, 1, 16, 128), jnp.bfloat16),
            pltpu.VMEM((2, n_made, rows, width), jnp.bfloat16),
            dma,
            dma((len(weights),)),
            dma((2, slots)),
            dma((2, n_made)),
        ]
        + [dma((size, pieces))] * 6,
        compiler_params=pltpu.CompilerParams(collective_id=ident, has_side_effects=True, vmem_limit_bytes=60000000),
        cost_estimate=pl.CostEstimate(flops=0, bytes_accessed=200000000, transcendentals=0),
    )(x, *weights, *extra)


def mask_into(bias_ref, first, seg_ref, place_ref):
    keys, rows = bias_ref.shape
    key_index = lax.broadcasted_iota(jnp.int32, (keys, rows), 0)
    row_index = lax.broadcasted_iota(jnp.int32, (keys, rows), 1) + first
    place = jnp.broadcast_to(place_ref[...], (keys, rows))
    start = jnp.broadcast_to(seg_ref[...], (keys, rows))
    allowed = ((place >= start) & (place <= row_index)) | (key_index == row_index)
    bias_ref[...] = jnp.where(allowed, 0.0, VERY_LOW)


def attend_kernel(scale, first_ref, seg_ref, place_ref, q_ref, k_ref, vt_ref, o_ref, lse_ref, bias_ref):
    @pl.when(pl.program_id(1) == 0)
    def _():
        mask_into(bias_ref, first_ref[0] + pl.program_id(0) * q_ref.shape[0], seg_ref, place_ref)

    scores = matmul_nt(k_ref[...], q_ref[...]) * scale + bias_ref[...]
    top = jnp.max(scores, axis=0, keepdims=True)
    powers = jnp.exp(scores - top)
    total = jnp.sum(powers, axis=0, keepdims=True)
    mixture = nn(vt_ref[...], powers.astype(jnp.bfloat16)) / total
    o_ref[...] = mixture.T.astype(jnp.bfloat16)
    lse_ref[0] = top + jnp.log(total)


def attend_back_kernel(
    scale, first_ref, seg_ref, place_ref, q_ref, do_ref, lse_ref, k_ref, v_ref, kt_ref,
    dq_ref, dkv_ref, bias_ref, dk_ref, dv_ref,
):
    block, head = pl.program_id(0), pl.program_id(1)

    @pl.when(head == 0)
    def _():
        mask_into(bias_ref, first_ref[0] + block * q_ref.shape[0], seg_ref, place_ref)

    @pl.when((head == 0) & (block == 0))
    def _():
        dk_ref[...] = jnp.zeros_like(dk_ref)
        dv_ref[...] = jnp.zeros_like(dv_ref)

    query, grad = q_ref[...], do_ref[...]
    scores = matmul_nt(k_ref[...], query) * scale + bias_ref[...]
    probs = jnp.exp(scores - lse_ref[0])
    grad_probs = matmul_nt(v_ref[...], grad)
    delta = jnp.sum(probs * grad_probs, axis=0, keepdims=True)
    grad_scores = (probs * (grad_probs - delta)).astype(jnp.bfloat16)
    dv_ref[...] += nn(probs.astype(jnp.bfloat16), grad)
    dk_ref[...] += nn(grad_scores, query)
    dq_ref[...] = (nn(kt_ref[...], grad_scores) * scale).T

    @pl.when((head == pl.num_programs(1) - 1) & (block == pl.num_programs(0) - 1))
    def _():
        dkv_ref[:, :HEAD] = (dk_ref[...] * scale).astype(jnp.bfloat16)
        dkv_ref[:, HEAD:] = dv_ref[...].astype(jnp.bfloat16)


def attention_calls(rows, keys, heads):
    block = math.gcd(256, rows)
    scale = 1.0 / math.sqrt(HEAD)
    smem = pl.BlockSpec(memory_space=pltpu.SMEM)
    seg = pl.BlockSpec((1, block), lambda i, h: (0, i))
    place = pl.BlockSpec((keys, 1), lambda i, h: (0, 0))
    head = pl.BlockSpec((block, HEAD), lambda i, h: (i, h))
    lse = pl.BlockSpec((1, 1, block), lambda i, h: (h, 0, i))
    tall = pl.BlockSpec((keys, HEAD), lambda i, h: (0, 0))
    wide = pl.BlockSpec((HEAD, keys), lambda i, h: (0, 0))
    params = pltpu.CompilerParams(vmem_limit_bytes=60000000)
    grid = (rows // block, heads)
    size = heads * rows * keys
    forward = pl.pallas_call(
        functools.partial(attend_kernel, scale),
        grid=grid,
        in_specs=[smem, seg, place, head, tall, wide],
        out_specs=[head, lse],
        out_shape=[
            jax.ShapeDtypeStruct((rows, heads * HEAD), jnp.bfloat16),
            jax.ShapeDtypeStruct((heads, 1, rows), jnp.float32),
        ],
        scratch_shapes=[pltpu.VMEM((keys, block), jnp.float32)],
        compiler_params=params,
        cost_estimate=pl.CostEstimate(flops=4 * size * HEAD, bytes_accessed=4 * rows * heads * HEAD, transcendentals=size),
        name="attend",
    )
    backward = pl.pallas_call(
        functools.partial(attend_back_kernel, scale),
        grid=grid,
        in_specs=[smem, seg, place, head, head, lse, tall, tall, wide],
        out_specs=[head, pl.BlockSpec((keys, 2 * HEAD), lambda i, h: (0, 0))],
        out_shape=[
            jax.ShapeDtypeStruct((rows, heads * HEAD), jnp.float32),
            jax.ShapeDtypeStruct((keys, 2 * HEAD), jnp.bfloat16),
        ],
        scratch_shapes=[
            pltpu.VMEM((keys, block), jnp.float32),
            pltpu.VMEM((keys, HEAD), jnp.float32),
            pltpu.VMEM((keys, HEAD), jnp.float32),
        ],
        compiler_params=params,
        cost_estimate=pl.CostEstimate(flops=10 * size * HEAD, bytes_accessed=8 * rows * heads * HEAD, transcendentals=size),
        name="attend_back",
    )
    return forward, backward


def per_device(
    layer_input,
    teacher,
    cotangent,
    segment_ids,
    positions,
    valid_mask,
    gain_attn,
    query_weight,
    query_bias,
    key_weight,
    key_bias,
    value_weight,
    value_bias,
    out_weight,
    gain_mlp,
    gate_weight,
    up_weight,
    down_weight,
):
    tensor_rank = lax.axis_index("tensor")
    ctx_rank = lax.axis_index("ctx")
    tensor_size, ctx_size = lax.axis_size("tensor"), lax.axis_size("ctx")
    own_rows = layer_input.shape[0]
    shard_rows = own_rows * tensor_size
    seq_len = segment_ids.shape[0]
    q_width = query_weight.shape[1]
    kv_width = key_weight.shape[1]
    kv_local = kv_width // HEAD
    group = q_width // kv_width
    hidden_width = gate_weight.shape[1]
    slice_width = -(-hidden_width // (128 * ctx_size)) * 128
    first_row = ctx_rank * shard_rows
    own_first = first_row + tensor_rank * own_rows

    inputs = layer_input.astype(jnp.float32)
    gain_one = gain_attn.astype(jnp.float32)
    gain_two = gain_mlp.astype(jnp.float32)
    scale_attn = lax.rsqrt(jnp.mean(inputs * inputs, axis=1, keepdims=True) + EPS)
    normed_attn = inputs * scale_attn
    extra = ((0, 0), (0, ctx_size * slice_width - hidden_width))
    full_qkv, full_out, *slices = front(
        jnp.concatenate([query_weight, key_weight, value_weight], axis=1),
        out_weight.T,
        [jnp.pad(w, extra) for w in (gate_weight, up_weight, down_weight.T)],
        slice_width,
        1,
    )
    full_gate, full_up, full_down = [lax.all_gather(w, "dp", axis=0, tiled=True) for w in slices]
    normed_rows = gather((normed_attn * gain_one).astype(jnp.bfloat16), 1, True, 2)
    valid_count = jnp.sum(valid_mask.astype(jnp.float32))
    counts = [valid_count]
    dp_size = lax.axis_size("dp")
    for step in range(1, dp_size):
        counts.append(
            lax.ppermute(
                jnp.full((8, 128), valid_count), "dp", [(i, (i + step) % dp_size) for i in range(dp_size)]
            )[0, 0]
        )
    valid_count = sum(counts)

    bias = jnp.concatenate(
        [
            lax.dynamic_slice_in_dim(query_bias, tensor_rank * q_width, q_width),
            lax.dynamic_slice_in_dim(key_bias, tensor_rank * kv_width, kv_width),
            lax.dynamic_slice_in_dim(value_bias, tensor_rank * kv_width, kv_width),
        ]
    ).astype(jnp.float32)
    places = lax.dynamic_slice_in_dim(positions, first_row, shard_rows)
    cosine, sine_table = rope_tables(places)
    qkv_pre = matmul(normed_rows, full_qkv) + bias
    turned = q_width + kv_width
    rotated = (
        rotate(qkv_pre[:, :turned].reshape(shard_rows, turned // HEAD, HEAD), cosine, sine_table)
        .astype(jnp.bfloat16)
        .reshape(shard_rows, turned)
    )
    queries = rotated[:, :q_width]
    own_kv = jnp.concatenate([rotated[:, q_width:], qkv_pre[:, turned:].astype(jnp.bfloat16)], axis=1)
    all_kv = gather(own_kv, ctx_size, False, 3)

    key_index = jnp.arange(seq_len, dtype=jnp.int32)
    key_place = jnp.where(valid_mask > 0, key_index, -1)[:, None]
    seq_first = lax.axis_index("dp") * seq_len
    doc_start = (lax.dynamic_slice_in_dim(segment_ids, first_row, shard_rows) - seq_first)[None, :]
    first = jnp.reshape(first_row, (1,)).astype(jnp.int32)
    forward, backward = attention_calls(shard_rows, seq_len, group)
    kept = []
    for c in range(kv_local):
        key = all_kv[:, c * HEAD : (c + 1) * HEAD]
        value = all_kv[:, kv_width + c * HEAD : kv_width + (c + 1) * HEAD]
        query = queries[:, c * group * HEAD : (c + 1) * group * HEAD]
        kept.append((query, key, value) + tuple(forward(first, doc_start, key_place, query, key, value.T)))
    heads_out = jnp.concatenate([k[3] for k in kept], axis=1)
    attention = scatter(matmul_nt(heads_out, full_out), 1, True, 4)
    residual_mid = inputs + attention
    scale_mlp = lax.rsqrt(jnp.mean(residual_mid * residual_mid, axis=1, keepdims=True) + EPS)
    normed_mlp = residual_mid * scale_mlp
    mlp_rows, gate_act, up_act, hidden = gather_apply(
        (normed_mlp * gain_two).astype(jnp.bfloat16), [full_gate, full_up], [], expand_block, 3, 5
    )
    branch = scatter(matmul_nt(hidden, full_down).astype(jnp.bfloat16), ctx_size, True, 6)
    layer_result = residual_mid + branch
    valid_own = lax.dynamic_slice_in_dim(valid_mask, own_first, own_rows).astype(jnp.float32)
    difference = layer_result - teacher.astype(jnp.float32)
    squared_sum = jnp.sum(valid_own[:, None] * difference * difference)
    grad_result = cotangent.astype(jnp.float32) + 2.0 * valid_own[:, None] * difference / (
        valid_count * D
    )
    grad_branch, grad_gate_act, grad_up_act = gather_apply(
        grad_result.astype(jnp.bfloat16), [full_down], [gate_act, up_act], shrink_block, 2, 9
    )
    summed = []
    for left, right in ((grad_branch, hidden), (mlp_rows, grad_gate_act), (mlp_rows, grad_up_act)):
        grad = matmul_tn(left, right).astype(jnp.bfloat16)
        grad_gate_act, grad_up_act, grad = lax.optimization_barrier((grad_gate_act, grad_up_act, grad))
        summed.append(lax.psum_scatter(grad, "dp", scatter_dimension=0, tiled=True))
    grad_mlp_rows = (matmul_nt(grad_gate_act, full_gate) + matmul_nt(grad_up_act, full_up)).astype(jnp.bfloat16)
    grad_mlp_rows = scatter(grad_mlp_rows, ctx_size, True, 6)
    grad_gain_mlp = jnp.sum(grad_mlp_rows * normed_mlp, axis=0)
    grad_mid = grad_result + norm_back(grad_mlp_rows, normed_mlp, scale_mlp, gain_two)
    grad_attn_rows = gather(grad_mid.astype(jnp.bfloat16), 1, True, 2)
    grad_heads = matmul(grad_attn_rows, full_out).astype(jnp.bfloat16)
    grad_out = matmul_tn(grad_attn_rows, heads_out).astype(jnp.bfloat16)

    grad_out = lax.psum_scatter(grad_out, "dp", scatter_dimension=0, tiled=True)
    query_grads, key_grads, value_grads = [], [], []
    for c in range(kv_local):
        query, key, value, _, log_total = kept[c]
        span = slice(c * group * HEAD, (c + 1) * group * HEAD)
        grad_query, grad_kv = backward(
            first, doc_start, key_place, query, grad_heads[:, span], log_total, key, value, key.T
        )
        query_grads.append(grad_query)
        key_grads.append(grad_kv[:, :HEAD])
        value_grads.append(grad_kv[:, HEAD:])
    grad_kv = grad_kv if kv_local == 1 else jnp.concatenate(key_grads + value_grads, axis=1)
    grad_kv, *summed = lax.optimization_barrier((grad_kv, *summed))
    shard_down, shard_gate, shard_up = to_rows(summed, hidden_width)
    shard_down = shard_down.T
    grad_kv = scatter(grad_kv, ctx_size, False, 7)
    grad_turned = jnp.concatenate(query_grads + [grad_kv[:, :kv_width]], axis=1)
    grad_pre = jnp.concatenate(
        [
            rotate(grad_turned.reshape(shard_rows, turned // HEAD, HEAD), cosine, -sine_table)
            .reshape(shard_rows, turned)
            .astype(jnp.bfloat16),
            grad_kv[:, kv_width:].astype(jnp.bfloat16),
        ],
        axis=1,
    )
    grad_pre, grad_out = lax.optimization_barrier((grad_pre, grad_out))
    shard_out = lax.psum_scatter(grad_out, "ctx", scatter_dimension=0, tiled=True)
    shard_out = shard_out.astype(jnp.float32).T
    grad_normed = scatter(matmul_nt(grad_pre, full_qkv), 1, True, 4)
    grad_gain_attn = jnp.sum(grad_normed * normed_attn, axis=0)
    grad_input = grad_mid + norm_back(grad_normed, normed_attn, scale_attn, gain_one)
    bias_sum = jnp.sum(grad_pre.astype(jnp.float32), axis=0)

    def spread(part, size):
        return lax.dynamic_update_slice_in_dim(
            jnp.zeros((size,), jnp.float32), part, tensor_rank * part.shape[0], 0
        )

    loss_part = jnp.zeros((128,), jnp.float32).at[0].set(squared_sum)
    parts = [
        grad_gain_attn,
        grad_gain_mlp,
        spread(bias_sum[:q_width], query_bias.shape[0]),
        spread(bias_sum[q_width:turned], key_bias.shape[0]),
        spread(bias_sum[turned:], value_bias.shape[0]),
        loss_part,
    ]
    flat = jnp.concatenate(parts)
    small = jnp.pad(flat, (0, -flat.shape[0] % 1024)).reshape(-1, 128)
    grad_qkv = matmul_tn(normed_rows, grad_pre).astype(jnp.bfloat16)
    shard_qkv, sums = back(grad_qkv, small, 8)
    sums = sums.reshape(-1)
    pieces, offset = [], 0
    for part in parts:
        pieces.append(sums[offset : offset + part.shape[0]])
        offset += part.shape[0]
    return (
        layer_result.astype(jnp.bfloat16),
        pieces[5][0] / (valid_count * D),
        grad_input,
        pieces[0],
        shard_qkv[:, :q_width],
        pieces[2],
        shard_qkv[:, q_width:turned],
        pieces[3],
        shard_qkv[:, turned:],
        pieces[4],
        shard_out,
        pieces[1],
        shard_gate,
        shard_up,
        shard_down,
    )


def solution(mesh):
    in_specs = (
        P(("dp", "ctx", "tensor"), None),
        P(("dp", "ctx", "tensor"), None),
        P(("dp", "ctx", "tensor"), None),
        P("dp"),
        P("dp"),
        P("dp"),
        P(),
        P(("dp", "ctx"), "tensor"),
        P(),
        P(("dp", "ctx"), "tensor"),
        P(),
        P(("dp", "ctx"), "tensor"),
        P(),
        P("tensor", ("dp", "ctx")),
        P(),
        P(("dp", "ctx"), "tensor"),
        P(("dp", "ctx"), "tensor"),
        P("tensor", ("dp", "ctx")),
    )
    out_specs = (
        P(("dp", "ctx", "tensor"), None),
        P(),
        P(("dp", "ctx", "tensor"), None),
        P(),
        P(("dp", "ctx"), "tensor"),
        P(),
        P(("dp", "ctx"), "tensor"),
        P(),
        P(("dp", "ctx"), "tensor"),
        P(),
        P("tensor", ("dp", "ctx")),
        P(),
        P(("dp", "ctx"), "tensor"),
        P(("dp", "ctx"), "tensor"),
        P("tensor", ("dp", "ctx")),
    )

    return jax.shard_map(per_device, mesh=mesh, in_specs=in_specs, out_specs=out_specs, check_vma=False)
```

```python
import functools
import math

import jax
import jax.numpy as jnp
from jax import lax
from jax.experimental import pallas as pl
from jax.experimental.pallas import tpu as pltpu
from jax.sharding import PartitionSpec as P


D = 1536
HEAD = 128


EPS = 1e-06
THETA = 10000.0
VERY_LOW = -1e30


def rope_tables(places):
    half_dim = HEAD // 2
    frequency = THETA ** (-(jnp.arange(half_dim, dtype=jnp.float32) * 2.0 / HEAD))
    angles = places.astype(jnp.float32)[:, None] * frequency[None, :]
    return (jnp.cos(angles), jnp.sin(angles))


def rotate(stacked, cosine, sine_table):
    half_dim = HEAD // 2
    first_half = stacked[..., :half_dim]
    second_half = stacked[..., half_dim:]
    cosine = cosine[:, None, :]
    sine_table = sine_table[:, None, :]
    return jnp.concatenate(
        [
            first_half * cosine - second_half * sine_table,
            second_half * cosine + first_half * sine_table,
        ],
        axis=-1,
    )


def matmul(first_op, second_op):
    return jnp.dot(first_op, second_op, preferred_element_type=jnp.float32)


def matmul_tn(first_op, second_op):
    return lax.dot_general(
        first_op, second_op, (((0,), (0,)), ((), ())), preferred_element_type=jnp.float32
    )


def matmul_nt(first_op, second_op):
    return lax.dot_general(
        first_op, second_op, (((1,), (1,)), ((), ())), preferred_element_type=jnp.float32
    )


def norm_back(grad_normed, normed, inverse, gain):
    scaled = grad_normed * gain
    return inverse * (scaled - normed * jnp.mean(scaled * normed, axis=1, keepdims=True))


def exchange(blocks, axis):
    size = lax.axis_size(axis)
    rank = lax.axis_index(axis)
    received = [(rank, lax.dynamic_index_in_dim(blocks, rank, 0, keepdims=False))]
    for step in range(1, size):
        going = lax.dynamic_index_in_dim(blocks, (rank + step) % size, 0, keepdims=False)
        came = lax.ppermute(going, axis, [(i, (i + step) % size) for i in range(size)])
        received.append(((rank - step + size) % size, came))
    return received


def to_rows(summed, columns):
    size = lax.axis_size("ctx")
    rows, width = summed[0].shape[0] // size, summed[0].shape[1]
    blocks = jnp.stack([s.reshape(size, rows, width) for s in summed], axis=1)
    return assemble(exchange(blocks, "ctx"), columns)


def nn(first_op, second_op):
    return jnp.dot(first_op, second_op, preferred_element_type=jnp.float32)


MESH = pl.DeviceIdType.MESH
ANY = pl.BlockSpec(memory_space=pl.ANY)
IN_VMEM = pl.BlockSpec(memory_space=pltpu.VMEM)


def remote(source, target, send_sem, recv_sem, device):
    return pltpu.make_async_remote_copy(
        src_ref=source,
        dst_ref=target,
        send_sem=send_sem,
        recv_sem=recv_sem,
        device_id=device,
        device_id_type=MESH,
    )


def greet(barrier, device):
    pl.semaphore_signal(barrier, inc=1, device_id=device, device_id_type=MESH)


def greet_chain(size, paired):
    place = lax.axis_index("ctx")
    barrier = pltpu.get_barrier_semaphore()
    if size > 1:
        pl.when(place < size - 1)(lambda: greet(barrier, {"ctx": place + 1}))
        pl.when(place > 0)(lambda: greet(barrier, {"ctx": place - 1}))
    if paired:
        greet(barrier, {"tensor": 1 - lax.axis_index("tensor")})
    if size == 1:
        pl.semaphore_wait(barrier, 1)
        return
    ends = (place == 0) | (place == size - 1)
    pl.when(ends)(lambda: pl.semaphore_wait(barrier, 1 + paired))
    pl.when(jnp.logical_not(ends))(lambda: pl.semaphore_wait(barrier, 2 + paired))


def gather_kernel(size, paired, pieces, x_ref, o_ref, local_sem, up_send, up_recv, down_send, down_recv, mate_send, mate_recv):
    place = lax.axis_index("ctx") if size > 1 else 0
    core = lax.axis_index("tensor")
    rows = x_ref.shape[0]
    part = rows // pieces
    greet_chain(size, paired)

    def block(rank, which, p):
        index = rank * 2 + which if paired else rank
        return o_ref.at[pl.ds(pl.multiple_of(index * rows + p * part, part), part)]

    def source(rank, k, p):
        return x_ref.at[pl.ds(p * part, part)] if k == 0 else block(rank, core, p)

    def going_up(k, p):
        return remote(
            source(place - k, k, p), block(place - k, core, p), up_send.at[k, p], up_recv.at[k, p], {"ctx": place + 1}
        )

    def going_down(k, p):
        return remote(
            source(place + k, k, p), block(place + k, core, p), down_send.at[k, p], down_recv.at[k, p], {"ctx": place - 1}
        )

    def to_mate(rank, k, p):
        return remote(
            source(rank, k, p), block(rank, core, p), mate_send.at[k, p], mate_recv.at[rank, p], {"tensor": 1 - core}
        )

    def from_mate(rank, p):
        there = block(rank, 1 - core, p)
        return remote(there, there, mate_send.at[0, p], mate_recv.at[rank, p], {"tensor": 1 - core})

    own = pltpu.make_async_copy(x_ref, o_ref.at[pl.ds(pl.multiple_of((place * 2 + core if paired else place) * rows, rows), rows)], local_sem)
    for p in range(pieces):
        if size > 1:
            pl.when(place < size - 1)(lambda p=p: going_up(0, p).start())
            pl.when(place > 0)(lambda p=p: going_down(0, p).start())
    for p in range(pieces):
        if paired:
            to_mate(place, 0, p).start()
    own.start()
    for k in range(size - 1):
        for p in range(pieces):

            @pl.when(place - 1 - k >= 0)
            def _(k=k, p=p):
                there = block(place - 1 - k, core, p)
                remote(there, there, up_send.at[k, p], up_recv.at[k, p], {"ctx": place - 1}).wait_recv()
                if k + 1 < size - 1:
                    pl.when(place < size - 1)(lambda: going_up(k + 1, p).start())
                if paired:
                    to_mate(place - 1 - k, 1 + k, p).start()

            @pl.when(place + 1 + k <= size - 1)
            def _(k=k, p=p):
                there = block(place + 1 + k, core, p)
                remote(there, there, down_send.at[k, p], down_recv.at[k, p], {"ctx": place + 1}).wait_recv()
                if k + 1 < size - 1:
                    pl.when(place > 0)(lambda: going_down(k + 1, p).start())
                if paired:
                    to_mate(place + 1 + k, size + k, p).start()

    own.wait()
    for p in range(pieces):
        if paired:
            for rank in range(size):
                from_mate(rank, p).wait_recv()
            to_mate(place, 0, p).wait_send()
        for k in range(size - 1):
            pl.when((place < size - 1) & (place - k >= 0))(lambda k=k, p=p: going_up(k, p).wait_send())
            pl.when((place > 0) & (place + k <= size - 1))(lambda k=k, p=p: going_down(k, p).wait_send())
            if paired:
                pl.when(place - 1 - k >= 0)(lambda k=k, p=p: to_mate(place - 1 - k, 1 + k, p).wait_send())
                pl.when(place + 1 + k <= size - 1)(lambda k=k, p=p: to_mate(place + 1 + k, size + k, p).wait_send())


def pieces_of(rows, columns):
    return math.gcd(4, rows // 64) if rows * columns >= 1 << 18 else 1


def gather(x, size, paired, ident):
    copies = size * 2 if paired else size
    wide = max(size, 2)
    pieces = pieces_of(*x.shape)
    dma = pltpu.SemaphoreType.DMA
    return pl.pallas_call(
        functools.partial(gather_kernel, size, paired, pieces),
        in_specs=[IN_VMEM],
        out_specs=ANY,
        out_shape=jax.ShapeDtypeStruct((copies * x.shape[0], x.shape[1]), x.dtype),
        scratch_shapes=[dma] + [dma((wide, pieces))] * 4 + [dma((2 * wide, pieces)), dma((wide, pieces))],
        compiler_params=pltpu.CompilerParams(collective_id=ident, has_side_effects=True),
        cost_estimate=pl.CostEstimate(flops=0, bytes_accessed=30 * copies * x.size, transcendentals=0),
        name="gather",
    )(x)


def add_blocks(target, parts):
    rows = target.shape[0]
    step = math.gcd(rows, 32)

    def some(i, carry):
        span = pl.ds(pl.multiple_of(i * step, step), step)
        total = parts[0][span].astype(jnp.float32)
        for part in parts[1:]:
            total += part[span].astype(jnp.float32)
        target[span] = total.astype(target.dtype)
        return carry

    lax.fori_loop(0, rows // step, some, 0)


def scatter_kernel(
    size, paired, pieces, x_ref, o_ref, mine, mate, above, below, own_sem, mate_send, mate_recv, up_send, up_recv, down_send, down_recv
):
    place = lax.axis_index("ctx") if size > 1 else 0
    core = lax.axis_index("tensor")
    rows = o_ref.shape[0]
    part = rows // pieces
    order = sorted(range(size), key=lambda d: min(d, size - 1 - d))
    every = [(d, p) for d in order for p in range(pieces)]

    def block(rank, which, p):
        index = rank * 2 + which if paired else rank
        return x_ref.at[pl.ds(pl.multiple_of(index * rows + p * part, part), part)]

    def at(ref, d, p):
        return ref.at[d, pl.ds(p * part, part)]

    def load(d, p):
        return pltpu.make_async_copy(block(d, core, p), at(mine, d, p), own_sem.at[d, p])

    def to_mate(d, p):
        return remote(
            block(d, 1 - core, p), at(mate, d, p), mate_send.at[d, p], mate_recv.at[d, p], {"tensor": 1 - core}
        )

    def going_up(d, p):
        return remote(at(mine, d, p), at(below, d, p), up_send.at[d, p], up_recv.at[d, p], {"ctx": place + 1})

    def going_down(d, p):
        return remote(at(mine, d, p), at(above, d, p), down_send.at[d, p], down_recv.at[d, p], {"ctx": place - 1})

    for d, p in every:
        load(d, p).start()
    greet_chain(size, paired)
    if paired:
        for d, p in every:
            to_mate(d, p).start()

    def here(d, p):
        load(d, p).wait()
        if paired:
            to_mate(d, p).wait_recv()
            return [at(mine, d, p), at(mate, d, p)]
        return [at(mine, d, p)]

    for k in range(size - 1):
        for p in range(pieces):

            @pl.when(place < size - 1 - k)
            def _(d=size - 1 - k, p=p):
                parts = here(d, p)

                @pl.when(place > 0)
                def _():
                    going_up(d, p).wait_recv()
                    add_blocks(at(mine, d, p), parts + [at(below, d, p)])

                if paired:
                    pl.when(place == 0)(lambda: add_blocks(at(mine, d, p), parts))
                going_up(d, p).start()

            @pl.when(place > k)
            def _(d=k, p=p):
                parts = here(d, p)

                @pl.when(place < size - 1)
                def _():
                    going_down(d, p).wait_recv()
                    add_blocks(at(mine, d, p), parts + [at(above, d, p)])

                if paired:
                    pl.when(place == size - 1)(lambda: add_blocks(at(mine, d, p), parts))
                going_down(d, p).start()

    for d in range(size):

        @pl.when(place == d)
        def _(d=d):
            for p in range(pieces):
                parts = here(d, p)
                if d > 0:
                    going_up(d, p).wait_recv()
                    parts = parts + [at(below, d, p)]
                if d < size - 1:
                    going_down(d, p).wait_recv()
                    parts = parts + [at(above, d, p)]
                add_blocks(o_ref.at[pl.ds(p * part, part)], parts)

    for d, p in every:
        if d > 0:
            pl.when(place < d)(lambda d=d, p=p: going_up(d, p).wait_send())
        if d < size - 1:
            pl.when(place > d)(lambda d=d, p=p: going_down(d, p).wait_send())
        if paired:
            to_mate(d, p).wait_send()


def scatter(x, size, paired, ident):
    copies = size * 2 if paired else size
    rows = x.shape[0] // copies
    pieces = pieces_of(rows, x.shape[1])
    dma = pltpu.SemaphoreType.DMA
    slots = pltpu.VMEM((size, rows, x.shape[1]), x.dtype)
    one = pltpu.VMEM((1, 32, 128), x.dtype)
    chain = slots if size > 1 else one
    return pl.pallas_call(
        functools.partial(scatter_kernel, size, paired, pieces),
        in_specs=[ANY],
        out_specs=IN_VMEM,
        out_shape=jax.ShapeDtypeStruct((rows, x.shape[1]), jnp.float32),
        scratch_shapes=[slots, slots if paired else one, chain, chain] + [dma((size, pieces))] * 7,
        compiler_params=pltpu.CompilerParams(collective_id=ident, has_side_effects=True, vmem_limit_bytes=60000000),
        cost_estimate=pl.CostEstimate(flops=0, bytes_accessed=30 * x.size, transcendentals=0),
        name="scatter",
    )(x)


def front_kernel(
    size, groups, a_ref, b_ref, g_ref, u_ref, d_ref, fa_ref, fb_ref, og_ref, ou_ref, od_ref,
    local_sem, up_send, up_recv, down_send, down_recv, far_send, far_recv, swap_send, swap_recv,
):
    place, group = lax.axis_index("ctx"), lax.axis_index("dp")
    rows, width = a_ref.shape[0], og_ref.shape[1]
    wholes, owns = (fa_ref, fb_ref), (a_ref, b_ref)
    parts, slices = (g_ref, u_ref, d_ref), (og_ref, ou_ref, od_ref)
    barrier = pltpu.get_barrier_semaphore()
    for step in range(1, size):
        greet(barrier, {"ctx": lax.rem(place + step, size)})
    for step in range(1, groups):
        greet(barrier, {"dp": lax.rem(group + step, groups)})
    pl.semaphore_wait(barrier, size + groups - 2)

    def chunk(which, in_group, rank):
        return wholes[which].at[pl.ds(pl.multiple_of((in_group * size + rank) * rows, rows), rows)]

    def source(which, rank, k):
        return owns[which] if k == 0 else chunk(which, group, rank)

    def going_up(which, k):
        return remote(
            source(which, place - k, k), chunk(which, group, place - k),
            up_send.at[which, k], up_recv.at[which, k], {"ctx": place + 1},
        )

    def going_down(which, k):
        return remote(
            source(which, place + k, k), chunk(which, group, place + k),
            down_send.at[which, k], down_recv.at[which, k], {"ctx": place - 1},
        )

    def across(which, rank, step, k):
        return remote(
            source(which, rank, k), chunk(which, group, rank),
            far_send.at[which, rank, step], far_recv.at[which, rank, step], {"dp": lax.rem(group + step, groups)},
        )

    def from_across(which, rank, step):
        there = chunk(which, lax.rem(group - step + groups, groups), rank)
        return remote(there, there, far_send.at[which, rank, step], far_recv.at[which, rank, step], {"dp": lax.rem(group + step, groups)})

    def columns(which, rank):
        return parts[which].at[:, pl.ds(pl.multiple_of(rank * width, 128), width)]

    def swap(which, step):
        return remote(
            columns(which, lax.rem(place + step, size)),
            slices[which].at[pl.ds(pl.multiple_of(place * rows, rows), rows)],
            swap_send.at[which, step], swap_recv.at[which, step], {"ctx": lax.rem(place + step, size)},
        )

    def swapped(which, step):
        there = slices[which].at[pl.ds(pl.multiple_of(lax.rem(place - step + size, size) * rows, rows), rows)]
        return remote(there, there, swap_send.at[which, step], swap_recv.at[which, step], {"ctx": lax.rem(place + step, size)})

    locals_ = [pltpu.make_async_copy(owns[w], chunk(w, group, place), local_sem.at[w]) for w in range(2)]
    locals_ += [
        pltpu.make_async_copy(
            columns(w, place), slices[w].at[pl.ds(pl.multiple_of(place * rows, rows), rows)], local_sem.at[2 + w]
        )
        for w in range(3)
    ]
    for w in range(2):
        pl.when(place < size - 1)(lambda w=w: going_up(w, 0).start())
        pl.when(place > 0)(lambda w=w: going_down(w, 0).start())
        for step in range(1, groups):
            across(w, place, step, 0).start()
    for copy in locals_:
        copy.start()
    for k in range(size - 1):
        for w in range(2):

            @pl.when(place - 1 - k >= 0)
            def _(k=k, w=w):
                there = chunk(w, group, place - 1 - k)
                remote(there, there, up_send.at[w, k], up_recv.at[w, k], {"ctx": place - 1}).wait_recv()
                if k + 1 < size - 1:
                    pl.when(place < size - 1)(lambda: going_up(w, k + 1).start())
                for step in range(1, groups):
                    across(w, place - 1 - k, step, 1).start()

            @pl.when(place + 1 + k <= size - 1)
            def _(k=k, w=w):
                there = chunk(w, group, place + 1 + k)
                remote(there, there, down_send.at[w, k], down_recv.at[w, k], {"ctx": place + 1}).wait_recv()
                if k + 1 < size - 1:
                    pl.when(place > 0)(lambda: going_down(w, k + 1).start())
                for step in range(1, groups):
                    across(w, place + 1 + k, step, 1).start()

    for w in range(3):
        for step in range(1, size):
            swap(w, step).start()
    for rank in range(size):
        for w in range(2):
            for step in range(1, groups):
                from_across(w, rank, step).wait_recv()
    for w in range(3):
        for step in range(1, size):
            swapped(w, step).wait_recv()
    for copy in locals_:
        copy.wait()
    for w in range(2):
        for k in range(size - 1):
            pl.when((place < size - 1) & (place - k >= 0))(lambda k=k, w=w: going_up(w, k).wait_send())
            pl.when((place > 0) & (place + k <= size - 1))(lambda k=k, w=w: going_down(w, k).wait_send())
        for rank in range(size):
            for step in range(1, groups):
                across(w, rank, step, 1).wait_send()
    for w in range(3):
        for step in range(1, size):
            swap(w, step).wait_send()


def front(a, b, parts, width, ident):
    size, groups = lax.axis_size("ctx"), lax.axis_size("dp")
    rows = a.shape[0]
    dma = pltpu.SemaphoreType.DMA
    slices = jax.ShapeDtypeStruct((size * rows, width), a.dtype)
    return pl.pallas_call(
        functools.partial(front_kernel, size, groups),
        in_specs=[IN_VMEM] * 5,
        out_specs=[ANY] * 5,
        out_shape=[jax.ShapeDtypeStruct((groups * size * rows, x.shape[1]), x.dtype) for x in (a, b)] + [slices] * 3,
        scratch_shapes=[dma((5,))] + [dma((2, size))] * 4 + [dma((2, size, groups))] * 2 + [dma((3, size))] * 2,
        compiler_params=pltpu.CompilerParams(collective_id=ident, has_side_effects=True),
        cost_estimate=pl.CostEstimate(flops=0, bytes_accessed=200000000, transcendentals=0),
        name="front",
    )(a, b, *parts)


def back_kernel(
    size, groups, x_ref, s_ref, o_ref, t_ref, mine, far, near, pair, crowd, row,
    own_sem, far_send, far_recv, near_send, near_recv, pair_sems, crowd_send, crowd_recv, row_send, row_recv,
):
    place, group = lax.axis_index("ctx"), lax.axis_index("dp")
    core = lax.axis_index("tensor")
    rows = o_ref.shape[0]
    barrier = pltpu.get_barrier_semaphore()

    def rank_at(k):
        return lax.rem(place + 1 + k, size)

    def block(in_group, rank):
        return x_ref.at[pl.ds(pl.multiple_of((in_group * size + rank) * rows, rows), rows)]

    def load(k):
        return pltpu.make_async_copy(block(group, rank_at(k)), mine.at[k], own_sem.at[k])

    def across(k, step):
        to = lax.rem(group + step, groups)
        return remote(block(to, rank_at(k)), far.at[k, step], far_send.at[k, step], far_recv.at[k, step], {"dp": to})

    def along(k):
        return remote(mine.at[k], near.at[k], near_send.at[k], near_recv.at[k], {"ctx": rank_at(k)})

    to_mate = remote(s_ref, pair, pair_sems.at[0], pair_sems.at[1], {"tensor": 1 - core})

    def to_crowd(step):
        return remote(
            crowd.at[group], crowd.at[group], crowd_send.at[step], crowd_recv.at[step],
            {"dp": lax.rem(group + step, groups)},
        )

    def to_row(step):
        return remote(
            row.at[place], row.at[place], row_send.at[step], row_recv.at[step], {"ctx": lax.rem(place + step, size)}
        )

    for k in range(size):
        load(k).start()
    for step in range(1, size):
        greet(barrier, {"ctx": lax.rem(place + step, size)})
    for step in range(1, groups):
        greet(barrier, {"dp": lax.rem(group + step, groups)})
    greet(barrier, {"tensor": 1 - core})
    pl.semaphore_wait(barrier, size + groups - 1)
    to_mate.start()
    to_mate.wait_recv()
    crowd[group] = s_ref[...] + pair[...]
    for step in range(1, groups):
        to_crowd(step).start()
    for k in range(size):
        for step in range(1, groups):
            across(k, step).start()
    for step in range(1, groups):
        to_crowd(step).wait_recv()
    total = crowd[0]
    for g in range(1, groups):
        total += crowd[g]
    row[place] = total
    for step in range(1, size):
        to_row(step).start()
    for k in range(size):
        load(k).wait()
        for step in range(1, groups):
            across(k, step).wait_recv()
        parts = [mine.at[k]] + [far.at[k, step] for step in range(1, groups)]
        if k < size - 1:
            add_blocks(mine.at[k], parts)
            along(k).start()
    for k in range(size - 1):
        along(k).wait_recv()
        parts.append(near.at[k])
    add_blocks(o_ref, parts)
    for step in range(1, size):
        to_row(step).wait_recv()
    total = row[0]
    for c in range(1, size):
        total += row[c]
    t_ref[...] = total
    to_mate.wait_send()
    for step in range(1, groups):
        to_crowd(step).wait_send()
    for step in range(1, size):
        to_row(step).wait_send()
    for k in range(size):
        for step in range(1, groups):
            across(k, step).wait_send()
        if k < size - 1:
            along(k).wait_send()


def back(x, small, ident):
    size, groups = lax.axis_size("ctx"), lax.axis_size("dp")
    rows, columns = x.shape[0] // (size * groups), x.shape[1]
    dma = pltpu.SemaphoreType.DMA
    return pl.pallas_call(
        functools.partial(back_kernel, size, groups),
        in_specs=[ANY, IN_VMEM],
        out_specs=[IN_VMEM, IN_VMEM],
        out_shape=[
            jax.ShapeDtypeStruct((rows, columns), jnp.float32),
            jax.ShapeDtypeStruct(small.shape, jnp.float32),
        ],
        scratch_shapes=[
            pltpu.VMEM((size, rows, columns), x.dtype),
            pltpu.VMEM((size, groups, rows, columns), x.dtype),
            pltpu.VMEM((size, rows, columns), x.dtype),
            pltpu.VMEM(small.shape, jnp.float32),
            pltpu.VMEM((groups,) + small.shape, jnp.float32),
            pltpu.VMEM((size,) + small.shape, jnp.float32),
            dma((size,)),
            dma((size, groups)),
            dma((size, groups)),
            dma((size,)),
            dma((size,)),
            dma((2,)),
            dma((groups,)),
            dma((groups,)),
            dma((size,)),
            dma((size,)),
        ],
        compiler_params=pltpu.CompilerParams(collective_id=ident, has_side_effects=True, vmem_limit_bytes=60000000),
        cost_estimate=pl.CostEstimate(flops=0, bytes_accessed=100 * x.size, transcendentals=0),
        name="back",
    )(x, small)


def column_step(width):
    return max(t for t in (768, 384, 256, 128) if width % t == 0)


def expand_block(x_ref, weights, extra, stage):
    step = column_step(weights[0].shape[1])

    def some(j, carry):
        span = pl.ds(pl.multiple_of(j * step, step), step)
        gate = nn(x_ref[...], weights[0][:, span])
        up = nn(x_ref[...], weights[1][:, span])
        stage[0, :, span] = gate.astype(jnp.bfloat16)
        stage[1, :, span] = up.astype(jnp.bfloat16)
        stage[2, :, span] = (gate * jax.nn.sigmoid(gate) * up).astype(jnp.bfloat16)
        return carry

    lax.fori_loop(0, weights[0].shape[1] // step, some, 0)


def shrink_block(x_ref, weights, extra, stage):
    step = column_step(weights[0].shape[1])

    def some(j, carry):
        span = pl.ds(pl.multiple_of(j * step, step), step)
        grad = nn(x_ref[...], weights[0][:, span])
        gate = extra[0, :, span].astype(jnp.float32)
        up = extra[1, :, span].astype(jnp.float32)
        sigmoid = jax.nn.sigmoid(gate)
        stage[0, :, span] = (grad * up * sigmoid * (1.0 + gate * (1.0 - sigmoid))).astype(jnp.bfloat16)
        stage[1, :, span] = (grad * gate * sigmoid).astype(jnp.bfloat16)
        return carry

    lax.fori_loop(0, weights[0].shape[1] // step, some, 0)


def gather_apply_kernel(size, pieces, work, n_weights, n_extra, n_made, *refs):
    x_ref, refs = refs[0], refs[1:]
    weights_from, refs = refs[:n_weights], refs[n_weights:]
    extra_from, refs = refs[:n_extra], refs[n_extra:]
    o_ref, refs = refs[0], refs[1:]
    made_to, refs = refs[:n_made], refs[n_made:]
    weights, refs = refs[:n_weights], refs[n_weights:]
    extra, stage, refs = refs[0], refs[1], refs[2:]
    local_sem, weight_sem, extra_sem, stage_sem = refs[:4]
    up_send, up_recv, down_send, down_recv, mate_send, mate_recv = refs[4:]
    place = lax.axis_index("ctx")
    core = lax.axis_index("tensor")
    rows = x_ref.shape[0]
    part = rows // pieces
    last = size - 1

    loads = [pltpu.make_async_copy(weights_from[w], weights[w], weight_sem.at[w]) for w in range(n_weights)]
    for load in loads:
        load.start()

    def first_of(rank, which):
        return pl.multiple_of((rank * 2 + which) * rows, rows)

    def block(rank, which, p):
        return o_ref.at[pl.ds(pl.multiple_of((rank * 2 + which) * rows + p * part, part), part)]

    def going_up(k, p):
        there = block(place - k, core, p)
        return remote(there, there, up_send.at[k, p], up_recv.at[k, p], {"ctx": place + 1})

    def going_down(k, p):
        there = block(place + k, core, p)
        return remote(there, there, down_send.at[k, p], down_recv.at[k, p], {"ctx": place - 1})

    def coming_up(k, p):
        there = block(place - 1 - k, core, p)
        return remote(there, there, up_send.at[k, p], up_recv.at[k, p], {"ctx": place - 1})

    def coming_down(k, p):
        there = block(place + 1 + k, core, p)
        return remote(there, there, down_send.at[k, p], down_recv.at[k, p], {"ctx": place + 1})

    def to_mate(rank, p):
        there = block(rank, core, p)
        return remote(there, there, mate_send.at[rank, p], mate_recv.at[rank, p], {"tensor": 1 - core})

    def from_mate(rank, p):
        there = block(rank, 1 - core, p)
        return remote(there, there, mate_send.at[rank, p], mate_recv.at[rank, p], {"tensor": 1 - core})

    own = pltpu.make_async_copy(x_ref, o_ref.at[pl.ds(first_of(place, core), rows)], local_sem)
    own.start()
    greet_chain(size, True)
    own.wait()
    for p in range(pieces):
        pl.when(place < last)(lambda p=p: going_up(0, p).start())
        pl.when(place > 0)(lambda p=p: going_down(0, p).start())
    for p in range(pieces):
        to_mate(place, p).start()

    def forward(d):
        for p in range(pieces):

            @pl.when(place - d >= 0)
            def _(p=p):
                coming_up(d - 1, p).wait_recv()
                pl.when(place < last)(lambda: going_up(d, p).start())
                to_mate(place - d, p).start()

            @pl.when(place + d <= last)
            def _(p=p):
                coming_down(d - 1, p).wait_recv()
                pl.when(place > 0)(lambda: going_down(d, p).start())
                to_mate(place + d, p).start()

    for load in loads:
        load.wait()
    short = jnp.minimum(place, last - place)

    def distance(s):
        return jnp.where(s <= 2 * short, (s + 1) // 2, s - short)

    def extra_load(rank, which, slot, e):
        return pltpu.make_async_copy(
            extra_from[e].at[pl.ds(first_of(rank, which), rows)], extra.at[slot, e], extra_sem.at[slot, e]
        )

    def store(rank, which, slot, m):
        return pltpu.make_async_copy(
            stage.at[slot, m], made_to[m].at[pl.ds(first_of(rank, which), rows)], stage_sem.at[slot, m]
        )

    def visit(s, carry):
        d = distance(s)
        below = jnp.where(s <= 2 * short, s % 2 == 1, place > last - place)
        rank = jnp.where(below, place - d, place + d)
        for slot, which in enumerate((core, 1 - core)):
            for e in range(n_extra):
                extra_load(rank, which, slot, e).start()
        pl.when((s > 0) & (d != distance(s - 1)))(lambda: forward(d))
        for slot, which in enumerate((core, 1 - core)):
            if slot == 1:
                for p in range(pieces):
                    from_mate(rank, p).wait_recv()
            for e in range(n_extra):
                extra_load(rank, which, slot, e).wait()

            @pl.when(s > 0)
            def _():
                for m in range(n_made):
                    store(rank, which, slot, m).wait()

            work(o_ref.at[pl.ds(first_of(rank, which), rows)], weights, extra.at[slot], stage.at[slot])
            for m in range(n_made):
                store(rank, which, slot, m).start()
        return carry

    lax.fori_loop(0, size, visit, 0)
    for slot, which in enumerate((core, 1 - core)):
        for m in range(n_made):
            store(place, which, slot, m).wait()
    for p in range(pieces):
        for k in range(last):
            pl.when((place < last) & (place - k >= 0))(lambda k=k, p=p: going_up(k, p).wait_send())
            pl.when((place > 0) & (place + k <= last))(lambda k=k, p=p: going_down(k, p).wait_send())
        for rank in range(size):
            to_mate(rank, p).wait_send()


def gather_apply(x, weights, extra, work, n_made, ident):
    size = lax.axis_size("ctx")
    rows, width = x.shape[0], weights[0].shape[1]
    total = 2 * size * rows
    pieces = pieces_of(*x.shape)
    dma = pltpu.SemaphoreType.DMA
    made = jax.ShapeDtypeStruct((total, width), jnp.bfloat16)
    slots = max(1, len(extra))
    return pl.pallas_call(
        functools.partial(gather_apply_kernel, size, pieces, work, len(weights), len(extra), n_made),
        in_specs=[IN_VMEM] + [ANY] * (len(weights) + len(extra)),
        out_specs=[IN_VMEM] + [ANY] * n_made,
        out_shape=[jax.ShapeDtypeStruct((total, x.shape[1]), x.dtype)] + [made] * n_made,
        scratch_shapes=[pltpu.VMEM(w.shape, w.dtype) for w in weights]
        + [
            pltpu.VMEM((2, slots, rows, width) if extra else (2, 1, 16, 128), jnp.bfloat16),
            pltpu.VMEM((2, n_made, rows, width), jnp.bfloat16),
            dma,
            dma((len(weights),)),
            dma((2, slots)),
            dma((2, n_made)),
        ]
        + [dma((size, pieces))] * 6,
        compiler_params=pltpu.CompilerParams(collective_id=ident, has_side_effects=True, vmem_limit_bytes=60000000),
        cost_estimate=pl.CostEstimate(flops=0, bytes_accessed=200000000, transcendentals=0),
    )(x, *weights, *extra)


def sum_apply_kernel(size, pieces, count, *refs):
    acts_from, refs = refs[:count], refs[count:]
    weights_from, refs = refs[:count], refs[count:]
    o_ref, acts, weights, mine, sent, mate, came, load_sem = refs[:8]
    mate_send, mate_recv, up_send, up_recv, down_send, down_recv = refs[8:]
    place, core = lax.axis_index("ctx"), lax.axis_index("tensor")
    rows, depth = o_ref.shape
    part = rows // pieces
    last = size - 1

    loads = []
    for a in range(count):
        loads.append(pltpu.make_async_copy(weights_from[a], weights.at[a], load_sem.at[a]))
        loads.append(pltpu.make_async_copy(acts_from[a], acts.at[a], load_sem.at[count + a]))
    for load in loads:
        load.start()
    greet_chain(size, True)
    for load in loads:
        load.wait()

    def at(ref, d, p):
        return ref.at[d, pl.ds(p * part, part)]

    def to_mate(i, d, p):
        slot = lax.rem(i, 2)
        return remote(at(sent, slot, p), at(mate, d, p), mate_send.at[slot, p], mate_recv.at[d, p], {"tensor": 1 - core})

    def going_up(d, p):
        return remote(at(mine, d, p), at(came, d, p), up_send.at[d, p], up_recv.at[d, p], {"ctx": place + 1})

    def going_down(d, p):
        there = jnp.where(d == place - 1, size, d)
        return remote(at(mine, d, p), at(came, there, p), down_send.at[d, p], down_recv.at[d, p], {"ctx": place - 1})

    def coming_up(d, p):
        there = at(came, d, p)
        return remote(there, there, up_send.at[d, p], up_recv.at[d, p], {"ctx": place - 1})

    def coming_down(d, p):
        there = at(came, jnp.where(d == place, size, d), p)
        return remote(there, there, down_send.at[d, p], down_recv.at[d, p], {"ctx": place + 1})

    def compute(d, which, target):
        step = column_step(depth)
        span = pl.ds(pl.multiple_of((d * 2 + which) * rows, rows), rows)

        def some(j, carry):
            columns = pl.ds(pl.multiple_of(j * step, step), step)
            total = matmul_nt(acts[0, span, :], weights[0, columns, :])
            for a in range(1, count):
                total += matmul_nt(acts[a, span, :], weights[a, columns, :])
            target[:, columns] = total.astype(target.dtype)
            return carry

        lax.fori_loop(0, depth // step, some, 0)

    def with_mate(d, p):
        to_mate(0, d, p).wait_recv()
        return [at(mine, d, p), at(mate, d, p)]

    short = jnp.minimum(place, last - place)

    def first_part(i, carry):
        s = last - i
        near = s <= 2 * short
        d = jnp.where(near, (s + 1) // 2, s - short)
        d = jnp.where(jnp.where(near, s % 2 == 1, place > last - place), place - d, place + d)
        for p in range(pieces):
            pl.when(i >= 2)(lambda p=p: to_mate(i, d, p).wait_send())
        compute(d, 1 - core, sent.at[lax.rem(i, 2)])
        for p in range(pieces):
            to_mate(i, d, p).start()
        compute(d, core, mine.at[d])

        @pl.when((place == 0) & (d > 0))
        def _():
            for p in range(pieces):
                add_blocks(at(mine, d, p), with_mate(d, p))
                going_up(d, p).start()

        @pl.when((place == last) & (d < last))
        def _():
            for p in range(pieces):
                add_blocks(at(mine, d, p), with_mate(d, p))
                going_down(d, p).start()

        return carry

    lax.fori_loop(0, size, first_part, 0)

    def second_part(s, carry):
        k, p = s // pieces, s % pieces

        @pl.when((place > 0) & (place < last - k))
        def _():
            d = last - k
            parts = with_mate(d, p)
            coming_up(d, p).wait_recv()
            add_blocks(at(mine, d, p), parts + [at(came, d, p)])
            going_up(d, p).start()

        @pl.when((place < last) & (place > k))
        def _():
            parts = with_mate(k, p)
            coming_down(k, p).wait_recv()
            add_blocks(at(mine, k, p), parts + [at(came, k, p)])
            going_down(k, p).start()

        return carry

    lax.fori_loop(0, last * pieces, second_part, 0)

    def final(p, carry):
        target = o_ref.at[pl.ds(pl.multiple_of(p * part, part), part)]
        parts = with_mate(place, p)
        pl.when(place > 0)(lambda: coming_up(place, p).wait_recv())
        pl.when(place < last)(lambda: coming_down(place, p).wait_recv())
        up, down = at(came, place, p), at(came, size, p)
        pl.when(place == 0)(lambda: add_blocks(target, parts + [down]))
        pl.when(place == last)(lambda: add_blocks(target, parts + [up]))
        pl.when((place > 0) & (place < last))(lambda: add_blocks(target, parts + [up, down]))
        return carry

    lax.fori_loop(0, pieces, final, 0)
    for p in range(pieces):
        for i in range(size - 2, size):
            to_mate(i, 0, p).wait_send()
        for d in range(size):
            pl.when(place < d)(lambda d=d, p=p: going_up(d, p).wait_send())
            pl.when(place > d)(lambda d=d, p=p: going_down(d, p).wait_send())


def sum_apply(acts, weights, ident):
    size, count = lax.axis_size("ctx"), len(acts)
    total, width = acts[0].shape
    depth = weights[0].shape[0]
    block = total // (2 * size)
    pieces = pieces_of(block, depth)
    dma = pltpu.SemaphoreType.DMA

    def slots(n):
        return pltpu.VMEM((n, block, depth), jnp.bfloat16)

    scratch = [
        pltpu.VMEM((count, total, width), jnp.bfloat16),
        pltpu.VMEM((count, depth, width), jnp.bfloat16),
        slots(size),
        slots(2),
        slots(size),
        slots(size + 1),
        dma((2 * count,)),
        dma((2, pieces)),
    ] + [dma((size, pieces))] * 5
    return pl.pallas_call(
        functools.partial(sum_apply_kernel, size, pieces, count),
        in_specs=[ANY] * (2 * count),
        out_specs=IN_VMEM,
        out_shape=jax.ShapeDtypeStruct((block, depth), jnp.float32),
        scratch_shapes=scratch,
        compiler_params=pltpu.CompilerParams(collective_id=ident, has_side_effects=True, vmem_limit_bytes=60000000),
        cost_estimate=pl.CostEstimate(flops=0, bytes_accessed=200000000, transcendentals=0),
    )(*acts, *weights)


def assemble_kernel(size, ranks_ref, *refs):
    parts, (down_ref, gate_ref, up_ref, whole) = refs[:size], refs[size:]
    width = parts[0].shape[2]
    for which, target in enumerate((down_ref, gate_ref, up_ref)):
        for part, k in zip(parts, range(size)):
            whole[:, pl.ds(pl.multiple_of(ranks_ref[k] * width, 128), width)] = part[which].astype(jnp.float32)
        kept = whole[:, : gate_ref.shape[1]]
        target[...] = kept.T if which == 0 else kept


def assemble(received, columns):
    ranks = jnp.stack([rank for rank, _ in received]).astype(jnp.int32)
    blocks = [block for _, block in received]
    _, rows, width = blocks[0].shape
    f32 = jnp.float32
    return pl.pallas_call(
        functools.partial(assemble_kernel, len(blocks)),
        in_specs=[pl.BlockSpec(memory_space=pltpu.SMEM)] + [IN_VMEM] * len(blocks),
        out_specs=[IN_VMEM] * 3,
        out_shape=[jax.ShapeDtypeStruct((columns, rows), f32)] + [jax.ShapeDtypeStruct((rows, columns), f32)] * 2,
        scratch_shapes=[pltpu.VMEM((rows, len(blocks) * width), f32)],
        compiler_params=pltpu.CompilerParams(vmem_limit_bytes=60000000),
        cost_estimate=pl.CostEstimate(flops=0, bytes_accessed=20 * rows * columns, transcendentals=0),
        name="assemble",
    )(ranks, *blocks)


def mask_into(bias_ref, first, seg_ref, place_ref):
    keys, rows = bias_ref.shape
    key_index = lax.broadcasted_iota(jnp.int32, (keys, rows), 0)
    row_index = lax.broadcasted_iota(jnp.int32, (keys, rows), 1) + first
    place = jnp.broadcast_to(place_ref[...], (keys, rows))
    start = jnp.broadcast_to(seg_ref[...], (keys, rows))
    allowed = ((place >= start) & (place <= row_index)) | (key_index == row_index)
    bias_ref[...] = jnp.where(allowed, 0.0, VERY_LOW)


def attend_kernel(scale, first_ref, seg_ref, place_ref, q_ref, k_ref, vt_ref, o_ref, lse_ref, bias_ref):
    @pl.when(pl.program_id(1) == 0)
    def _():
        mask_into(bias_ref, first_ref[0] + pl.program_id(0) * q_ref.shape[0], seg_ref, place_ref)

    scores = matmul_nt(k_ref[...], q_ref[...]) * scale + bias_ref[...]
    top = jnp.max(scores, axis=0, keepdims=True)
    powers = jnp.exp(scores - top)
    total = jnp.sum(powers, axis=0, keepdims=True)
    mixture = nn(vt_ref[...], powers.astype(jnp.bfloat16)) / total
    o_ref[...] = mixture.T.astype(jnp.bfloat16)
    lse_ref[0] = top + jnp.log(total)


def attend_back_kernel(
    scale, first_ref, seg_ref, place_ref, q_ref, do_ref, lse_ref, k_ref, v_ref, kt_ref,
    dq_ref, dkv_ref, bias_ref, dk_ref, dv_ref,
):
    block, head = pl.program_id(0), pl.program_id(1)

    @pl.when(head == 0)
    def _():
        mask_into(bias_ref, first_ref[0] + block * q_ref.shape[0], seg_ref, place_ref)

    @pl.when((head == 0) & (block == 0))
    def _():
        dk_ref[...] = jnp.zeros_like(dk_ref)
        dv_ref[...] = jnp.zeros_like(dv_ref)

    query, grad = q_ref[...], do_ref[...]
    scores = matmul_nt(k_ref[...], query) * scale + bias_ref[...]
    probs = jnp.exp(scores - lse_ref[0])
    grad_probs = matmul_nt(v_ref[...], grad)
    delta = jnp.sum(probs * grad_probs, axis=0, keepdims=True)
    grad_scores = (probs * (grad_probs - delta)).astype(jnp.bfloat16)
    dv_ref[...] += nn(probs.astype(jnp.bfloat16), grad)
    dk_ref[...] += nn(grad_scores, query)
    dq_ref[...] = (nn(kt_ref[...], grad_scores) * scale).T

    @pl.when((head == pl.num_programs(1) - 1) & (block == pl.num_programs(0) - 1))
    def _():
        dkv_ref[:, :HEAD] = (dk_ref[...] * scale).astype(jnp.bfloat16)
        dkv_ref[:, HEAD:] = dv_ref[...].astype(jnp.bfloat16)


def attention_calls(rows, keys, heads):
    block = math.gcd(256, rows)
    scale = 1.0 / math.sqrt(HEAD)
    smem = pl.BlockSpec(memory_space=pltpu.SMEM)
    seg = pl.BlockSpec((1, block), lambda i, h: (0, i))
    place = pl.BlockSpec((keys, 1), lambda i, h: (0, 0))
    head = pl.BlockSpec((block, HEAD), lambda i, h: (i, h))
    lse = pl.BlockSpec((1, 1, block), lambda i, h: (h, 0, i))
    tall = pl.BlockSpec((keys, HEAD), lambda i, h: (0, 0))
    wide = pl.BlockSpec((HEAD, keys), lambda i, h: (0, 0))
    params = pltpu.CompilerParams(vmem_limit_bytes=60000000)
    grid = (rows // block, heads)
    size = heads * rows * keys
    forward = pl.pallas_call(
        functools.partial(attend_kernel, scale),
        grid=grid,
        in_specs=[smem, seg, place, head, tall, wide],
        out_specs=[head, lse],
        out_shape=[
            jax.ShapeDtypeStruct((rows, heads * HEAD), jnp.bfloat16),
            jax.ShapeDtypeStruct((heads, 1, rows), jnp.float32),
        ],
        scratch_shapes=[pltpu.VMEM((keys, block), jnp.float32)],
        compiler_params=params,
        cost_estimate=pl.CostEstimate(flops=4 * size * HEAD, bytes_accessed=4 * rows * heads * HEAD, transcendentals=size),
        name="attend",
    )
    backward = pl.pallas_call(
        functools.partial(attend_back_kernel, scale),
        grid=grid,
        in_specs=[smem, seg, place, head, head, lse, tall, tall, wide],
        out_specs=[head, pl.BlockSpec((keys, 2 * HEAD), lambda i, h: (0, 0))],
        out_shape=[
            jax.ShapeDtypeStruct((rows, heads * HEAD), jnp.float32),
            jax.ShapeDtypeStruct((keys, 2 * HEAD), jnp.bfloat16),
        ],
        scratch_shapes=[
            pltpu.VMEM((keys, block), jnp.float32),
            pltpu.VMEM((keys, HEAD), jnp.float32),
            pltpu.VMEM((keys, HEAD), jnp.float32),
        ],
        compiler_params=params,
        cost_estimate=pl.CostEstimate(flops=10 * size * HEAD, bytes_accessed=8 * rows * heads * HEAD, transcendentals=size),
        name="attend_back",
    )
    return forward, backward


def per_device(
    layer_input,
    teacher,
    cotangent,
    segment_ids,
    positions,
    valid_mask,
    gain_attn,
    query_weight,
    query_bias,
    key_weight,
    key_bias,
    value_weight,
    value_bias,
    out_weight,
    gain_mlp,
    gate_weight,
    up_weight,
    down_weight,
):
    tensor_rank = lax.axis_index("tensor")
    ctx_rank = lax.axis_index("ctx")
    tensor_size, ctx_size = lax.axis_size("tensor"), lax.axis_size("ctx")
    own_rows = layer_input.shape[0]
    shard_rows = own_rows * tensor_size
    seq_len = segment_ids.shape[0]
    q_width = query_weight.shape[1]
    kv_width = key_weight.shape[1]
    kv_local = kv_width // HEAD
    group = q_width // kv_width
    hidden_width = gate_weight.shape[1]
    slice_width = -(-hidden_width // (128 * ctx_size)) * 128
    first_row = ctx_rank * shard_rows
    own_first = first_row + tensor_rank * own_rows

    inputs = layer_input.astype(jnp.float32)
    gain_one = gain_attn.astype(jnp.float32)
    gain_two = gain_mlp.astype(jnp.float32)
    scale_attn = lax.rsqrt(jnp.mean(inputs * inputs, axis=1, keepdims=True) + EPS)
    normed_attn = inputs * scale_attn
    extra = ((0, 0), (0, ctx_size * slice_width - hidden_width))
    full_qkv, full_out, *slices = front(
        jnp.concatenate([query_weight, key_weight, value_weight], axis=1),
        out_weight.T,
        [jnp.pad(w, extra) for w in (gate_weight, up_weight, down_weight.T)],
        slice_width,
        1,
    )
    full_gate, full_up, full_down = [lax.all_gather(w, "dp", axis=0, tiled=True) for w in slices]
    normed_rows = gather((normed_attn * gain_one).astype(jnp.bfloat16), 1, True, 2)
    valid_count = jnp.sum(valid_mask.astype(jnp.float32))
    counts = [valid_count]
    dp_size = lax.axis_size("dp")
    for step in range(1, dp_size):
        counts.append(
            lax.ppermute(
                jnp.full((8, 128), valid_count), "dp", [(i, (i + step) % dp_size) for i in range(dp_size)]
            )[0, 0]
        )
    valid_count = sum(counts)

    bias = jnp.concatenate(
        [
            lax.dynamic_slice_in_dim(query_bias, tensor_rank * q_width, q_width),
            lax.dynamic_slice_in_dim(key_bias, tensor_rank * kv_width, kv_width),
            lax.dynamic_slice_in_dim(value_bias, tensor_rank * kv_width, kv_width),
        ]
    ).astype(jnp.float32)
    places = lax.dynamic_slice_in_dim(positions, first_row, shard_rows)
    cosine, sine_table = rope_tables(places)
    qkv_pre = matmul(normed_rows, full_qkv) + bias
    turned = q_width + kv_width
    rotated = (
        rotate(qkv_pre[:, :turned].reshape(shard_rows, turned // HEAD, HEAD), cosine, sine_table)
        .astype(jnp.bfloat16)
        .reshape(shard_rows, turned)
    )
    queries = rotated[:, :q_width]
    own_kv = jnp.concatenate([rotated[:, q_width:], qkv_pre[:, turned:].astype(jnp.bfloat16)], axis=1)
    all_kv = gather(own_kv, ctx_size, False, 3)

    key_index = jnp.arange(seq_len, dtype=jnp.int32)
    key_place = jnp.where(valid_mask > 0, key_index, -1)[:, None]
    seq_first = lax.axis_index("dp") * seq_len
    doc_start = (lax.dynamic_slice_in_dim(segment_ids, first_row, shard_rows) - seq_first)[None, :]
    first = jnp.reshape(first_row, (1,)).astype(jnp.int32)
    forward, backward = attention_calls(shard_rows, seq_len, group)
    kept = []
    for c in range(kv_local):
        key = all_kv[:, c * HEAD : (c + 1) * HEAD]
        value = all_kv[:, kv_width + c * HEAD : kv_width + (c + 1) * HEAD]
        query = queries[:, c * group * HEAD : (c + 1) * group * HEAD]
        kept.append((query, key, value) + tuple(forward(first, doc_start, key_place, query, key, value.T)))
    heads_out = jnp.concatenate([k[3] for k in kept], axis=1)
    attention = scatter(matmul_nt(heads_out, full_out), 1, True, 4)
    residual_mid = inputs + attention
    scale_mlp = lax.rsqrt(jnp.mean(residual_mid * residual_mid, axis=1, keepdims=True) + EPS)
    normed_mlp = residual_mid * scale_mlp
    mlp_rows, gate_act, up_act, hidden = gather_apply(
        (normed_mlp * gain_two).astype(jnp.bfloat16), [full_gate, full_up], [], expand_block, 3, 5
    )
    branch = sum_apply([hidden], [full_down], 6)
    layer_result = residual_mid + branch
    valid_own = lax.dynamic_slice_in_dim(valid_mask, own_first, own_rows).astype(jnp.float32)
    difference = layer_result - teacher.astype(jnp.float32)
    squared_sum = jnp.sum(valid_own[:, None] * difference * difference)
    grad_result = cotangent.astype(jnp.float32) + 2.0 * valid_own[:, None] * difference / (
        valid_count * D
    )
    grad_branch, grad_gate_act, grad_up_act = gather_apply(
        grad_result.astype(jnp.bfloat16), [full_down], [gate_act, up_act], shrink_block, 2, 9
    )
    summed = []
    for left, right in ((grad_branch, hidden), (mlp_rows, grad_gate_act), (mlp_rows, grad_up_act)):
        grad = matmul_tn(left, right).astype(jnp.bfloat16)
        grad_gate_act, grad_up_act, grad = lax.optimization_barrier((grad_gate_act, grad_up_act, grad))
        summed.append(lax.psum_scatter(grad, "dp", scatter_dimension=0, tiled=True))
    grad_mlp_rows = sum_apply([grad_gate_act, grad_up_act], [full_gate, full_up], 10)
    grad_gain_mlp = jnp.sum(grad_mlp_rows * normed_mlp, axis=0)
    grad_mid = grad_result + norm_back(grad_mlp_rows, normed_mlp, scale_mlp, gain_two)
    grad_attn_rows = gather(grad_mid.astype(jnp.bfloat16), 1, True, 2)
    grad_heads = matmul(grad_attn_rows, full_out).astype(jnp.bfloat16)
    grad_out = matmul_tn(grad_attn_rows, heads_out).astype(jnp.bfloat16)

    grad_out = lax.psum_scatter(grad_out, "dp", scatter_dimension=0, tiled=True)
    query_grads, key_grads, value_grads = [], [], []
    for c in range(kv_local):
        query, key, value, _, log_total = kept[c]
        span = slice(c * group * HEAD, (c + 1) * group * HEAD)
        grad_query, grad_kv = backward(
            first, doc_start, key_place, query, grad_heads[:, span], log_total, key, value, key.T
        )
        query_grads.append(grad_query)
        key_grads.append(grad_kv[:, :HEAD])
        value_grads.append(grad_kv[:, HEAD:])
    grad_kv = grad_kv if kv_local == 1 else jnp.concatenate(key_grads + value_grads, axis=1)
    grad_kv = scatter(grad_kv, ctx_size, False, 7)
    grad_kv, *summed = lax.optimization_barrier((grad_kv, *summed))
    shard_down, shard_gate, shard_up = to_rows(summed, hidden_width)
    grad_turned = jnp.concatenate(query_grads + [grad_kv[:, :kv_width]], axis=1)
    grad_pre = jnp.concatenate(
        [
            rotate(grad_turned.reshape(shard_rows, turned // HEAD, HEAD), cosine, -sine_table)
            .reshape(shard_rows, turned)
            .astype(jnp.bfloat16),
            grad_kv[:, kv_width:].astype(jnp.bfloat16),
        ],
        axis=1,
    )
    grad_pre, grad_out = lax.optimization_barrier((grad_pre, grad_out))
    shard_out = lax.psum_scatter(grad_out, "ctx", scatter_dimension=0, tiled=True)
    shard_out = shard_out.astype(jnp.float32).T
    grad_normed = scatter(matmul_nt(grad_pre, full_qkv), 1, True, 4)
    grad_gain_attn = jnp.sum(grad_normed * normed_attn, axis=0)
    grad_input = grad_mid + norm_back(grad_normed, normed_attn, scale_attn, gain_one)
    bias_sum = jnp.sum(grad_pre.astype(jnp.float32), axis=0)

    def spread(part, size):
        return lax.dynamic_update_slice_in_dim(
            jnp.zeros((size,), jnp.float32), part, tensor_rank * part.shape[0], 0
        )

    loss_part = jnp.zeros((128,), jnp.float32).at[0].set(squared_sum)
    parts = [
        grad_gain_attn,
        grad_gain_mlp,
        spread(bias_sum[:q_width], query_bias.shape[0]),
        spread(bias_sum[q_width:turned], key_bias.shape[0]),
        spread(bias_sum[turned:], value_bias.shape[0]),
        loss_part,
    ]
    flat = jnp.concatenate(parts)
    small = jnp.pad(flat, (0, -flat.shape[0] % 1024)).reshape(-1, 128)
    grad_qkv = matmul_tn(normed_rows, grad_pre).astype(jnp.bfloat16)
    shard_qkv, sums = back(grad_qkv, small, 8)
    sums = sums.reshape(-1)
    pieces, offset = [], 0
    for part in parts:
        pieces.append(sums[offset : offset + part.shape[0]])
        offset += part.shape[0]
    return (
        layer_result.astype(jnp.bfloat16),
        pieces[5][0] / (valid_count * D),
        grad_input,
        pieces[0],
        shard_qkv[:, :q_width],
        pieces[2],
        shard_qkv[:, q_width:turned],
        pieces[3],
        shard_qkv[:, turned:],
        pieces[4],
        shard_out,
        pieces[1],
        shard_gate,
        shard_up,
        shard_down,
    )


def solution(mesh):
    in_specs = (
        P(("dp", "ctx", "tensor"), None),
        P(("dp", "ctx", "tensor"), None),
        P(("dp", "ctx", "tensor"), None),
        P("dp"),
        P("dp"),
        P("dp"),
        P(),
        P(("dp", "ctx"), "tensor"),
        P(),
        P(("dp", "ctx"), "tensor"),
        P(),
        P(("dp", "ctx"), "tensor"),
        P(),
        P("tensor", ("dp", "ctx")),
        P(),
        P(("dp", "ctx"), "tensor"),
        P(("dp", "ctx"), "tensor"),
        P("tensor", ("dp", "ctx")),
    )
    out_specs = (
        P(("dp", "ctx", "tensor"), None),
        P(),
        P(("dp", "ctx", "tensor"), None),
        P(),
        P(("dp", "ctx"), "tensor"),
        P(),
        P(("dp", "ctx"), "tensor"),
        P(),
        P(("dp", "ctx"), "tensor"),
        P(),
        P("tensor", ("dp", "ctx")),
        P(),
        P(("dp", "ctx"), "tensor"),
        P(("dp", "ctx"), "tensor"),
        P("tensor", ("dp", "ctx")),
    )

    return jax.shard_map(per_device, mesh=mesh, in_specs=in_specs, out_specs=out_specs, check_vma=False)
```

```python
import functools
import math

import jax
import jax.numpy as jnp
from jax import lax
from jax.experimental import pallas as pl
from jax.experimental.pallas import tpu as pltpu
from jax.sharding import PartitionSpec as P


D = 1536
HEAD = 128


EPS = 1e-06
THETA = 10000.0
VERY_LOW = -1e30


def rope_tables(places):
    half_dim = HEAD // 2
    frequency = THETA ** (-(jnp.arange(half_dim, dtype=jnp.float32) * 2.0 / HEAD))
    angles = places.astype(jnp.float32)[:, None] * frequency[None, :]
    return (jnp.cos(angles), jnp.sin(angles))


def rotate(stacked, cosine, sine_table):
    half_dim = HEAD // 2
    first_half = stacked[..., :half_dim]
    second_half = stacked[..., half_dim:]
    cosine = cosine[:, None, :]
    sine_table = sine_table[:, None, :]
    return jnp.concatenate(
        [
            first_half * cosine - second_half * sine_table,
            second_half * cosine + first_half * sine_table,
        ],
        axis=-1,
    )


def matmul(first_op, second_op):
    return jnp.dot(first_op, second_op, preferred_element_type=jnp.float32)


def matmul_tn(first_op, second_op):
    return lax.dot_general(
        first_op, second_op, (((0,), (0,)), ((), ())), preferred_element_type=jnp.float32
    )


def matmul_nt(first_op, second_op):
    return lax.dot_general(
        first_op, second_op, (((1,), (1,)), ((), ())), preferred_element_type=jnp.float32
    )


def norm_back(grad_normed, normed, inverse, gain):
    scaled = grad_normed * gain
    return inverse * (scaled - normed * jnp.mean(scaled * normed, axis=1, keepdims=True))


def exchange(blocks, axis):
    size = lax.axis_size(axis)
    rank = lax.axis_index(axis)
    received = [(rank, lax.dynamic_index_in_dim(blocks, rank, 0, keepdims=False))]
    for step in range(1, size):
        going = lax.dynamic_index_in_dim(blocks, (rank + step) % size, 0, keepdims=False)
        came = lax.ppermute(going, axis, [(i, (i + step) % size) for i in range(size)])
        received.append(((rank - step + size) % size, came))
    return received


def to_rows(summed, columns):
    size = lax.axis_size("ctx")
    rows, width = summed[0].shape[0] // size, summed[0].shape[1]
    blocks = jnp.stack([s.reshape(size, rows, width) for s in summed], axis=1)
    return assemble(exchange(blocks, "ctx"), columns)


def nn(first_op, second_op):
    return jnp.dot(first_op, second_op, preferred_element_type=jnp.float32)


MESH = pl.DeviceIdType.MESH
ANY = pl.BlockSpec(memory_space=pl.ANY)
IN_VMEM = pl.BlockSpec(memory_space=pltpu.VMEM)


def remote(source, target, send_sem, recv_sem, device):
    return pltpu.make_async_remote_copy(
        src_ref=source,
        dst_ref=target,
        send_sem=send_sem,
        recv_sem=recv_sem,
        device_id=device,
        device_id_type=MESH,
    )


def greet(barrier, device):
    pl.semaphore_signal(barrier, inc=1, device_id=device, device_id_type=MESH)


def greet_chain(size, paired):
    place = lax.axis_index("ctx")
    barrier = pltpu.get_barrier_semaphore()
    if size > 1:
        pl.when(place < size - 1)(lambda: greet(barrier, {"ctx": place + 1}))
        pl.when(place > 0)(lambda: greet(barrier, {"ctx": place - 1}))
    if paired:
        greet(barrier, {"tensor": 1 - lax.axis_index("tensor")})
    if size == 1:
        pl.semaphore_wait(barrier, 1)
        return
    ends = (place == 0) | (place == size - 1)
    pl.when(ends)(lambda: pl.semaphore_wait(barrier, 1 + paired))
    pl.when(jnp.logical_not(ends))(lambda: pl.semaphore_wait(barrier, 2 + paired))


def gather_kernel(size, paired, pieces, x_ref, o_ref, local_sem, up_send, up_recv, down_send, down_recv, mate_send, mate_recv):
    place = lax.axis_index("ctx") if size > 1 else 0
    core = lax.axis_index("tensor")
    rows = x_ref.shape[0]
    part = rows // pieces
    greet_chain(size, paired)

    def block(rank, which, p):
        index = rank * 2 + which if paired else rank
        return o_ref.at[pl.ds(pl.multiple_of(index * rows + p * part, part), part)]

    def source(rank, k, p):
        return x_ref.at[pl.ds(p * part, part)] if k == 0 else block(rank, core, p)

    def going_up(k, p):
        return remote(
            source(place - k, k, p), block(place - k, core, p), up_send.at[k, p], up_recv.at[k, p], {"ctx": place + 1}
        )

    def going_down(k, p):
        return remote(
            source(place + k, k, p), block(place + k, core, p), down_send.at[k, p], down_recv.at[k, p], {"ctx": place - 1}
        )

    def to_mate(rank, k, p):
        return remote(
            source(rank, k, p), block(rank, core, p), mate_send.at[k, p], mate_recv.at[rank, p], {"tensor": 1 - core}
        )

    def from_mate(rank, p):
        there = block(rank, 1 - core, p)
        return remote(there, there, mate_send.at[0, p], mate_recv.at[rank, p], {"tensor": 1 - core})

    own = pltpu.make_async_copy(x_ref, o_ref.at[pl.ds(pl.multiple_of((place * 2 + core if paired else place) * rows, rows), rows)], local_sem)
    for p in range(pieces):
        if size > 1:
            pl.when(place < size - 1)(lambda p=p: going_up(0, p).start())
            pl.when(place > 0)(lambda p=p: going_down(0, p).start())
    for p in range(pieces):
        if paired:
            to_mate(place, 0, p).start()
    own.start()
    for k in range(size - 1):
        for p in range(pieces):

            @pl.when(place - 1 - k >= 0)
            def _(k=k, p=p):
                there = block(place - 1 - k, core, p)
                remote(there, there, up_send.at[k, p], up_recv.at[k, p], {"ctx": place - 1}).wait_recv()
                if k + 1 < size - 1:
                    pl.when(place < size - 1)(lambda: going_up(k + 1, p).start())
                if paired:
                    to_mate(place - 1 - k, 1 + k, p).start()

            @pl.when(place + 1 + k <= size - 1)
            def _(k=k, p=p):
                there = block(place + 1 + k, core, p)
                remote(there, there, down_send.at[k, p], down_recv.at[k, p], {"ctx": place + 1}).wait_recv()
                if k + 1 < size - 1:
                    pl.when(place > 0)(lambda: going_down(k + 1, p).start())
                if paired:
                    to_mate(place + 1 + k, size + k, p).start()

    own.wait()
    for p in range(pieces):
        if paired:
            for rank in range(size):
                from_mate(rank, p).wait_recv()
            to_mate(place, 0, p).wait_send()
        for k in range(size - 1):
            pl.when((place < size - 1) & (place - k >= 0))(lambda k=k, p=p: going_up(k, p).wait_send())
            pl.when((place > 0) & (place + k <= size - 1))(lambda k=k, p=p: going_down(k, p).wait_send())
            if paired:
                pl.when(place - 1 - k >= 0)(lambda k=k, p=p: to_mate(place - 1 - k, 1 + k, p).wait_send())
                pl.when(place + 1 + k <= size - 1)(lambda k=k, p=p: to_mate(place + 1 + k, size + k, p).wait_send())


def pieces_of(rows, columns):
    return math.gcd(4, rows // 64) if rows * columns >= 1 << 18 else 1


def gather(x, size, paired, ident):
    copies = size * 2 if paired else size
    wide = max(size, 2)
    pieces = pieces_of(*x.shape)
    dma = pltpu.SemaphoreType.DMA
    return pl.pallas_call(
        functools.partial(gather_kernel, size, paired, pieces),
        in_specs=[IN_VMEM],
        out_specs=ANY,
        out_shape=jax.ShapeDtypeStruct((copies * x.shape[0], x.shape[1]), x.dtype),
        scratch_shapes=[dma] + [dma((wide, pieces))] * 4 + [dma((2 * wide, pieces)), dma((wide, pieces))],
        compiler_params=pltpu.CompilerParams(collective_id=ident, has_side_effects=True),
        cost_estimate=pl.CostEstimate(flops=0, bytes_accessed=30 * copies * x.size, transcendentals=0),
        name="gather",
    )(x)


def add_blocks(target, parts):
    rows = target.shape[0]
    step = math.gcd(rows, 32)

    def some(i, carry):
        span = pl.ds(pl.multiple_of(i * step, step), step)
        total = parts[0][span].astype(jnp.float32)
        for part in parts[1:]:
            total += part[span].astype(jnp.float32)
        target[span] = total.astype(target.dtype)
        return carry

    lax.fori_loop(0, rows // step, some, 0)


def scatter_kernel(
    size, paired, pieces, x_ref, o_ref, mine, mate, above, below, own_sem, mate_send, mate_recv, up_send, up_recv, down_send, down_recv
):
    place = lax.axis_index("ctx") if size > 1 else 0
    core = lax.axis_index("tensor")
    rows = o_ref.shape[0]
    part = rows // pieces
    order = sorted(range(size), key=lambda d: min(d, size - 1 - d))
    every = [(d, p) for d in order for p in range(pieces)]

    def block(rank, which, p):
        index = rank * 2 + which if paired else rank
        return x_ref.at[pl.ds(pl.multiple_of(index * rows + p * part, part), part)]

    def at(ref, d, p):
        return ref.at[d, pl.ds(p * part, part)]

    def load(d, p):
        return pltpu.make_async_copy(block(d, core, p), at(mine, d, p), own_sem.at[d, p])

    def to_mate(d, p):
        return remote(
            block(d, 1 - core, p), at(mate, d, p), mate_send.at[d, p], mate_recv.at[d, p], {"tensor": 1 - core}
        )

    def going_up(d, p):
        return remote(at(mine, d, p), at(below, d, p), up_send.at[d, p], up_recv.at[d, p], {"ctx": place + 1})

    def going_down(d, p):
        return remote(at(mine, d, p), at(above, d, p), down_send.at[d, p], down_recv.at[d, p], {"ctx": place - 1})

    for d, p in every:
        load(d, p).start()
    greet_chain(size, paired)
    if paired:
        for d, p in every:
            to_mate(d, p).start()

    def here(d, p):
        load(d, p).wait()
        if paired:
            to_mate(d, p).wait_recv()
            return [at(mine, d, p), at(mate, d, p)]
        return [at(mine, d, p)]

    for k in range(size - 1):
        for p in range(pieces):

            @pl.when(place < size - 1 - k)
            def _(d=size - 1 - k, p=p):
                parts = here(d, p)

                @pl.when(place > 0)
                def _():
                    going_up(d, p).wait_recv()
                    add_blocks(at(mine, d, p), parts + [at(below, d, p)])

                if paired:
                    pl.when(place == 0)(lambda: add_blocks(at(mine, d, p), parts))
                going_up(d, p).start()

            @pl.when(place > k)
            def _(d=k, p=p):
                parts = here(d, p)

                @pl.when(place < size - 1)
                def _():
                    going_down(d, p).wait_recv()
                    add_blocks(at(mine, d, p), parts + [at(above, d, p)])

                if paired:
                    pl.when(place == size - 1)(lambda: add_blocks(at(mine, d, p), parts))
                going_down(d, p).start()

    for d in range(size):

        @pl.when(place == d)
        def _(d=d):
            for p in range(pieces):
                parts = here(d, p)
                if d > 0:
                    going_up(d, p).wait_recv()
                    parts = parts + [at(below, d, p)]
                if d < size - 1:
                    going_down(d, p).wait_recv()
                    parts = parts + [at(above, d, p)]
                add_blocks(o_ref.at[pl.ds(p * part, part)], parts)

    for d, p in every:
        if d > 0:
            pl.when(place < d)(lambda d=d, p=p: going_up(d, p).wait_send())
        if d < size - 1:
            pl.when(place > d)(lambda d=d, p=p: going_down(d, p).wait_send())
        if paired:
            to_mate(d, p).wait_send()


def scatter(x, size, paired, ident):
    copies = size * 2 if paired else size
    rows = x.shape[0] // copies
    pieces = pieces_of(rows, x.shape[1])
    dma = pltpu.SemaphoreType.DMA
    slots = pltpu.VMEM((size, rows, x.shape[1]), x.dtype)
    one = pltpu.VMEM((1, 32, 128), x.dtype)
    chain = slots if size > 1 else one
    return pl.pallas_call(
        functools.partial(scatter_kernel, size, paired, pieces),
        in_specs=[ANY],
        out_specs=IN_VMEM,
        out_shape=jax.ShapeDtypeStruct((rows, x.shape[1]), jnp.float32),
        scratch_shapes=[slots, slots if paired else one, chain, chain] + [dma((size, pieces))] * 7,
        compiler_params=pltpu.CompilerParams(collective_id=ident, has_side_effects=True, vmem_limit_bytes=60000000),
        cost_estimate=pl.CostEstimate(flops=0, bytes_accessed=30 * x.size, transcendentals=0),
        name="scatter",
    )(x)


def front_kernel(
    size, groups, a_ref, b_ref, g_ref, u_ref, d_ref, fa_ref, fb_ref, og_ref, ou_ref, od_ref,
    local_sem, up_send, up_recv, down_send, down_recv, far_send, far_recv, swap_send, swap_recv,
):
    place, group = lax.axis_index("ctx"), lax.axis_index("dp")
    rows, width = a_ref.shape[0], og_ref.shape[1]
    wholes, owns = (fa_ref, fb_ref), (a_ref, b_ref)
    parts, slices = (g_ref, u_ref, d_ref), (og_ref, ou_ref, od_ref)
    barrier = pltpu.get_barrier_semaphore()
    for step in range(1, size):
        greet(barrier, {"ctx": lax.rem(place + step, size)})
    for step in range(1, groups):
        greet(barrier, {"dp": lax.rem(group + step, groups)})
    pl.semaphore_wait(barrier, size + groups - 2)

    def chunk(which, in_group, rank):
        return wholes[which].at[pl.ds(pl.multiple_of((in_group * size + rank) * rows, rows), rows)]

    def source(which, rank, k):
        return owns[which] if k == 0 else chunk(which, group, rank)

    def going_up(which, k):
        return remote(
            source(which, place - k, k), chunk(which, group, place - k),
            up_send.at[which, k], up_recv.at[which, k], {"ctx": place + 1},
        )

    def going_down(which, k):
        return remote(
            source(which, place + k, k), chunk(which, group, place + k),
            down_send.at[which, k], down_recv.at[which, k], {"ctx": place - 1},
        )

    def across(which, rank, step, k):
        return remote(
            source(which, rank, k), chunk(which, group, rank),
            far_send.at[which, rank, step], far_recv.at[which, rank, step], {"dp": lax.rem(group + step, groups)},
        )

    def from_across(which, rank, step):
        there = chunk(which, lax.rem(group - step + groups, groups), rank)
        return remote(there, there, far_send.at[which, rank, step], far_recv.at[which, rank, step], {"dp": lax.rem(group + step, groups)})

    def columns(which, rank):
        return parts[which].at[:, pl.ds(pl.multiple_of(rank * width, 128), width)]

    def swap(which, step):
        return remote(
            columns(which, lax.rem(place + step, size)),
            slices[which].at[pl.ds(pl.multiple_of(place * rows, rows), rows)],
            swap_send.at[which, step], swap_recv.at[which, step], {"ctx": lax.rem(place + step, size)},
        )

    def swapped(which, step):
        there = slices[which].at[pl.ds(pl.multiple_of(lax.rem(place - step + size, size) * rows, rows), rows)]
        return remote(there, there, swap_send.at[which, step], swap_recv.at[which, step], {"ctx": lax.rem(place + step, size)})

    locals_ = [pltpu.make_async_copy(owns[w], chunk(w, group, place), local_sem.at[w]) for w in range(2)]
    locals_ += [
        pltpu.make_async_copy(
            columns(w, place), slices[w].at[pl.ds(pl.multiple_of(place * rows, rows), rows)], local_sem.at[2 + w]
        )
        for w in range(3)
    ]
    for w in range(2):
        pl.when(place < size - 1)(lambda w=w: going_up(w, 0).start())
        pl.when(place > 0)(lambda w=w: going_down(w, 0).start())
        for step in range(1, groups):
            across(w, place, step, 0).start()
    for copy in locals_:
        copy.start()
    for k in range(size - 1):
        for w in range(2):

            @pl.when(place - 1 - k >= 0)
            def _(k=k, w=w):
                there = chunk(w, group, place - 1 - k)
                remote(there, there, up_send.at[w, k], up_recv.at[w, k], {"ctx": place - 1}).wait_recv()
                if k + 1 < size - 1:
                    pl.when(place < size - 1)(lambda: going_up(w, k + 1).start())
                for step in range(1, groups):
                    across(w, place - 1 - k, step, 1).start()

            @pl.when(place + 1 + k <= size - 1)
            def _(k=k, w=w):
                there = chunk(w, group, place + 1 + k)
                remote(there, there, down_send.at[w, k], down_recv.at[w, k], {"ctx": place + 1}).wait_recv()
                if k + 1 < size - 1:
                    pl.when(place > 0)(lambda: going_down(w, k + 1).start())
                for step in range(1, groups):
                    across(w, place + 1 + k, step, 1).start()

    for w in range(3):
        for step in range(1, size):
            swap(w, step).start()
    for rank in range(size):
        for w in range(2):
            for step in range(1, groups):
                from_across(w, rank, step).wait_recv()
    for w in range(3):
        for step in range(1, size):
            swapped(w, step).wait_recv()
    for copy in locals_:
        copy.wait()
    for w in range(2):
        for k in range(size - 1):
            pl.when((place < size - 1) & (place - k >= 0))(lambda k=k, w=w: going_up(w, k).wait_send())
            pl.when((place > 0) & (place + k <= size - 1))(lambda k=k, w=w: going_down(w, k).wait_send())
        for rank in range(size):
            for step in range(1, groups):
                across(w, rank, step, 1).wait_send()
    for w in range(3):
        for step in range(1, size):
            swap(w, step).wait_send()


def front(a, b, parts, width, ident):
    size, groups = lax.axis_size("ctx"), lax.axis_size("dp")
    rows = a.shape[0]
    dma = pltpu.SemaphoreType.DMA
    slices = jax.ShapeDtypeStruct((size * rows, width), a.dtype)
    return pl.pallas_call(
        functools.partial(front_kernel, size, groups),
        in_specs=[IN_VMEM] * 5,
        out_specs=[ANY] * 5,
        out_shape=[jax.ShapeDtypeStruct((groups * size * rows, x.shape[1]), x.dtype) for x in (a, b)] + [slices] * 3,
        scratch_shapes=[dma((5,))] + [dma((2, size))] * 4 + [dma((2, size, groups))] * 2 + [dma((3, size))] * 2,
        compiler_params=pltpu.CompilerParams(collective_id=ident, has_side_effects=True),
        cost_estimate=pl.CostEstimate(flops=0, bytes_accessed=200000000, transcendentals=0),
        name="front",
    )(a, b, *parts)


def back_kernel(
    size, groups, x_ref, s_ref, p_ref, w_ref, n_ref, o_ref, t_ref, g_ref, mine, far, near, part, pair, crowd, row, give, got,
    give_sems, own_sem, far_send, far_recv, near_send, near_recv, pair_sems, crowd_send, crowd_recv, row_send, row_recv,
):
    place, group = lax.axis_index("ctx"), lax.axis_index("dp")
    core = lax.axis_index("tensor")
    rows = o_ref.shape[0]
    barrier = pltpu.get_barrier_semaphore()

    def rank_at(k):
        return lax.rem(place + 1 + k, size)

    def block(in_group, rank):
        return x_ref.at[pl.ds(pl.multiple_of((in_group * size + rank) * rows, rows), rows)]

    def load(k):
        return pltpu.make_async_copy(block(group, rank_at(k)), mine.at[k], own_sem.at[k])

    def across(k, step):
        to = lax.rem(group + step, groups)
        return remote(block(to, rank_at(k)), far.at[k, step], far_send.at[k, step], far_recv.at[k, step], {"dp": to})

    def along(k):
        return remote(mine.at[k], near.at[k], near_send.at[k], near_recv.at[k], {"ctx": rank_at(k)})

    to_mate = remote(part, pair, pair_sems.at[0], pair_sems.at[1], {"tensor": 1 - core})
    half = remote(give, got, give_sems.at[0], give_sems.at[1], {"tensor": 1 - core})

    def product(which, target):
        own_rows, depth = target.shape
        step = column_step(depth)
        span = pl.ds(pl.multiple_of(which * own_rows, own_rows), own_rows)

        def some(j, carry):
            columns = pl.ds(pl.multiple_of(j * step, step), step)
            target[:, columns] = matmul_nt(p_ref[span, :], w_ref[columns, :])
            return carry

        lax.fori_loop(0, depth // step, some, 0)

    def gain_sums(i, total):
        span = pl.ds(pl.multiple_of(i * 32, 32), 32)
        grad = g_ref[span, :] + got[span, :]
        g_ref[span, :] = grad
        return total + jnp.sum(grad * n_ref[span, :], axis=0, keepdims=True)

    def to_crowd(step):
        return remote(
            crowd.at[group], crowd.at[group], crowd_send.at[step], crowd_recv.at[step],
            {"dp": lax.rem(group + step, groups)},
        )

    def to_row(step):
        return remote(
            row.at[place], row.at[place], row_send.at[step], row_recv.at[step], {"ctx": lax.rem(place + step, size)}
        )

    for k in range(size):
        load(k).start()
    for step in range(1, size):
        greet(barrier, {"ctx": lax.rem(place + step, size)})
    for step in range(1, groups):
        greet(barrier, {"dp": lax.rem(group + step, groups)})
    greet(barrier, {"tensor": 1 - core})
    pl.semaphore_wait(barrier, size + groups - 1)
    for k in range(size):
        for step in range(1, groups):
            across(k, step).start()
    product(1 - core, give)
    half.start()
    product(core, g_ref)
    part[...] = s_ref[...]
    half.wait_recv()
    gains = lax.fori_loop(0, g_ref.shape[0] // 32, gain_sums, jnp.zeros((1, g_ref.shape[1]), jnp.float32))
    for j in range(g_ref.shape[1] // 128):
        part[j : j + 1, :] = gains[:, j * 128 : (j + 1) * 128]
    to_mate.start()
    to_mate.wait_recv()
    crowd[group] = part[...] + pair[...]
    for step in range(1, groups):
        to_crowd(step).start()
    for step in range(1, groups):
        to_crowd(step).wait_recv()
    total = crowd[0]
    for g in range(1, groups):
        total += crowd[g]
    row[place] = total
    for step in range(1, size):
        to_row(step).start()
    for k in range(size):
        load(k).wait()
        for step in range(1, groups):
            across(k, step).wait_recv()
        parts = [mine.at[k]] + [far.at[k, step] for step in range(1, groups)]
        if k < size - 1:
            add_blocks(mine.at[k], parts)
            along(k).start()
    for k in range(size - 1):
        along(k).wait_recv()
        parts.append(near.at[k])
    add_blocks(o_ref, parts)
    for step in range(1, size):
        to_row(step).wait_recv()
    total = row[0]
    for c in range(1, size):
        total += row[c]
    t_ref[...] = total
    half.wait_send()
    to_mate.wait_send()
    for step in range(1, groups):
        to_crowd(step).wait_send()
    for step in range(1, size):
        to_row(step).wait_send()
    for k in range(size):
        for step in range(1, groups):
            across(k, step).wait_send()
        if k < size - 1:
            along(k).wait_send()


def back(x, small, grad_pre, weight, normed, ident):
    size, groups = lax.axis_size("ctx"), lax.axis_size("dp")
    rows, columns = x.shape[0] // (size * groups), x.shape[1]
    dma = pltpu.SemaphoreType.DMA
    return pl.pallas_call(
        functools.partial(back_kernel, size, groups),
        in_specs=[ANY] + [IN_VMEM] * 4,
        out_specs=[IN_VMEM] * 3,
        out_shape=[
            jax.ShapeDtypeStruct((rows, columns), jnp.float32),
            jax.ShapeDtypeStruct(small.shape, jnp.float32),
            jax.ShapeDtypeStruct(normed.shape, jnp.float32),
        ],
        scratch_shapes=[
            pltpu.VMEM((size, rows, columns), x.dtype),
            pltpu.VMEM((size, groups, rows, columns), x.dtype),
            pltpu.VMEM((size, rows, columns), x.dtype),
            pltpu.VMEM(small.shape, jnp.float32),
            pltpu.VMEM(small.shape, jnp.float32),
            pltpu.VMEM((groups,) + small.shape, jnp.float32),
            pltpu.VMEM((size,) + small.shape, jnp.float32),
            pltpu.VMEM(normed.shape, jnp.float32),
            pltpu.VMEM(normed.shape, jnp.float32),
            dma((2,)),
            dma((size,)),
            dma((size, groups)),
            dma((size, groups)),
            dma((size,)),
            dma((size,)),
            dma((2,)),
            dma((groups,)),
            dma((groups,)),
            dma((size,)),
            dma((size,)),
        ],
        compiler_params=pltpu.CompilerParams(collective_id=ident, has_side_effects=True, vmem_limit_bytes=60000000),
        cost_estimate=pl.CostEstimate(flops=0, bytes_accessed=100 * x.size, transcendentals=0),
        name="back",
    )(x, small, grad_pre, weight, normed)


def column_step(width):
    return max(t for t in (768, 384, 256, 128) if width % t == 0)


def expand_block(x_ref, weights, extra, stage):
    step = column_step(weights[0].shape[1])

    def some(j, carry):
        span = pl.ds(pl.multiple_of(j * step, step), step)
        gate = nn(x_ref[...], weights[0][:, span])
        up = nn(x_ref[...], weights[1][:, span])
        stage[0, :, span] = gate.astype(jnp.bfloat16)
        stage[1, :, span] = up.astype(jnp.bfloat16)
        stage[2, :, span] = (gate * jax.nn.sigmoid(gate) * up).astype(jnp.bfloat16)
        return carry

    lax.fori_loop(0, weights[0].shape[1] // step, some, 0)


def shrink_block(x_ref, weights, extra, stage):
    step = column_step(weights[0].shape[1])

    def some(j, carry):
        span = pl.ds(pl.multiple_of(j * step, step), step)
        grad = nn(x_ref[...], weights[0][:, span])
        gate = extra[0, :, span].astype(jnp.float32)
        up = extra[1, :, span].astype(jnp.float32)
        sigmoid = jax.nn.sigmoid(gate)
        stage[0, :, span] = (grad * up * sigmoid * (1.0 + gate * (1.0 - sigmoid))).astype(jnp.bfloat16)
        stage[1, :, span] = (grad * gate * sigmoid).astype(jnp.bfloat16)
        return carry

    lax.fori_loop(0, weights[0].shape[1] // step, some, 0)


def gather_apply_kernel(size, pieces, work, n_weights, n_extra, n_made, *refs):
    x_ref, refs = refs[0], refs[1:]
    weights_from, refs = refs[:n_weights], refs[n_weights:]
    extra_from, refs = refs[:n_extra], refs[n_extra:]
    o_ref, refs = refs[0], refs[1:]
    made_to, refs = refs[:n_made], refs[n_made:]
    weights, refs = refs[:n_weights], refs[n_weights:]
    extra, stage, refs = refs[0], refs[1], refs[2:]
    local_sem, weight_sem, extra_sem, stage_sem = refs[:4]
    up_send, up_recv, down_send, down_recv, mate_send, mate_recv = refs[4:]
    place = lax.axis_index("ctx")
    core = lax.axis_index("tensor")
    rows = x_ref.shape[0]
    part = rows // pieces
    last = size - 1

    loads = [pltpu.make_async_copy(weights_from[w], weights[w], weight_sem.at[w]) for w in range(n_weights)]
    for load in loads:
        load.start()

    def first_of(rank, which):
        return pl.multiple_of((rank * 2 + which) * rows, rows)

    def block(rank, which, p):
        return o_ref.at[pl.ds(pl.multiple_of((rank * 2 + which) * rows + p * part, part), part)]

    def going_up(k, p):
        there = block(place - k, core, p)
        return remote(there, there, up_send.at[k, p], up_recv.at[k, p], {"ctx": place + 1})

    def going_down(k, p):
        there = block(place + k, core, p)
        return remote(there, there, down_send.at[k, p], down_recv.at[k, p], {"ctx": place - 1})

    def coming_up(k, p):
        there = block(place - 1 - k, core, p)
        return remote(there, there, up_send.at[k, p], up_recv.at[k, p], {"ctx": place - 1})

    def coming_down(k, p):
        there = block(place + 1 + k, core, p)
        return remote(there, there, down_send.at[k, p], down_recv.at[k, p], {"ctx": place + 1})

    def to_mate(rank, p):
        there = block(rank, core, p)
        return remote(there, there, mate_send.at[rank, p], mate_recv.at[rank, p], {"tensor": 1 - core})

    def from_mate(rank, p):
        there = block(rank, 1 - core, p)
        return remote(there, there, mate_send.at[rank, p], mate_recv.at[rank, p], {"tensor": 1 - core})

    own = pltpu.make_async_copy(x_ref, o_ref.at[pl.ds(first_of(place, core), rows)], local_sem)
    own.start()
    greet_chain(size, True)
    own.wait()
    for p in range(pieces):
        pl.when(place < last)(lambda p=p: going_up(0, p).start())
        pl.when(place > 0)(lambda p=p: going_down(0, p).start())
    for p in range(pieces):
        to_mate(place, p).start()

    def forward(d):
        for p in range(pieces):

            @pl.when(place - d >= 0)
            def _(p=p):
                coming_up(d - 1, p).wait_recv()
                pl.when(place < last)(lambda: going_up(d, p).start())
                to_mate(place - d, p).start()

            @pl.when(place + d <= last)
            def _(p=p):
                coming_down(d - 1, p).wait_recv()
                pl.when(place > 0)(lambda: going_down(d, p).start())
                to_mate(place + d, p).start()

    for load in loads:
        load.wait()
    short = jnp.minimum(place, last - place)

    def distance(s):
        return jnp.where(s <= 2 * short, (s + 1) // 2, s - short)

    def extra_load(rank, which, slot, e):
        return pltpu.make_async_copy(
            extra_from[e].at[pl.ds(first_of(rank, which), rows)], extra.at[slot, e], extra_sem.at[slot, e]
        )

    def store(rank, which, slot, m):
        return pltpu.make_async_copy(
            stage.at[slot, m], made_to[m].at[pl.ds(first_of(rank, which), rows)], stage_sem.at[slot, m]
        )

    def visit(s, carry):
        d = distance(s)
        below = jnp.where(s <= 2 * short, s % 2 == 1, place > last - place)
        rank = jnp.where(below, place - d, place + d)
        for slot, which in enumerate((core, 1 - core)):
            for e in range(n_extra):
                extra_load(rank, which, slot, e).start()
        pl.when((s > 0) & (d != distance(s - 1)))(lambda: forward(d))
        for slot, which in enumerate((core, 1 - core)):
            if slot == 1:
                for p in range(pieces):
                    from_mate(rank, p).wait_recv()
            for e in range(n_extra):
                extra_load(rank, which, slot, e).wait()

            @pl.when(s > 0)
            def _():
                for m in range(n_made):
                    store(rank, which, slot, m).wait()

            work(o_ref.at[pl.ds(first_of(rank, which), rows)], weights, extra.at[slot], stage.at[slot])
            for m in range(n_made):
                store(rank, which, slot, m).start()
        return carry

    lax.fori_loop(0, size, visit, 0)
    for slot, which in enumerate((core, 1 - core)):
        for m in range(n_made):
            store(place, which, slot, m).wait()
    for p in range(pieces):
        for k in range(last):
            pl.when((place < last) & (place - k >= 0))(lambda k=k, p=p: going_up(k, p).wait_send())
            pl.when((place > 0) & (place + k <= last))(lambda k=k, p=p: going_down(k, p).wait_send())
        for rank in range(size):
            to_mate(rank, p).wait_send()


def gather_apply(x, weights, extra, work, n_made, ident):
    size = lax.axis_size("ctx")
    rows, width = x.shape[0], weights[0].shape[1]
    total = 2 * size * rows
    pieces = pieces_of(*x.shape)
    dma = pltpu.SemaphoreType.DMA
    made = jax.ShapeDtypeStruct((total, width), jnp.bfloat16)
    slots = max(1, len(extra))
    return pl.pallas_call(
        functools.partial(gather_apply_kernel, size, pieces, work, len(weights), len(extra), n_made),
        in_specs=[IN_VMEM] + [ANY] * (len(weights) + len(extra)),
        out_specs=[IN_VMEM] + [ANY] * n_made,
        out_shape=[jax.ShapeDtypeStruct((total, x.shape[1]), x.dtype)] + [made] * n_made,
        scratch_shapes=[pltpu.VMEM(w.shape, w.dtype) for w in weights]
        + [
            pltpu.VMEM((2, slots, rows, width) if extra else (2, 1, 16, 128), jnp.bfloat16),
            pltpu.VMEM((2, n_made, rows, width), jnp.bfloat16),
            dma,
            dma((len(weights),)),
            dma((2, slots)),
            dma((2, n_made)),
        ]
        + [dma((size, pieces))] * 6,
        compiler_params=pltpu.CompilerParams(collective_id=ident, has_side_effects=True, vmem_limit_bytes=60000000),
        cost_estimate=pl.CostEstimate(flops=0, bytes_accessed=200000000, transcendentals=0),
    )(x, *weights, *extra)


def sum_apply_kernel(size, pieces, count, *refs):
    acts_from, refs = refs[:count], refs[count:]
    weights_from, refs = refs[:count], refs[count:]
    o_ref, acts, weights, mine, sent, mate, came, load_sem = refs[:8]
    mate_send, mate_recv, up_send, up_recv, down_send, down_recv = refs[8:]
    place, core = lax.axis_index("ctx"), lax.axis_index("tensor")
    rows, depth = o_ref.shape
    part = rows // pieces
    last = size - 1

    loads = []
    for a in range(count):
        loads.append(pltpu.make_async_copy(weights_from[a], weights.at[a], load_sem.at[a]))
        loads.append(pltpu.make_async_copy(acts_from[a], acts.at[a], load_sem.at[count + a]))
    for load in loads:
        load.start()
    greet_chain(size, True)
    for load in loads:
        load.wait()

    def at(ref, d, p):
        return ref.at[d, pl.ds(p * part, part)]

    def to_mate(i, d, p):
        slot = lax.rem(i, 2)
        return remote(at(sent, slot, p), at(mate, d, p), mate_send.at[slot, p], mate_recv.at[d, p], {"tensor": 1 - core})

    def going_up(d, p):
        return remote(at(mine, d, p), at(came, d, p), up_send.at[d, p], up_recv.at[d, p], {"ctx": place + 1})

    def going_down(d, p):
        there = jnp.where(d == place - 1, size, d)
        return remote(at(mine, d, p), at(came, there, p), down_send.at[d, p], down_recv.at[d, p], {"ctx": place - 1})

    def coming_up(d, p):
        there = at(came, d, p)
        return remote(there, there, up_send.at[d, p], up_recv.at[d, p], {"ctx": place - 1})

    def coming_down(d, p):
        there = at(came, jnp.where(d == place, size, d), p)
        return remote(there, there, down_send.at[d, p], down_recv.at[d, p], {"ctx": place + 1})

    def compute(d, which, target):
        step = column_step(depth)
        span = pl.ds(pl.multiple_of((d * 2 + which) * rows, rows), rows)

        def some(j, carry):
            columns = pl.ds(pl.multiple_of(j * step, step), step)
            total = matmul_nt(acts[0, span, :], weights[0, columns, :])
            for a in range(1, count):
                total += matmul_nt(acts[a, span, :], weights[a, columns, :])
            target[:, columns] = total.astype(target.dtype)
            return carry

        lax.fori_loop(0, depth // step, some, 0)

    def with_mate(d, p):
        to_mate(0, d, p).wait_recv()
        return [at(mine, d, p), at(mate, d, p)]

    short = jnp.minimum(place, last - place)

    def first_part(i, carry):
        s = last - i
        near = s <= 2 * short
        d = jnp.where(near, (s + 1) // 2, s - short)
        d = jnp.where(jnp.where(near, s % 2 == 1, place > last - place), place - d, place + d)
        for p in range(pieces):
            pl.when(i >= 2)(lambda p=p: to_mate(i, d, p).wait_send())
        compute(d, 1 - core, sent.at[lax.rem(i, 2)])
        for p in range(pieces):
            to_mate(i, d, p).start()
        compute(d, core, mine.at[d])

        @pl.when((place == 0) & (d > 0))
        def _():
            for p in range(pieces):
                add_blocks(at(mine, d, p), with_mate(d, p))
                going_up(d, p).start()

        @pl.when((place == last) & (d < last))
        def _():
            for p in range(pieces):
                add_blocks(at(mine, d, p), with_mate(d, p))
                going_down(d, p).start()

        return carry

    lax.fori_loop(0, size, first_part, 0)

    def second_part(s, carry):
        k, p = s // pieces, s % pieces

        @pl.when((place > 0) & (place < last - k))
        def _():
            d = last - k
            parts = with_mate(d, p)
            coming_up(d, p).wait_recv()
            add_blocks(at(mine, d, p), parts + [at(came, d, p)])
            going_up(d, p).start()

        @pl.when((place < last) & (place > k))
        def _():
            parts = with_mate(k, p)
            coming_down(k, p).wait_recv()
            add_blocks(at(mine, k, p), parts + [at(came, k, p)])
            going_down(k, p).start()

        return carry

    lax.fori_loop(0, last * pieces, second_part, 0)

    def final(p, carry):
        target = o_ref.at[pl.ds(pl.multiple_of(p * part, part), part)]
        parts = with_mate(place, p)
        pl.when(place > 0)(lambda: coming_up(place, p).wait_recv())
        pl.when(place < last)(lambda: coming_down(place, p).wait_recv())
        up, down = at(came, place, p), at(came, size, p)
        pl.when(place == 0)(lambda: add_blocks(target, parts + [down]))
        pl.when(place == last)(lambda: add_blocks(target, parts + [up]))
        pl.when((place > 0) & (place < last))(lambda: add_blocks(target, parts + [up, down]))
        return carry

    lax.fori_loop(0, pieces, final, 0)
    for p in range(pieces):
        for i in range(size - 2, size):
            to_mate(i, 0, p).wait_send()
        for d in range(size):
            pl.when(place < d)(lambda d=d, p=p: going_up(d, p).wait_send())
            pl.when(place > d)(lambda d=d, p=p: going_down(d, p).wait_send())


def sum_apply(acts, weights, ident):
    size, count = lax.axis_size("ctx"), len(acts)
    total, width = acts[0].shape
    depth = weights[0].shape[0]
    block = total // (2 * size)
    pieces = pieces_of(block, depth)
    dma = pltpu.SemaphoreType.DMA

    def slots(n):
        return pltpu.VMEM((n, block, depth), jnp.bfloat16)

    scratch = [
        pltpu.VMEM((count, total, width), jnp.bfloat16),
        pltpu.VMEM((count, depth, width), jnp.bfloat16),
        slots(size),
        slots(2),
        slots(size),
        slots(size + 1),
        dma((2 * count,)),
        dma((2, pieces)),
    ] + [dma((size, pieces))] * 5
    return pl.pallas_call(
        functools.partial(sum_apply_kernel, size, pieces, count),
        in_specs=[ANY] * (2 * count),
        out_specs=IN_VMEM,
        out_shape=jax.ShapeDtypeStruct((block, depth), jnp.float32),
        scratch_shapes=scratch,
        compiler_params=pltpu.CompilerParams(collective_id=ident, has_side_effects=True, vmem_limit_bytes=60000000),
        cost_estimate=pl.CostEstimate(flops=0, bytes_accessed=200000000, transcendentals=0),
    )(*acts, *weights)


def assemble_kernel(size, ranks_ref, *refs):
    parts, (down_ref, gate_ref, up_ref, whole) = refs[:size], refs[size:]
    width = parts[0].shape[2]
    for which, target in enumerate((down_ref, gate_ref, up_ref)):
        for part, k in zip(parts, range(size)):
            whole[:, pl.ds(pl.multiple_of(ranks_ref[k] * width, 128), width)] = part[which].astype(jnp.float32)
        target[...] = whole[:, : gate_ref.shape[1]]


def assemble(received, columns):
    ranks = jnp.stack([rank for rank, _ in received]).astype(jnp.int32)
    blocks = [block for _, block in received]
    _, rows, width = blocks[0].shape
    f32 = jnp.float32
    return pl.pallas_call(
        functools.partial(assemble_kernel, len(blocks)),
        in_specs=[pl.BlockSpec(memory_space=pltpu.SMEM)] + [IN_VMEM] * len(blocks),
        out_specs=[IN_VMEM] * 3,
        out_shape=[jax.ShapeDtypeStruct((rows, columns), f32)] * 3,
        scratch_shapes=[pltpu.VMEM((rows, len(blocks) * width), f32)],
        compiler_params=pltpu.CompilerParams(vmem_limit_bytes=60000000),
        cost_estimate=pl.CostEstimate(flops=0, bytes_accessed=20 * rows * columns, transcendentals=0),
        name="assemble",
    )(ranks, *blocks)


def mask_into(bias_ref, first, seg_ref, place_ref):
    keys, rows = bias_ref.shape
    key_index = lax.broadcasted_iota(jnp.int32, (keys, rows), 0)
    row_index = lax.broadcasted_iota(jnp.int32, (keys, rows), 1) + first
    place = jnp.broadcast_to(place_ref[...], (keys, rows))
    start = jnp.broadcast_to(seg_ref[...], (keys, rows))
    allowed = ((place >= start) & (place <= row_index)) | (key_index == row_index)
    bias_ref[...] = jnp.where(allowed, 0.0, VERY_LOW)


def attend_kernel(scale, first_ref, seg_ref, place_ref, q_ref, k_ref, vt_ref, o_ref, lse_ref, bias_ref):
    @pl.when(pl.program_id(1) == 0)
    def _():
        mask_into(bias_ref, first_ref[0] + pl.program_id(0) * q_ref.shape[0], seg_ref, place_ref)

    scores = matmul_nt(k_ref[...], q_ref[...]) * scale + bias_ref[...]
    top = jnp.max(scores, axis=0, keepdims=True)
    powers = jnp.exp(scores - top)
    total = jnp.sum(powers, axis=0, keepdims=True)
    mixture = nn(vt_ref[...], powers.astype(jnp.bfloat16)) / total
    o_ref[...] = mixture.T.astype(jnp.bfloat16)
    lse_ref[0] = top + jnp.log(total)


def attend_back_kernel(
    scale, first_ref, seg_ref, place_ref, q_ref, do_ref, lse_ref, k_ref, v_ref, kt_ref,
    dq_ref, dkv_ref, bias_ref, dk_ref, dv_ref,
):
    block, head = pl.program_id(0), pl.program_id(1)

    @pl.when(head == 0)
    def _():
        mask_into(bias_ref, first_ref[0] + block * q_ref.shape[0], seg_ref, place_ref)

    @pl.when((head == 0) & (block == 0))
    def _():
        dk_ref[...] = jnp.zeros_like(dk_ref)
        dv_ref[...] = jnp.zeros_like(dv_ref)

    query, grad = q_ref[...], do_ref[...]
    scores = matmul_nt(k_ref[...], query) * scale + bias_ref[...]
    probs = jnp.exp(scores - lse_ref[0])
    grad_probs = matmul_nt(v_ref[...], grad)
    delta = jnp.sum(probs * grad_probs, axis=0, keepdims=True)
    grad_scores = (probs * (grad_probs - delta)).astype(jnp.bfloat16)
    dv_ref[...] += nn(probs.astype(jnp.bfloat16), grad)
    dk_ref[...] += nn(grad_scores, query)
    dq_ref[...] = (nn(kt_ref[...], grad_scores) * scale).T

    @pl.when((head == pl.num_programs(1) - 1) & (block == pl.num_programs(0) - 1))
    def _():
        dkv_ref[:, :HEAD] = (dk_ref[...] * scale).astype(jnp.bfloat16)
        dkv_ref[:, HEAD:] = dv_ref[...].astype(jnp.bfloat16)


def attention_calls(rows, keys, heads):
    block = math.gcd(256, rows)
    scale = 1.0 / math.sqrt(HEAD)
    smem = pl.BlockSpec(memory_space=pltpu.SMEM)
    seg = pl.BlockSpec((1, block), lambda i, h: (0, i))
    place = pl.BlockSpec((keys, 1), lambda i, h: (0, 0))
    head = pl.BlockSpec((block, HEAD), lambda i, h: (i, h))
    lse = pl.BlockSpec((1, 1, block), lambda i, h: (h, 0, i))
    tall = pl.BlockSpec((keys, HEAD), lambda i, h: (0, 0))
    wide = pl.BlockSpec((HEAD, keys), lambda i, h: (0, 0))
    params = pltpu.CompilerParams(vmem_limit_bytes=60000000)
    grid = (rows // block, heads)
    size = heads * rows * keys
    forward = pl.pallas_call(
        functools.partial(attend_kernel, scale),
        grid=grid,
        in_specs=[smem, seg, place, head, tall, wide],
        out_specs=[head, lse],
        out_shape=[
            jax.ShapeDtypeStruct((rows, heads * HEAD), jnp.bfloat16),
            jax.ShapeDtypeStruct((heads, 1, rows), jnp.float32),
        ],
        scratch_shapes=[pltpu.VMEM((keys, block), jnp.float32)],
        compiler_params=params,
        cost_estimate=pl.CostEstimate(flops=4 * size * HEAD, bytes_accessed=4 * rows * heads * HEAD, transcendentals=size),
        name="attend",
    )
    backward = pl.pallas_call(
        functools.partial(attend_back_kernel, scale),
        grid=grid,
        in_specs=[smem, seg, place, head, head, lse, tall, tall, wide],
        out_specs=[head, pl.BlockSpec((keys, 2 * HEAD), lambda i, h: (0, 0))],
        out_shape=[
            jax.ShapeDtypeStruct((rows, heads * HEAD), jnp.float32),
            jax.ShapeDtypeStruct((keys, 2 * HEAD), jnp.bfloat16),
        ],
        scratch_shapes=[
            pltpu.VMEM((keys, block), jnp.float32),
            pltpu.VMEM((keys, HEAD), jnp.float32),
            pltpu.VMEM((keys, HEAD), jnp.float32),
        ],
        compiler_params=params,
        cost_estimate=pl.CostEstimate(flops=10 * size * HEAD, bytes_accessed=8 * rows * heads * HEAD, transcendentals=size),
        name="attend_back",
    )
    return forward, backward


def per_device(
    layer_input,
    teacher,
    cotangent,
    segment_ids,
    positions,
    valid_mask,
    gain_attn,
    query_weight,
    query_bias,
    key_weight,
    key_bias,
    value_weight,
    value_bias,
    out_weight,
    gain_mlp,
    gate_weight,
    up_weight,
    down_weight,
):
    tensor_rank = lax.axis_index("tensor")
    ctx_rank = lax.axis_index("ctx")
    tensor_size, ctx_size = lax.axis_size("tensor"), lax.axis_size("ctx")
    own_rows = layer_input.shape[0]
    shard_rows = own_rows * tensor_size
    seq_len = segment_ids.shape[0]
    q_width = query_weight.shape[1]
    kv_width = key_weight.shape[1]
    kv_local = kv_width // HEAD
    group = q_width // kv_width
    hidden_width = gate_weight.shape[1]
    slice_width = -(-hidden_width // (128 * ctx_size)) * 128
    first_row = ctx_rank * shard_rows
    own_first = first_row + tensor_rank * own_rows

    inputs = layer_input.astype(jnp.float32)
    gain_one = gain_attn.astype(jnp.float32)
    gain_two = gain_mlp.astype(jnp.float32)
    scale_attn = lax.rsqrt(jnp.mean(inputs * inputs, axis=1, keepdims=True) + EPS)
    normed_attn = inputs * scale_attn
    extra = ((0, 0), (0, ctx_size * slice_width - hidden_width))
    full_qkv, full_out, *slices = front(
        jnp.concatenate([query_weight, key_weight, value_weight], axis=1),
        out_weight.T,
        [jnp.pad(w, extra) for w in (gate_weight, up_weight, down_weight.T)],
        slice_width,
        1,
    )
    full_gate, full_up, full_down = [lax.all_gather(w, "dp", axis=0, tiled=True) for w in slices]
    normed_rows = gather((normed_attn * gain_one).astype(jnp.bfloat16), 1, True, 2)
    valid_count = jnp.sum(valid_mask.astype(jnp.float32))
    counts = [valid_count]
    dp_size = lax.axis_size("dp")
    for step in range(1, dp_size):
        counts.append(
            lax.ppermute(
                jnp.full((8, 128), valid_count), "dp", [(i, (i + step) % dp_size) for i in range(dp_size)]
            )[0, 0]
        )
    valid_count = sum(counts)

    bias = jnp.concatenate(
        [
            lax.dynamic_slice_in_dim(query_bias, tensor_rank * q_width, q_width),
            lax.dynamic_slice_in_dim(key_bias, tensor_rank * kv_width, kv_width),
            lax.dynamic_slice_in_dim(value_bias, tensor_rank * kv_width, kv_width),
        ]
    ).astype(jnp.float32)
    places = lax.dynamic_slice_in_dim(positions, first_row, shard_rows)
    cosine, sine_table = rope_tables(places)
    qkv_pre = matmul(normed_rows, full_qkv) + bias
    turned = q_width + kv_width
    rotated = (
        rotate(qkv_pre[:, :turned].reshape(shard_rows, turned // HEAD, HEAD), cosine, sine_table)
        .astype(jnp.bfloat16)
        .reshape(shard_rows, turned)
    )
    queries = rotated[:, :q_width]
    own_kv = jnp.concatenate([rotated[:, q_width:], qkv_pre[:, turned:].astype(jnp.bfloat16)], axis=1)
    all_kv = gather(own_kv, ctx_size, False, 3)

    key_index = jnp.arange(seq_len, dtype=jnp.int32)
    key_place = jnp.where(valid_mask > 0, key_index, -1)[:, None]
    seq_first = lax.axis_index("dp") * seq_len
    doc_start = (lax.dynamic_slice_in_dim(segment_ids, first_row, shard_rows) - seq_first)[None, :]
    first = jnp.reshape(first_row, (1,)).astype(jnp.int32)
    forward, backward = attention_calls(shard_rows, seq_len, group)
    kept = []
    for c in range(kv_local):
        key = all_kv[:, c * HEAD : (c + 1) * HEAD]
        value = all_kv[:, kv_width + c * HEAD : kv_width + (c + 1) * HEAD]
        query = queries[:, c * group * HEAD : (c + 1) * group * HEAD]
        kept.append((query, key, value) + tuple(forward(first, doc_start, key_place, query, key, value.T)))
    heads_out = jnp.concatenate([k[3] for k in kept], axis=1)
    attention = scatter(matmul_nt(heads_out, full_out), 1, True, 4)
    residual_mid = inputs + attention
    scale_mlp = lax.rsqrt(jnp.mean(residual_mid * residual_mid, axis=1, keepdims=True) + EPS)
    normed_mlp = residual_mid * scale_mlp
    mlp_rows, gate_act, up_act, hidden = gather_apply(
        (normed_mlp * gain_two).astype(jnp.bfloat16), [full_gate, full_up], [], expand_block, 3, 5
    )
    branch = sum_apply([hidden], [full_down], 6)
    layer_result = residual_mid + branch
    valid_own = lax.dynamic_slice_in_dim(valid_mask, own_first, own_rows).astype(jnp.float32)
    difference = layer_result - teacher.astype(jnp.float32)
    squared_sum = jnp.sum(valid_own[:, None] * difference * difference)
    grad_result = cotangent.astype(jnp.float32) + 2.0 * valid_own[:, None] * difference / (
        valid_count * D
    )
    grad_branch, grad_gate_act, grad_up_act = gather_apply(
        grad_result.astype(jnp.bfloat16), [full_down], [gate_act, up_act], shrink_block, 2, 9
    )
    summed = []
    for left, right in ((grad_branch, hidden), (mlp_rows, grad_gate_act), (mlp_rows, grad_up_act)):
        grad = matmul_tn(left, right).astype(jnp.bfloat16)
        grad_gate_act, grad_up_act, grad = lax.optimization_barrier((grad_gate_act, grad_up_act, grad))
        summed.append(lax.psum_scatter(grad, "dp", scatter_dimension=0, tiled=True))
    grad_mlp_rows = sum_apply([grad_gate_act, grad_up_act], [full_gate, full_up], 10)
    grad_gain_mlp = jnp.sum(grad_mlp_rows * normed_mlp, axis=0)
    grad_mid = grad_result + norm_back(grad_mlp_rows, normed_mlp, scale_mlp, gain_two)
    grad_attn_rows = gather(grad_mid.astype(jnp.bfloat16), 1, True, 2)
    grad_heads = matmul(grad_attn_rows, full_out).astype(jnp.bfloat16)
    grad_out = matmul_tn(grad_attn_rows, heads_out).astype(jnp.bfloat16)

    grad_out = lax.psum_scatter(grad_out, "dp", scatter_dimension=0, tiled=True)
    query_grads, key_grads, value_grads = [], [], []
    for c in range(kv_local):
        query, key, value, _, log_total = kept[c]
        span = slice(c * group * HEAD, (c + 1) * group * HEAD)
        grad_query, grad_kv = backward(
            first, doc_start, key_place, query, grad_heads[:, span], log_total, key, value, key.T
        )
        query_grads.append(grad_query)
        key_grads.append(grad_kv[:, :HEAD])
        value_grads.append(grad_kv[:, HEAD:])
    grad_kv = grad_kv if kv_local == 1 else jnp.concatenate(key_grads + value_grads, axis=1)
    grad_kv = scatter(grad_kv, ctx_size, False, 7)
    grad_kv, *summed = lax.optimization_barrier((grad_kv, *summed))
    shard_down, shard_gate, shard_up = to_rows(summed, hidden_width)
    shard_down = shard_down.T
    grad_turned = jnp.concatenate(query_grads + [grad_kv[:, :kv_width]], axis=1)
    grad_pre = jnp.concatenate(
        [
            rotate(grad_turned.reshape(shard_rows, turned // HEAD, HEAD), cosine, -sine_table)
            .reshape(shard_rows, turned)
            .astype(jnp.bfloat16),
            grad_kv[:, kv_width:].astype(jnp.bfloat16),
        ],
        axis=1,
    )
    grad_pre, grad_out = lax.optimization_barrier((grad_pre, grad_out))
    shard_out = lax.psum_scatter(grad_out, "ctx", scatter_dimension=0, tiled=True)
    shard_out = shard_out.astype(jnp.float32).T
    bias_sum = jnp.sum(grad_pre.astype(jnp.float32), axis=0)

    def spread(part, size):
        return lax.dynamic_update_slice_in_dim(
            jnp.zeros((size,), jnp.float32), part, tensor_rank * part.shape[0], 0
        )

    loss_part = jnp.zeros((128,), jnp.float32).at[0].set(squared_sum)
    parts = [
        jnp.zeros((D,), jnp.float32),
        grad_gain_mlp,
        spread(bias_sum[:q_width], query_bias.shape[0]),
        spread(bias_sum[q_width:turned], key_bias.shape[0]),
        spread(bias_sum[turned:], value_bias.shape[0]),
        loss_part,
    ]
    flat = jnp.concatenate(parts)
    small = jnp.pad(flat, (0, -flat.shape[0] % 1024)).reshape(-1, 128)
    grad_qkv = matmul_tn(normed_rows, grad_pre).astype(jnp.bfloat16)
    shard_qkv, sums, grad_normed = back(grad_qkv, small, grad_pre, full_qkv, normed_attn, 8)
    grad_input = grad_mid + norm_back(grad_normed, normed_attn, scale_attn, gain_one)
    sums = sums.reshape(-1)
    pieces, offset = [], 0
    for part in parts:
        pieces.append(sums[offset : offset + part.shape[0]])
        offset += part.shape[0]
    return (
        layer_result.astype(jnp.bfloat16),
        pieces[5][0] / (valid_count * D),
        grad_input,
        pieces[0],
        shard_qkv[:, :q_width],
        pieces[2],
        shard_qkv[:, q_width:turned],
        pieces[3],
        shard_qkv[:, turned:],
        pieces[4],
        shard_out,
        pieces[1],
        shard_gate,
        shard_up,
        shard_down,
    )


def solution(mesh):
    in_specs = (
        P(("dp", "ctx", "tensor"), None),
        P(("dp", "ctx", "tensor"), None),
        P(("dp", "ctx", "tensor"), None),
        P("dp"),
        P("dp"),
        P("dp"),
        P(),
        P(("dp", "ctx"), "tensor"),
        P(),
        P(("dp", "ctx"), "tensor"),
        P(),
        P(("dp", "ctx"), "tensor"),
        P(),
        P("tensor", ("dp", "ctx")),
        P(),
        P(("dp", "ctx"), "tensor"),
        P(("dp", "ctx"), "tensor"),
        P("tensor", ("dp", "ctx")),
    )
    out_specs = (
        P(("dp", "ctx", "tensor"), None),
        P(),
        P(("dp", "ctx", "tensor"), None),
        P(),
        P(("dp", "ctx"), "tensor"),
        P(),
        P(("dp", "ctx"), "tensor"),
        P(),
        P(("dp", "ctx"), "tensor"),
        P(),
        P("tensor", ("dp", "ctx")),
        P(),
        P(("dp", "ctx"), "tensor"),
        P(("dp", "ctx"), "tensor"),
        P("tensor", ("dp", "ctx")),
    )

    return jax.shard_map(per_device, mesh=mesh, in_specs=in_specs, out_specs=out_specs, check_vma=False)
```

```python
import functools
import math

import jax
import jax.numpy as jnp
from jax import lax
from jax.experimental import pallas as pl
from jax.experimental.pallas import tpu as pltpu
from jax.sharding import PartitionSpec as P


D = 1536
HEAD = 128


EPS = 1e-06
THETA = 10000.0
VERY_LOW = -1e30


def rope_tables(places):
    half_dim = HEAD // 2
    frequency = THETA ** (-(jnp.arange(half_dim, dtype=jnp.float32) * 2.0 / HEAD))
    angles = places.astype(jnp.float32)[:, None] * frequency[None, :]
    return (jnp.cos(angles), jnp.sin(angles))


def rotate(stacked, cosine, sine_table):
    half_dim = HEAD // 2
    first_half = stacked[..., :half_dim]
    second_half = stacked[..., half_dim:]
    cosine = cosine[:, None, :]
    sine_table = sine_table[:, None, :]
    return jnp.concatenate(
        [
            first_half * cosine - second_half * sine_table,
            second_half * cosine + first_half * sine_table,
        ],
        axis=-1,
    )


def matmul(first_op, second_op):
    return jnp.dot(first_op, second_op, preferred_element_type=jnp.float32)


def matmul_tn(first_op, second_op):
    return lax.dot_general(
        first_op, second_op, (((0,), (0,)), ((), ())), preferred_element_type=jnp.float32
    )


def matmul_nt(first_op, second_op):
    return lax.dot_general(
        first_op, second_op, (((1,), (1,)), ((), ())), preferred_element_type=jnp.float32
    )


def norm_back(grad_normed, normed, inverse, gain):
    scaled = grad_normed * gain
    return inverse * (scaled - normed * jnp.mean(scaled * normed, axis=1, keepdims=True))


def exchange(blocks, axis):
    size = lax.axis_size(axis)
    rank = lax.axis_index(axis)
    received = [(rank, lax.dynamic_index_in_dim(blocks, rank, 0, keepdims=False))]
    for step in range(1, size):
        going = lax.dynamic_index_in_dim(blocks, (rank + step) % size, 0, keepdims=False)
        came = lax.ppermute(going, axis, [(i, (i + step) % size) for i in range(size)])
        received.append(((rank - step + size) % size, came))
    return received


def to_rows(summed, columns):
    size = lax.axis_size("ctx")
    rows, width = summed[0].shape[0] // size, summed[0].shape[1]
    blocks = jnp.stack([s.reshape(size, rows, width) for s in summed], axis=1)
    return assemble(exchange(blocks, "ctx"), columns)


def nn(first_op, second_op):
    return jnp.dot(first_op, second_op, preferred_element_type=jnp.float32)


MESH = pl.DeviceIdType.MESH
ANY = pl.BlockSpec(memory_space=pl.ANY)
IN_VMEM = pl.BlockSpec(memory_space=pltpu.VMEM)


def remote(source, target, send_sem, recv_sem, device):
    return pltpu.make_async_remote_copy(
        src_ref=source,
        dst_ref=target,
        send_sem=send_sem,
        recv_sem=recv_sem,
        device_id=device,
        device_id_type=MESH,
    )


def greet(barrier, device):
    pl.semaphore_signal(barrier, inc=1, device_id=device, device_id_type=MESH)


def greet_chain(size, paired):
    place = lax.axis_index("ctx")
    barrier = pltpu.get_barrier_semaphore()
    if size > 1:
        pl.when(place < size - 1)(lambda: greet(barrier, {"ctx": place + 1}))
        pl.when(place > 0)(lambda: greet(barrier, {"ctx": place - 1}))
    if paired:
        greet(barrier, {"tensor": 1 - lax.axis_index("tensor")})
    if size == 1:
        pl.semaphore_wait(barrier, 1)
        return
    ends = (place == 0) | (place == size - 1)
    pl.when(ends)(lambda: pl.semaphore_wait(barrier, 1 + paired))
    pl.when(jnp.logical_not(ends))(lambda: pl.semaphore_wait(barrier, 2 + paired))


def gather_kernel(size, paired, pieces, x_ref, o_ref, local_sem, up_send, up_recv, down_send, down_recv, mate_send, mate_recv):
    place = lax.axis_index("ctx") if size > 1 else 0
    core = lax.axis_index("tensor")
    rows = x_ref.shape[0]
    part = rows // pieces
    greet_chain(size, paired)

    def block(rank, which, p):
        index = rank * 2 + which if paired else rank
        return o_ref.at[pl.ds(pl.multiple_of(index * rows + p * part, part), part)]

    def source(rank, k, p):
        return x_ref.at[pl.ds(p * part, part)] if k == 0 else block(rank, core, p)

    def going_up(k, p):
        return remote(
            source(place - k, k, p), block(place - k, core, p), up_send.at[k, p], up_recv.at[k, p], {"ctx": place + 1}
        )

    def going_down(k, p):
        return remote(
            source(place + k, k, p), block(place + k, core, p), down_send.at[k, p], down_recv.at[k, p], {"ctx": place - 1}
        )

    def to_mate(rank, k, p):
        return remote(
            source(rank, k, p), block(rank, core, p), mate_send.at[k, p], mate_recv.at[rank, p], {"tensor": 1 - core}
        )

    def from_mate(rank, p):
        there = block(rank, 1 - core, p)
        return remote(there, there, mate_send.at[0, p], mate_recv.at[rank, p], {"tensor": 1 - core})

    own = pltpu.make_async_copy(x_ref, o_ref.at[pl.ds(pl.multiple_of((place * 2 + core if paired else place) * rows, rows), rows)], local_sem)
    for p in range(pieces):
        if size > 1:
            pl.when(place < size - 1)(lambda p=p: going_up(0, p).start())
            pl.when(place > 0)(lambda p=p: going_down(0, p).start())
    for p in range(pieces):
        if paired:
            to_mate(place, 0, p).start()
    own.start()
    for k in range(size - 1):
        for p in range(pieces):

            @pl.when(place - 1 - k >= 0)
            def _(k=k, p=p):
                there = block(place - 1 - k, core, p)
                remote(there, there, up_send.at[k, p], up_recv.at[k, p], {"ctx": place - 1}).wait_recv()
                if k + 1 < size - 1:
                    pl.when(place < size - 1)(lambda: going_up(k + 1, p).start())
                if paired:
                    to_mate(place - 1 - k, 1 + k, p).start()

            @pl.when(place + 1 + k <= size - 1)
            def _(k=k, p=p):
                there = block(place + 1 + k, core, p)
                remote(there, there, down_send.at[k, p], down_recv.at[k, p], {"ctx": place + 1}).wait_recv()
                if k + 1 < size - 1:
                    pl.when(place > 0)(lambda: going_down(k + 1, p).start())
                if paired:
                    to_mate(place + 1 + k, size + k, p).start()

    own.wait()
    for p in range(pieces):
        if paired:
            for rank in range(size):
                from_mate(rank, p).wait_recv()
            to_mate(place, 0, p).wait_send()
        for k in range(size - 1):
            pl.when((place < size - 1) & (place - k >= 0))(lambda k=k, p=p: going_up(k, p).wait_send())
            pl.when((place > 0) & (place + k <= size - 1))(lambda k=k, p=p: going_down(k, p).wait_send())
            if paired:
                pl.when(place - 1 - k >= 0)(lambda k=k, p=p: to_mate(place - 1 - k, 1 + k, p).wait_send())
                pl.when(place + 1 + k <= size - 1)(lambda k=k, p=p: to_mate(place + 1 + k, size + k, p).wait_send())


def pieces_of(rows, columns):
    return math.gcd(4, rows // 64) if rows * columns >= 1 << 18 else 1


def gather(x, size, paired, ident):
    copies = size * 2 if paired else size
    wide = max(size, 2)
    pieces = pieces_of(*x.shape)
    dma = pltpu.SemaphoreType.DMA
    return pl.pallas_call(
        functools.partial(gather_kernel, size, paired, pieces),
        in_specs=[IN_VMEM],
        out_specs=ANY,
        out_shape=jax.ShapeDtypeStruct((copies * x.shape[0], x.shape[1]), x.dtype),
        scratch_shapes=[dma] + [dma((wide, pieces))] * 4 + [dma((2 * wide, pieces)), dma((wide, pieces))],
        compiler_params=pltpu.CompilerParams(collective_id=ident, has_side_effects=True),
        cost_estimate=pl.CostEstimate(flops=0, bytes_accessed=30 * copies * x.size, transcendentals=0),
        name="gather",
    )(x)


def add_blocks(target, parts):
    rows = target.shape[0]
    step = math.gcd(rows, 32)

    def some(i, carry):
        span = pl.ds(pl.multiple_of(i * step, step), step)
        total = parts[0][span].astype(jnp.float32)
        for part in parts[1:]:
            total += part[span].astype(jnp.float32)
        target[span] = total.astype(target.dtype)
        return carry

    lax.fori_loop(0, rows // step, some, 0)


def scatter_kernel(
    size, paired, pieces, x_ref, o_ref, mine, mate, above, below, own_sem, mate_send, mate_recv, up_send, up_recv, down_send, down_recv
):
    place = lax.axis_index("ctx") if size > 1 else 0
    core = lax.axis_index("tensor")
    rows = o_ref.shape[0]
    part = rows // pieces
    order = sorted(range(size), key=lambda d: min(d, size - 1 - d))
    every = [(d, p) for d in order for p in range(pieces)]

    def block(rank, which, p):
        index = rank * 2 + which if paired else rank
        return x_ref.at[pl.ds(pl.multiple_of(index * rows + p * part, part), part)]

    def at(ref, d, p):
        return ref.at[d, pl.ds(p * part, part)]

    def load(d, p):
        return pltpu.make_async_copy(block(d, core, p), at(mine, d, p), own_sem.at[d, p])

    def to_mate(d, p):
        return remote(
            block(d, 1 - core, p), at(mate, d, p), mate_send.at[d, p], mate_recv.at[d, p], {"tensor": 1 - core}
        )

    def going_up(d, p):
        return remote(at(mine, d, p), at(below, d, p), up_send.at[d, p], up_recv.at[d, p], {"ctx": place + 1})

    def going_down(d, p):
        return remote(at(mine, d, p), at(above, d, p), down_send.at[d, p], down_recv.at[d, p], {"ctx": place - 1})

    for d, p in every:
        load(d, p).start()
    greet_chain(size, paired)
    if paired:
        for d, p in every:
            to_mate(d, p).start()

    def here(d, p):
        load(d, p).wait()
        if paired:
            to_mate(d, p).wait_recv()
            return [at(mine, d, p), at(mate, d, p)]
        return [at(mine, d, p)]

    for k in range(size - 1):
        for p in range(pieces):

            @pl.when(place < size - 1 - k)
            def _(d=size - 1 - k, p=p):
                parts = here(d, p)

                @pl.when(place > 0)
                def _():
                    going_up(d, p).wait_recv()
                    add_blocks(at(mine, d, p), parts + [at(below, d, p)])

                if paired:
                    pl.when(place == 0)(lambda: add_blocks(at(mine, d, p), parts))
                going_up(d, p).start()

            @pl.when(place > k)
            def _(d=k, p=p):
                parts = here(d, p)

                @pl.when(place < size - 1)
                def _():
                    going_down(d, p).wait_recv()
                    add_blocks(at(mine, d, p), parts + [at(above, d, p)])

                if paired:
                    pl.when(place == size - 1)(lambda: add_blocks(at(mine, d, p), parts))
                going_down(d, p).start()

    for d in range(size):

        @pl.when(place == d)
        def _(d=d):
            for p in range(pieces):
                parts = here(d, p)
                if d > 0:
                    going_up(d, p).wait_recv()
                    parts = parts + [at(below, d, p)]
                if d < size - 1:
                    going_down(d, p).wait_recv()
                    parts = parts + [at(above, d, p)]
                add_blocks(o_ref.at[pl.ds(p * part, part)], parts)

    for d, p in every:
        if d > 0:
            pl.when(place < d)(lambda d=d, p=p: going_up(d, p).wait_send())
        if d < size - 1:
            pl.when(place > d)(lambda d=d, p=p: going_down(d, p).wait_send())
        if paired:
            to_mate(d, p).wait_send()


def scatter(x, size, paired, ident):
    copies = size * 2 if paired else size
    rows = x.shape[0] // copies
    pieces = pieces_of(rows, x.shape[1])
    dma = pltpu.SemaphoreType.DMA
    slots = pltpu.VMEM((size, rows, x.shape[1]), x.dtype)
    one = pltpu.VMEM((1, 32, 128), x.dtype)
    chain = slots if size > 1 else one
    return pl.pallas_call(
        functools.partial(scatter_kernel, size, paired, pieces),
        in_specs=[ANY],
        out_specs=IN_VMEM,
        out_shape=jax.ShapeDtypeStruct((rows, x.shape[1]), jnp.float32),
        scratch_shapes=[slots, slots if paired else one, chain, chain] + [dma((size, pieces))] * 7,
        compiler_params=pltpu.CompilerParams(collective_id=ident, has_side_effects=True, vmem_limit_bytes=60000000),
        cost_estimate=pl.CostEstimate(flops=0, bytes_accessed=30 * x.size, transcendentals=0),
        name="scatter",
    )(x)


def share_kernel(size, groups, kinds, count, *refs):
    whole = len(kinds)
    owns, refs = refs[:whole], refs[whole:]
    parts, refs = refs[:count], refs[count:]
    wholes, refs = refs[:whole], refs[whole:]
    slices, refs = refs[:count], refs[count:]
    local_sem, up_send, up_recv, down_send, down_recv, far_send, far_recv, swap_send, swap_recv = refs
    place, group = lax.axis_index("ctx"), lax.axis_index("dp")
    rows, width = slices[0].shape[0] // size, slices[0].shape[1]
    chained = [w for w in range(whole) if kinds[w][0]]
    crossing = [w for w in range(whole) if kinds[w][1]]
    last = size - 1
    barrier = pltpu.get_barrier_semaphore()
    for step in range(1, size):
        greet(barrier, {"ctx": lax.rem(place + step, size)})
    for step in range(1, groups):
        greet(barrier, {"dp": lax.rem(group + step, groups)})
    pl.semaphore_wait(barrier, size + groups - 2)

    def chunk(w, in_group, rank):
        along, over = kinds[w]
        index = (in_group * size + rank if along else in_group) if over else rank
        n = owns[w].shape[0]
        return wholes[w].at[pl.ds(pl.multiple_of(index * n, n), n)]

    def source(w, rank, k):
        return owns[w] if k == 0 else chunk(w, group, rank)

    def going_up(w, k):
        return remote(
            source(w, place - k, k), chunk(w, group, place - k), up_send.at[w, k], up_recv.at[w, k], {"ctx": place + 1}
        )

    def going_down(w, k):
        return remote(
            source(w, place + k, k), chunk(w, group, place + k), down_send.at[w, k], down_recv.at[w, k], {"ctx": place - 1}
        )

    def across(w, rank, step, k):
        slot = rank if kinds[w][0] else 0
        return remote(
            source(w, rank, k), chunk(w, group, rank),
            far_send.at[w, slot, step], far_recv.at[w, slot, step], {"dp": lax.rem(group + step, groups)},
        )

    def from_across(w, rank, step):
        slot = rank if kinds[w][0] else 0
        there = chunk(w, lax.rem(group - step + groups, groups), rank)
        return remote(
            there, there, far_send.at[w, slot, step], far_recv.at[w, slot, step], {"dp": lax.rem(group + step, groups)}
        )

    def columns(w, rank):
        return parts[w].at[:, pl.ds(pl.multiple_of(rank * width, 128), width)]

    def at_rank(w, rank):
        return slices[w].at[pl.ds(pl.multiple_of(rank * rows, rows), rows)]

    def swap(w, step):
        to = lax.rem(place + step, size)
        return remote(columns(w, to), at_rank(w, place), swap_send.at[w, step], swap_recv.at[w, step], {"ctx": to})

    def swapped(w, step):
        there = at_rank(w, lax.rem(place - step + size, size))
        return remote(
            there, there, swap_send.at[w, step], swap_recv.at[w, step], {"ctx": lax.rem(place + step, size)}
        )

    copies = [pltpu.make_async_copy(owns[w], chunk(w, group, place), local_sem.at[w]) for w in range(whole)]
    copies += [pltpu.make_async_copy(columns(w, place), at_rank(w, place), local_sem.at[whole + w]) for w in range(count)]
    for w in range(whole):
        if w in chained:
            pl.when(place < last)(lambda w=w: going_up(w, 0).start())
            pl.when(place > 0)(lambda w=w: going_down(w, 0).start())
        if w in crossing:
            for step in range(1, groups):
                across(w, place, step, 0).start()
    for copy in copies:
        copy.start()
    for k in range(last):
        for w in chained:

            @pl.when(place - 1 - k >= 0)
            def _(k=k, w=w):
                there = chunk(w, group, place - 1 - k)
                remote(there, there, up_send.at[w, k], up_recv.at[w, k], {"ctx": place - 1}).wait_recv()
                if k + 1 < last:
                    pl.when(place < last)(lambda: going_up(w, k + 1).start())
                if w in crossing:
                    for step in range(1, groups):
                        across(w, place - 1 - k, step, 1).start()

            @pl.when(place + 1 + k <= last)
            def _(k=k, w=w):
                there = chunk(w, group, place + 1 + k)
                remote(there, there, down_send.at[w, k], down_recv.at[w, k], {"ctx": place + 1}).wait_recv()
                if k + 1 < last:
                    pl.when(place > 0)(lambda: going_down(w, k + 1).start())
                if w in crossing:
                    for step in range(1, groups):
                        across(w, place + 1 + k, step, 1).start()

    for w in range(count):
        for step in range(1, size):
            swap(w, step).start()
    for w in crossing:
        for rank in range(size) if w in chained else [place]:
            for step in range(1, groups):
                from_across(w, rank, step).wait_recv()
    for w in range(count):
        for step in range(1, size):
            swapped(w, step).wait_recv()
    for copy in copies:
        copy.wait()
    for w in range(whole):
        if w in chained:
            for k in range(last):
                pl.when((place < last) & (place - k >= 0))(lambda k=k, w=w: going_up(w, k).wait_send())
                pl.when((place > 0) & (place + k <= last))(lambda k=k, w=w: going_down(w, k).wait_send())
        if w in crossing:
            for rank in range(size) if w in chained else [place]:
                for step in range(1, groups):
                    across(w, rank, step, 1).wait_send()
    for w in range(count):
        for step in range(1, size):
            swap(w, step).wait_send()


def share(wholes, kinds, parts, width, ident):
    size, groups = lax.axis_size("ctx"), lax.axis_size("dp")
    rows = parts[0].shape[0]
    dma = pltpu.SemaphoreType.DMA
    n, m = len(wholes), len(parts)
    shapes = [
        jax.ShapeDtypeStruct(((size if along else 1) * (groups if over else 1) * x.shape[0], x.shape[1]), x.dtype)
        for x, (along, over) in zip(wholes, kinds)
    ]
    shapes += [jax.ShapeDtypeStruct((size * rows, width), parts[0].dtype)] * m
    return pl.pallas_call(
        functools.partial(share_kernel, size, groups, kinds, m),
        in_specs=[IN_VMEM] * (n + m),
        out_specs=[ANY] * (n + m),
        out_shape=shapes,
        scratch_shapes=[dma((n + m,))] + [dma((n, size))] * 4 + [dma((n, size, groups))] * 2 + [dma((m, size))] * 2,
        compiler_params=pltpu.CompilerParams(collective_id=ident, has_side_effects=True),
        cost_estimate=pl.CostEstimate(flops=0, bytes_accessed=150000000, transcendentals=0),
    )(*wholes, *parts)


def back_kernel(
    size, groups, x_ref, s_ref, p_ref, w_ref, n_ref, o_ref, t_ref, g_ref, mine, far, near, part, pair, crowd, row, give, got,
    give_sems, own_sem, far_send, far_recv, near_send, near_recv, pair_sems, crowd_send, crowd_recv, row_send, row_recv,
):
    place, group = lax.axis_index("ctx"), lax.axis_index("dp")
    core = lax.axis_index("tensor")
    rows = o_ref.shape[0]
    barrier = pltpu.get_barrier_semaphore()

    def rank_at(k):
        return lax.rem(place + 1 + k, size)

    def block(in_group, rank):
        return x_ref.at[pl.ds(pl.multiple_of((in_group * size + rank) * rows, rows), rows)]

    def load(k):
        return pltpu.make_async_copy(block(group, rank_at(k)), mine.at[k], own_sem.at[k])

    def across(k, step):
        to = lax.rem(group + step, groups)
        return remote(block(to, rank_at(k)), far.at[k, step], far_send.at[k, step], far_recv.at[k, step], {"dp": to})

    def along(k):
        return remote(mine.at[k], near.at[k], near_send.at[k], near_recv.at[k], {"ctx": rank_at(k)})

    to_mate = remote(part, pair, pair_sems.at[0], pair_sems.at[1], {"tensor": 1 - core})
    half = remote(give, got, give_sems.at[0], give_sems.at[1], {"tensor": 1 - core})

    def product(which, target):
        own_rows, depth = target.shape
        step = column_step(depth)
        span = pl.ds(pl.multiple_of(which * own_rows, own_rows), own_rows)

        def some(j, carry):
            columns = pl.ds(pl.multiple_of(j * step, step), step)
            target[:, columns] = matmul_nt(p_ref[span, :], w_ref[columns, :])
            return carry

        lax.fori_loop(0, depth // step, some, 0)

    def gain_sums(i, total):
        span = pl.ds(pl.multiple_of(i * 32, 32), 32)
        grad = g_ref[span, :] + got[span, :]
        g_ref[span, :] = grad
        return total + jnp.sum(grad * n_ref[span, :], axis=0, keepdims=True)

    def to_crowd(step):
        return remote(
            crowd.at[group], crowd.at[group], crowd_send.at[step], crowd_recv.at[step],
            {"dp": lax.rem(group + step, groups)},
        )

    def to_row(step):
        return remote(
            row.at[place], row.at[place], row_send.at[step], row_recv.at[step], {"ctx": lax.rem(place + step, size)}
        )

    for k in range(size):
        load(k).start()
    for step in range(1, size):
        greet(barrier, {"ctx": lax.rem(place + step, size)})
    for step in range(1, groups):
        greet(barrier, {"dp": lax.rem(group + step, groups)})
    greet(barrier, {"tensor": 1 - core})
    pl.semaphore_wait(barrier, size + groups - 1)
    for k in range(size):
        for step in range(1, groups):
            across(k, step).start()
    product(1 - core, give)
    half.start()
    product(core, g_ref)
    part[...] = s_ref[...]
    half.wait_recv()
    gains = lax.fori_loop(0, g_ref.shape[0] // 32, gain_sums, jnp.zeros((1, g_ref.shape[1]), jnp.float32))
    for j in range(g_ref.shape[1] // 128):
        part[j : j + 1, :] = gains[:, j * 128 : (j + 1) * 128]
    to_mate.start()
    to_mate.wait_recv()
    crowd[group] = part[...] + pair[...]
    for step in range(1, groups):
        to_crowd(step).start()
    for step in range(1, groups):
        to_crowd(step).wait_recv()
    total = crowd[0]
    for g in range(1, groups):
        total += crowd[g]
    row[place] = total
    for step in range(1, size):
        to_row(step).start()
    for k in range(size):
        load(k).wait()
        for step in range(1, groups):
            across(k, step).wait_recv()
        parts = [mine.at[k]] + [far.at[k, step] for step in range(1, groups)]
        if k < size - 1:
            add_blocks(mine.at[k], parts)
            along(k).start()
    for k in range(size - 1):
        along(k).wait_recv()
        parts.append(near.at[k])
    add_blocks(o_ref, parts)
    for step in range(1, size):
        to_row(step).wait_recv()
    total = row[0]
    for c in range(1, size):
        total += row[c]
    t_ref[...] = total
    half.wait_send()
    to_mate.wait_send()
    for step in range(1, groups):
        to_crowd(step).wait_send()
    for step in range(1, size):
        to_row(step).wait_send()
    for k in range(size):
        for step in range(1, groups):
            across(k, step).wait_send()
        if k < size - 1:
            along(k).wait_send()


def back(x, small, grad_pre, weight, normed, ident):
    size, groups = lax.axis_size("ctx"), lax.axis_size("dp")
    rows, columns = x.shape[0] // (size * groups), x.shape[1]
    dma = pltpu.SemaphoreType.DMA
    return pl.pallas_call(
        functools.partial(back_kernel, size, groups),
        in_specs=[ANY] + [IN_VMEM] * 4,
        out_specs=[IN_VMEM] * 3,
        out_shape=[
            jax.ShapeDtypeStruct((rows, columns), jnp.float32),
            jax.ShapeDtypeStruct(small.shape, jnp.float32),
            jax.ShapeDtypeStruct(normed.shape, jnp.float32),
        ],
        scratch_shapes=[
            pltpu.VMEM((size, rows, columns), x.dtype),
            pltpu.VMEM((size, groups, rows, columns), x.dtype),
            pltpu.VMEM((size, rows, columns), x.dtype),
            pltpu.VMEM(small.shape, jnp.float32),
            pltpu.VMEM(small.shape, jnp.float32),
            pltpu.VMEM((groups,) + small.shape, jnp.float32),
            pltpu.VMEM((size,) + small.shape, jnp.float32),
            pltpu.VMEM(normed.shape, jnp.float32),
            pltpu.VMEM(normed.shape, jnp.float32),
            dma((2,)),
            dma((size,)),
            dma((size, groups)),
            dma((size, groups)),
            dma((size,)),
            dma((size,)),
            dma((2,)),
            dma((groups,)),
            dma((groups,)),
            dma((size,)),
            dma((size,)),
        ],
        compiler_params=pltpu.CompilerParams(collective_id=ident, has_side_effects=True, vmem_limit_bytes=60000000),
        cost_estimate=pl.CostEstimate(flops=0, bytes_accessed=100 * x.size, transcendentals=0),
        name="back",
    )(x, small, grad_pre, weight, normed)


def column_step(width):
    return max(t for t in (768, 384, 256, 128) if width % t == 0)


def expand_block(x_ref, weights, extra, stage):
    step = column_step(weights[0].shape[1])

    def some(j, carry):
        span = pl.ds(pl.multiple_of(j * step, step), step)
        gate = nn(x_ref[...], weights[0][:, span])
        up = nn(x_ref[...], weights[1][:, span])
        stage[0, :, span] = gate.astype(jnp.bfloat16)
        stage[1, :, span] = up.astype(jnp.bfloat16)
        stage[2, :, span] = (gate * jax.nn.sigmoid(gate) * up).astype(jnp.bfloat16)
        return carry

    lax.fori_loop(0, weights[0].shape[1] // step, some, 0)


def shrink_block(x_ref, weights, extra, stage):
    step = column_step(weights[0].shape[1])

    def some(j, carry):
        span = pl.ds(pl.multiple_of(j * step, step), step)
        grad = nn(x_ref[...], weights[0][:, span])
        gate = extra[0, :, span].astype(jnp.float32)
        up = extra[1, :, span].astype(jnp.float32)
        sigmoid = jax.nn.sigmoid(gate)
        stage[0, :, span] = (grad * up * sigmoid * (1.0 + gate * (1.0 - sigmoid))).astype(jnp.bfloat16)
        stage[1, :, span] = (grad * gate * sigmoid).astype(jnp.bfloat16)
        return carry

    lax.fori_loop(0, weights[0].shape[1] // step, some, 0)


def gather_apply_kernel(size, pieces, work, n_weights, n_extra, n_made, *refs):
    x_ref, refs = refs[0], refs[1:]
    weights_from, refs = refs[:n_weights], refs[n_weights:]
    extra_from, refs = refs[:n_extra], refs[n_extra:]
    o_ref, refs = refs[0], refs[1:]
    made_to, refs = refs[:n_made], refs[n_made:]
    weights, refs = refs[:n_weights], refs[n_weights:]
    extra, stage, refs = refs[0], refs[1], refs[2:]
    local_sem, weight_sem, extra_sem, stage_sem = refs[:4]
    up_send, up_recv, down_send, down_recv, mate_send, mate_recv = refs[4:]
    place = lax.axis_index("ctx")
    core = lax.axis_index("tensor")
    rows = x_ref.shape[0]
    part = rows // pieces
    last = size - 1

    loads = [pltpu.make_async_copy(weights_from[w], weights[w], weight_sem.at[w]) for w in range(n_weights)]
    for load in loads:
        load.start()

    def first_of(rank, which):
        return pl.multiple_of((rank * 2 + which) * rows, rows)

    def block(rank, which, p):
        return o_ref.at[pl.ds(pl.multiple_of((rank * 2 + which) * rows + p * part, part), part)]

    def going_up(k, p):
        there = block(place - k, core, p)
        return remote(there, there, up_send.at[k, p], up_recv.at[k, p], {"ctx": place + 1})

    def going_down(k, p):
        there = block(place + k, core, p)
        return remote(there, there, down_send.at[k, p], down_recv.at[k, p], {"ctx": place - 1})

    def coming_up(k, p):
        there = block(place - 1 - k, core, p)
        return remote(there, there, up_send.at[k, p], up_recv.at[k, p], {"ctx": place - 1})

    def coming_down(k, p):
        there = block(place + 1 + k, core, p)
        return remote(there, there, down_send.at[k, p], down_recv.at[k, p], {"ctx": place + 1})

    def to_mate(rank, p):
        there = block(rank, core, p)
        return remote(there, there, mate_send.at[rank, p], mate_recv.at[rank, p], {"tensor": 1 - core})

    def from_mate(rank, p):
        there = block(rank, 1 - core, p)
        return remote(there, there, mate_send.at[rank, p], mate_recv.at[rank, p], {"tensor": 1 - core})

    own = pltpu.make_async_copy(x_ref, o_ref.at[pl.ds(first_of(place, core), rows)], local_sem)
    own.start()
    greet_chain(size, True)
    own.wait()
    for p in range(pieces):
        pl.when(place < last)(lambda p=p: going_up(0, p).start())
        pl.when(place > 0)(lambda p=p: going_down(0, p).start())
    for p in range(pieces):
        to_mate(place, p).start()

    def forward(d):
        for p in range(pieces):

            @pl.when(place - d >= 0)
            def _(p=p):
                coming_up(d - 1, p).wait_recv()
                pl.when(place < last)(lambda: going_up(d, p).start())
                to_mate(place - d, p).start()

            @pl.when(place + d <= last)
            def _(p=p):
                coming_down(d - 1, p).wait_recv()
                pl.when(place > 0)(lambda: going_down(d, p).start())
                to_mate(place + d, p).start()

    for load in loads:
        load.wait()
    short = jnp.minimum(place, last - place)

    def distance(s):
        return jnp.where(s <= 2 * short, (s + 1) // 2, s - short)

    def extra_load(rank, which, slot, e):
        return pltpu.make_async_copy(
            extra_from[e].at[pl.ds(first_of(rank, which), rows)], extra.at[slot, e], extra_sem.at[slot, e]
        )

    def store(rank, which, slot, m):
        return pltpu.make_async_copy(
            stage.at[slot, m], made_to[m].at[pl.ds(first_of(rank, which), rows)], stage_sem.at[slot, m]
        )

    def visit(s, carry):
        d = distance(s)
        below = jnp.where(s <= 2 * short, s % 2 == 1, place > last - place)
        rank = jnp.where(below, place - d, place + d)
        for slot, which in enumerate((core, 1 - core)):
            for e in range(n_extra):
                extra_load(rank, which, slot, e).start()
        pl.when((s > 0) & (d != distance(s - 1)))(lambda: forward(d))
        for slot, which in enumerate((core, 1 - core)):
            if slot == 1:
                for p in range(pieces):
                    from_mate(rank, p).wait_recv()
            for e in range(n_extra):
                extra_load(rank, which, slot, e).wait()

            @pl.when(s > 0)
            def _():
                for m in range(n_made):
                    store(rank, which, slot, m).wait()

            work(o_ref.at[pl.ds(first_of(rank, which), rows)], weights, extra.at[slot], stage.at[slot])
            for m in range(n_made):
                store(rank, which, slot, m).start()
        return carry

    lax.fori_loop(0, size, visit, 0)
    for slot, which in enumerate((core, 1 - core)):
        for m in range(n_made):
            store(place, which, slot, m).wait()
    for p in range(pieces):
        for k in range(last):
            pl.when((place < last) & (place - k >= 0))(lambda k=k, p=p: going_up(k, p).wait_send())
            pl.when((place > 0) & (place + k <= last))(lambda k=k, p=p: going_down(k, p).wait_send())
        for rank in range(size):
            to_mate(rank, p).wait_send()


def gather_apply(x, weights, extra, work, n_made, ident):
    size = lax.axis_size("ctx")
    rows, width = x.shape[0], weights[0].shape[1]
    total = 2 * size * rows
    pieces = pieces_of(*x.shape)
    dma = pltpu.SemaphoreType.DMA
    made = jax.ShapeDtypeStruct((total, width), jnp.bfloat16)
    slots = max(1, len(extra))
    return pl.pallas_call(
        functools.partial(gather_apply_kernel, size, pieces, work, len(weights), len(extra), n_made),
        in_specs=[IN_VMEM] + [ANY] * (len(weights) + len(extra)),
        out_specs=[IN_VMEM] + [ANY] * n_made,
        out_shape=[jax.ShapeDtypeStruct((total, x.shape[1]), x.dtype)] + [made] * n_made,
        scratch_shapes=[pltpu.VMEM(w.shape, w.dtype) for w in weights]
        + [
            pltpu.VMEM((2, slots, rows, width) if extra else (2, 1, 16, 128), jnp.bfloat16),
            pltpu.VMEM((2, n_made, rows, width), jnp.bfloat16),
            dma,
            dma((len(weights),)),
            dma((2, slots)),
            dma((2, n_made)),
        ]
        + [dma((size, pieces))] * 6,
        compiler_params=pltpu.CompilerParams(collective_id=ident, has_side_effects=True, vmem_limit_bytes=60000000),
        cost_estimate=pl.CostEstimate(flops=0, bytes_accessed=200000000, transcendentals=0),
    )(x, *weights, *extra)


def sum_apply_kernel(size, pieces, count, *refs):
    acts_from, refs = refs[:count], refs[count:]
    weights_from, refs = refs[:count], refs[count:]
    o_ref, acts, weights, mine, sent, mate, came, load_sem = refs[:8]
    mate_send, mate_recv, up_send, up_recv, down_send, down_recv = refs[8:]
    place, core = lax.axis_index("ctx"), lax.axis_index("tensor")
    rows, depth = o_ref.shape
    part = rows // pieces
    last = size - 1

    loads = []
    for a in range(count):
        loads.append(pltpu.make_async_copy(weights_from[a], weights.at[a], load_sem.at[a]))
        loads.append(pltpu.make_async_copy(acts_from[a], acts.at[a], load_sem.at[count + a]))
    for load in loads:
        load.start()
    greet_chain(size, True)
    for load in loads:
        load.wait()

    def at(ref, d, p):
        return ref.at[d, pl.ds(p * part, part)]

    def to_mate(i, d, p):
        slot = lax.rem(i, 2)
        return remote(at(sent, slot, p), at(mate, d, p), mate_send.at[slot, p], mate_recv.at[d, p], {"tensor": 1 - core})

    def going_up(d, p):
        return remote(at(mine, d, p), at(came, d, p), up_send.at[d, p], up_recv.at[d, p], {"ctx": place + 1})

    def going_down(d, p):
        there = jnp.where(d == place - 1, size, d)
        return remote(at(mine, d, p), at(came, there, p), down_send.at[d, p], down_recv.at[d, p], {"ctx": place - 1})

    def coming_up(d, p):
        there = at(came, d, p)
        return remote(there, there, up_send.at[d, p], up_recv.at[d, p], {"ctx": place - 1})

    def coming_down(d, p):
        there = at(came, jnp.where(d == place, size, d), p)
        return remote(there, there, down_send.at[d, p], down_recv.at[d, p], {"ctx": place + 1})

    def compute(d, which, target):
        step = column_step(depth)
        span = pl.ds(pl.multiple_of((d * 2 + which) * rows, rows), rows)

        def some(j, carry):
            columns = pl.ds(pl.multiple_of(j * step, step), step)
            total = matmul_nt(acts[0, span, :], weights[0, columns, :])
            for a in range(1, count):
                total += matmul_nt(acts[a, span, :], weights[a, columns, :])
            target[:, columns] = total.astype(target.dtype)
            return carry

        lax.fori_loop(0, depth // step, some, 0)

    def with_mate(d, p):
        to_mate(0, d, p).wait_recv()
        return [at(mine, d, p), at(mate, d, p)]

    short = jnp.minimum(place, last - place)

    def first_part(i, carry):
        s = last - i
        near = s <= 2 * short
        d = jnp.where(near, (s + 1) // 2, s - short)
        d = jnp.where(jnp.where(near, s % 2 == 1, place > last - place), place - d, place + d)
        for p in range(pieces):
            pl.when(i >= 2)(lambda p=p: to_mate(i, d, p).wait_send())
        compute(d, 1 - core, sent.at[lax.rem(i, 2)])
        for p in range(pieces):
            to_mate(i, d, p).start()
        compute(d, core, mine.at[d])

        @pl.when((place == 0) & (d > 0))
        def _():
            for p in range(pieces):
                add_blocks(at(mine, d, p), with_mate(d, p))
                going_up(d, p).start()

        @pl.when((place == last) & (d < last))
        def _():
            for p in range(pieces):
                add_blocks(at(mine, d, p), with_mate(d, p))
                going_down(d, p).start()

        return carry

    lax.fori_loop(0, size, first_part, 0)

    def second_part(s, carry):
        k, p = s // pieces, s % pieces

        @pl.when((place > 0) & (place < last - k))
        def _():
            d = last - k
            parts = with_mate(d, p)
            coming_up(d, p).wait_recv()
            add_blocks(at(mine, d, p), parts + [at(came, d, p)])
            going_up(d, p).start()

        @pl.when((place < last) & (place > k))
        def _():
            parts = with_mate(k, p)
            coming_down(k, p).wait_recv()
            add_blocks(at(mine, k, p), parts + [at(came, k, p)])
            going_down(k, p).start()

        return carry

    lax.fori_loop(0, last * pieces, second_part, 0)

    def final(p, carry):
        target = o_ref.at[pl.ds(pl.multiple_of(p * part, part), part)]
        parts = with_mate(place, p)
        pl.when(place > 0)(lambda: coming_up(place, p).wait_recv())
        pl.when(place < last)(lambda: coming_down(place, p).wait_recv())
        up, down = at(came, place, p), at(came, size, p)
        pl.when(place == 0)(lambda: add_blocks(target, parts + [down]))
        pl.when(place == last)(lambda: add_blocks(target, parts + [up]))
        pl.when((place > 0) & (place < last))(lambda: add_blocks(target, parts + [up, down]))
        return carry

    lax.fori_loop(0, pieces, final, 0)
    for p in range(pieces):
        for i in range(size - 2, size):
            to_mate(i, 0, p).wait_send()
        for d in range(size):
            pl.when(place < d)(lambda d=d, p=p: going_up(d, p).wait_send())
            pl.when(place > d)(lambda d=d, p=p: going_down(d, p).wait_send())


def sum_apply(acts, weights, ident):
    size, count = lax.axis_size("ctx"), len(acts)
    total, width = acts[0].shape
    depth = weights[0].shape[0]
    block = total // (2 * size)
    pieces = pieces_of(block, depth)
    dma = pltpu.SemaphoreType.DMA

    def slots(n):
        return pltpu.VMEM((n, block, depth), jnp.bfloat16)

    scratch = [
        pltpu.VMEM((count, total, width), jnp.bfloat16),
        pltpu.VMEM((count, depth, width), jnp.bfloat16),
        slots(size),
        slots(2),
        slots(size),
        slots(size + 1),
        dma((2 * count,)),
        dma((2, pieces)),
    ] + [dma((size, pieces))] * 5
    return pl.pallas_call(
        functools.partial(sum_apply_kernel, size, pieces, count),
        in_specs=[ANY] * (2 * count),
        out_specs=IN_VMEM,
        out_shape=jax.ShapeDtypeStruct((block, depth), jnp.float32),
        scratch_shapes=scratch,
        compiler_params=pltpu.CompilerParams(collective_id=ident, has_side_effects=True, vmem_limit_bytes=60000000),
        cost_estimate=pl.CostEstimate(flops=0, bytes_accessed=200000000, transcendentals=0),
    )(*acts, *weights)


def assemble_kernel(size, ranks_ref, *refs):
    parts, (down_ref, gate_ref, up_ref, whole) = refs[:size], refs[size:]
    width = parts[0].shape[2]
    for which, target in enumerate((down_ref, gate_ref, up_ref)):
        for part, k in zip(parts, range(size)):
            whole[:, pl.ds(pl.multiple_of(ranks_ref[k] * width, 128), width)] = part[which].astype(jnp.float32)
        target[...] = whole[:, : gate_ref.shape[1]]


def assemble(received, columns):
    ranks = jnp.stack([rank for rank, _ in received]).astype(jnp.int32)
    blocks = [block for _, block in received]
    _, rows, width = blocks[0].shape
    f32 = jnp.float32
    return pl.pallas_call(
        functools.partial(assemble_kernel, len(blocks)),
        in_specs=[pl.BlockSpec(memory_space=pltpu.SMEM)] + [IN_VMEM] * len(blocks),
        out_specs=[IN_VMEM] * 3,
        out_shape=[jax.ShapeDtypeStruct((rows, columns), f32)] * 3,
        scratch_shapes=[pltpu.VMEM((rows, len(blocks) * width), f32)],
        compiler_params=pltpu.CompilerParams(vmem_limit_bytes=60000000),
        cost_estimate=pl.CostEstimate(flops=0, bytes_accessed=20 * rows * columns, transcendentals=0),
        name="assemble",
    )(ranks, *blocks)


def mask_into(bias_ref, first, seg_ref, place_ref):
    keys, rows = bias_ref.shape
    key_index = lax.broadcasted_iota(jnp.int32, (keys, rows), 0)
    row_index = lax.broadcasted_iota(jnp.int32, (keys, rows), 1) + first
    place = jnp.broadcast_to(place_ref[...], (keys, rows))
    start = jnp.broadcast_to(seg_ref[...], (keys, rows))
    allowed = ((place >= start) & (place <= row_index)) | (key_index == row_index)
    bias_ref[...] = jnp.where(allowed, 0.0, VERY_LOW)


def attend_kernel(scale, first_ref, seg_ref, place_ref, q_ref, k_ref, vt_ref, o_ref, lse_ref, bias_ref):
    @pl.when(pl.program_id(1) == 0)
    def _():
        mask_into(bias_ref, first_ref[0] + pl.program_id(0) * q_ref.shape[0], seg_ref, place_ref)

    scores = matmul_nt(k_ref[...], q_ref[...]) * scale + bias_ref[...]
    top = jnp.max(scores, axis=0, keepdims=True)
    powers = jnp.exp(scores - top)
    total = jnp.sum(powers, axis=0, keepdims=True)
    mixture = nn(vt_ref[...], powers.astype(jnp.bfloat16)) / total
    o_ref[...] = mixture.T.astype(jnp.bfloat16)
    lse_ref[0] = top + jnp.log(total)


def attend_back_kernel(
    scale, first_ref, seg_ref, place_ref, q_ref, do_ref, lse_ref, k_ref, v_ref, kt_ref,
    dq_ref, dkv_ref, bias_ref, dk_ref, dv_ref,
):
    block, head = pl.program_id(0), pl.program_id(1)

    @pl.when(head == 0)
    def _():
        mask_into(bias_ref, first_ref[0] + block * q_ref.shape[0], seg_ref, place_ref)

    @pl.when((head == 0) & (block == 0))
    def _():
        dk_ref[...] = jnp.zeros_like(dk_ref)
        dv_ref[...] = jnp.zeros_like(dv_ref)

    query, grad = q_ref[...], do_ref[...]
    scores = matmul_nt(k_ref[...], query) * scale + bias_ref[...]
    probs = jnp.exp(scores - lse_ref[0])
    grad_probs = matmul_nt(v_ref[...], grad)
    delta = jnp.sum(probs * grad_probs, axis=0, keepdims=True)
    grad_scores = (probs * (grad_probs - delta)).astype(jnp.bfloat16)
    dv_ref[...] += nn(probs.astype(jnp.bfloat16), grad)
    dk_ref[...] += nn(grad_scores, query)
    dq_ref[...] = (nn(kt_ref[...], grad_scores) * scale).T

    @pl.when((head == pl.num_programs(1) - 1) & (block == pl.num_programs(0) - 1))
    def _():
        dkv_ref[:, :HEAD] = (dk_ref[...] * scale).astype(jnp.bfloat16)
        dkv_ref[:, HEAD:] = dv_ref[...].astype(jnp.bfloat16)


def attention_calls(rows, keys, heads):
    block = math.gcd(256, rows)
    scale = 1.0 / math.sqrt(HEAD)
    smem = pl.BlockSpec(memory_space=pltpu.SMEM)
    seg = pl.BlockSpec((1, block), lambda i, h: (0, i))
    place = pl.BlockSpec((keys, 1), lambda i, h: (0, 0))
    head = pl.BlockSpec((block, HEAD), lambda i, h: (i, h))
    lse = pl.BlockSpec((1, 1, block), lambda i, h: (h, 0, i))
    tall = pl.BlockSpec((keys, HEAD), lambda i, h: (0, 0))
    wide = pl.BlockSpec((HEAD, keys), lambda i, h: (0, 0))
    params = pltpu.CompilerParams(vmem_limit_bytes=60000000)
    grid = (rows // block, heads)
    size = heads * rows * keys
    forward = pl.pallas_call(
        functools.partial(attend_kernel, scale),
        grid=grid,
        in_specs=[smem, seg, place, head, tall, wide],
        out_specs=[head, lse],
        out_shape=[
            jax.ShapeDtypeStruct((rows, heads * HEAD), jnp.bfloat16),
            jax.ShapeDtypeStruct((heads, 1, rows), jnp.float32),
        ],
        scratch_shapes=[pltpu.VMEM((keys, block), jnp.float32)],
        compiler_params=params,
        cost_estimate=pl.CostEstimate(flops=4 * size * HEAD, bytes_accessed=4 * rows * heads * HEAD, transcendentals=size),
        name="attend",
    )
    backward = pl.pallas_call(
        functools.partial(attend_back_kernel, scale),
        grid=grid,
        in_specs=[smem, seg, place, head, head, lse, tall, tall, wide],
        out_specs=[head, pl.BlockSpec((keys, 2 * HEAD), lambda i, h: (0, 0))],
        out_shape=[
            jax.ShapeDtypeStruct((rows, heads * HEAD), jnp.float32),
            jax.ShapeDtypeStruct((keys, 2 * HEAD), jnp.bfloat16),
        ],
        scratch_shapes=[
            pltpu.VMEM((keys, block), jnp.float32),
            pltpu.VMEM((keys, HEAD), jnp.float32),
            pltpu.VMEM((keys, HEAD), jnp.float32),
        ],
        compiler_params=params,
        cost_estimate=pl.CostEstimate(flops=10 * size * HEAD, bytes_accessed=8 * rows * heads * HEAD, transcendentals=size),
        name="attend_back",
    )
    return forward, backward


def per_device(
    layer_input,
    teacher,
    cotangent,
    segment_ids,
    positions,
    valid_mask,
    gain_attn,
    query_weight,
    query_bias,
    key_weight,
    key_bias,
    value_weight,
    value_bias,
    out_weight,
    gain_mlp,
    gate_weight,
    up_weight,
    down_weight,
):
    tensor_rank = lax.axis_index("tensor")
    ctx_rank = lax.axis_index("ctx")
    tensor_size, ctx_size = lax.axis_size("tensor"), lax.axis_size("ctx")
    own_rows = layer_input.shape[0]
    shard_rows = own_rows * tensor_size
    seq_len = segment_ids.shape[0]
    q_width = query_weight.shape[1]
    kv_width = key_weight.shape[1]
    kv_local = kv_width // HEAD
    group = q_width // kv_width
    hidden_width = gate_weight.shape[1]
    slice_width = -(-hidden_width // (128 * ctx_size)) * 128
    first_row = ctx_rank * shard_rows
    own_first = first_row + tensor_rank * own_rows

    inputs = layer_input.astype(jnp.float32)
    gain_one = gain_attn.astype(jnp.float32)
    gain_two = gain_mlp.astype(jnp.float32)
    scale_attn = lax.rsqrt(jnp.mean(inputs * inputs, axis=1, keepdims=True) + EPS)
    normed_attn = inputs * scale_attn
    extra = ((0, 0), (0, ctx_size * slice_width - hidden_width))
    full_qkv, *slices = share(
        [jnp.concatenate([query_weight, key_weight, value_weight], axis=1)],
        ((True, True),),
        [jnp.pad(w, extra) for w in (gate_weight, up_weight)],
        slice_width,
        1,
    )
    full_gate, full_up = [lax.all_gather(w, "dp", axis=0, tiled=True) for w in slices]
    normed_rows = gather((normed_attn * gain_one).astype(jnp.bfloat16), 1, True, 2)
    bias = jnp.concatenate(
        [
            lax.dynamic_slice_in_dim(query_bias, tensor_rank * q_width, q_width),
            lax.dynamic_slice_in_dim(key_bias, tensor_rank * kv_width, kv_width),
            lax.dynamic_slice_in_dim(value_bias, tensor_rank * kv_width, kv_width),
        ]
    ).astype(jnp.float32)
    places = lax.dynamic_slice_in_dim(positions, first_row, shard_rows)
    cosine, sine_table = rope_tables(places)
    qkv_pre = matmul(normed_rows, full_qkv) + bias
    turned = q_width + kv_width
    rotated = (
        rotate(qkv_pre[:, :turned].reshape(shard_rows, turned // HEAD, HEAD), cosine, sine_table)
        .astype(jnp.bfloat16)
        .reshape(shard_rows, turned)
    )
    queries = rotated[:, :q_width]
    own_kv = jnp.concatenate([rotated[:, q_width:], qkv_pre[:, turned:].astype(jnp.bfloat16)], axis=1)
    own_count = jnp.full((8, 128), jnp.sum(valid_mask.astype(jnp.float32)))
    all_kv, full_out, counts, down_slice = share(
        [own_kv, out_weight.T, own_count],
        ((True, False), (True, True), (False, True)),
        [jnp.pad(down_weight.T, extra)],
        slice_width,
        3,
    )
    full_down = lax.all_gather(down_slice, "dp", axis=0, tiled=True)
    valid_count = jnp.sum(counts[::8, 0])

    key_index = jnp.arange(seq_len, dtype=jnp.int32)
    key_place = jnp.where(valid_mask > 0, key_index, -1)[:, None]
    seq_first = lax.axis_index("dp") * seq_len
    doc_start = (lax.dynamic_slice_in_dim(segment_ids, first_row, shard_rows) - seq_first)[None, :]
    first = jnp.reshape(first_row, (1,)).astype(jnp.int32)
    forward, backward = attention_calls(shard_rows, seq_len, group)
    kept = []
    for c in range(kv_local):
        key = all_kv[:, c * HEAD : (c + 1) * HEAD]
        value = all_kv[:, kv_width + c * HEAD : kv_width + (c + 1) * HEAD]
        query = queries[:, c * group * HEAD : (c + 1) * group * HEAD]
        kept.append((query, key, value) + tuple(forward(first, doc_start, key_place, query, key, value.T)))
    heads_out = jnp.concatenate([k[3] for k in kept], axis=1)
    attention = scatter(matmul_nt(heads_out, full_out), 1, True, 4)
    residual_mid = inputs + attention
    scale_mlp = lax.rsqrt(jnp.mean(residual_mid * residual_mid, axis=1, keepdims=True) + EPS)
    normed_mlp = residual_mid * scale_mlp
    mlp_rows, gate_act, up_act, hidden = gather_apply(
        (normed_mlp * gain_two).astype(jnp.bfloat16), [full_gate, full_up], [], expand_block, 3, 5
    )
    branch = sum_apply([hidden], [full_down], 6)
    layer_result = residual_mid + branch
    valid_own = lax.dynamic_slice_in_dim(valid_mask, own_first, own_rows).astype(jnp.float32)
    difference = layer_result - teacher.astype(jnp.float32)
    squared_sum = jnp.sum(valid_own[:, None] * difference * difference)
    grad_result = cotangent.astype(jnp.float32) + 2.0 * valid_own[:, None] * difference / (
        valid_count * D
    )
    grad_branch, grad_gate_act, grad_up_act = gather_apply(
        grad_result.astype(jnp.bfloat16), [full_down], [gate_act, up_act], shrink_block, 2, 9
    )
    summed = []
    for left, right in ((grad_branch, hidden), (mlp_rows, grad_gate_act), (mlp_rows, grad_up_act)):
        grad = matmul_tn(left, right).astype(jnp.bfloat16)
        grad_gate_act, grad_up_act, grad = lax.optimization_barrier((grad_gate_act, grad_up_act, grad))
        summed.append(lax.psum_scatter(grad, "dp", scatter_dimension=0, tiled=True))
    grad_mlp_rows = sum_apply([grad_gate_act, grad_up_act], [full_gate, full_up], 10)
    grad_gain_mlp = jnp.sum(grad_mlp_rows * normed_mlp, axis=0)
    grad_mid = grad_result + norm_back(grad_mlp_rows, normed_mlp, scale_mlp, gain_two)
    grad_attn_rows = gather(grad_mid.astype(jnp.bfloat16), 1, True, 2)
    grad_heads = matmul(grad_attn_rows, full_out).astype(jnp.bfloat16)
    grad_out = matmul_tn(grad_attn_rows, heads_out).astype(jnp.bfloat16)

    grad_out = lax.psum_scatter(grad_out, "dp", scatter_dimension=0, tiled=True)
    query_grads, key_grads, value_grads = [], [], []
    for c in range(kv_local):
        query, key, value, _, log_total = kept[c]
        span = slice(c * group * HEAD, (c + 1) * group * HEAD)
        grad_query, grad_kv = backward(
            first, doc_start, key_place, query, grad_heads[:, span], log_total, key, value, key.T
        )
        query_grads.append(grad_query)
        key_grads.append(grad_kv[:, :HEAD])
        value_grads.append(grad_kv[:, HEAD:])
    grad_kv = grad_kv if kv_local == 1 else jnp.concatenate(key_grads + value_grads, axis=1)
    grad_kv = scatter(grad_kv, ctx_size, False, 7)
    grad_kv, *summed = lax.optimization_barrier((grad_kv, *summed))
    shard_down, shard_gate, shard_up = to_rows(summed, hidden_width)
    shard_down = shard_down.T
    grad_turned = jnp.concatenate(query_grads + [grad_kv[:, :kv_width]], axis=1)
    grad_pre = jnp.concatenate(
        [
            rotate(grad_turned.reshape(shard_rows, turned // HEAD, HEAD), cosine, -sine_table)
            .reshape(shard_rows, turned)
            .astype(jnp.bfloat16),
            grad_kv[:, kv_width:].astype(jnp.bfloat16),
        ],
        axis=1,
    )
    grad_pre, grad_out = lax.optimization_barrier((grad_pre, grad_out))
    shard_out = lax.psum_scatter(grad_out, "ctx", scatter_dimension=0, tiled=True)
    shard_out = shard_out.astype(jnp.float32).T
    bias_sum = jnp.sum(grad_pre.astype(jnp.float32), axis=0)

    def spread(part, size):
        return lax.dynamic_update_slice_in_dim(
            jnp.zeros((size,), jnp.float32), part, tensor_rank * part.shape[0], 0
        )

    loss_part = jnp.zeros((128,), jnp.float32).at[0].set(squared_sum)
    parts = [
        jnp.zeros((D,), jnp.float32),
        grad_gain_mlp,
        spread(bias_sum[:q_width], query_bias.shape[0]),
        spread(bias_sum[q_width:turned], key_bias.shape[0]),
        spread(bias_sum[turned:], value_bias.shape[0]),
        loss_part,
    ]
    flat = jnp.concatenate(parts)
    small = jnp.pad(flat, (0, -flat.shape[0] % 1024)).reshape(-1, 128)
    grad_qkv = matmul_tn(normed_rows, grad_pre).astype(jnp.bfloat16)
    shard_qkv, sums, grad_normed = back(grad_qkv, small, grad_pre, full_qkv, normed_attn, 8)
    grad_input = grad_mid + norm_back(grad_normed, normed_attn, scale_attn, gain_one)
    sums = sums.reshape(-1)
    pieces, offset = [], 0
    for part in parts:
        pieces.append(sums[offset : offset + part.shape[0]])
        offset += part.shape[0]
    return (
        layer_result.astype(jnp.bfloat16),
        pieces[5][0] / (valid_count * D),
        grad_input,
        pieces[0],
        shard_qkv[:, :q_width],
        pieces[2],
        shard_qkv[:, q_width:turned],
        pieces[3],
        shard_qkv[:, turned:],
        pieces[4],
        shard_out,
        pieces[1],
        shard_gate,
        shard_up,
        shard_down,
    )


def solution(mesh):
    in_specs = (
        P(("dp", "ctx", "tensor"), None),
        P(("dp", "ctx", "tensor"), None),
        P(("dp", "ctx", "tensor"), None),
        P("dp"),
        P("dp"),
        P("dp"),
        P(),
        P(("dp", "ctx"), "tensor"),
        P(),
        P(("dp", "ctx"), "tensor"),
        P(),
        P(("dp", "ctx"), "tensor"),
        P(),
        P("tensor", ("dp", "ctx")),
        P(),
        P(("dp", "ctx"), "tensor"),
        P(("dp", "ctx"), "tensor"),
        P("tensor", ("dp", "ctx")),
    )
    out_specs = (
        P(("dp", "ctx", "tensor"), None),
        P(),
        P(("dp", "ctx", "tensor"), None),
        P(),
        P(("dp", "ctx"), "tensor"),
        P(),
        P(("dp", "ctx"), "tensor"),
        P(),
        P(("dp", "ctx"), "tensor"),
        P(),
        P("tensor", ("dp", "ctx")),
        P(),
        P(("dp", "ctx"), "tensor"),
        P(("dp", "ctx"), "tensor"),
        P("tensor", ("dp", "ctx")),
    )

    return jax.shard_map(per_device, mesh=mesh, in_specs=in_specs, out_specs=out_specs, check_vma=False)
```

```python
import functools
import math

import jax
import jax.numpy as jnp
from jax import lax
from jax.experimental import pallas as pl
from jax.experimental.pallas import tpu as pltpu
from jax.sharding import PartitionSpec as P


D = 1536
HEAD = 128


EPS = 1e-06
THETA = 10000.0
VERY_LOW = -1e30


def rope_tables(places):
    half_dim = HEAD // 2
    frequency = THETA ** (-(jnp.arange(half_dim, dtype=jnp.float32) * 2.0 / HEAD))
    angles = places.astype(jnp.float32)[:, None] * frequency[None, :]
    return (jnp.cos(angles), jnp.sin(angles))


def rotate(stacked, cosine, sine_table):
    half_dim = HEAD // 2
    first_half = stacked[..., :half_dim]
    second_half = stacked[..., half_dim:]
    cosine = cosine[:, None, :]
    sine_table = sine_table[:, None, :]
    return jnp.concatenate(
        [
            first_half * cosine - second_half * sine_table,
            second_half * cosine + first_half * sine_table,
        ],
        axis=-1,
    )


def matmul(first_op, second_op):
    return jnp.dot(first_op, second_op, preferred_element_type=jnp.float32)


def matmul_tn(first_op, second_op):
    return lax.dot_general(
        first_op, second_op, (((0,), (0,)), ((), ())), preferred_element_type=jnp.float32
    )


def matmul_nt(first_op, second_op):
    return lax.dot_general(
        first_op, second_op, (((1,), (1,)), ((), ())), preferred_element_type=jnp.float32
    )


def norm_back(grad_normed, normed, inverse, gain):
    scaled = grad_normed * gain
    return inverse * (scaled - normed * jnp.mean(scaled * normed, axis=1, keepdims=True))


def exchange(blocks, axis):
    size = lax.axis_size(axis)
    rank = lax.axis_index(axis)
    received = [(rank, lax.dynamic_index_in_dim(blocks, rank, 0, keepdims=False))]
    for step in range(1, size):
        going = lax.dynamic_index_in_dim(blocks, (rank + step) % size, 0, keepdims=False)
        came = lax.ppermute(going, axis, [(i, (i + step) % size) for i in range(size)])
        received.append(((rank - step + size) % size, came))
    return received


def to_rows(summed, columns):
    size = lax.axis_size("ctx")
    rows, width = summed[0].shape[0] // size, summed[0].shape[1]
    blocks = jnp.stack([s.reshape(size, rows, width) for s in summed], axis=1)
    return assemble(exchange(blocks, "ctx"), columns)


def nn(first_op, second_op):
    return jnp.dot(first_op, second_op, preferred_element_type=jnp.float32)


MESH = pl.DeviceIdType.MESH
ANY = pl.BlockSpec(memory_space=pl.ANY)
IN_VMEM = pl.BlockSpec(memory_space=pltpu.VMEM)


def remote(source, target, send_sem, recv_sem, device):
    return pltpu.make_async_remote_copy(
        src_ref=source,
        dst_ref=target,
        send_sem=send_sem,
        recv_sem=recv_sem,
        device_id=device,
        device_id_type=MESH,
    )


def greet(barrier, device):
    pl.semaphore_signal(barrier, inc=1, device_id=device, device_id_type=MESH)


def greet_chain(size, paired):
    place = lax.axis_index("ctx")
    barrier = pltpu.get_barrier_semaphore()
    if size > 1:
        pl.when(place < size - 1)(lambda: greet(barrier, {"ctx": place + 1}))
        pl.when(place > 0)(lambda: greet(barrier, {"ctx": place - 1}))
    if paired:
        greet(barrier, {"tensor": 1 - lax.axis_index("tensor")})
    if size == 1:
        pl.semaphore_wait(barrier, 1)
        return
    ends = (place == 0) | (place == size - 1)
    pl.when(ends)(lambda: pl.semaphore_wait(barrier, 1 + paired))
    pl.when(jnp.logical_not(ends))(lambda: pl.semaphore_wait(barrier, 2 + paired))


def gather_kernel(size, paired, pieces, x_ref, o_ref, local_sem, up_send, up_recv, down_send, down_recv, mate_send, mate_recv):
    place = lax.axis_index("ctx") if size > 1 else 0
    core = lax.axis_index("tensor")
    rows = x_ref.shape[0]
    part = rows // pieces
    greet_chain(size, paired)

    def block(rank, which, p):
        index = rank * 2 + which if paired else rank
        return o_ref.at[pl.ds(pl.multiple_of(index * rows + p * part, part), part)]

    def source(rank, k, p):
        return x_ref.at[pl.ds(p * part, part)] if k == 0 else block(rank, core, p)

    def going_up(k, p):
        return remote(
            source(place - k, k, p), block(place - k, core, p), up_send.at[k, p], up_recv.at[k, p], {"ctx": place + 1}
        )

    def going_down(k, p):
        return remote(
            source(place + k, k, p), block(place + k, core, p), down_send.at[k, p], down_recv.at[k, p], {"ctx": place - 1}
        )

    def to_mate(rank, k, p):
        return remote(
            source(rank, k, p), block(rank, core, p), mate_send.at[k, p], mate_recv.at[rank, p], {"tensor": 1 - core}
        )

    def from_mate(rank, p):
        there = block(rank, 1 - core, p)
        return remote(there, there, mate_send.at[0, p], mate_recv.at[rank, p], {"tensor": 1 - core})

    own = pltpu.make_async_copy(x_ref, o_ref.at[pl.ds(pl.multiple_of((place * 2 + core if paired else place) * rows, rows), rows)], local_sem)
    for p in range(pieces):
        if size > 1:
            pl.when(place < size - 1)(lambda p=p: going_up(0, p).start())
            pl.when(place > 0)(lambda p=p: going_down(0, p).start())
    for p in range(pieces):
        if paired:
            to_mate(place, 0, p).start()
    own.start()
    for k in range(size - 1):
        for p in range(pieces):

            @pl.when(place - 1 - k >= 0)
            def _(k=k, p=p):
                there = block(place - 1 - k, core, p)
                remote(there, there, up_send.at[k, p], up_recv.at[k, p], {"ctx": place - 1}).wait_recv()
                if k + 1 < size - 1:
                    pl.when(place < size - 1)(lambda: going_up(k + 1, p).start())
                if paired:
                    to_mate(place - 1 - k, 1 + k, p).start()

            @pl.when(place + 1 + k <= size - 1)
            def _(k=k, p=p):
                there = block(place + 1 + k, core, p)
                remote(there, there, down_send.at[k, p], down_recv.at[k, p], {"ctx": place + 1}).wait_recv()
                if k + 1 < size - 1:
                    pl.when(place > 0)(lambda: going_down(k + 1, p).start())
                if paired:
                    to_mate(place + 1 + k, size + k, p).start()

    own.wait()
    for p in range(pieces):
        if paired:
            for rank in range(size):
                from_mate(rank, p).wait_recv()
            to_mate(place, 0, p).wait_send()
        for k in range(size - 1):
            pl.when((place < size - 1) & (place - k >= 0))(lambda k=k, p=p: going_up(k, p).wait_send())
            pl.when((place > 0) & (place + k <= size - 1))(lambda k=k, p=p: going_down(k, p).wait_send())
            if paired:
                pl.when(place - 1 - k >= 0)(lambda k=k, p=p: to_mate(place - 1 - k, 1 + k, p).wait_send())
                pl.when(place + 1 + k <= size - 1)(lambda k=k, p=p: to_mate(place + 1 + k, size + k, p).wait_send())


def pieces_of(rows, columns):
    return math.gcd(4, rows // 64) if rows * columns >= 1 << 18 else 1


def gather(x, size, paired, ident):
    copies = size * 2 if paired else size
    wide = max(size, 2)
    pieces = pieces_of(*x.shape)
    dma = pltpu.SemaphoreType.DMA
    return pl.pallas_call(
        functools.partial(gather_kernel, size, paired, pieces),
        in_specs=[IN_VMEM],
        out_specs=ANY,
        out_shape=jax.ShapeDtypeStruct((copies * x.shape[0], x.shape[1]), x.dtype),
        scratch_shapes=[dma] + [dma((wide, pieces))] * 4 + [dma((2 * wide, pieces)), dma((wide, pieces))],
        compiler_params=pltpu.CompilerParams(collective_id=ident, has_side_effects=True),
        cost_estimate=pl.CostEstimate(flops=0, bytes_accessed=30 * copies * x.size, transcendentals=0),
        name="gather",
    )(x)


def add_blocks(target, parts):
    rows = target.shape[0]
    step = math.gcd(rows, 32)

    def some(i, carry):
        span = pl.ds(pl.multiple_of(i * step, step), step)
        total = parts[0][span].astype(jnp.float32)
        for part in parts[1:]:
            total += part[span].astype(jnp.float32)
        target[span] = total.astype(target.dtype)
        return carry

    lax.fori_loop(0, rows // step, some, 0)


def scatter_kernel(
    size, paired, pieces, x_ref, o_ref, mine, mate, above, below, own_sem, mate_send, mate_recv, up_send, up_recv, down_send, down_recv
):
    place = lax.axis_index("ctx") if size > 1 else 0
    core = lax.axis_index("tensor")
    rows = o_ref.shape[0]
    part = rows // pieces
    order = sorted(range(size), key=lambda d: min(d, size - 1 - d))
    every = [(d, p) for d in order for p in range(pieces)]

    def block(rank, which, p):
        index = rank * 2 + which if paired else rank
        return x_ref.at[pl.ds(pl.multiple_of(index * rows + p * part, part), part)]

    def at(ref, d, p):
        return ref.at[d, pl.ds(p * part, part)]

    def load(d, p):
        return pltpu.make_async_copy(block(d, core, p), at(mine, d, p), own_sem.at[d, p])

    def to_mate(d, p):
        return remote(
            block(d, 1 - core, p), at(mate, d, p), mate_send.at[d, p], mate_recv.at[d, p], {"tensor": 1 - core}
        )

    def going_up(d, p):
        return remote(at(mine, d, p), at(below, d, p), up_send.at[d, p], up_recv.at[d, p], {"ctx": place + 1})

    def going_down(d, p):
        return remote(at(mine, d, p), at(above, d, p), down_send.at[d, p], down_recv.at[d, p], {"ctx": place - 1})

    for d, p in every:
        load(d, p).start()
    greet_chain(size, paired)
    if paired:
        for d, p in every:
            to_mate(d, p).start()

    def here(d, p):
        load(d, p).wait()
        if paired:
            to_mate(d, p).wait_recv()
            return [at(mine, d, p), at(mate, d, p)]
        return [at(mine, d, p)]

    for k in range(size - 1):
        for p in range(pieces):

            @pl.when(place < size - 1 - k)
            def _(d=size - 1 - k, p=p):
                parts = here(d, p)

                @pl.when(place > 0)
                def _():
                    going_up(d, p).wait_recv()
                    add_blocks(at(mine, d, p), parts + [at(below, d, p)])

                if paired:
                    pl.when(place == 0)(lambda: add_blocks(at(mine, d, p), parts))
                going_up(d, p).start()

            @pl.when(place > k)
            def _(d=k, p=p):
                parts = here(d, p)

                @pl.when(place < size - 1)
                def _():
                    going_down(d, p).wait_recv()
                    add_blocks(at(mine, d, p), parts + [at(above, d, p)])

                if paired:
                    pl.when(place == size - 1)(lambda: add_blocks(at(mine, d, p), parts))
                going_down(d, p).start()

    for d in range(size):

        @pl.when(place == d)
        def _(d=d):
            for p in range(pieces):
                parts = here(d, p)
                if d > 0:
                    going_up(d, p).wait_recv()
                    parts = parts + [at(below, d, p)]
                if d < size - 1:
                    going_down(d, p).wait_recv()
                    parts = parts + [at(above, d, p)]
                add_blocks(o_ref.at[pl.ds(p * part, part)], parts)

    for d, p in every:
        if d > 0:
            pl.when(place < d)(lambda d=d, p=p: going_up(d, p).wait_send())
        if d < size - 1:
            pl.when(place > d)(lambda d=d, p=p: going_down(d, p).wait_send())
        if paired:
            to_mate(d, p).wait_send()


def scatter(x, size, paired, ident):
    copies = size * 2 if paired else size
    rows = x.shape[0] // copies
    pieces = pieces_of(rows, x.shape[1])
    dma = pltpu.SemaphoreType.DMA
    slots = pltpu.VMEM((size, rows, x.shape[1]), x.dtype)
    one = pltpu.VMEM((1, 32, 128), x.dtype)
    chain = slots if size > 1 else one
    return pl.pallas_call(
        functools.partial(scatter_kernel, size, paired, pieces),
        in_specs=[ANY],
        out_specs=IN_VMEM,
        out_shape=jax.ShapeDtypeStruct((rows, x.shape[1]), jnp.float32),
        scratch_shapes=[slots, slots if paired else one, chain, chain] + [dma((size, pieces))] * 7,
        compiler_params=pltpu.CompilerParams(collective_id=ident, has_side_effects=True, vmem_limit_bytes=60000000),
        cost_estimate=pl.CostEstimate(flops=0, bytes_accessed=30 * x.size, transcendentals=0),
        name="scatter",
    )(x)


def share_kernel(size, groups, kinds, count, *refs):
    whole = len(kinds)
    owns, refs = refs[:whole], refs[whole:]
    parts, refs = refs[:count], refs[count:]
    wholes, refs = refs[:whole], refs[whole:]
    slices, refs = refs[:count], refs[count:]
    local_sem, up_send, up_recv, down_send, down_recv, far_send, far_recv, swap_send, swap_recv = refs
    place, group = lax.axis_index("ctx"), lax.axis_index("dp")
    rows, width = slices[0].shape[0] // size, slices[0].shape[1]
    chained = [w for w in range(whole) if kinds[w][0]]
    crossing = [w for w in range(whole) if kinds[w][1]]
    last = size - 1
    barrier = pltpu.get_barrier_semaphore()
    for step in range(1, size):
        greet(barrier, {"ctx": lax.rem(place + step, size)})
    for step in range(1, groups):
        greet(barrier, {"dp": lax.rem(group + step, groups)})
    pl.semaphore_wait(barrier, size + groups - 2)

    def chunk(w, in_group, rank):
        along, over = kinds[w]
        index = (in_group * size + rank if along else in_group) if over else rank
        n = owns[w].shape[0]
        return wholes[w].at[pl.ds(pl.multiple_of(index * n, n), n)]

    def source(w, rank, k):
        return owns[w] if k == 0 else chunk(w, group, rank)

    def going_up(w, k):
        return remote(
            source(w, place - k, k), chunk(w, group, place - k), up_send.at[w, k], up_recv.at[w, k], {"ctx": place + 1}
        )

    def going_down(w, k):
        return remote(
            source(w, place + k, k), chunk(w, group, place + k), down_send.at[w, k], down_recv.at[w, k], {"ctx": place - 1}
        )

    def across(w, rank, step, k):
        slot = rank if kinds[w][0] else 0
        return remote(
            source(w, rank, k), chunk(w, group, rank),
            far_send.at[w, slot, step], far_recv.at[w, slot, step], {"dp": lax.rem(group + step, groups)},
        )

    def from_across(w, rank, step):
        slot = rank if kinds[w][0] else 0
        there = chunk(w, lax.rem(group - step + groups, groups), rank)
        return remote(
            there, there, far_send.at[w, slot, step], far_recv.at[w, slot, step], {"dp": lax.rem(group + step, groups)}
        )

    def columns(w, rank):
        return parts[w].at[:, pl.ds(pl.multiple_of(rank * width, 128), width)]

    def at_rank(w, rank):
        return slices[w].at[pl.ds(pl.multiple_of(rank * rows, rows), rows)]

    def swap(w, step):
        to = lax.rem(place + step, size)
        return remote(columns(w, to), at_rank(w, place), swap_send.at[w, step], swap_recv.at[w, step], {"ctx": to})

    def swapped(w, step):
        there = at_rank(w, lax.rem(place - step + size, size))
        return remote(
            there, there, swap_send.at[w, step], swap_recv.at[w, step], {"ctx": lax.rem(place + step, size)}
        )

    copies = [pltpu.make_async_copy(owns[w], chunk(w, group, place), local_sem.at[w]) for w in range(whole)]
    copies += [pltpu.make_async_copy(columns(w, place), at_rank(w, place), local_sem.at[whole + w]) for w in range(count)]
    for w in range(whole):
        if w in chained:
            pl.when(place < last)(lambda w=w: going_up(w, 0).start())
            pl.when(place > 0)(lambda w=w: going_down(w, 0).start())
        if w in crossing:
            for step in range(1, groups):
                across(w, place, step, 0).start()
    for copy in copies:
        copy.start()
    for k in range(last):
        for w in chained:

            @pl.when(place - 1 - k >= 0)
            def _(k=k, w=w):
                there = chunk(w, group, place - 1 - k)
                remote(there, there, up_send.at[w, k], up_recv.at[w, k], {"ctx": place - 1}).wait_recv()
                if k + 1 < last:
                    pl.when(place < last)(lambda: going_up(w, k + 1).start())
                if w in crossing:
                    for step in range(1, groups):
                        across(w, place - 1 - k, step, 1).start()

            @pl.when(place + 1 + k <= last)
            def _(k=k, w=w):
                there = chunk(w, group, place + 1 + k)
                remote(there, there, down_send.at[w, k], down_recv.at[w, k], {"ctx": place + 1}).wait_recv()
                if k + 1 < last:
                    pl.when(place > 0)(lambda: going_down(w, k + 1).start())
                if w in crossing:
                    for step in range(1, groups):
                        across(w, place + 1 + k, step, 1).start()

    for w in range(count):
        for step in range(1, size):
            swap(w, step).start()
    for w in crossing:
        for rank in range(size) if w in chained else [place]:
            for step in range(1, groups):
                from_across(w, rank, step).wait_recv()
    for w in range(count):
        for step in range(1, size):
            swapped(w, step).wait_recv()
    for copy in copies:
        copy.wait()
    for w in range(whole):
        if w in chained:
            for k in range(last):
                pl.when((place < last) & (place - k >= 0))(lambda k=k, w=w: going_up(w, k).wait_send())
                pl.when((place > 0) & (place + k <= last))(lambda k=k, w=w: going_down(w, k).wait_send())
        if w in crossing:
            for rank in range(size) if w in chained else [place]:
                for step in range(1, groups):
                    across(w, rank, step, 1).wait_send()
    for w in range(count):
        for step in range(1, size):
            swap(w, step).wait_send()


def share(wholes, kinds, parts, width, ident):
    size, groups = lax.axis_size("ctx"), lax.axis_size("dp")
    rows = parts[0].shape[0]
    dma = pltpu.SemaphoreType.DMA
    n, m = len(wholes), len(parts)
    shapes = [
        jax.ShapeDtypeStruct(((size if along else 1) * (groups if over else 1) * x.shape[0], x.shape[1]), x.dtype)
        for x, (along, over) in zip(wholes, kinds)
    ]
    shapes += [jax.ShapeDtypeStruct((size * rows, width), parts[0].dtype)] * m
    return pl.pallas_call(
        functools.partial(share_kernel, size, groups, kinds, m),
        in_specs=[IN_VMEM] * (n + m),
        out_specs=[ANY] * (n + m),
        out_shape=shapes,
        scratch_shapes=[dma((n + m,))] + [dma((n, size))] * 4 + [dma((n, size, groups))] * 2 + [dma((m, size))] * 2,
        compiler_params=pltpu.CompilerParams(collective_id=ident, has_side_effects=True),
        cost_estimate=pl.CostEstimate(flops=0, bytes_accessed=150000000, transcendentals=0),
    )(*wholes, *parts)


def back_kernel(
    size, groups, x_ref, s_ref, p_ref, w_ref, n_ref, o_ref, t_ref, g_ref, mine, far, near, part, pair, crowd, row, give, got,
    give_sems, own_sem, far_send, far_recv, near_send, near_recv, pair_sems, crowd_send, crowd_recv, row_send, row_recv,
):
    place, group = lax.axis_index("ctx"), lax.axis_index("dp")
    core = lax.axis_index("tensor")
    rows = o_ref.shape[0]
    barrier = pltpu.get_barrier_semaphore()

    def rank_at(k):
        return lax.rem(place + 1 + k, size)

    def block(in_group, rank):
        return x_ref.at[pl.ds(pl.multiple_of((in_group * size + rank) * rows, rows), rows)]

    def load(k):
        return pltpu.make_async_copy(block(group, rank_at(k)), mine.at[k], own_sem.at[k])

    def across(k, step):
        to = lax.rem(group + step, groups)
        return remote(block(to, rank_at(k)), far.at[k, step], far_send.at[k, step], far_recv.at[k, step], {"dp": to})

    def along(k):
        return remote(mine.at[k], near.at[k], near_send.at[k], near_recv.at[k], {"ctx": rank_at(k)})

    to_mate = remote(part, pair, pair_sems.at[0], pair_sems.at[1], {"tensor": 1 - core})
    half = remote(give, got, give_sems.at[0], give_sems.at[1], {"tensor": 1 - core})

    def product(which, target):
        own_rows, depth = target.shape
        step = column_step(depth)
        span = pl.ds(pl.multiple_of(which * own_rows, own_rows), own_rows)

        def some(j, carry):
            columns = pl.ds(pl.multiple_of(j * step, step), step)
            target[:, columns] = matmul_nt(p_ref[span, :], w_ref[columns, :])
            return carry

        lax.fori_loop(0, depth // step, some, 0)

    def gain_sums(i, total):
        span = pl.ds(pl.multiple_of(i * 32, 32), 32)
        grad = g_ref[span, :] + got[span, :]
        g_ref[span, :] = grad
        return total + jnp.sum(grad * n_ref[span, :], axis=0, keepdims=True)

    def to_crowd(step):
        return remote(
            crowd.at[group], crowd.at[group], crowd_send.at[step], crowd_recv.at[step],
            {"dp": lax.rem(group + step, groups)},
        )

    def to_row(step):
        return remote(
            row.at[place], row.at[place], row_send.at[step], row_recv.at[step], {"ctx": lax.rem(place + step, size)}
        )

    for k in range(size):
        load(k).start()
    for step in range(1, size):
        greet(barrier, {"ctx": lax.rem(place + step, size)})
    for step in range(1, groups):
        greet(barrier, {"dp": lax.rem(group + step, groups)})
    greet(barrier, {"tensor": 1 - core})
    pl.semaphore_wait(barrier, size + groups - 1)
    for k in range(size):
        for step in range(1, groups):
            across(k, step).start()
    product(1 - core, give)
    half.start()
    product(core, g_ref)
    part[...] = s_ref[...]
    half.wait_recv()
    gains = lax.fori_loop(0, g_ref.shape[0] // 32, gain_sums, jnp.zeros((1, g_ref.shape[1]), jnp.float32))
    for j in range(g_ref.shape[1] // 128):
        part[j : j + 1, :] = gains[:, j * 128 : (j + 1) * 128]
    to_mate.start()
    to_mate.wait_recv()
    crowd[group] = part[...] + pair[...]
    for step in range(1, groups):
        to_crowd(step).start()
    for step in range(1, groups):
        to_crowd(step).wait_recv()
    total = crowd[0]
    for g in range(1, groups):
        total += crowd[g]
    row[place] = total
    for step in range(1, size):
        to_row(step).start()
    for k in range(size):
        load(k).wait()
        for step in range(1, groups):
            across(k, step).wait_recv()
        parts = [mine.at[k]] + [far.at[k, step] for step in range(1, groups)]
        if k < size - 1:
            add_blocks(mine.at[k], parts)
            along(k).start()
    for k in range(size - 1):
        along(k).wait_recv()
        parts.append(near.at[k])
    add_blocks(o_ref, parts)
    for step in range(1, size):
        to_row(step).wait_recv()
    total = row[0]
    for c in range(1, size):
        total += row[c]
    t_ref[...] = total
    half.wait_send()
    to_mate.wait_send()
    for step in range(1, groups):
        to_crowd(step).wait_send()
    for step in range(1, size):
        to_row(step).wait_send()
    for k in range(size):
        for step in range(1, groups):
            across(k, step).wait_send()
        if k < size - 1:
            along(k).wait_send()


def back(x, small, grad_pre, weight, normed, ident):
    size, groups = lax.axis_size("ctx"), lax.axis_size("dp")
    rows, columns = x.shape[0] // (size * groups), x.shape[1]
    dma = pltpu.SemaphoreType.DMA
    return pl.pallas_call(
        functools.partial(back_kernel, size, groups),
        in_specs=[ANY] + [IN_VMEM] * 4,
        out_specs=[IN_VMEM] * 3,
        out_shape=[
            jax.ShapeDtypeStruct((rows, columns), jnp.float32),
            jax.ShapeDtypeStruct(small.shape, jnp.float32),
            jax.ShapeDtypeStruct(normed.shape, jnp.float32),
        ],
        scratch_shapes=[
            pltpu.VMEM((size, rows, columns), x.dtype),
            pltpu.VMEM((size, groups, rows, columns), x.dtype),
            pltpu.VMEM((size, rows, columns), x.dtype),
            pltpu.VMEM(small.shape, jnp.float32),
            pltpu.VMEM(small.shape, jnp.float32),
            pltpu.VMEM((groups,) + small.shape, jnp.float32),
            pltpu.VMEM((size,) + small.shape, jnp.float32),
            pltpu.VMEM(normed.shape, jnp.float32),
            pltpu.VMEM(normed.shape, jnp.float32),
            dma((2,)),
            dma((size,)),
            dma((size, groups)),
            dma((size, groups)),
            dma((size,)),
            dma((size,)),
            dma((2,)),
            dma((groups,)),
            dma((groups,)),
            dma((size,)),
            dma((size,)),
        ],
        compiler_params=pltpu.CompilerParams(collective_id=ident, has_side_effects=True, vmem_limit_bytes=60000000),
        cost_estimate=pl.CostEstimate(flops=0, bytes_accessed=100 * x.size, transcendentals=0),
        name="back",
    )(x, small, grad_pre, weight, normed)


def column_step(width):
    return max(t for t in (768, 384, 256, 128) if width % t == 0)


def expand_block(x_ref, weights, extra, stage):
    step = column_step(weights[0].shape[1])

    def some(j, carry):
        span = pl.ds(pl.multiple_of(j * step, step), step)
        gate = nn(x_ref[...], weights[0][:, span])
        up = nn(x_ref[...], weights[1][:, span])
        stage[0, :, span] = gate.astype(jnp.bfloat16)
        stage[1, :, span] = up.astype(jnp.bfloat16)
        stage[2, :, span] = (gate * jax.nn.sigmoid(gate) * up).astype(jnp.bfloat16)
        return carry

    lax.fori_loop(0, weights[0].shape[1] // step, some, 0)


def shrink_block(x_ref, weights, extra, stage):
    step = column_step(weights[0].shape[1])

    def some(j, carry):
        span = pl.ds(pl.multiple_of(j * step, step), step)
        grad = nn(x_ref[...], weights[0][:, span])
        gate = extra[0, :, span].astype(jnp.float32)
        up = extra[1, :, span].astype(jnp.float32)
        sigmoid = jax.nn.sigmoid(gate)
        stage[0, :, span] = (grad * up * sigmoid * (1.0 + gate * (1.0 - sigmoid))).astype(jnp.bfloat16)
        stage[1, :, span] = (grad * gate * sigmoid).astype(jnp.bfloat16)
        return carry

    lax.fori_loop(0, weights[0].shape[1] // step, some, 0)


def gather_apply_kernel(size, pieces, work, n_weights, n_extra, n_made, *refs):
    x_ref, refs = refs[0], refs[1:]
    weights_from, refs = refs[:n_weights], refs[n_weights:]
    extra_from, refs = refs[:n_extra], refs[n_extra:]
    o_ref, refs = refs[0], refs[1:]
    made_to, refs = refs[:n_made], refs[n_made:]
    weights, refs = refs[:n_weights], refs[n_weights:]
    extra, stage, refs = refs[0], refs[1], refs[2:]
    local_sem, weight_sem, extra_sem, stage_sem = refs[:4]
    up_send, up_recv, down_send, down_recv, mate_send, mate_recv = refs[4:]
    place = lax.axis_index("ctx")
    core = lax.axis_index("tensor")
    rows = x_ref.shape[0]
    part = rows // pieces
    last = size - 1

    loads = [pltpu.make_async_copy(weights_from[w], weights[w], weight_sem.at[w]) for w in range(n_weights)]
    for load in loads:
        load.start()

    def first_of(rank, which):
        return pl.multiple_of((rank * 2 + which) * rows, rows)

    def block(rank, which, p):
        return o_ref.at[pl.ds(pl.multiple_of((rank * 2 + which) * rows + p * part, part), part)]

    def going_up(k, p):
        there = block(place - k, core, p)
        return remote(there, there, up_send.at[k, p], up_recv.at[k, p], {"ctx": place + 1})

    def going_down(k, p):
        there = block(place + k, core, p)
        return remote(there, there, down_send.at[k, p], down_recv.at[k, p], {"ctx": place - 1})

    def coming_up(k, p):
        there = block(place - 1 - k, core, p)
        return remote(there, there, up_send.at[k, p], up_recv.at[k, p], {"ctx": place - 1})

    def coming_down(k, p):
        there = block(place + 1 + k, core, p)
        return remote(there, there, down_send.at[k, p], down_recv.at[k, p], {"ctx": place + 1})

    def to_mate(rank, p):
        there = block(rank, core, p)
        return remote(there, there, mate_send.at[rank, p], mate_recv.at[rank, p], {"tensor": 1 - core})

    def from_mate(rank, p):
        there = block(rank, 1 - core, p)
        return remote(there, there, mate_send.at[rank, p], mate_recv.at[rank, p], {"tensor": 1 - core})

    own = pltpu.make_async_copy(x_ref, o_ref.at[pl.ds(first_of(place, core), rows)], local_sem)
    own.start()
    greet_chain(size, True)
    own.wait()
    for p in range(pieces):
        pl.when(place < last)(lambda p=p: going_up(0, p).start())
        pl.when(place > 0)(lambda p=p: going_down(0, p).start())
    for p in range(pieces):
        to_mate(place, p).start()

    def forward(d):
        for p in range(pieces):

            @pl.when(place - d >= 0)
            def _(p=p):
                coming_up(d - 1, p).wait_recv()
                pl.when(place < last)(lambda: going_up(d, p).start())
                to_mate(place - d, p).start()

            @pl.when(place + d <= last)
            def _(p=p):
                coming_down(d - 1, p).wait_recv()
                pl.when(place > 0)(lambda: going_down(d, p).start())
                to_mate(place + d, p).start()

    for load in loads:
        load.wait()
    short = jnp.minimum(place, last - place)

    def distance(s):
        return jnp.where(s <= 2 * short, (s + 1) // 2, s - short)

    def extra_load(rank, which, slot, e):
        return pltpu.make_async_copy(
            extra_from[e].at[pl.ds(first_of(rank, which), rows)], extra.at[slot, e], extra_sem.at[slot, e]
        )

    def store(rank, which, slot, m):
        return pltpu.make_async_copy(
            stage.at[slot, m], made_to[m].at[pl.ds(first_of(rank, which), rows)], stage_sem.at[slot, m]
        )

    def visit(s, carry):
        d = distance(s)
        below = jnp.where(s <= 2 * short, s % 2 == 1, place > last - place)
        rank = jnp.where(below, place - d, place + d)
        for slot, which in enumerate((core, 1 - core)):
            for e in range(n_extra):
                extra_load(rank, which, slot, e).start()
        pl.when((s > 0) & (d != distance(s - 1)))(lambda: forward(d))
        for slot, which in enumerate((core, 1 - core)):
            if slot == 1:
                for p in range(pieces):
                    from_mate(rank, p).wait_recv()
            for e in range(n_extra):
                extra_load(rank, which, slot, e).wait()

            @pl.when(s > 0)
            def _():
                for m in range(n_made):
                    store(rank, which, slot, m).wait()

            work(o_ref.at[pl.ds(first_of(rank, which), rows)], weights, extra.at[slot], stage.at[slot])
            for m in range(n_made):
                store(rank, which, slot, m).start()
        return carry

    lax.fori_loop(0, size, visit, 0)
    for slot, which in enumerate((core, 1 - core)):
        for m in range(n_made):
            store(place, which, slot, m).wait()
    for p in range(pieces):
        for k in range(last):
            pl.when((place < last) & (place - k >= 0))(lambda k=k, p=p: going_up(k, p).wait_send())
            pl.when((place > 0) & (place + k <= last))(lambda k=k, p=p: going_down(k, p).wait_send())
        for rank in range(size):
            to_mate(rank, p).wait_send()


def gather_apply(x, weights, extra, work, n_made, ident):
    size = lax.axis_size("ctx")
    rows, width = x.shape[0], weights[0].shape[1]
    total = 2 * size * rows
    pieces = pieces_of(*x.shape)
    dma = pltpu.SemaphoreType.DMA
    made = jax.ShapeDtypeStruct((total, width), jnp.bfloat16)
    slots = max(1, len(extra))
    return pl.pallas_call(
        functools.partial(gather_apply_kernel, size, pieces, work, len(weights), len(extra), n_made),
        in_specs=[IN_VMEM] + [ANY] * (len(weights) + len(extra)),
        out_specs=[IN_VMEM] + [ANY] * n_made,
        out_shape=[jax.ShapeDtypeStruct((total, x.shape[1]), x.dtype)] + [made] * n_made,
        scratch_shapes=[pltpu.VMEM(w.shape, w.dtype) for w in weights]
        + [
            pltpu.VMEM((2, slots, rows, width) if extra else (2, 1, 16, 128), jnp.bfloat16),
            pltpu.VMEM((2, n_made, rows, width), jnp.bfloat16),
            dma,
            dma((len(weights),)),
            dma((2, slots)),
            dma((2, n_made)),
        ]
        + [dma((size, pieces))] * 6,
        compiler_params=pltpu.CompilerParams(collective_id=ident, has_side_effects=True, vmem_limit_bytes=60000000),
        cost_estimate=pl.CostEstimate(flops=0, bytes_accessed=200000000, transcendentals=0),
    )(x, *weights, *extra)


def sum_apply_kernel(size, pieces, count, *refs):
    acts_from, refs = refs[:count], refs[count:]
    weights_from, refs = refs[:count], refs[count:]
    o_ref, acts, weights, mine, sent, mate, came, load_sem, act_sem = refs[:9]
    mate_send, mate_recv, up_send, up_recv, down_send, down_recv = refs[9:]
    place, core = lax.axis_index("ctx"), lax.axis_index("tensor")
    rows, depth = o_ref.shape
    part = rows // pieces
    last = size - 1

    loads = []
    for a in range(count):
        loads.append(pltpu.make_async_copy(weights_from[a], weights.at[a], load_sem.at[a]))
    for load in loads:
        load.start()

    def load_acts(a, d):
        span = pl.ds(pl.multiple_of(d * 2 * rows, rows), 2 * rows)
        return pltpu.make_async_copy(acts_from[a].at[span], acts.at[a, span], act_sem.at[a, d])

    short = jnp.minimum(place, last - place)

    def visited(i):
        s = last - i
        near = s <= 2 * short
        d = jnp.where(near, (s + 1) // 2, s - short)
        return jnp.where(jnp.where(near, s % 2 == 1, place > last - place), place - d, place + d)

    for i in range(size):
        for a in range(count):
            load_acts(a, visited(i)).start()
    greet_chain(size, True)
    for load in loads:
        load.wait()

    def at(ref, d, p):
        return ref.at[d, pl.ds(p * part, part)]

    def to_mate(i, d, p):
        slot = lax.rem(i, 2)
        return remote(at(sent, slot, p), at(mate, d, p), mate_send.at[slot, p], mate_recv.at[d, p], {"tensor": 1 - core})

    def going_up(d, p):
        return remote(at(mine, d, p), at(came, d, p), up_send.at[d, p], up_recv.at[d, p], {"ctx": place + 1})

    def going_down(d, p):
        there = jnp.where(d == place - 1, size, d)
        return remote(at(mine, d, p), at(came, there, p), down_send.at[d, p], down_recv.at[d, p], {"ctx": place - 1})

    def coming_up(d, p):
        there = at(came, d, p)
        return remote(there, there, up_send.at[d, p], up_recv.at[d, p], {"ctx": place - 1})

    def coming_down(d, p):
        there = at(came, jnp.where(d == place, size, d), p)
        return remote(there, there, down_send.at[d, p], down_recv.at[d, p], {"ctx": place + 1})

    def compute(d, which, target):
        step = column_step(depth)
        span = pl.ds(pl.multiple_of((d * 2 + which) * rows, rows), rows)

        def some(j, carry):
            columns = pl.ds(pl.multiple_of(j * step, step), step)
            total = matmul_nt(acts[0, span, :], weights[0, columns, :])
            for a in range(1, count):
                total += matmul_nt(acts[a, span, :], weights[a, columns, :])
            target[:, columns] = total.astype(target.dtype)
            return carry

        lax.fori_loop(0, depth // step, some, 0)

    def with_mate(d, p):
        to_mate(0, d, p).wait_recv()
        return [at(mine, d, p), at(mate, d, p)]

    def first_part(i, carry):
        d = visited(i)
        for a in range(count):
            load_acts(a, d).wait()
        for p in range(pieces):
            pl.when(i >= 2)(lambda p=p: to_mate(i, d, p).wait_send())
        compute(d, 1 - core, sent.at[lax.rem(i, 2)])
        for p in range(pieces):
            to_mate(i, d, p).start()
        compute(d, core, mine.at[d])

        @pl.when((place == 0) & (d > 0))
        def _():
            for p in range(pieces):
                add_blocks(at(mine, d, p), with_mate(d, p))
                going_up(d, p).start()

        @pl.when((place == last) & (d < last))
        def _():
            for p in range(pieces):
                add_blocks(at(mine, d, p), with_mate(d, p))
                going_down(d, p).start()

        return carry

    lax.fori_loop(0, size, first_part, 0)

    def second_part(s, carry):
        k, p = s // pieces, s % pieces

        @pl.when((place > 0) & (place < last - k))
        def _():
            d = last - k
            parts = with_mate(d, p)
            coming_up(d, p).wait_recv()
            add_blocks(at(mine, d, p), parts + [at(came, d, p)])
            going_up(d, p).start()

        @pl.when((place < last) & (place > k))
        def _():
            parts = with_mate(k, p)
            coming_down(k, p).wait_recv()
            add_blocks(at(mine, k, p), parts + [at(came, k, p)])
            going_down(k, p).start()

        return carry

    lax.fori_loop(0, last * pieces, second_part, 0)

    def final(p, carry):
        target = o_ref.at[pl.ds(pl.multiple_of(p * part, part), part)]
        parts = with_mate(place, p)
        pl.when(place > 0)(lambda: coming_up(place, p).wait_recv())
        pl.when(place < last)(lambda: coming_down(place, p).wait_recv())
        up, down = at(came, place, p), at(came, size, p)
        pl.when(place == 0)(lambda: add_blocks(target, parts + [down]))
        pl.when(place == last)(lambda: add_blocks(target, parts + [up]))
        pl.when((place > 0) & (place < last))(lambda: add_blocks(target, parts + [up, down]))
        return carry

    lax.fori_loop(0, pieces, final, 0)
    for p in range(pieces):
        for i in range(size - 2, size):
            to_mate(i, 0, p).wait_send()
        for d in range(size):
            pl.when(place < d)(lambda d=d, p=p: going_up(d, p).wait_send())
            pl.when(place > d)(lambda d=d, p=p: going_down(d, p).wait_send())


def sum_apply(acts, weights, ident):
    size, count = lax.axis_size("ctx"), len(acts)
    total, width = acts[0].shape
    depth = weights[0].shape[0]
    block = total // (2 * size)
    pieces = pieces_of(block, depth)
    dma = pltpu.SemaphoreType.DMA

    def slots(n):
        return pltpu.VMEM((n, block, depth), jnp.bfloat16)

    scratch = [
        pltpu.VMEM((count, total, width), jnp.bfloat16),
        pltpu.VMEM((count, depth, width), jnp.bfloat16),
        slots(size),
        slots(2),
        slots(size),
        slots(size + 1),
        dma((count,)),
        dma((count, size)),
        dma((2, pieces)),
    ] + [dma((size, pieces))] * 5
    return pl.pallas_call(
        functools.partial(sum_apply_kernel, size, pieces, count),
        in_specs=[ANY] * (2 * count),
        out_specs=IN_VMEM,
        out_shape=jax.ShapeDtypeStruct((block, depth), jnp.float32),
        scratch_shapes=scratch,
        compiler_params=pltpu.CompilerParams(collective_id=ident, has_side_effects=True, vmem_limit_bytes=60000000),
        cost_estimate=pl.CostEstimate(flops=0, bytes_accessed=200000000, transcendentals=0),
    )(*acts, *weights)


def assemble_kernel(size, ranks_ref, *refs):
    parts, (down_ref, gate_ref, up_ref, whole) = refs[:size], refs[size:]
    width = parts[0].shape[2]
    for which, target in enumerate((down_ref, gate_ref, up_ref)):
        for part, k in zip(parts, range(size)):
            whole[:, pl.ds(pl.multiple_of(ranks_ref[k] * width, 128), width)] = part[which].astype(jnp.float32)
        target[...] = whole[:, : gate_ref.shape[1]]


def assemble(received, columns):
    ranks = jnp.stack([rank for rank, _ in received]).astype(jnp.int32)
    blocks = [block for _, block in received]
    _, rows, width = blocks[0].shape
    f32 = jnp.float32
    return pl.pallas_call(
        functools.partial(assemble_kernel, len(blocks)),
        in_specs=[pl.BlockSpec(memory_space=pltpu.SMEM)] + [IN_VMEM] * len(blocks),
        out_specs=[IN_VMEM] * 3,
        out_shape=[jax.ShapeDtypeStruct((rows, columns), f32)] * 3,
        scratch_shapes=[pltpu.VMEM((rows, len(blocks) * width), f32)],
        compiler_params=pltpu.CompilerParams(vmem_limit_bytes=60000000),
        cost_estimate=pl.CostEstimate(flops=0, bytes_accessed=20 * rows * columns, transcendentals=0),
        name="assemble",
    )(ranks, *blocks)


def mask_into(bias_ref, first, seg_ref, place_ref):
    keys, rows = bias_ref.shape
    key_index = lax.broadcasted_iota(jnp.int32, (keys, rows), 0)
    row_index = lax.broadcasted_iota(jnp.int32, (keys, rows), 1) + first
    place = jnp.broadcast_to(place_ref[...], (keys, rows))
    start = jnp.broadcast_to(seg_ref[...], (keys, rows))
    allowed = ((place >= start) & (place <= row_index)) | (key_index == row_index)
    bias_ref[...] = jnp.where(allowed, 0.0, VERY_LOW)


def attend_kernel(scale, first_ref, seg_ref, place_ref, q_ref, k_ref, v_ref, o_ref, lse_ref, bias_ref, vt_ref):
    @pl.when((pl.program_id(0) == 0) & (pl.program_id(1) == 0))
    def _():
        vt_ref[...] = v_ref[...].T

    @pl.when(pl.program_id(1) == 0)
    def _():
        mask_into(bias_ref, first_ref[0] + pl.program_id(0) * q_ref.shape[0], seg_ref, place_ref)

    scores = matmul_nt(k_ref[...], q_ref[...]) * scale + bias_ref[...]
    top = jnp.max(scores, axis=0, keepdims=True)
    powers = jnp.exp(scores - top)
    total = jnp.sum(powers, axis=0, keepdims=True)
    mixture = nn(vt_ref[...], powers.astype(jnp.bfloat16)) / total
    o_ref[...] = mixture.T.astype(jnp.bfloat16)
    lse_ref[0] = top + jnp.log(total)


def attend_back_kernel(
    scale, first_ref, seg_ref, place_ref, q_ref, do_ref, lse_ref, k_ref, v_ref,
    dq_ref, dkv_ref, bias_ref, dk_ref, dv_ref, kt_ref,
):
    block, head = pl.program_id(0), pl.program_id(1)

    @pl.when(head == 0)
    def _():
        mask_into(bias_ref, first_ref[0] + block * q_ref.shape[0], seg_ref, place_ref)

    @pl.when((head == 0) & (block == 0))
    def _():
        kt_ref[...] = k_ref[...].T
        dk_ref[...] = jnp.zeros_like(dk_ref)
        dv_ref[...] = jnp.zeros_like(dv_ref)

    query, grad = q_ref[...], do_ref[...]
    scores = matmul_nt(k_ref[...], query) * scale + bias_ref[...]
    probs = jnp.exp(scores - lse_ref[0])
    grad_probs = matmul_nt(v_ref[...], grad)
    delta = jnp.sum(probs * grad_probs, axis=0, keepdims=True)
    grad_scores = (probs * (grad_probs - delta)).astype(jnp.bfloat16)
    dv_ref[...] += nn(probs.astype(jnp.bfloat16), grad)
    dk_ref[...] += nn(grad_scores, query)
    dq_ref[...] = (nn(kt_ref[...], grad_scores) * scale).T

    @pl.when((head == pl.num_programs(1) - 1) & (block == pl.num_programs(0) - 1))
    def _():
        dkv_ref[:, :HEAD] = (dk_ref[...] * scale).astype(jnp.bfloat16)
        dkv_ref[:, HEAD:] = dv_ref[...].astype(jnp.bfloat16)


def attention_calls(rows, keys, heads, which):
    block = math.gcd(256, rows)
    scale = 1.0 / math.sqrt(HEAD)
    smem = pl.BlockSpec(memory_space=pltpu.SMEM)
    seg = pl.BlockSpec((1, block), lambda i, h: (0, i))
    place = pl.BlockSpec((keys, 1), lambda i, h: (0, 0))
    head = pl.BlockSpec((block, HEAD), lambda i, h: (i, h))
    of_all = pl.BlockSpec((block, HEAD), lambda i, h: (i, which * heads + h))
    lse = pl.BlockSpec((1, 1, block), lambda i, h: (h, 0, i))
    tall = pl.BlockSpec((keys, HEAD), lambda i, h: (0, which))
    turned = pltpu.VMEM((HEAD, keys), jnp.bfloat16)
    params = pltpu.CompilerParams(vmem_limit_bytes=60000000)
    grid = (rows // block, heads)
    size = heads * rows * keys
    forward = pl.pallas_call(
        functools.partial(attend_kernel, scale),
        grid=grid,
        in_specs=[smem, seg, place, of_all, tall, tall],
        out_specs=[head, lse],
        out_shape=[
            jax.ShapeDtypeStruct((rows, heads * HEAD), jnp.bfloat16),
            jax.ShapeDtypeStruct((heads, 1, rows), jnp.float32),
        ],
        scratch_shapes=[pltpu.VMEM((keys, block), jnp.float32), turned],
        compiler_params=params,
        cost_estimate=pl.CostEstimate(flops=4 * size * HEAD, bytes_accessed=4 * rows * heads * HEAD, transcendentals=size),
        name="attend",
    )
    backward = pl.pallas_call(
        functools.partial(attend_back_kernel, scale),
        grid=grid,
        in_specs=[smem, seg, place, of_all, of_all, lse, tall, tall],
        out_specs=[head, pl.BlockSpec((keys, 2 * HEAD), lambda i, h: (0, 0))],
        out_shape=[
            jax.ShapeDtypeStruct((rows, heads * HEAD), jnp.float32),
            jax.ShapeDtypeStruct((keys, 2 * HEAD), jnp.bfloat16),
        ],
        scratch_shapes=[
            pltpu.VMEM((keys, block), jnp.float32),
            pltpu.VMEM((keys, HEAD), jnp.float32),
            pltpu.VMEM((keys, HEAD), jnp.float32),
            turned,
        ],
        compiler_params=params,
        cost_estimate=pl.CostEstimate(flops=10 * size * HEAD, bytes_accessed=8 * rows * heads * HEAD, transcendentals=size),
        name="attend_back",
    )
    return forward, backward


def per_device(
    layer_input,
    teacher,
    cotangent,
    segment_ids,
    positions,
    valid_mask,
    gain_attn,
    query_weight,
    query_bias,
    key_weight,
    key_bias,
    value_weight,
    value_bias,
    out_weight,
    gain_mlp,
    gate_weight,
    up_weight,
    down_weight,
):
    tensor_rank = lax.axis_index("tensor")
    ctx_rank = lax.axis_index("ctx")
    tensor_size, ctx_size = lax.axis_size("tensor"), lax.axis_size("ctx")
    own_rows = layer_input.shape[0]
    shard_rows = own_rows * tensor_size
    seq_len = segment_ids.shape[0]
    q_width = query_weight.shape[1]
    kv_width = key_weight.shape[1]
    kv_local = kv_width // HEAD
    group = q_width // kv_width
    hidden_width = gate_weight.shape[1]
    slice_width = -(-hidden_width // (128 * ctx_size)) * 128
    first_row = ctx_rank * shard_rows
    own_first = first_row + tensor_rank * own_rows

    inputs = layer_input.astype(jnp.float32)
    gain_one = gain_attn.astype(jnp.float32)
    gain_two = gain_mlp.astype(jnp.float32)
    scale_attn = lax.rsqrt(jnp.mean(inputs * inputs, axis=1, keepdims=True) + EPS)
    normed_attn = inputs * scale_attn
    extra = ((0, 0), (0, ctx_size * slice_width - hidden_width))
    full_qkv, full_out, *slices = share(
        [jnp.concatenate([query_weight, key_weight, value_weight], axis=1), out_weight.T],
        ((True, True), (True, True)),
        [jnp.pad(w, extra) for w in (gate_weight, up_weight)],
        slice_width,
        1,
    )
    full_gate, full_up = [lax.all_gather(w, "dp", axis=0, tiled=True) for w in slices]
    normed_rows = gather((normed_attn * gain_one).astype(jnp.bfloat16), 1, True, 2)
    bias = jnp.concatenate(
        [
            lax.dynamic_slice_in_dim(query_bias, tensor_rank * q_width, q_width),
            lax.dynamic_slice_in_dim(key_bias, tensor_rank * kv_width, kv_width),
            lax.dynamic_slice_in_dim(value_bias, tensor_rank * kv_width, kv_width),
        ]
    ).astype(jnp.float32)
    places = lax.dynamic_slice_in_dim(positions, first_row, shard_rows)
    cosine, sine_table = rope_tables(places)
    qkv_pre = matmul(normed_rows, full_qkv) + bias
    turned = q_width + kv_width
    rotated = (
        rotate(qkv_pre[:, :turned].reshape(shard_rows, turned // HEAD, HEAD), cosine, sine_table)
        .astype(jnp.bfloat16)
        .reshape(shard_rows, turned)
    )
    own_count = jnp.full((8, 128), jnp.sum(valid_mask.astype(jnp.float32)))
    all_keys, all_values, counts, down_slice = share(
        [rotated[:, q_width:], qkv_pre[:, turned:].astype(jnp.bfloat16), own_count],
        ((True, False), (True, False), (False, True)),
        [jnp.pad(down_weight.T, extra)],
        slice_width,
        3,
    )
    full_down = lax.all_gather(down_slice, "dp", axis=0, tiled=True)
    valid_count = jnp.sum(counts[::8, 0])

    key_index = jnp.arange(seq_len, dtype=jnp.int32)
    key_place = jnp.where(valid_mask > 0, key_index, -1)[:, None]
    seq_first = lax.axis_index("dp") * seq_len
    doc_start = (lax.dynamic_slice_in_dim(segment_ids, first_row, shard_rows) - seq_first)[None, :]
    first = jnp.reshape(first_row, (1,)).astype(jnp.int32)
    kept = []
    for c in range(kv_local):
        forward, backward = attention_calls(shard_rows, seq_len, group, c)
        kept.append((backward,) + tuple(forward(first, doc_start, key_place, rotated, all_keys, all_values)))
    heads_out = jnp.concatenate([k[1] for k in kept], axis=1)
    attention = scatter(matmul_nt(heads_out, full_out), 1, True, 4)
    residual_mid = inputs + attention
    scale_mlp = lax.rsqrt(jnp.mean(residual_mid * residual_mid, axis=1, keepdims=True) + EPS)
    normed_mlp = residual_mid * scale_mlp
    mlp_rows, gate_act, up_act, hidden = gather_apply(
        (normed_mlp * gain_two).astype(jnp.bfloat16), [full_gate, full_up], [], expand_block, 3, 5
    )
    branch = sum_apply([hidden], [full_down], 6)
    layer_result = residual_mid + branch
    valid_own = lax.dynamic_slice_in_dim(valid_mask, own_first, own_rows).astype(jnp.float32)
    difference = layer_result - teacher.astype(jnp.float32)
    squared_sum = jnp.sum(valid_own[:, None] * difference * difference)
    grad_result = cotangent.astype(jnp.float32) + 2.0 * valid_own[:, None] * difference / (
        valid_count * D
    )
    grad_branch, grad_gate_act, grad_up_act = gather_apply(
        grad_result.astype(jnp.bfloat16), [full_down], [gate_act, up_act], shrink_block, 2, 9
    )
    summed = []
    for left, right in ((grad_branch, hidden), (mlp_rows, grad_gate_act), (mlp_rows, grad_up_act)):
        grad = matmul_tn(left, right).astype(jnp.bfloat16)
        grad_gate_act, grad_up_act, grad = lax.optimization_barrier((grad_gate_act, grad_up_act, grad))
        summed.append(lax.psum_scatter(grad, "dp", scatter_dimension=0, tiled=True))
    grad_mlp_rows = sum_apply([grad_gate_act, grad_up_act], [full_gate, full_up], 10)
    grad_gain_mlp = jnp.sum(grad_mlp_rows * normed_mlp, axis=0)
    grad_mid = grad_result + norm_back(grad_mlp_rows, normed_mlp, scale_mlp, gain_two)
    grad_attn_rows = gather(grad_mid.astype(jnp.bfloat16), 1, True, 2)
    grad_heads = matmul(grad_attn_rows, full_out).astype(jnp.bfloat16)
    grad_out = matmul_tn(grad_attn_rows, heads_out).astype(jnp.bfloat16)

    grad_out = lax.psum_scatter(grad_out, "dp", scatter_dimension=0, tiled=True)
    query_grads, key_grads, value_grads = [], [], []
    for c in range(kv_local):
        backward, _, log_total = kept[c]
        grad_query, grad_kv = backward(
            first, doc_start, key_place, rotated, grad_heads, log_total, all_keys, all_values
        )
        query_grads.append(grad_query)
        key_grads.append(grad_kv[:, :HEAD])
        value_grads.append(grad_kv[:, HEAD:])
    grad_kv = grad_kv if kv_local == 1 else jnp.concatenate(key_grads + value_grads, axis=1)
    grad_kv = scatter(grad_kv, ctx_size, False, 7)
    grad_kv, *summed = lax.optimization_barrier((grad_kv, *summed))
    shard_down, shard_gate, shard_up = to_rows(summed, hidden_width)
    shard_down = shard_down.T
    grad_turned = jnp.concatenate(query_grads + [grad_kv[:, :kv_width]], axis=1)
    grad_pre = jnp.concatenate(
        [
            rotate(grad_turned.reshape(shard_rows, turned // HEAD, HEAD), cosine, -sine_table)
            .reshape(shard_rows, turned)
            .astype(jnp.bfloat16),
            grad_kv[:, kv_width:].astype(jnp.bfloat16),
        ],
        axis=1,
    )
    grad_pre, grad_out = lax.optimization_barrier((grad_pre, grad_out))
    shard_out = lax.psum_scatter(grad_out, "ctx", scatter_dimension=0, tiled=True)
    shard_out = shard_out.astype(jnp.float32).T
    bias_sum = jnp.sum(grad_pre.astype(jnp.float32), axis=0)

    def spread(part, size):
        return lax.dynamic_update_slice_in_dim(
            jnp.zeros((size,), jnp.float32), part, tensor_rank * part.shape[0], 0
        )

    loss_part = jnp.zeros((128,), jnp.float32).at[0].set(squared_sum)
    parts = [
        jnp.zeros((D,), jnp.float32),
        grad_gain_mlp,
        spread(bias_sum[:q_width], query_bias.shape[0]),
        spread(bias_sum[q_width:turned], key_bias.shape[0]),
        spread(bias_sum[turned:], value_bias.shape[0]),
        loss_part,
    ]
    flat = jnp.concatenate(parts)
    small = jnp.pad(flat, (0, -flat.shape[0] % 1024)).reshape(-1, 128)
    grad_qkv = matmul_tn(normed_rows, grad_pre).astype(jnp.bfloat16)
    shard_qkv, sums, grad_normed = back(grad_qkv, small, grad_pre, full_qkv, normed_attn, 8)
    grad_input = grad_mid + norm_back(grad_normed, normed_attn, scale_attn, gain_one)
    sums = sums.reshape(-1)
    pieces, offset = [], 0
    for part in parts:
        pieces.append(sums[offset : offset + part.shape[0]])
        offset += part.shape[0]
    return (
        layer_result.astype(jnp.bfloat16),
        pieces[5][0] / (valid_count * D),
        grad_input,
        pieces[0],
        shard_qkv[:, :q_width],
        pieces[2],
        shard_qkv[:, q_width:turned],
        pieces[3],
        shard_qkv[:, turned:],
        pieces[4],
        shard_out,
        pieces[1],
        shard_gate,
        shard_up,
        shard_down,
    )


def solution(mesh):
    in_specs = (
        P(("dp", "ctx", "tensor"), None),
        P(("dp", "ctx", "tensor"), None),
        P(("dp", "ctx", "tensor"), None),
        P("dp"),
        P("dp"),
        P("dp"),
        P(),
        P(("dp", "ctx"), "tensor"),
        P(),
        P(("dp", "ctx"), "tensor"),
        P(),
        P(("dp", "ctx"), "tensor"),
        P(),
        P("tensor", ("dp", "ctx")),
        P(),
        P(("dp", "ctx"), "tensor"),
        P(("dp", "ctx"), "tensor"),
        P("tensor", ("dp", "ctx")),
    )
    out_specs = (
        P(("dp", "ctx", "tensor"), None),
        P(),
        P(("dp", "ctx", "tensor"), None),
        P(),
        P(("dp", "ctx"), "tensor"),
        P(),
        P(("dp", "ctx"), "tensor"),
        P(),
        P(("dp", "ctx"), "tensor"),
        P(),
        P("tensor", ("dp", "ctx")),
        P(),
        P(("dp", "ctx"), "tensor"),
        P(("dp", "ctx"), "tensor"),
        P("tensor", ("dp", "ctx")),
    )

    return jax.shard_map(per_device, mesh=mesh, in_specs=in_specs, out_specs=out_specs, check_vma=False)
```

```python
import functools
import math

import jax
import jax.numpy as jnp
from jax import lax
from jax.experimental import pallas as pl
from jax.experimental.pallas import tpu as pltpu
from jax.sharding import PartitionSpec as P


D = 1536
HEAD = 128


EPS = 1e-06
THETA = 10000.0
VERY_LOW = -1e30


def rope_tables(places):
    half_dim = HEAD // 2
    frequency = THETA ** (-(jnp.arange(half_dim, dtype=jnp.float32) * 2.0 / HEAD))
    angles = places.astype(jnp.float32)[:, None] * frequency[None, :]
    return (jnp.cos(angles), jnp.sin(angles))


def matmul(first_op, second_op):
    return jnp.dot(first_op, second_op, preferred_element_type=jnp.float32)


def matmul_tn(first_op, second_op):
    return lax.dot_general(
        first_op, second_op, (((0,), (0,)), ((), ())), preferred_element_type=jnp.float32
    )


def matmul_nt(first_op, second_op):
    return lax.dot_general(
        first_op, second_op, (((1,), (1,)), ((), ())), preferred_element_type=jnp.float32
    )


def norm_back(grad_normed, normed, inverse, gain):
    scaled = grad_normed * gain
    return inverse * (scaled - normed * jnp.mean(scaled * normed, axis=1, keepdims=True))


def exchange(blocks, axis):
    size = lax.axis_size(axis)
    rank = lax.axis_index(axis)
    received = [(rank, lax.dynamic_index_in_dim(blocks, rank, 0, keepdims=False))]
    for step in range(1, size):
        going = lax.dynamic_index_in_dim(blocks, (rank + step) % size, 0, keepdims=False)
        came = lax.ppermute(going, axis, [(i, (i + step) % size) for i in range(size)])
        received.append(((rank - step + size) % size, came))
    return received


def swapped_rows(summed):
    size = lax.axis_size("ctx")
    rows, width = summed[0].shape[0] // size, summed[0].shape[1]
    return exchange(jnp.stack([s.reshape(size, rows, width) for s in summed], axis=1), "ctx")


def nn(first_op, second_op):
    return jnp.dot(first_op, second_op, preferred_element_type=jnp.float32)


MESH = pl.DeviceIdType.MESH
ANY = pl.BlockSpec(memory_space=pl.ANY)
IN_VMEM = pl.BlockSpec(memory_space=pltpu.VMEM)


def remote(source, target, send_sem, recv_sem, device):
    return pltpu.make_async_remote_copy(
        src_ref=source,
        dst_ref=target,
        send_sem=send_sem,
        recv_sem=recv_sem,
        device_id=device,
        device_id_type=MESH,
    )


def greet(barrier, device):
    pl.semaphore_signal(barrier, inc=1, device_id=device, device_id_type=MESH)


def greet_chain(size, paired):
    place = lax.axis_index("ctx")
    barrier = pltpu.get_barrier_semaphore()
    if size > 1:
        pl.when(place < size - 1)(lambda: greet(barrier, {"ctx": place + 1}))
        pl.when(place > 0)(lambda: greet(barrier, {"ctx": place - 1}))
    if paired:
        greet(barrier, {"tensor": 1 - lax.axis_index("tensor")})
    if size == 1:
        pl.semaphore_wait(barrier, 1)
        return
    ends = (place == 0) | (place == size - 1)
    pl.when(ends)(lambda: pl.semaphore_wait(barrier, 1 + paired))
    pl.when(jnp.logical_not(ends))(lambda: pl.semaphore_wait(barrier, 2 + paired))


def gather_kernel(size, paired, pieces, x_ref, o_ref, local_sem, up_send, up_recv, down_send, down_recv, mate_send, mate_recv):
    place = lax.axis_index("ctx") if size > 1 else 0
    core = lax.axis_index("tensor")
    rows = x_ref.shape[0]
    part = rows // pieces
    greet_chain(size, paired)

    def block(rank, which, p):
        index = rank * 2 + which if paired else rank
        return o_ref.at[pl.ds(pl.multiple_of(index * rows + p * part, part), part)]

    def source(rank, k, p):
        return x_ref.at[pl.ds(p * part, part)] if k == 0 else block(rank, core, p)

    def going_up(k, p):
        return remote(
            source(place - k, k, p), block(place - k, core, p), up_send.at[k, p], up_recv.at[k, p], {"ctx": place + 1}
        )

    def going_down(k, p):
        return remote(
            source(place + k, k, p), block(place + k, core, p), down_send.at[k, p], down_recv.at[k, p], {"ctx": place - 1}
        )

    def to_mate(rank, k, p):
        return remote(
            source(rank, k, p), block(rank, core, p), mate_send.at[k, p], mate_recv.at[rank, p], {"tensor": 1 - core}
        )

    def from_mate(rank, p):
        there = block(rank, 1 - core, p)
        return remote(there, there, mate_send.at[0, p], mate_recv.at[rank, p], {"tensor": 1 - core})

    own = pltpu.make_async_copy(x_ref, o_ref.at[pl.ds(pl.multiple_of((place * 2 + core if paired else place) * rows, rows), rows)], local_sem)
    for p in range(pieces):
        if size > 1:
            pl.when(place < size - 1)(lambda p=p: going_up(0, p).start())
            pl.when(place > 0)(lambda p=p: going_down(0, p).start())
    for p in range(pieces):
        if paired:
            to_mate(place, 0, p).start()
    own.start()
    for k in range(size - 1):
        for p in range(pieces):

            @pl.when(place - 1 - k >= 0)
            def _(k=k, p=p):
                there = block(place - 1 - k, core, p)
                remote(there, there, up_send.at[k, p], up_recv.at[k, p], {"ctx": place - 1}).wait_recv()
                if k + 1 < size - 1:
                    pl.when(place < size - 1)(lambda: going_up(k + 1, p).start())
                if paired:
                    to_mate(place - 1 - k, 1 + k, p).start()

            @pl.when(place + 1 + k <= size - 1)
            def _(k=k, p=p):
                there = block(place + 1 + k, core, p)
                remote(there, there, down_send.at[k, p], down_recv.at[k, p], {"ctx": place + 1}).wait_recv()
                if k + 1 < size - 1:
                    pl.when(place > 0)(lambda: going_down(k + 1, p).start())
                if paired:
                    to_mate(place + 1 + k, size + k, p).start()

    own.wait()
    for p in range(pieces):
        if paired:
            for rank in range(size):
                from_mate(rank, p).wait_recv()
            to_mate(place, 0, p).wait_send()
        for k in range(size - 1):
            pl.when((place < size - 1) & (place - k >= 0))(lambda k=k, p=p: going_up(k, p).wait_send())
            pl.when((place > 0) & (place + k <= size - 1))(lambda k=k, p=p: going_down(k, p).wait_send())
            if paired:
                pl.when(place - 1 - k >= 0)(lambda k=k, p=p: to_mate(place - 1 - k, 1 + k, p).wait_send())
                pl.when(place + 1 + k <= size - 1)(lambda k=k, p=p: to_mate(place + 1 + k, size + k, p).wait_send())


def pieces_of(rows, columns):
    return math.gcd(4, rows // 64) if rows * columns >= 1 << 18 else 1


def gather(x, size, paired, ident):
    copies = size * 2 if paired else size
    wide = max(size, 2)
    pieces = pieces_of(*x.shape)
    dma = pltpu.SemaphoreType.DMA
    return pl.pallas_call(
        functools.partial(gather_kernel, size, paired, pieces),
        in_specs=[IN_VMEM],
        out_specs=ANY,
        out_shape=jax.ShapeDtypeStruct((copies * x.shape[0], x.shape[1]), x.dtype),
        scratch_shapes=[dma] + [dma((wide, pieces))] * 4 + [dma((2 * wide, pieces)), dma((wide, pieces))],
        compiler_params=pltpu.CompilerParams(collective_id=ident, has_side_effects=True),
        cost_estimate=pl.CostEstimate(flops=0, bytes_accessed=30 * copies * x.size, transcendentals=0),
        name="gather",
    )(x)


def add_blocks(target, parts):
    rows = target.shape[0]
    step = math.gcd(rows, 32)

    def some(i, carry):
        span = pl.ds(pl.multiple_of(i * step, step), step)
        total = parts[0][span].astype(jnp.float32)
        for part in parts[1:]:
            total += part[span].astype(jnp.float32)
        target[span] = total.astype(target.dtype)
        return carry

    lax.fori_loop(0, rows // step, some, 0)


def scatter_kernel(
    size, paired, pieces, x_ref, o_ref, mine, mate, above, below, own_sem, mate_send, mate_recv, up_send, up_recv, down_send, down_recv
):
    place = lax.axis_index("ctx") if size > 1 else 0
    core = lax.axis_index("tensor")
    rows = o_ref.shape[0]
    part = rows // pieces
    order = sorted(range(size), key=lambda d: min(d, size - 1 - d))
    every = [(d, p) for d in order for p in range(pieces)]

    def block(rank, which, p):
        index = rank * 2 + which if paired else rank
        return x_ref.at[pl.ds(pl.multiple_of(index * rows + p * part, part), part)]

    def at(ref, d, p):
        return ref.at[d, pl.ds(p * part, part)]

    def load(d, p):
        return pltpu.make_async_copy(block(d, core, p), at(mine, d, p), own_sem.at[d, p])

    def to_mate(d, p):
        return remote(
            block(d, 1 - core, p), at(mate, d, p), mate_send.at[d, p], mate_recv.at[d, p], {"tensor": 1 - core}
        )

    def going_up(d, p):
        return remote(at(mine, d, p), at(below, d, p), up_send.at[d, p], up_recv.at[d, p], {"ctx": place + 1})

    def going_down(d, p):
        return remote(at(mine, d, p), at(above, d, p), down_send.at[d, p], down_recv.at[d, p], {"ctx": place - 1})

    for d, p in every:
        load(d, p).start()
    greet_chain(size, paired)
    if paired:
        for d, p in every:
            to_mate(d, p).start()

    def here(d, p):
        load(d, p).wait()
        if paired:
            to_mate(d, p).wait_recv()
            return [at(mine, d, p), at(mate, d, p)]
        return [at(mine, d, p)]

    for k in range(size - 1):
        for p in range(pieces):

            @pl.when(place < size - 1 - k)
            def _(d=size - 1 - k, p=p):
                parts = here(d, p)

                @pl.when(place > 0)
                def _():
                    going_up(d, p).wait_recv()
                    add_blocks(at(mine, d, p), parts + [at(below, d, p)])

                if paired:
                    pl.when(place == 0)(lambda: add_blocks(at(mine, d, p), parts))
                going_up(d, p).start()

            @pl.when(place > k)
            def _(d=k, p=p):
                parts = here(d, p)

                @pl.when(place < size - 1)
                def _():
                    going_down(d, p).wait_recv()
                    add_blocks(at(mine, d, p), parts + [at(above, d, p)])

                if paired:
                    pl.when(place == size - 1)(lambda: add_blocks(at(mine, d, p), parts))
                going_down(d, p).start()

    for d in range(size):

        @pl.when(place == d)
        def _(d=d):
            for p in range(pieces):
                parts = here(d, p)
                if d > 0:
                    going_up(d, p).wait_recv()
                    parts = parts + [at(below, d, p)]
                if d < size - 1:
                    going_down(d, p).wait_recv()
                    parts = parts + [at(above, d, p)]
                add_blocks(o_ref.at[pl.ds(p * part, part)], parts)

    for d, p in every:
        if d > 0:
            pl.when(place < d)(lambda d=d, p=p: going_up(d, p).wait_send())
        if d < size - 1:
            pl.when(place > d)(lambda d=d, p=p: going_down(d, p).wait_send())
        if paired:
            to_mate(d, p).wait_send()


def scatter(x, size, paired, ident):
    copies = size * 2 if paired else size
    rows = x.shape[0] // copies
    pieces = pieces_of(rows, x.shape[1])
    dma = pltpu.SemaphoreType.DMA
    slots = pltpu.VMEM((size, rows, x.shape[1]), x.dtype)
    one = pltpu.VMEM((1, 32, 128), x.dtype)
    chain = slots if size > 1 else one
    return pl.pallas_call(
        functools.partial(scatter_kernel, size, paired, pieces),
        in_specs=[ANY],
        out_specs=IN_VMEM,
        out_shape=jax.ShapeDtypeStruct((rows, x.shape[1]), jnp.float32),
        scratch_shapes=[slots, slots if paired else one, chain, chain] + [dma((size, pieces))] * 7,
        compiler_params=pltpu.CompilerParams(collective_id=ident, has_side_effects=True, vmem_limit_bytes=60000000),
        cost_estimate=pl.CostEstimate(flops=0, bytes_accessed=30 * x.size, transcendentals=0),
        name="scatter",
    )(x)


def share_kernel(size, groups, kinds, count, *refs):
    whole = len(kinds)
    owns, refs = refs[:whole], refs[whole:]
    parts, refs = refs[:count], refs[count:]
    wholes, refs = refs[:whole], refs[whole:]
    slices, refs = refs[:count], refs[count:]
    local_sem, up_send, up_recv, down_send, down_recv, far_send, far_recv, swap_send, swap_recv = refs
    place, group = lax.axis_index("ctx"), lax.axis_index("dp")
    rows, width = slices[0].shape[0] // size, slices[0].shape[1]
    chained = [w for w in range(whole) if kinds[w][0]]
    crossing = [w for w in range(whole) if kinds[w][1]]
    last = size - 1
    barrier = pltpu.get_barrier_semaphore()
    for step in range(1, size):
        greet(barrier, {"ctx": lax.rem(place + step, size)})
    for step in range(1, groups):
        greet(barrier, {"dp": lax.rem(group + step, groups)})
    pl.semaphore_wait(barrier, size + groups - 2)

    def chunk(w, in_group, rank):
        along, over = kinds[w]
        index = (in_group * size + rank if along else in_group) if over else rank
        n = owns[w].shape[0]
        return wholes[w].at[pl.ds(pl.multiple_of(index * n, n), n)]

    def source(w, rank, k):
        return owns[w] if k == 0 else chunk(w, group, rank)

    def going_up(w, k):
        return remote(
            source(w, place - k, k), chunk(w, group, place - k), up_send.at[w, k], up_recv.at[w, k], {"ctx": place + 1}
        )

    def going_down(w, k):
        return remote(
            source(w, place + k, k), chunk(w, group, place + k), down_send.at[w, k], down_recv.at[w, k], {"ctx": place - 1}
        )

    def across(w, rank, step, k):
        slot = rank if kinds[w][0] else 0
        return remote(
            source(w, rank, k), chunk(w, group, rank),
            far_send.at[w, slot, step], far_recv.at[w, slot, step], {"dp": lax.rem(group + step, groups)},
        )

    def from_across(w, rank, step):
        slot = rank if kinds[w][0] else 0
        there = chunk(w, lax.rem(group - step + groups, groups), rank)
        return remote(
            there, there, far_send.at[w, slot, step], far_recv.at[w, slot, step], {"dp": lax.rem(group + step, groups)}
        )

    def columns(w, rank):
        return parts[w].at[:, pl.ds(pl.multiple_of(rank * width, 128), width)]

    def at_rank(w, rank):
        return slices[w].at[pl.ds(pl.multiple_of(rank * rows, rows), rows)]

    def swap(w, step):
        to = lax.rem(place + step, size)
        return remote(columns(w, to), at_rank(w, place), swap_send.at[w, step], swap_recv.at[w, step], {"ctx": to})

    def swapped(w, step):
        there = at_rank(w, lax.rem(place - step + size, size))
        return remote(
            there, there, swap_send.at[w, step], swap_recv.at[w, step], {"ctx": lax.rem(place + step, size)}
        )

    copies = [pltpu.make_async_copy(owns[w], chunk(w, group, place), local_sem.at[w]) for w in range(whole)]
    copies += [pltpu.make_async_copy(columns(w, place), at_rank(w, place), local_sem.at[whole + w]) for w in range(count)]
    for w in range(whole):
        if w in chained:
            pl.when(place < last)(lambda w=w: going_up(w, 0).start())
            pl.when(place > 0)(lambda w=w: going_down(w, 0).start())
        if w in crossing:
            for step in range(1, groups):
                across(w, place, step, 0).start()
    for copy in copies:
        copy.start()
    for k in range(last):
        for w in chained:

            @pl.when(place - 1 - k >= 0)
            def _(k=k, w=w):
                there = chunk(w, group, place - 1 - k)
                remote(there, there, up_send.at[w, k], up_recv.at[w, k], {"ctx": place - 1}).wait_recv()
                if k + 1 < last:
                    pl.when(place < last)(lambda: going_up(w, k + 1).start())
                if w in crossing:
                    for step in range(1, groups):
                        across(w, place - 1 - k, step, 1).start()

            @pl.when(place + 1 + k <= last)
            def _(k=k, w=w):
                there = chunk(w, group, place + 1 + k)
                remote(there, there, down_send.at[w, k], down_recv.at[w, k], {"ctx": place + 1}).wait_recv()
                if k + 1 < last:
                    pl.when(place > 0)(lambda: going_down(w, k + 1).start())
                if w in crossing:
                    for step in range(1, groups):
                        across(w, place + 1 + k, step, 1).start()

    for w in range(count):
        for step in range(1, size):
            swap(w, step).start()
    for w in crossing:
        for rank in range(size) if w in chained else [place]:
            for step in range(1, groups):
                from_across(w, rank, step).wait_recv()
    for w in range(count):
        for step in range(1, size):
            swapped(w, step).wait_recv()
    for copy in copies:
        copy.wait()
    for w in range(whole):
        if w in chained:
            for k in range(last):
                pl.when((place < last) & (place - k >= 0))(lambda k=k, w=w: going_up(w, k).wait_send())
                pl.when((place > 0) & (place + k <= last))(lambda k=k, w=w: going_down(w, k).wait_send())
        if w in crossing:
            for rank in range(size) if w in chained else [place]:
                for step in range(1, groups):
                    across(w, rank, step, 1).wait_send()
    for w in range(count):
        for step in range(1, size):
            swap(w, step).wait_send()


def share(wholes, kinds, parts, width, ident):
    size, groups = lax.axis_size("ctx"), lax.axis_size("dp")
    rows = parts[0].shape[0]
    dma = pltpu.SemaphoreType.DMA
    n, m = len(wholes), len(parts)
    shapes = [
        jax.ShapeDtypeStruct(((size if along else 1) * (groups if over else 1) * x.shape[0], x.shape[1]), x.dtype)
        for x, (along, over) in zip(wholes, kinds)
    ]
    shapes += [jax.ShapeDtypeStruct((size * rows, width), parts[0].dtype)] * m
    return pl.pallas_call(
        functools.partial(share_kernel, size, groups, kinds, m),
        in_specs=[IN_VMEM] * (n + m),
        out_specs=[ANY] * (n + m),
        out_shape=shapes,
        scratch_shapes=[dma((n + m,))] + [dma((n, size))] * 4 + [dma((n, size, groups))] * 2 + [dma((m, size))] * 2,
        compiler_params=pltpu.CompilerParams(collective_id=ident, has_side_effects=True),
        cost_estimate=pl.CostEstimate(flops=0, bytes_accessed=150000000, transcendentals=0),
    )(*wholes, *parts)


def back_kernel(
    size, groups, x_ref, s_ref, p_ref, w_ref, n_ref, mid_ref, scale_ref, gain_ref, o_ref, t_ref, g_ref, mine, far, near, part, pair, crowd, row, give, got,
    give_sems, own_sem, far_send, far_recv, near_send, near_recv, pair_sems, crowd_send, crowd_recv, row_send, row_recv,
):
    place, group = lax.axis_index("ctx"), lax.axis_index("dp")
    core = lax.axis_index("tensor")
    rows = o_ref.shape[0]
    barrier = pltpu.get_barrier_semaphore()

    def rank_at(k):
        return lax.rem(place + 1 + k, size)

    def block(in_group, rank):
        return x_ref.at[pl.ds(pl.multiple_of((in_group * size + rank) * rows, rows), rows)]

    def load(k):
        return pltpu.make_async_copy(block(group, rank_at(k)), mine.at[k], own_sem.at[k])

    def across(k, step):
        to = lax.rem(group + step, groups)
        return remote(block(to, rank_at(k)), far.at[k, step], far_send.at[k, step], far_recv.at[k, step], {"dp": to})

    def along(k):
        return remote(mine.at[k], near.at[k], near_send.at[k], near_recv.at[k], {"ctx": rank_at(k)})

    to_mate = remote(part, pair, pair_sems.at[0], pair_sems.at[1], {"tensor": 1 - core})
    half = remote(give, got, give_sems.at[0], give_sems.at[1], {"tensor": 1 - core})

    def product(which, target):
        own_rows, depth = target.shape
        step = column_step(depth)
        span = pl.ds(pl.multiple_of(which * own_rows, own_rows), own_rows)

        def some(j, carry):
            columns = pl.ds(pl.multiple_of(j * step, step), step)
            target[:, columns] = matmul_nt(p_ref[span, :], w_ref[columns, :])
            return carry

        lax.fori_loop(0, depth // step, some, 0)

    def gain_sums(i, total):
        span = pl.ds(pl.multiple_of(i * 32, 32), 32)
        grad, normed = g_ref[span, :] + got[span, :], n_ref[span, :]
        scaled = grad * gain_ref[...]
        mean = jnp.mean(scaled * normed, axis=1, keepdims=True)
        g_ref[span, :] = mid_ref[span, :] + scale_ref[span, :] * (scaled - normed * mean)
        return total + jnp.sum(grad * normed, axis=0, keepdims=True)

    def to_crowd(step):
        return remote(
            crowd.at[group], crowd.at[group], crowd_send.at[step], crowd_recv.at[step],
            {"dp": lax.rem(group + step, groups)},
        )

    def to_row(step):
        return remote(
            row.at[place], row.at[place], row_send.at[step], row_recv.at[step], {"ctx": lax.rem(place + step, size)}
        )

    for k in range(size):
        load(k).start()
    for step in range(1, size):
        greet(barrier, {"ctx": lax.rem(place + step, size)})
    for step in range(1, groups):
        greet(barrier, {"dp": lax.rem(group + step, groups)})
    greet(barrier, {"tensor": 1 - core})
    pl.semaphore_wait(barrier, size + groups - 1)
    for k in range(size):
        for step in range(1, groups):
            across(k, step).start()
    product(1 - core, give)
    half.start()
    product(core, g_ref)
    part[...] = s_ref[...]
    half.wait_recv()
    gains = lax.fori_loop(0, g_ref.shape[0] // 32, gain_sums, jnp.zeros((1, g_ref.shape[1]), jnp.float32))
    for j in range(g_ref.shape[1] // 128):
        part[j : j + 1, :] = gains[:, j * 128 : (j + 1) * 128]
    to_mate.start()
    to_mate.wait_recv()
    crowd[group] = part[...] + pair[...]
    for step in range(1, groups):
        to_crowd(step).start()
    for step in range(1, groups):
        to_crowd(step).wait_recv()
    total = crowd[0]
    for g in range(1, groups):
        total += crowd[g]
    row[place] = total
    for step in range(1, size):
        to_row(step).start()
    for k in range(size):
        load(k).wait()
        for step in range(1, groups):
            across(k, step).wait_recv()
        parts = [mine.at[k]] + [far.at[k, step] for step in range(1, groups)]
        if k < size - 1:
            add_blocks(mine.at[k], parts)
            along(k).start()
    for k in range(size - 1):
        along(k).wait_recv()
        parts.append(near.at[k])
    add_blocks(o_ref, parts)
    for step in range(1, size):
        to_row(step).wait_recv()
    total = row[0]
    for c in range(1, size):
        total += row[c]
    t_ref[...] = total
    half.wait_send()
    to_mate.wait_send()
    for step in range(1, groups):
        to_crowd(step).wait_send()
    for step in range(1, size):
        to_row(step).wait_send()
    for k in range(size):
        for step in range(1, groups):
            across(k, step).wait_send()
        if k < size - 1:
            along(k).wait_send()


def back(x, small, grad_pre, weight, normed, mid, scale, gain, ident):
    size, groups = lax.axis_size("ctx"), lax.axis_size("dp")
    rows, columns = x.shape[0] // (size * groups), x.shape[1]
    dma = pltpu.SemaphoreType.DMA
    return pl.pallas_call(
        functools.partial(back_kernel, size, groups),
        in_specs=[ANY] + [IN_VMEM] * 7,
        out_specs=[IN_VMEM] * 3,
        out_shape=[
            jax.ShapeDtypeStruct((rows, columns), jnp.float32),
            jax.ShapeDtypeStruct(small.shape, jnp.float32),
            jax.ShapeDtypeStruct(normed.shape, jnp.float32),
        ],
        scratch_shapes=[
            pltpu.VMEM((size, rows, columns), x.dtype),
            pltpu.VMEM((size, groups, rows, columns), x.dtype),
            pltpu.VMEM((size, rows, columns), x.dtype),
            pltpu.VMEM(small.shape, jnp.float32),
            pltpu.VMEM(small.shape, jnp.float32),
            pltpu.VMEM((groups,) + small.shape, jnp.float32),
            pltpu.VMEM((size,) + small.shape, jnp.float32),
            pltpu.VMEM(normed.shape, jnp.float32),
            pltpu.VMEM(normed.shape, jnp.float32),
            dma((2,)),
            dma((size,)),
            dma((size, groups)),
            dma((size, groups)),
            dma((size,)),
            dma((size,)),
            dma((2,)),
            dma((groups,)),
            dma((groups,)),
            dma((size,)),
            dma((size,)),
        ],
        compiler_params=pltpu.CompilerParams(collective_id=ident, has_side_effects=True, vmem_limit_bytes=60000000),
        cost_estimate=pl.CostEstimate(flops=0, bytes_accessed=100 * x.size, transcendentals=0),
        name="back",
    )(x, small, grad_pre, weight, normed, mid, scale, gain)


def column_step(width):
    return max(t for t in (768, 384, 256, 128) if width % t == 0)


def expand_block(x_ref, weights, extra, stage):
    step = column_step(weights[0].shape[1])

    def some(j, carry):
        span = pl.ds(pl.multiple_of(j * step, step), step)
        gate = nn(x_ref[...], weights[0][:, span])
        up = nn(x_ref[...], weights[1][:, span])
        stage[0, :, span] = gate.astype(jnp.bfloat16)
        stage[1, :, span] = up.astype(jnp.bfloat16)
        stage[2, :, span] = (gate * jax.nn.sigmoid(gate) * up).astype(jnp.bfloat16)
        return carry

    lax.fori_loop(0, weights[0].shape[1] // step, some, 0)


def shrink_block(x_ref, weights, extra, stage):
    step = column_step(weights[0].shape[1])

    def some(j, carry):
        span = pl.ds(pl.multiple_of(j * step, step), step)
        grad = nn(x_ref[...], weights[0][:, span])
        gate = extra[0, :, span].astype(jnp.float32)
        up = extra[1, :, span].astype(jnp.float32)
        sigmoid = jax.nn.sigmoid(gate)
        stage[0, :, span] = (grad * up * sigmoid * (1.0 + gate * (1.0 - sigmoid))).astype(jnp.bfloat16)
        stage[1, :, span] = (grad * gate * sigmoid).astype(jnp.bfloat16)
        return carry

    lax.fori_loop(0, weights[0].shape[1] // step, some, 0)


def gather_apply_kernel(size, pieces, work, n_weights, n_extra, n_made, *refs):
    x_ref, refs = refs[0], refs[1:]
    weights_from, refs = refs[:n_weights], refs[n_weights:]
    extra_from, refs = refs[:n_extra], refs[n_extra:]
    o_ref, refs = refs[0], refs[1:]
    made_to, refs = refs[:n_made], refs[n_made:]
    weights, refs = refs[:n_weights], refs[n_weights:]
    extra, stage, refs = refs[0], refs[1], refs[2:]
    local_sem, weight_sem, extra_sem, stage_sem = refs[:4]
    up_send, up_recv, down_send, down_recv, mate_send, mate_recv = refs[4:]
    place = lax.axis_index("ctx")
    core = lax.axis_index("tensor")
    rows = x_ref.shape[0]
    part = rows // pieces
    last = size - 1

    loads = [pltpu.make_async_copy(weights_from[w], weights[w], weight_sem.at[w]) for w in range(n_weights)]
    for load in loads:
        load.start()

    def first_of(rank, which):
        return pl.multiple_of((rank * 2 + which) * rows, rows)

    def block(rank, which, p):
        return o_ref.at[pl.ds(pl.multiple_of((rank * 2 + which) * rows + p * part, part), part)]

    def going_up(k, p):
        there = block(place - k, core, p)
        return remote(there, there, up_send.at[k, p], up_recv.at[k, p], {"ctx": place + 1})

    def going_down(k, p):
        there = block(place + k, core, p)
        return remote(there, there, down_send.at[k, p], down_recv.at[k, p], {"ctx": place - 1})

    def coming_up(k, p):
        there = block(place - 1 - k, core, p)
        return remote(there, there, up_send.at[k, p], up_recv.at[k, p], {"ctx": place - 1})

    def coming_down(k, p):
        there = block(place + 1 + k, core, p)
        return remote(there, there, down_send.at[k, p], down_recv.at[k, p], {"ctx": place + 1})

    def to_mate(rank, p):
        there = block(rank, core, p)
        return remote(there, there, mate_send.at[rank, p], mate_recv.at[rank, p], {"tensor": 1 - core})

    def from_mate(rank, p):
        there = block(rank, 1 - core, p)
        return remote(there, there, mate_send.at[rank, p], mate_recv.at[rank, p], {"tensor": 1 - core})

    own = pltpu.make_async_copy(x_ref, o_ref.at[pl.ds(first_of(place, core), rows)], local_sem)
    own.start()
    greet_chain(size, True)
    own.wait()
    for p in range(pieces):
        pl.when(place < last)(lambda p=p: going_up(0, p).start())
        pl.when(place > 0)(lambda p=p: going_down(0, p).start())
    for p in range(pieces):
        to_mate(place, p).start()

    def forward(d):
        for p in range(pieces):

            @pl.when(place - d >= 0)
            def _(p=p):
                coming_up(d - 1, p).wait_recv()
                pl.when(place < last)(lambda: going_up(d, p).start())
                to_mate(place - d, p).start()

            @pl.when(place + d <= last)
            def _(p=p):
                coming_down(d - 1, p).wait_recv()
                pl.when(place > 0)(lambda: going_down(d, p).start())
                to_mate(place + d, p).start()

    for load in loads:
        load.wait()
    short = jnp.minimum(place, last - place)

    def distance(s):
        return jnp.where(s <= 2 * short, (s + 1) // 2, s - short)

    def extra_load(rank, which, slot, e):
        return pltpu.make_async_copy(
            extra_from[e].at[pl.ds(first_of(rank, which), rows)], extra.at[slot, e], extra_sem.at[slot, e]
        )

    def store(rank, which, slot, m):
        return pltpu.make_async_copy(
            stage.at[slot, m], made_to[m].at[pl.ds(first_of(rank, which), rows)], stage_sem.at[slot, m]
        )

    def visit(s, carry):
        d = distance(s)
        below = jnp.where(s <= 2 * short, s % 2 == 1, place > last - place)
        rank = jnp.where(below, place - d, place + d)
        for slot, which in enumerate((core, 1 - core)):
            for e in range(n_extra):
                extra_load(rank, which, slot, e).start()
        pl.when((s > 0) & (d != distance(s - 1)))(lambda: forward(d))
        for slot, which in enumerate((core, 1 - core)):
            if slot == 1:
                for p in range(pieces):
                    from_mate(rank, p).wait_recv()
            for e in range(n_extra):
                extra_load(rank, which, slot, e).wait()

            @pl.when(s > 0)
            def _():
                for m in range(n_made):
                    store(rank, which, slot, m).wait()

            work(o_ref.at[pl.ds(first_of(rank, which), rows)], weights, extra.at[slot], stage.at[slot])
            for m in range(n_made):
                store(rank, which, slot, m).start()
        return carry

    lax.fori_loop(0, size, visit, 0)
    for slot, which in enumerate((core, 1 - core)):
        for m in range(n_made):
            store(place, which, slot, m).wait()
    for p in range(pieces):
        for k in range(last):
            pl.when((place < last) & (place - k >= 0))(lambda k=k, p=p: going_up(k, p).wait_send())
            pl.when((place > 0) & (place + k <= last))(lambda k=k, p=p: going_down(k, p).wait_send())
        for rank in range(size):
            to_mate(rank, p).wait_send()


def gather_apply(x, weights, extra, work, n_made, ident):
    size = lax.axis_size("ctx")
    rows, width = x.shape[0], weights[0].shape[1]
    total = 2 * size * rows
    pieces = pieces_of(*x.shape)
    dma = pltpu.SemaphoreType.DMA
    made = jax.ShapeDtypeStruct((total, width), jnp.bfloat16)
    slots = max(1, len(extra))
    return pl.pallas_call(
        functools.partial(gather_apply_kernel, size, pieces, work, len(weights), len(extra), n_made),
        in_specs=[IN_VMEM] + [ANY] * (len(weights) + len(extra)),
        out_specs=[IN_VMEM] + [ANY] * n_made,
        out_shape=[jax.ShapeDtypeStruct((total, x.shape[1]), x.dtype)] + [made] * n_made,
        scratch_shapes=[pltpu.VMEM(w.shape, w.dtype) for w in weights]
        + [
            pltpu.VMEM((2, slots, rows, width) if extra else (2, 1, 16, 128), jnp.bfloat16),
            pltpu.VMEM((2, n_made, rows, width), jnp.bfloat16),
            dma,
            dma((len(weights),)),
            dma((2, slots)),
            dma((2, n_made)),
        ]
        + [dma((size, pieces))] * 6,
        compiler_params=pltpu.CompilerParams(collective_id=ident, has_side_effects=True, vmem_limit_bytes=60000000),
        cost_estimate=pl.CostEstimate(flops=0, bytes_accessed=200000000, transcendentals=0),
    )(x, *weights, *extra)


def sum_apply_kernel(size, pieces, count, *refs):
    acts_from, refs = refs[:count], refs[count:]
    weights_from, refs = refs[:count], refs[count:]
    o_ref, acts, weights, mine, sent, mate, came, load_sem, act_sem = refs[:9]
    mate_send, mate_recv, up_send, up_recv, down_send, down_recv = refs[9:]
    place, core = lax.axis_index("ctx"), lax.axis_index("tensor")
    rows, depth = o_ref.shape
    part = rows // pieces
    last = size - 1

    loads = []
    for a in range(count):
        loads.append(pltpu.make_async_copy(weights_from[a], weights.at[a], load_sem.at[a]))
    for load in loads:
        load.start()

    def load_acts(a, d):
        span = pl.ds(pl.multiple_of(d * 2 * rows, rows), 2 * rows)
        return pltpu.make_async_copy(acts_from[a].at[span], acts.at[a, span], act_sem.at[a, d])

    short = jnp.minimum(place, last - place)

    def visited(i):
        s = last - i
        near = s <= 2 * short
        d = jnp.where(near, (s + 1) // 2, s - short)
        return jnp.where(jnp.where(near, s % 2 == 1, place > last - place), place - d, place + d)

    for i in range(size):
        for a in range(count):
            load_acts(a, visited(i)).start()
    greet_chain(size, True)
    for load in loads:
        load.wait()

    def at(ref, d, p):
        return ref.at[d, pl.ds(p * part, part)]

    def to_mate(i, d, p):
        slot = lax.rem(i, 2)
        return remote(at(sent, slot, p), at(mate, d, p), mate_send.at[slot, p], mate_recv.at[d, p], {"tensor": 1 - core})

    def going_up(d, p):
        return remote(at(mine, d, p), at(came, d, p), up_send.at[d, p], up_recv.at[d, p], {"ctx": place + 1})

    def going_down(d, p):
        there = jnp.where(d == place - 1, size, d)
        return remote(at(mine, d, p), at(came, there, p), down_send.at[d, p], down_recv.at[d, p], {"ctx": place - 1})

    def coming_up(d, p):
        there = at(came, d, p)
        return remote(there, there, up_send.at[d, p], up_recv.at[d, p], {"ctx": place - 1})

    def coming_down(d, p):
        there = at(came, jnp.where(d == place, size, d), p)
        return remote(there, there, down_send.at[d, p], down_recv.at[d, p], {"ctx": place + 1})

    def compute(d, which, target):
        step = column_step(depth)
        span = pl.ds(pl.multiple_of((d * 2 + which) * rows, rows), rows)

        def some(j, carry):
            columns = pl.ds(pl.multiple_of(j * step, step), step)
            total = matmul_nt(acts[0, span, :], weights[0, columns, :])
            for a in range(1, count):
                total += matmul_nt(acts[a, span, :], weights[a, columns, :])
            target[:, columns] = total.astype(target.dtype)
            return carry

        lax.fori_loop(0, depth // step, some, 0)

    def with_mate(d, p):
        to_mate(0, d, p).wait_recv()
        return [at(mine, d, p), at(mate, d, p)]

    def first_part(i, carry):
        d = visited(i)
        for a in range(count):
            load_acts(a, d).wait()
        for p in range(pieces):
            pl.when(i >= 2)(lambda p=p: to_mate(i, d, p).wait_send())
        compute(d, 1 - core, sent.at[lax.rem(i, 2)])
        for p in range(pieces):
            to_mate(i, d, p).start()
        compute(d, core, mine.at[d])

        @pl.when((place == 0) & (d > 0))
        def _():
            for p in range(pieces):
                add_blocks(at(mine, d, p), with_mate(d, p))
                going_up(d, p).start()

        @pl.when((place == last) & (d < last))
        def _():
            for p in range(pieces):
                add_blocks(at(mine, d, p), with_mate(d, p))
                going_down(d, p).start()

        return carry

    lax.fori_loop(0, size, first_part, 0)

    def second_part(s, carry):
        k, p = s // pieces, s % pieces

        @pl.when((place > 0) & (place < last - k))
        def _():
            d = last - k
            parts = with_mate(d, p)
            coming_up(d, p).wait_recv()
            add_blocks(at(mine, d, p), parts + [at(came, d, p)])
            going_up(d, p).start()

        @pl.when((place < last) & (place > k))
        def _():
            parts = with_mate(k, p)
            coming_down(k, p).wait_recv()
            add_blocks(at(mine, k, p), parts + [at(came, k, p)])
            going_down(k, p).start()

        return carry

    lax.fori_loop(0, last * pieces, second_part, 0)

    def final(p, carry):
        target = o_ref.at[pl.ds(pl.multiple_of(p * part, part), part)]
        parts = with_mate(place, p)
        pl.when(place > 0)(lambda: coming_up(place, p).wait_recv())
        pl.when(place < last)(lambda: coming_down(place, p).wait_recv())
        up, down = at(came, place, p), at(came, size, p)
        pl.when(place == 0)(lambda: add_blocks(target, parts + [down]))
        pl.when(place == last)(lambda: add_blocks(target, parts + [up]))
        pl.when((place > 0) & (place < last))(lambda: add_blocks(target, parts + [up, down]))
        return carry

    lax.fori_loop(0, pieces, final, 0)
    for p in range(pieces):
        for i in range(size - 2, size):
            to_mate(i, 0, p).wait_send()
        for d in range(size):
            pl.when(place < d)(lambda d=d, p=p: going_up(d, p).wait_send())
            pl.when(place > d)(lambda d=d, p=p: going_down(d, p).wait_send())


def sum_apply(acts, weights, ident):
    size, count = lax.axis_size("ctx"), len(acts)
    total, width = acts[0].shape
    depth = weights[0].shape[0]
    block = total // (2 * size)
    pieces = pieces_of(block, depth)
    dma = pltpu.SemaphoreType.DMA

    def slots(n):
        return pltpu.VMEM((n, block, depth), jnp.bfloat16)

    scratch = [
        pltpu.VMEM((count, total, width), jnp.bfloat16),
        pltpu.VMEM((count, depth, width), jnp.bfloat16),
        slots(size),
        slots(2),
        slots(size),
        slots(size + 1),
        dma((count,)),
        dma((count, size)),
        dma((2, pieces)),
    ] + [dma((size, pieces))] * 5
    return pl.pallas_call(
        functools.partial(sum_apply_kernel, size, pieces, count),
        in_specs=[ANY] * (2 * count),
        out_specs=IN_VMEM,
        out_shape=jax.ShapeDtypeStruct((block, depth), jnp.float32),
        scratch_shapes=scratch,
        compiler_params=pltpu.CompilerParams(collective_id=ident, has_side_effects=True, vmem_limit_bytes=60000000),
        cost_estimate=pl.CostEstimate(flops=0, bytes_accessed=200000000, transcendentals=0),
    )(*acts, *weights)


def assemble_kernel(groups, size, ranks_ref, *refs):
    parts, targets, whole = refs[: size * len(groups)], refs[size * len(groups) : -1], refs[-1]
    width = parts[0].shape[2]
    taken = [(g, which) for g, held in enumerate(groups) for which in range(held)]
    for (g, which), target in zip(taken, targets):
        for k in range(size):
            span = pl.ds(pl.multiple_of(ranks_ref[k] * width, 128), width)
            whole[:, span] = parts[g * size + k][which].astype(jnp.float32)
        target[...] = whole[:, : target.shape[1]]


def assemble(received, columns):
    ranks = jnp.stack([rank for rank, _ in received[0]]).astype(jnp.int32)
    blocks = [block for group in received for _, block in group]
    groups, size = tuple(group[0][1].shape[0] for group in received), len(received[0])
    _, rows, width = blocks[0].shape
    f32 = jnp.float32
    return pl.pallas_call(
        functools.partial(assemble_kernel, groups, size),
        in_specs=[pl.BlockSpec(memory_space=pltpu.SMEM)] + [IN_VMEM] * len(blocks),
        out_specs=[IN_VMEM] * sum(groups),
        out_shape=[jax.ShapeDtypeStruct((rows, columns), f32)] * sum(groups),
        scratch_shapes=[pltpu.VMEM((rows, size * width), f32)],
        compiler_params=pltpu.CompilerParams(vmem_limit_bytes=60000000),
        cost_estimate=pl.CostEstimate(flops=0, bytes_accessed=20 * rows * columns, transcendentals=0),
        name="assemble",
    )(ranks, *blocks)


def turn(part, cosine, sine):
    return part * cosine + pltpu.roll(part, HEAD // 2, 1) * sine


def rope_kernel(x_ref, cosine_ref, sine_ref, q_ref, k_ref, v_ref):
    start = 0
    for target in (q_ref, k_ref, v_ref):
        for h in range(target.shape[1] // HEAD):
            part = x_ref[:, start : start + HEAD]
            if target is not v_ref:
                part = turn(part, cosine_ref[...], sine_ref[...])
            target[:, h * HEAD : (h + 1) * HEAD] = part.astype(jnp.bfloat16)
            start += HEAD


def rope_back_kernel(q_ref, kv_ref, cosine_ref, sine_ref, o_ref):
    start, kv_heads = 0, kv_ref.shape[1] // (2 * HEAD)
    for source, heads, turning in ((q_ref, q_ref.shape[1] // HEAD, True), (kv_ref, kv_heads, True), (kv_ref, kv_heads, False)):
        for h in range(heads):
            first = (h if turning else h + kv_heads) * HEAD
            part = source[:, first : first + HEAD]
            if turning:
                part = turn(part, cosine_ref[...], -sine_ref[...])
            o_ref[:, start : start + HEAD] = part.astype(jnp.bfloat16)
            start += HEAD


def rope_call(kernel, arrays, widths):
    rows = arrays[0].shape[0]
    return pl.pallas_call(
        kernel,
        in_specs=[IN_VMEM] * len(arrays),
        out_specs=[IN_VMEM] * len(widths),
        out_shape=[jax.ShapeDtypeStruct((rows, w), jnp.bfloat16) for w in widths],
        cost_estimate=pl.CostEstimate(flops=0, bytes_accessed=6 * rows * sum(widths), transcendentals=0),
    )(*arrays)


def mask_into(bias_ref, first, seg_ref, place_ref):
    keys, rows = bias_ref.shape
    key_index = lax.broadcasted_iota(jnp.int32, (keys, rows), 0)
    row_index = lax.broadcasted_iota(jnp.int32, (keys, rows), 1) + first
    place = jnp.broadcast_to(place_ref[...], (keys, rows))
    start = jnp.broadcast_to(seg_ref[...], (keys, rows))
    allowed = ((place >= start) & (place <= row_index)) | (key_index == row_index)
    bias_ref[...] = jnp.where(allowed, 0.0, VERY_LOW)


def attend_kernel(scale, first_ref, seg_ref, place_ref, q_ref, k_ref, v_ref, o_ref, lse_ref, bias_ref, vt_ref):
    @pl.when((pl.program_id(0) == 0) & (pl.program_id(1) == 0))
    def _():
        vt_ref[...] = v_ref[...].T

    @pl.when(pl.program_id(1) == 0)
    def _():
        mask_into(bias_ref, first_ref[0] + pl.program_id(0) * q_ref.shape[0], seg_ref, place_ref)

    scores = matmul_nt(k_ref[...], q_ref[...]) * scale + bias_ref[...]
    top = jnp.max(scores, axis=0, keepdims=True)
    powers = jnp.exp(scores - top)
    total = jnp.sum(powers, axis=0, keepdims=True)
    mixture = nn(vt_ref[...], powers.astype(jnp.bfloat16)) / total
    o_ref[...] = mixture.T.astype(jnp.bfloat16)
    lse_ref[0] = top + jnp.log(total)


def attend_back_kernel(
    scale, first_ref, seg_ref, place_ref, q_ref, do_ref, lse_ref, k_ref, v_ref,
    dq_ref, dkv_ref, bias_ref, dk_ref, dv_ref, kt_ref,
):
    block, head = pl.program_id(0), pl.program_id(1)

    @pl.when(head == 0)
    def _():
        mask_into(bias_ref, first_ref[0] + block * q_ref.shape[0], seg_ref, place_ref)

    @pl.when((head == 0) & (block == 0))
    def _():
        kt_ref[...] = k_ref[...].T
        dk_ref[...] = jnp.zeros_like(dk_ref)
        dv_ref[...] = jnp.zeros_like(dv_ref)

    query, grad = q_ref[...], do_ref[...]
    scores = matmul_nt(k_ref[...], query) * scale + bias_ref[...]
    probs = jnp.exp(scores - lse_ref[0])
    grad_probs = matmul_nt(v_ref[...], grad)
    delta = jnp.sum(probs * grad_probs, axis=0, keepdims=True)
    grad_scores = (probs * (grad_probs - delta)).astype(jnp.bfloat16)
    dv_ref[...] += nn(probs.astype(jnp.bfloat16), grad)
    dk_ref[...] += nn(grad_scores, query)
    dq_ref[...] = (nn(kt_ref[...], grad_scores) * scale).T

    @pl.when((head == pl.num_programs(1) - 1) & (block == pl.num_programs(0) - 1))
    def _():
        dkv_ref[:, :HEAD] = (dk_ref[...] * scale).astype(jnp.bfloat16)
        dkv_ref[:, HEAD:] = dv_ref[...].astype(jnp.bfloat16)


def attention_calls(rows, keys, heads, which):
    block = math.gcd(256, rows)
    scale = 1.0 / math.sqrt(HEAD)
    smem = pl.BlockSpec(memory_space=pltpu.SMEM)
    seg = pl.BlockSpec((1, block), lambda i, h: (0, i))
    place = pl.BlockSpec((keys, 1), lambda i, h: (0, 0))
    head = pl.BlockSpec((block, HEAD), lambda i, h: (i, h))
    of_all = pl.BlockSpec((block, HEAD), lambda i, h: (i, which * heads + h))
    lse = pl.BlockSpec((1, 1, block), lambda i, h: (h, 0, i))
    tall = pl.BlockSpec((keys, HEAD), lambda i, h: (0, which))
    turned = pltpu.VMEM((HEAD, keys), jnp.bfloat16)
    params = pltpu.CompilerParams(vmem_limit_bytes=60000000)
    grid = (rows // block, heads)
    size = heads * rows * keys
    forward = pl.pallas_call(
        functools.partial(attend_kernel, scale),
        grid=grid,
        in_specs=[smem, seg, place, of_all, tall, tall],
        out_specs=[head, lse],
        out_shape=[
            jax.ShapeDtypeStruct((rows, heads * HEAD), jnp.bfloat16),
            jax.ShapeDtypeStruct((heads, 1, rows), jnp.float32),
        ],
        scratch_shapes=[pltpu.VMEM((keys, block), jnp.float32), turned],
        compiler_params=params,
        cost_estimate=pl.CostEstimate(flops=4 * size * HEAD, bytes_accessed=4 * rows * heads * HEAD, transcendentals=size),
        name="attend",
    )
    backward = pl.pallas_call(
        functools.partial(attend_back_kernel, scale),
        grid=grid,
        in_specs=[smem, seg, place, of_all, of_all, lse, tall, tall],
        out_specs=[head, pl.BlockSpec((keys, 2 * HEAD), lambda i, h: (0, 0))],
        out_shape=[
            jax.ShapeDtypeStruct((rows, heads * HEAD), jnp.float32),
            jax.ShapeDtypeStruct((keys, 2 * HEAD), jnp.bfloat16),
        ],
        scratch_shapes=[
            pltpu.VMEM((keys, block), jnp.float32),
            pltpu.VMEM((keys, HEAD), jnp.float32),
            pltpu.VMEM((keys, HEAD), jnp.float32),
            turned,
        ],
        compiler_params=params,
        cost_estimate=pl.CostEstimate(flops=10 * size * HEAD, bytes_accessed=8 * rows * heads * HEAD, transcendentals=size),
        name="attend_back",
    )
    return forward, backward


def per_device(
    layer_input,
    teacher,
    cotangent,
    segment_ids,
    positions,
    valid_mask,
    gain_attn,
    query_weight,
    query_bias,
    key_weight,
    key_bias,
    value_weight,
    value_bias,
    out_weight,
    gain_mlp,
    gate_weight,
    up_weight,
    down_weight,
):
    tensor_rank = lax.axis_index("tensor")
    ctx_rank = lax.axis_index("ctx")
    tensor_size, ctx_size = lax.axis_size("tensor"), lax.axis_size("ctx")
    own_rows = layer_input.shape[0]
    shard_rows = own_rows * tensor_size
    seq_len = segment_ids.shape[0]
    q_width = query_weight.shape[1]
    kv_width = key_weight.shape[1]
    kv_local = kv_width // HEAD
    group = q_width // kv_width
    hidden_width = gate_weight.shape[1]
    slice_width = -(-hidden_width // (128 * ctx_size)) * 128
    first_row = ctx_rank * shard_rows
    own_first = first_row + tensor_rank * own_rows

    inputs = layer_input.astype(jnp.float32)
    gain_one = gain_attn.astype(jnp.float32)
    gain_two = gain_mlp.astype(jnp.float32)
    scale_attn = lax.rsqrt(jnp.mean(inputs * inputs, axis=1, keepdims=True) + EPS)
    normed_attn = inputs * scale_attn
    extra = ((0, 0), (0, ctx_size * slice_width - hidden_width))
    full_qkv, full_out, *slices = share(
        [jnp.concatenate([query_weight, key_weight, value_weight], axis=1), out_weight.T],
        ((True, True), (True, True)),
        [jnp.pad(w, extra) for w in (gate_weight, up_weight)],
        slice_width,
        1,
    )
    full_gate, full_up = [lax.all_gather(w, "dp", axis=0, tiled=True) for w in slices]
    normed_rows = gather((normed_attn * gain_one).astype(jnp.bfloat16), 1, True, 2)
    bias = jnp.concatenate(
        [
            lax.dynamic_slice_in_dim(query_bias, tensor_rank * q_width, q_width),
            lax.dynamic_slice_in_dim(key_bias, tensor_rank * kv_width, kv_width),
            lax.dynamic_slice_in_dim(value_bias, tensor_rank * kv_width, kv_width),
        ]
    ).astype(jnp.float32)
    places = lax.dynamic_slice_in_dim(positions, first_row, shard_rows)
    cosine, sine_table = rope_tables(places)
    qkv_pre = matmul(normed_rows, full_qkv) + bias
    turned = q_width + kv_width
    cosines = jnp.concatenate([cosine, cosine], axis=1)
    sines = jnp.concatenate([-sine_table, sine_table], axis=1)
    queries, own_keys, own_values = rope_call(rope_kernel, (qkv_pre, cosines, sines), (q_width, kv_width, kv_width))
    own_count = jnp.full((8, 128), jnp.sum(valid_mask.astype(jnp.float32)))
    all_keys, all_values, counts, down_slice = share(
        [own_keys, own_values, own_count],
        ((True, False), (True, False), (False, True)),
        [jnp.pad(down_weight.T, extra)],
        slice_width,
        3,
    )
    full_down = lax.all_gather(down_slice, "dp", axis=0, tiled=True)
    valid_count = jnp.sum(counts[::8, 0])

    key_index = jnp.arange(seq_len, dtype=jnp.int32)
    key_place = jnp.where(valid_mask > 0, key_index, -1)[:, None]
    seq_first = lax.axis_index("dp") * seq_len
    doc_start = (lax.dynamic_slice_in_dim(segment_ids, first_row, shard_rows) - seq_first)[None, :]
    first = jnp.reshape(first_row, (1,)).astype(jnp.int32)
    kept = []
    for c in range(kv_local):
        forward, backward = attention_calls(shard_rows, seq_len, group, c)
        kept.append((backward,) + tuple(forward(first, doc_start, key_place, queries, all_keys, all_values)))
    heads_out = jnp.concatenate([k[1] for k in kept], axis=1)
    attention = scatter(matmul_nt(heads_out, full_out), 1, True, 4)
    residual_mid = inputs + attention
    scale_mlp = lax.rsqrt(jnp.mean(residual_mid * residual_mid, axis=1, keepdims=True) + EPS)
    normed_mlp = residual_mid * scale_mlp
    mlp_rows, gate_act, up_act, hidden = gather_apply(
        (normed_mlp * gain_two).astype(jnp.bfloat16), [full_gate, full_up], [], expand_block, 3, 5
    )
    branch = sum_apply([hidden], [full_down], 6)
    layer_result = residual_mid + branch
    valid_own = lax.dynamic_slice_in_dim(valid_mask, own_first, own_rows).astype(jnp.float32)
    difference = layer_result - teacher.astype(jnp.float32)
    squared_sum = jnp.sum(valid_own[:, None] * difference * difference)
    grad_result = cotangent.astype(jnp.float32) + 2.0 * valid_own[:, None] * difference / (
        valid_count * D
    )
    grad_branch, grad_gate_act, grad_up_act = gather_apply(
        grad_result.astype(jnp.bfloat16), [full_down], [gate_act, up_act], shrink_block, 2, 9
    )
    summed = []
    for left, right in ((grad_branch, hidden), (mlp_rows, grad_gate_act), (mlp_rows, grad_up_act)):
        grad = matmul_tn(left, right).astype(jnp.bfloat16)
        grad_gate_act, grad_up_act, grad = lax.optimization_barrier((grad_gate_act, grad_up_act, grad))
        summed.append(lax.psum_scatter(grad, "dp", scatter_dimension=0, tiled=True))
    grad_mlp_rows = sum_apply([grad_gate_act, grad_up_act], [full_gate, full_up], 10)
    grad_gain_mlp = jnp.sum(grad_mlp_rows * normed_mlp, axis=0)
    grad_mid = grad_result + norm_back(grad_mlp_rows, normed_mlp, scale_mlp, gain_two)
    grad_attn_rows = gather(grad_mid.astype(jnp.bfloat16), 1, True, 2)
    grad_heads = matmul(grad_attn_rows, full_out).astype(jnp.bfloat16)
    grad_out = matmul_tn(grad_attn_rows, heads_out).astype(jnp.bfloat16)

    grad_out = lax.psum_scatter(grad_out, "dp", scatter_dimension=0, tiled=True)
    early = swapped_rows(summed[:2])
    query_grads, key_grads, value_grads = [], [], []
    for c in range(kv_local):
        backward, _, log_total = kept[c]
        grad_query, grad_kv = backward(
            first, doc_start, key_place, queries, grad_heads, log_total, all_keys, all_values
        )
        query_grads.append(grad_query)
        key_grads.append(grad_kv[:, :HEAD])
        value_grads.append(grad_kv[:, HEAD:])
    grad_kv = grad_kv if kv_local == 1 else jnp.concatenate(key_grads + value_grads, axis=1)
    grad_kv = scatter(grad_kv, ctx_size, False, 7)
    grad_kv, up_summed = lax.optimization_barrier((grad_kv, summed[2]))
    late = swapped_rows([up_summed])
    shard_down, shard_gate, shard_up = assemble([early, late], hidden_width)
    shard_down = shard_down.T
    grad_turned = query_grads[0] if kv_local == 1 else jnp.concatenate(query_grads, axis=1)
    (grad_pre,) = rope_call(rope_back_kernel, (grad_turned, grad_kv, cosines, sines), (turned + kv_width,))
    grad_pre, grad_out = lax.optimization_barrier((grad_pre, grad_out))
    shard_out = lax.psum_scatter(grad_out, "ctx", scatter_dimension=0, tiled=True)
    shard_out = shard_out.astype(jnp.float32).T
    bias_sum = jnp.sum(grad_pre.astype(jnp.float32), axis=0)

    def spread(part, size):
        return lax.dynamic_update_slice_in_dim(
            jnp.zeros((size,), jnp.float32), part, tensor_rank * part.shape[0], 0
        )

    loss_part = jnp.zeros((128,), jnp.float32).at[0].set(squared_sum)
    parts = [
        jnp.zeros((D,), jnp.float32),
        grad_gain_mlp,
        spread(bias_sum[:q_width], query_bias.shape[0]),
        spread(bias_sum[q_width:turned], key_bias.shape[0]),
        spread(bias_sum[turned:], value_bias.shape[0]),
        loss_part,
    ]
    flat = jnp.concatenate(parts)
    small = jnp.pad(flat, (0, -flat.shape[0] % 1024)).reshape(-1, 128)
    grad_qkv = matmul_tn(normed_rows, grad_pre).astype(jnp.bfloat16)
    shard_qkv, sums, grad_input = back(
        grad_qkv, small, grad_pre, full_qkv, normed_attn, grad_mid, scale_attn, gain_one[None, :], 8
    )
    sums = sums.reshape(-1)
    pieces, offset = [], 0
    for part in parts:
        pieces.append(sums[offset : offset + part.shape[0]])
        offset += part.shape[0]
    return (
        layer_result.astype(jnp.bfloat16),
        pieces[5][0] / (valid_count * D),
        grad_input,
        pieces[0],
        shard_qkv[:, :q_width],
        pieces[2],
        shard_qkv[:, q_width:turned],
        pieces[3],
        shard_qkv[:, turned:],
        pieces[4],
        shard_out,
        pieces[1],
        shard_gate,
        shard_up,
        shard_down,
    )


def solution(mesh):
    in_specs = (
        P(("dp", "ctx", "tensor"), None),
        P(("dp", "ctx", "tensor"), None),
        P(("dp", "ctx", "tensor"), None),
        P("dp"),
        P("dp"),
        P("dp"),
        P(),
        P(("dp", "ctx"), "tensor"),
        P(),
        P(("dp", "ctx"), "tensor"),
        P(),
        P(("dp", "ctx"), "tensor"),
        P(),
        P("tensor", ("dp", "ctx")),
        P(),
        P(("dp", "ctx"), "tensor"),
        P(("dp", "ctx"), "tensor"),
        P("tensor", ("dp", "ctx")),
    )
    out_specs = (
        P(("dp", "ctx", "tensor"), None),
        P(),
        P(("dp", "ctx", "tensor"), None),
        P(),
        P(("dp", "ctx"), "tensor"),
        P(),
        P(("dp", "ctx"), "tensor"),
        P(),
        P(("dp", "ctx"), "tensor"),
        P(),
        P("tensor", ("dp", "ctx")),
        P(),
        P(("dp", "ctx"), "tensor"),
        P(("dp", "ctx"), "tensor"),
        P("tensor", ("dp", "ctx")),
    )

    return jax.shard_map(per_device, mesh=mesh, in_specs=in_specs, out_specs=out_specs, check_vma=False)
```
